128 devices in a mesh: gx: 4 (over y), gy: 4 (over x_hi, core), gz: 8 (over z, x_lo).
Axes of the slice: x: 4 (x_hi: 2, x_lo: 2; x = x_hi * 2 + x_lo), y: 4, z: 4, core: 2. Of those that a mesh axis runs over, the one named last changes fastest.
Arguments:
- offset: float32 [3, 32, 32, 1024], P(None, 'gx', 'gy', 'gz'), may hold values from -0.25 to 0.25
- velocity: float32 [3, 32, 32, 1024], P(None, 'gx', 'gy', 'gz'), may hold values from -3 to 3
- spin: float32 [3, 32, 32, 1024], P(None, 'gx', 'gy', 'gz'), may hold values from -3 to 3
- radius: float32 [32, 32, 1024], P('gx', 'gy', 'gz'), may hold values from 0.62 to 0.82
- history: float32 [6, 3, 32, 32, 1024], P(None, None, 'gx', 'gy', 'gz'), may hold values from -0.3 to 0.3
- contacts: int32 [6, 32, 32, 1024], P(None, 'gx', 'gy', 'gz'), may hold values from -1 to 8, as said below
- leaving: int32 [4, 4, 8, 64], P('gx', 'gy', 'gz'), may hold values from -1 to 8191, as said below
Outputs:
- new_offset: float32 [3, 32, 32, 1024], P(None, 'gx', 'gy', 'gz')
- new_velocity: float32 [3, 32, 32, 1024], P(None, 'gx', 'gy', 'gz')
- new_spin: float32 [3, 32, 32, 1024], P(None, 'gx', 'gy', 'gz')
- new_history: float32 [6, 3, 32, 32, 1024], P(None, None, 'gx', 'gy', 'gz')
- arrivals: float32 [28, 4, 4, 8, 64], P(None, 'gx', 'gy', 'gz')
The draws below stay inside these ranges and needn't reach their ends.
Inputs may be any that keep to these rules, and one draw needn't show every extreme that they name: `contacts`: the live codes of one particle are distinct. `leaving`: each block's live entries are distinct cells with z index 0 or 1 within the block, listed first and followed by -1; at most 64 are live, and some block has 64 live.
All inputs are finite; a program needn't handle non-finite values.
Results may differ from the reference program's by a relative error of at most 0.0003.
Values sent between devices are 32-bit elements; how exact they have to be, the bound alone decides.
A program may use at most 512 MiB of HBM per device.

```python
import jax
import jax.numpy as jnp
import numpy as np
from jax import lax

CX = 8
CY = 8
CZ = 128
K = 6
DIRS = 9
CAP = 64
NX = 32
NY = 32
NZ = 1024
N_GX = 4
N_GY = 4
N_GZ = 8


def draw_contacts(key, part):
    alive_key = jax.random.fold_in(key, 11)
    ranking_key = jax.random.fold_in(key, 12)
    height = jnp.arange(NZ, dtype=jnp.int32)
    percent = 95 - 60 * height // NZ
    dice_rolls = jax.random.randint(alive_key, (K, NX, NY, NZ), 0, 100)
    slot_alive = dice_rolls < percent[None, None, None, :]
    scores = jax.random.randint(ranking_key, (DIRS, NX, NY, NZ), 0, 1 << 20) * DIRS + jnp.arange(DIRS, dtype=jnp.int32)[:, None, None, None]
    ranking = jnp.argsort(scores, axis=0, stable=True)[:K].astype(jnp.int32)
    return jnp.where(slot_alive, ranking, -1).astype(jnp.int32)


def draw_leaving(key, part):
    blocks_x = NX // CX
    blocks_y = NY // CY
    blocks_z = NZ // CZ
    choose_key = jax.random.fold_in(key, 21)
    count_key = jax.random.fold_in(key, 22)
    full_key = jax.random.fold_in(key, 23)
    candidates = 2 * CX * CY
    scores = jax.random.randint(choose_key, (blocks_x, blocks_y, blocks_z, candidates), 0, 1 << 20) * candidates + jnp.arange(candidates, dtype=jnp.int32)
    picks = jnp.argsort(scores, axis=-1, stable=True)[..., :CAP].astype(jnp.int32)
    local_x = picks // (2 * CY)
    local_y = picks // 2 % CY
    local_z = picks % 2
    local_cell = (local_x * CY + local_y) * CZ + local_z
    counts = jax.random.randint(count_key, (blocks_x, blocks_y, blocks_z), CAP // 3, CAP + 1)
    chosen_block = jax.random.randint(full_key, (), 0, blocks_x * blocks_y * blocks_z)
    block_number = jnp.arange(blocks_x * blocks_y * blocks_z, dtype=jnp.int32).reshape(blocks_x, blocks_y, blocks_z)
    counts = jnp.where(block_number == chosen_block, CAP, counts)
    slot_number = jnp.arange(CAP, dtype=jnp.int32)
    return jnp.where(slot_number < counts[..., None], local_cell, -1).astype(jnp.int32)


def steps_of(own_key, dims, cuts, low, largest):
    loudness = 1.0
    for axis_at, blocks in cuts:
        draws = jax.random.uniform(jax.random.fold_in(jax.random.fold_in(own_key, 6), axis_at), (blocks,), jnp.float32, low / len(cuts), largest / len(cuts))
        loudness = loudness * jnp.repeat(jnp.exp(draws), dims[axis_at] // blocks).reshape((-1,) + (1,) * (len(dims) - 1 - axis_at))
    return loudness


def bell_draw(own_key, extent, width, bound, shards=(), held_as=jnp.bfloat16):
    loudness = steps_of(own_key, extent, shards, -0.22, 0.18) if shards else 1.0
    entries = jax.random.normal(own_key, extent, jnp.float32) * width * loudness
    return jnp.minimum(jnp.maximum(entries, -bound), bound).astype(held_as)


def setup_inputs(seed: int = 0) -> dict:
    arg_keys = jax.random.split(jax.random.key(seed), 8)
    offset = bell_draw(arg_keys[0], (3, NX, NY, NZ), 0.06, 0.25, ((1, 4), (2, 4), (3, 8)), jnp.float32)
    velocity = bell_draw(arg_keys[1], (3, NX, NY, NZ), 0.5, 3.0, ((1, 4), (2, 4), (3, 8)), jnp.float32)
    spin = bell_draw(arg_keys[2], (3, NX, NY, NZ), 0.5, 3.0, ((1, 4), (2, 4), (3, 8)), jnp.float32)
    radius = jnp.clip(0.62 + 0.19999999 * jax.random.uniform(arg_keys[3], (NX, NY, NZ), jnp.float32) ** steps_of(arg_keys[3], (NX, NY, NZ), ((0, 4), (1, 4), (2, 8)), -0.2, 0.2), 0.62, 0.82)
    history = bell_draw(arg_keys[4], (K, 3, NX, NY, NZ), 0.05, 0.3, ((2, 4), (3, 4), (4, 8)), jnp.float32)
    contacts = draw_contacts(jax.random.fold_in(arg_keys[7], 71), 0)
    leaving = draw_leaving(jax.random.fold_in(arg_keys[7], 71), 0)
    return dict(offset=offset, velocity=velocity, spin=spin, radius=radius, history=history, contacts=contacts, leaving=leaving)


forward_dirs = np.array([[1, 0, 0], [0, 1, 0], [0, 0, 1], [1, 1, 0], [1, -1, 0], [1, 0, 1], [1, 0, -1], [0, 1, 1], [0, 1, -1]], np.int32)
stiff_normal = 10.0
damp_normal = 2.0
stiff_shear = 8.0
damp_shear = 1.5
friction = 0.4
shear_floor = 0.05
time_step = 0.05
gravity = 1.0

def cross_product(first_vec, second_vec):
    return jnp.stack([first_vec[1] * second_vec[2] - first_vec[2] * second_vec[1], first_vec[2] * second_vec[0] - first_vec[0] * second_vec[2], first_vec[0] * second_vec[1] - first_vec[1] * second_vec[0]], 0)

def contact_pair(centers, partner, direction, shear):
    separation = direction + partner[0:3] - centers[0:3]
    distance = jnp.sqrt(lax.optimization_barrier(jnp.sum(separation * separation, 0)))
    normal = separation / distance
    radius_center = centers[9]
    radius_partner = partner[9]
    radius_sum = radius_center + radius_partner
    intersection = jnp.maximum(radius_sum - distance, 0.0)
    contact = jnp.sqrt(radius_center * radius_partner / radius_sum * intersection)
    relative = partner[3:6] - centers[3:6] - cross_product(radius_center * centers[6:9] + radius_partner * partner[6:9], normal)
    approach = lax.optimization_barrier(jnp.sum(relative * normal, 0))
    sliding = relative - approach * normal
    repulsion = jnp.maximum(stiff_normal * contact * intersection - damp_normal * contact * approach, 0.0)
    spring = shear - lax.optimization_barrier(jnp.sum(shear * normal, 0)) * normal + time_step * sliding
    trial_force = stiff_shear * contact * spring + damp_shear * contact * sliding
    magnitude = jnp.sqrt(lax.optimization_barrier(jnp.sum(trial_force * trial_force, 0)))
    factor = jnp.minimum(1.0, friction * repulsion / jnp.maximum(magnitude, shear_floor))
    tangent = factor * trial_force
    pair_force = tangent - repulsion * normal
    twisting = cross_product(normal, tangent)
    return (pair_force, radius_center * twisting, radius_partner * twisting, factor * spring)

def contact_terms(centers, shear, codes, source, base_index, stride_x, stride_y):
    table = jnp.asarray(forward_dirs, dtype=jnp.int32)
    stride_table = table[:, 0] * stride_x + table[:, 1] * stride_y + table[:, 2]
    direction_table = jnp.asarray(forward_dirs.T, dtype=jnp.float32)
    own_terms = jnp.zeros((6, centers.shape[1]), jnp.float32)
    partner_terms = jnp.zeros((6, source.shape[1]), jnp.float32)
    springs = []
    for which_slot in range(codes.shape[0]):
        slot_code = codes[which_slot]
        slot_live = slot_code >= 0
        chosen = jnp.maximum(slot_code, 0)
        selector = chosen[None, :] == jnp.arange(table.shape[0], dtype=jnp.int32)[:, None]
        direction = jnp.dot(direction_table, selector.astype(jnp.float32), precision=lax.Precision.HIGHEST)
        target = base_index + lax.optimization_barrier(jnp.sum(jnp.where(selector, stride_table[:, None], 0), 0)).astype(jnp.int32)
        partner = jnp.take(source, target, axis=1)
        pair_force, torque_center, torque_partner, spring = contact_pair(centers, partner, direction, shear[which_slot])
        own_terms = own_terms + jnp.where(slot_live[None], jnp.concatenate([pair_force, torque_center], 0), 0.0)
        partner_terms = partner_terms.at[:, target].add(jnp.where(slot_live[None], jnp.concatenate([-pair_force, torque_partner], 0), 0.0))
        springs.append(jnp.where(slot_live[None], spring, 0.0))
    return (own_terms, partner_terms, jnp.stack(springs, 0))

def cell_index(count_x, count_y, count_z, margin, span_y, span_z):
    across_x = jnp.arange(count_x, dtype=jnp.int32)[:, None, None] + margin
    across_y = jnp.arange(count_y, dtype=jnp.int32)[None, :, None] + margin
    across_z = jnp.arange(count_z, dtype=jnp.int32)[None, None, :] + margin
    return ((across_x * span_y + across_y) * span_z + across_z).reshape(-1)

def reference(offset, velocity, spin, radius, history, contacts, leaving):
    fields = jnp.concatenate([offset, velocity, spin, radius[None]], 0)
    padded = jnp.pad(fields, ((0, 0), (1, 1), (1, 1), (1, 1)))
    span_y = NY + 2
    span_z = NZ + 2
    base_index = cell_index(NX, NY, NZ, 1, span_y, span_z)
    own_terms, partner_terms, springs = contact_terms(fields.reshape(10, -1), history.reshape(K, 3, -1), contacts.reshape(K, -1), padded.reshape(10, -1), base_index, span_y * span_z, span_z)
    received = partner_terms.reshape(6, NX + 2, span_y, span_z)[:, 1:-1, 1:-1, 1:-1]
    totals = own_terms.reshape(6, NX, NY, NZ) + received
    slot_history = springs.reshape(K, 3, NX, NY, NZ)
    particle_mass = radius ** 3
    downward = jnp.asarray([0.0, 0.0, -gravity], dtype=jnp.float32).reshape(3, 1, 1, 1)
    moved_velocity = velocity + time_step * (totals[0:3] / particle_mass + downward)
    moved_spin = spin + time_step * totals[3:6] / (0.4 * particle_mass * radius * radius)
    moved_offset = offset + time_step * moved_velocity
    coord_x = jnp.broadcast_to(jnp.arange(NX, dtype=jnp.float32)[:, None, None], (NX, NY, NZ))
    coord_y = jnp.broadcast_to(jnp.arange(NY, dtype=jnp.float32)[None, :, None], (NX, NY, NZ))
    coord_z = jnp.broadcast_to(jnp.arange(NZ, dtype=jnp.float32)[None, None, :], (NX, NY, NZ))
    position = jnp.stack([coord_x, coord_y, coord_z], 0) + moved_offset
    leave_live = leaving >= 0
    picked = jnp.maximum(leaving, 0)
    block_x = jnp.arange(N_GX, dtype=jnp.int32)[:, None, None, None]
    block_y = jnp.arange(N_GY, dtype=jnp.int32)[None, :, None, None]
    block_z = jnp.arange(N_GZ, dtype=jnp.int32)[None, None, :, None]
    global_x = block_x * CX + picked // (CY * CZ)
    global_y = block_y * CY + picked // CZ % CY
    global_z = block_z * CZ + picked % CZ
    pieces = [position, moved_velocity, moved_spin, radius[None], slot_history.reshape(3 * K, NX, NY, NZ)]
    outbox = jnp.concatenate([piece[:, global_x, global_y, global_z] for piece in pieces], 0)
    outbox = jnp.where(leave_live[None], outbox, 0.0)
    arrivals = jnp.concatenate([outbox[:, :, :, 1:], jnp.zeros_like(outbox[:, :, :, :1])], 3)
    departed = jnp.zeros((NX, NY, NZ), jnp.float32).at[global_x, global_y, global_z].add(leave_live.astype(jnp.float32))
    staying = 1.0 - departed
    return (moved_offset * staying, moved_velocity * staying, moved_spin * staying, slot_history * staying, arrivals)
```

```python
import functools

import jax
import jax.numpy as jnp
from jax import lax
from jax.experimental import pallas as pl
from jax.experimental.pallas import tpu as pltpu
from jax.sharding import PartitionSpec as P

MESH = pl.DeviceIdType.MESH
AXES = ("gx", "gy", "gz")
DIRS = (
    (1, 0, 0),
    (0, 1, 0),
    (0, 0, 1),
    (1, 1, 0),
    (1, -1, 0),
    (1, 0, 1),
    (1, 0, -1),
    (0, 1, 1),
    (0, 1, -1),
)
SLOTS = 6
FIELDS = 10
SHEAR = FIELDS
CODES = FIELDS + 3 * SLOTS
FULL = CODES + SLOTS
PACKS = (FULL * 8 + 127) // 128
STEP = 0.05
TINY = 1e-30

ROWS = 24
HEIGHT = 10 * ROWS

PACK_FROM = (
    (0, 0, -1),
    (0, 0, 1),
    (-1, 0, -1),
    (-1, 0, 1),
    (1, 0, -1),
    (1, 0, 1),
    (0, -1, -1),
    (0, -1, 1),
    (0, 1, -1),
    (0, 1, 1),
)
FLAT_FROM = (
    (-1, 0, 0),
    (1, 0, 0),
    (0, -1, 0),
    (0, 1, 0),
    (-1, -1, 0),
    (-1, 1, 0),
    (1, -1, 0),
    (1, 1, 0),
)
SENDERS = FLAT_FROM + PACK_FROM


def plane(x):
    return (x + 1) * ROWS + 8


def halo_kernel(
    off_hbm, vel_hbm, spin_hbm, rad_hbm, hist_hbm, con_hbm,
    xlo, xhi, ylo, yhi, edges, packs, own_packs,
    cells, codes, yrows, rows, local_sems, send_sems, recv_sems,
):
    here = [lax.axis_index(a) for a in AXES]
    size = [lax.axis_size(a) for a in AXES]

    def exists(step):
        ok = None
        for at, n, s in zip(here, size, step):
            if s == 0:
                continue
            test = at + s < n if s > 0 else at + s >= 0
            ok = test if ok is None else jnp.logical_and(ok, test)
        return ok

    def place(step):
        return tuple(at + s for at, s in zip(here, step))

    loads = [
        pltpu.make_async_copy(off_hbm, cells.at[0:3], local_sems.at[0]),
        pltpu.make_async_copy(vel_hbm, cells.at[3:6], local_sems.at[1]),
        pltpu.make_async_copy(spin_hbm, cells.at[6:9], local_sems.at[2]),
        pltpu.make_async_copy(rad_hbm, cells.at[9:10], local_sems.at[3]),
        pltpu.make_async_copy(hist_hbm, cells.at[SHEAR:CODES], local_sems.at[4]),
        pltpu.make_async_copy(con_hbm, codes, local_sems.at[5]),
    ]
    for load in loads:
        load.start()
    barrier = pltpu.get_barrier_semaphore()
    expected = jnp.int32(0)
    for step in SENDERS:
        there = exists(step)
        expected = expected + there.astype(jnp.int32)

        @pl.when(there)
        def _():
            pl.semaphore_signal(barrier, inc=1, device_id=place(step), device_id_type=MESH)

    for load in loads:
        load.wait()
    for s in range(SLOTS):
        cells[CODES + s] = codes[s].astype(jnp.float32)
    lane = lax.broadcasted_iota(jnp.int32, (8, 128), 1)
    for k in range(PACKS):
        low = jnp.zeros((8, 128), jnp.float32)
        top = jnp.zeros((8, 128), jnp.float32)
        for c in range(k * 16, min(FULL, k * 16 + 16)):
            for x in range(8):
                p = (c % 16) * 8 + x
                value = cells[c, x * 8 : x * 8 + 8, :]
                if p:
                    value = pltpu.roll(value, p, 1)
                low = jnp.where(lane == p, value, low)
                top = jnp.where(lane == (p - 1) % 128, value, top)
        own_packs[0, k] = low
        own_packs[1, k] = top
    for c in range(FULL):
        yrows[0, c] = cells[c, pl.ds(0, 8, stride=8), :]
        yrows[1, c] = cells[c, pl.ds(7, 8, stride=8), :]
    for which, row in enumerate((63, 56, 7, 0)):
        for c in range(FULL if which < 2 else FIELDS):
            rows[which, c : c + 1, :] = cells[c, row : row + 1, :]

    targets = [xlo, xhi, ylo, yhi] + [edges.at[k] for k in range(4)] + [
        packs.at[k] for k in range(len(PACK_FROM))
    ]
    sources = (
        [cells.at[:, 56:64, :], cells.at[0:FIELDS, 0:8, :], yrows.at[1], yrows.at[0]]
        + [rows.at[k] for k in range(4)]
        + [own_packs.at[0 if s[2] > 0 else 1] for s in PACK_FROM]
    )

    def copy(k):
        to = tuple(-s for s in SENDERS[k])
        return pltpu.make_async_remote_copy(
            src_ref=sources[k],
            dst_ref=targets[k],
            send_sem=send_sems.at[k],
            recv_sem=recv_sems.at[k],
            device_id=place(to),
            device_id_type=MESH,
        )

    for k, step in enumerate(SENDERS):

        @pl.when(jnp.logical_not(exists(step)))
        def _():
            targets[k][...] = jnp.zeros(targets[k].shape, jnp.float32)

    pl.semaphore_wait(barrier, expected)
    for k, step in enumerate(SENDERS):

        @pl.when(exists(tuple(-s for s in step)))
        def _():
            copy(k).start()

    for k, step in enumerate(SENDERS):

        @pl.when(exists(step))
        def _():
            copy(k).wait_recv()

        @pl.when(exists(tuple(-s for s in step)))
        def _():
            copy(k).wait_send()


def cross(a, b):
    return [
        a[1] * b[2] - a[2] * b[1],
        a[2] * b[0] - a[0] * b[2],
        a[0] * b[1] - a[1] * b[0],
    ]


def dot3(a, b):
    return a[0] * b[0] + a[1] * b[1] + a[2] * b[2]


def pair(first, second, direction, shear, live):
    sep = []
    for k in range(3):
        gap = second[k] - first[k]
        sep.append(gap + float(direction[k]) if direction[k] else gap)
    square = dot3(sep, sep)
    inverse = lax.rsqrt(square)
    normal = [s * inverse for s in sep]
    radii = first[9] + second[9]
    overlap = jnp.maximum(radii - square * inverse, 0.0)
    product = first[9] * second[9] * overlap
    contact = product * lax.rsqrt(jnp.maximum(product * radii, TINY))
    contact = jnp.where(live, contact, 0.0)
    surface = cross([first[6 + k] + second[6 + k] for k in range(3)], normal)
    relative = [second[3 + k] - first[3 + k] - surface[k] for k in range(3)]
    approach = dot3(relative, normal)
    sliding = [relative[k] - approach * normal[k] for k in range(3)]
    repulsion = contact * jnp.maximum(10.0 * overlap - 2.0 * approach, 0.0)
    along = dot3(shear, normal)
    spring = [shear[k] - along * normal[k] + STEP * sliding[k] for k in range(3)]
    pull = [8.0 * spring[k] + 1.5 * sliding[k] for k in range(3)]
    size = contact * contact * dot3(pull, pull)
    factor = jnp.minimum(1.0, 0.4 * repulsion * lax.rsqrt(jnp.maximum(size, 0.0025)))
    scale = factor * contact
    tangent = [scale * pull[k] for k in range(3)]
    force = [tangent[k] - repulsion * normal[k] for k in range(3)]
    return force, cross(normal, tangent), [factor * spring[k] for k in range(3)]


def pick_shear(load, code, number):
    masks = [code(s) == number for s in range(SLOTS)]
    live = masks[0]
    shear = [jnp.where(masks[0], load(k), 0.0) for k in range(3)]
    for s in range(1, SLOTS):
        live = jnp.logical_or(live, masks[s])
        shear = [jnp.where(masks[s], load(3 * s + k), shear[k]) for k in range(3)]
    return shear, live, masks


def compute_kernel(
    off, vel, spin, rad, hist, con, leaving, xlo, xhi, ylo, yhi, edges, packs, own_packs,
    new_off, new_vel, new_spin, new_hist, outbox,
    pad, pad_up, pad_down, level, rising, falling, side, zside,
):
    lane = lax.broadcasted_iota(jnp.int32, (8, 128), 1)
    sub = lax.broadcasted_iota(jnp.int32, (8, 128), 0)
    zero = jnp.zeros((8, 128), jnp.float32)

    def scaled(values):
        return values[:6] + [v * values[9] for v in values[6:9]] + [values[9]]

    for x in range(8):
        rows = pl.ds(plane(x), 8)
        here = slice(x * 8, x * 8 + 8)
        values = [off[k, here] for k in range(3)] + [vel[k, here] for k in range(3)]
        values += [spin[k, here] for k in range(3)] + [rad[0, here]]
        for c, v in enumerate(scaled(values)):
            pad[c, rows, :] = v
    for source, first in ((ylo, plane(0) - 1), (yhi, plane(0) + 8)):
        for c, v in enumerate(scaled([source[c] for c in range(FIELDS)])):
            pad[c, pl.ds(first, 8, stride=ROWS), :] = v
    for c, v in enumerate(scaled([xhi[c] for c in range(FIELDS)])):
        pad[c, pl.ds(plane(8), 8), :] = v
    for which, row in ((2, plane(8) - 1), (3, plane(8) + 8)):
        for c, v in enumerate(scaled([edges[which, c : c + 1, :] for c in range(FIELDS)])):
            pad[c, row : row + 1, :] = v

    def first_pack(pack):
        shift = [pltpu.roll(pack, 128 - 8 * (9 - c), 1) for c in (6, 7, 8)]
        group = lane // 8
        return jnp.where(
            group == 6, pack * shift[0],
            jnp.where(group == 7, pack * shift[1], jnp.where(group == 8, pack * shift[2], pack)),
        )

    def first_top(pack):
        shift = [pltpu.roll(pack, 128 - 8 * (9 - c), 1) for c in (6, 7, 8)]
        group = (lane + 1) // 8
        return jnp.where(
            group == 6, pack * shift[0],
            jnp.where(group == 7, pack * shift[1], jnp.where(group == 8, pack * shift[2], pack)),
        )

    above = [first_pack(packs[k, 0]) for k in (1, 5, 9)]
    below = [first_top(packs[k, 0]) for k in (0, 4, 8)]
    for c in range(FIELDS):
        for x in range(9):
            for tile in range(2 if x < 8 else 1):
                which = 1 if x == 8 else 2 * tile
                p = c * 8 + x % 8
                rows = pl.ds(plane(x) + 8 * tile, 8)
                value = pad[c, rows, :]
                up = pltpu.roll(value, 127, 1)
                pad_up[c, rows, :] = jnp.where(
                    lane == 127, pltpu.roll(above[which], 127 - p, 1), up
                )
                down = pltpu.roll(value, 1, 1)
                pad_down[c, rows, :] = jnp.where(
                    lane == 0, pltpu.roll(below[which], (129 - p) % 128, 1), down
                )

    for total in (level, rising, falling):
        for c in range(6):
            for x in range(9):
                total[c, pl.ds(plane(x), 8), :] = zero
                total[c, pl.ds(plane(x) - 8, 8), :] = zero
                total[c, pl.ds(plane(x) + 8, 8), :] = zero

    def add(total, rows, force, twist, sign):
        for k in range(3):
            total[k, rows, :] = total[k, rows, :] + (force[k] if sign > 0 else -force[k])
            total[3 + k, rows, :] = total[3 + k, rows, :] + twist[k]

    def body(x, carry):
        base = pl.multiple_of((x + 1) * ROWS + 8, 8)
        here = pl.ds(pl.multiple_of(x * 8, 8), 8)
        first = [pad[c, pl.ds(base, 8), :] for c in range(FIELDS)]
        forces = [zero] * 3
        twists = [zero] * 3
        springs = [zero] * (3 * SLOTS)
        for number, (dx, dy, dz) in enumerate(DIRS):
            rows = pl.ds(base + dx * ROWS + dy, 8)
            source = (pad, pad_up, pad_down)[dz]
            total = (level, rising, falling)[dz]
            second = [source[c, rows, :] for c in range(FIELDS)]
            shear, live, masks = pick_shear(
                lambda c: hist[c, here, :], lambda s: con[s, here, :], number
            )
            force, twist, spring = pair(first, second, (dx, dy, dz), shear, live)
            for k in range(3):
                forces[k] = forces[k] + force[k]
                twists[k] = twists[k] + twist[k]
                for s in range(SLOTS):
                    springs[3 * s + k] = jnp.where(masks[s], spring[k], springs[3 * s + k])
            add(total, rows, force, twist, -1)
        add(level, pl.ds(base, 8), forces, twists, 1)
        for c in range(3 * SLOTS):
            new_hist[c, here, :] = springs[c]
        return carry

    lax.fori_loop(0, 8, body, 0)

    def shifted(values, amount):
        return [pltpu.roll(v, amount, 1) for v in values]

    def outer(rows, load, number, second, dead=None, turn=0):
        first = scaled([load(c, rows) for c in range(FIELDS)])
        shear, live, _ = pick_shear(
            lambda c: load(SHEAR + c, rows), lambda s: load(CODES + s, rows), float(number)
        )
        if turn:
            alive = jnp.where(live, 1.0, 0.0)
            moved = shifted(first + shear + [alive], turn)
            first, shear, live = moved[:10], moved[10:13], moved[13] > 0.5
        if dead is not None:
            live = jnp.logical_and(live, jnp.logical_not(dead))
        force, twist, _ = pair(first, second, DIRS[number], shear, live)
        return force, twist

    def load_side(c, rows):
        return side[c, rows, :]

    for c in range(FULL):
        side[c, 8:16, :] = xlo[c]
        side[c, 7:8, :] = edges[0, c : c + 1, :]
        side[c, 16:17, :] = edges[1, c : c + 1, :]
    mine = pl.ds(plane(0), 8)
    second = [pad[c, mine, :] for c in range(FIELDS)]
    for number in (0, 3, 4, 5, 6):
        dx, dy, dz = DIRS[number]
        dead = None if dz == 0 else lane == (0 if dz > 0 else 127)
        force, twist = outer(
            pl.ds(8 - dy, 8), load_side, number, second, dead, (0, 1, 127)[dz]
        )
        add(level, mine, force, twist, -1)
    for c in range(FULL):
        side[c, 8:16, :] = ylo[c]
    mine = pl.ds(plane(0), 8, stride=ROWS)
    second = [pad[c, mine, :] for c in range(FIELDS)]
    for number in (1, 3, 7, 8):
        dx, dy, dz = DIRS[number]
        dead = sub == 0 if dx else (None if dz == 0 else lane == (0 if dz > 0 else 127))
        force, twist = outer(
            pl.ds(8 - dx, 8), load_side, number, second, dead, (0, 1, 127)[dz]
        )
        add(level, mine, force, twist, -1)
    for c in range(FULL):
        side[c, 8:16, :] = yhi[c]
    mine = pl.ds(plane(0) + 7, 8, stride=ROWS)
    second = [pad[c, mine, :] for c in range(FIELDS)]
    force, twist = outer(pl.ds(7, 8), load_side, 4, second, sub == 0)
    add(level, mine, force, twist, -1)

    def spread(pack, c, top):
        p = (c % 16) * 8 - top
        return pltpu.roll(pack, (128 - p) % 128, 1) if p % 128 else pack

    for end in range(2):
        top = 1 - end
        for k in range(PACKS):
            straight, behind, left = packs[end, k], packs[2 + end, k], packs[6 + end, k]
            for c in range(16 * k, min(FULL, 16 * k + 16)):
                before = pltpu.roll(spread(behind, c, top), 120, 1)
                zside[end, c, 8:16, :] = jnp.where(
                    lane == 127, before, spread(straight, c, top)
                )
                zside[end, c, 0:8, :] = spread(left, c, top)

    for end, numbers in ((0, (2, 5, 7)), (1, (6, 8))):
        mine = own_packs[end, 0]
        second = scaled([spread(mine, c, end) for c in range(FIELDS)])
        forces = [zero] * 3
        twists = [zero] * 3
        for number in numbers:
            dx, dy, dz = DIRS[number]
            force, twist = outer(
                pl.ds(8 - dy, 8), lambda c, rows: zside[end, c, rows, :], number, second,
                None, dx,
            )
            forces = [forces[k] + force[k] for k in range(3)]
            twists = [twists[k] + twist[k] for k in range(3)]
        edge = 127 * end
        for x in range(8):
            turn = (edge - x) % 128
            rows = pl.ds(plane(x), 8)
            hold = lane == edge
            add(
                level, rows,
                [jnp.where(hold, pltpu.roll(v, turn, 1) if turn else v, 0.0) for v in forces],
                [jnp.where(hold, pltpu.roll(v, turn, 1) if turn else v, 0.0) for v in twists],
                -1,
            )

    names = leaving[...]
    wide = jnp.broadcast_to(names, (8, 64))
    deep = lax.broadcasted_iota(jnp.int32, (8, 64), 0)
    starts = [(lax.axis_index(a) * n).astype(jnp.float32) for a, n in zip(AXES, (8, 8, 128))]
    boxes = [jnp.zeros((8, 64), jnp.float32) for _ in range(28)]
    for x in range(8):
        rows = pl.ds(plane(x), 8)
        here = slice(x * 8, x * 8 + 8)
        sums = []
        for c in range(6):
            up = jnp.where(lane == 0, 0.0, pltpu.roll(rising[c, rows, :], 1, 1))
            down = jnp.where(lane == 127, 0.0, pltpu.roll(falling[c, rows, :], 127, 1))
            sums.append(level[c, rows, :] + up + down)
        radius = rad[0, here, :]
        inverse = 1.0 / radius
        push = STEP * inverse * inverse * inverse
        turn = 0.125 * (inverse * inverse) * (inverse * inverse)
        velocity = [vel[k, here, :] + push * sums[k] for k in range(3)]
        velocity[2] = velocity[2] - STEP
        offset = [off[k, here, :] + STEP * velocity[k] for k in range(3)]
        rotation = [spin[k, here, :] + turn * sums[3 + k] for k in range(3)]
        springs = [new_hist[c, here, :] for c in range(3 * SLOTS)]
        bottom = [wide == (x * 8 + deep) * 128 + z for z in range(2)]
        left = [
            jnp.max(jnp.where(b, 1.0, 0.0), axis=1, keepdims=True) for b in bottom
        ]
        staying = 1.0 - jnp.where(lane == 0, left[0], jnp.where(lane == 1, left[1], 0.0))
        lanes = lane.astype(jnp.float32)
        position = [
            offset[0] + (starts[0] + float(x)),
            offset[1] + (starts[1] + sub.astype(jnp.float32)),
            offset[2] + (starts[2] + lanes),
        ]
        for c, v in enumerate(position + velocity + rotation + [radius] + springs):
            for z in range(2):
                value = jnp.broadcast_to(v[:, z : z + 1], (8, 64))
                boxes[c] = boxes[c] + jnp.where(bottom[z], value, 0.0)
        for k in range(3):
            new_off[k, here, :] = offset[k] * staying
            new_vel[k, here, :] = velocity[k] * staying
            new_spin[k, here, :] = rotation[k] * staying
        for c in range(3 * SLOTS):
            new_hist[c, here, :] = springs[c] * staying
    for c in range(28):
        outbox[c : c + 1, :] = jnp.sum(boxes[c], axis=0, keepdims=True)


def on_device(offset, velocity, spin, radius, history, contacts, leaving):
    f32 = jnp.float32
    off = offset.reshape(3, 64, 128)
    vel = velocity.reshape(3, 64, 128)
    spn = spin.reshape(3, 64, 128)
    rad = radius.reshape(1, 64, 128)
    hist = history.reshape(3 * SLOTS, 64, 128)
    con = contacts.reshape(SLOTS, 64, 128)
    vmem = pl.BlockSpec(memory_space=pltpu.VMEM)
    anywhere = pl.BlockSpec(memory_space=pl.ANY)
    halo_shapes = (
        (FULL, 8, 128),
        (FIELDS, 8, 128),
        (FULL, 8, 128),
        (FULL, 8, 128),
        (4, 40, 128),
        (len(PACK_FROM), PACKS, 8, 128),
        (2, PACKS, 8, 128),
    )
    halos = pl.pallas_call(
        halo_kernel,
        out_shape=[jax.ShapeDtypeStruct(s, f32) for s in halo_shapes],
        in_specs=[anywhere] * 6,
        out_specs=[vmem] * len(halo_shapes),
        scratch_shapes=[
            pltpu.VMEM((FULL, 64, 128), f32),
            pltpu.VMEM((SLOTS, 64, 128), jnp.int32),
            pltpu.VMEM((2, FULL, 8, 128), f32),
            pltpu.VMEM((4, 40, 128), f32),
            pltpu.SemaphoreType.DMA((6,)),
            pltpu.SemaphoreType.DMA((len(SENDERS),)),
            pltpu.SemaphoreType.DMA((len(SENDERS),)),
        ],
        compiler_params=pltpu.CompilerParams(collective_id=0, has_side_effects=True),
        name="halo",
    )(off, vel, spn, rad, hist, con)
    state = jax.ShapeDtypeStruct((3, 64, 128), f32)
    new_off, new_vel, new_spin, new_hist, outbox = pl.pallas_call(
        compute_kernel,
        out_shape=[
            state, state, state,
            jax.ShapeDtypeStruct((3 * SLOTS, 64, 128), f32),
            jax.ShapeDtypeStruct((28, 64), f32),
        ],
        in_specs=[vmem] * 14,
        out_specs=[vmem] * 5,
        scratch_shapes=[
            pltpu.VMEM((FIELDS, HEIGHT, 128), f32),
            pltpu.VMEM((FIELDS, HEIGHT, 128), f32),
            pltpu.VMEM((FIELDS, HEIGHT, 128), f32),
            pltpu.VMEM((6, HEIGHT, 128), f32),
            pltpu.VMEM((6, HEIGHT, 128), f32),
            pltpu.VMEM((6, HEIGHT, 128), f32),
            pltpu.VMEM((FULL, ROWS, 128), f32),
            pltpu.VMEM((2, FULL, ROWS, 128), f32),
        ],
        name="pairs",
    )(off, vel, spn, rad, hist, con, leaving.reshape(1, 64), *halos)
    count = lax.axis_size("gz")
    arrivals = lax.ppermute(outbox, "gz", [(i + 1, i) for i in range(count - 1)])
    return (
        new_off.reshape(3, 8, 8, 128),
        new_vel.reshape(3, 8, 8, 128),
        new_spin.reshape(3, 8, 8, 128),
        new_hist.reshape(SLOTS, 3, 8, 8, 128),
        arrivals.reshape(28, 1, 1, 1, 64),
    )


def solution(mesh):
    placed = (
        P(None, "gx", "gy", "gz"),
        P(None, "gx", "gy", "gz"),
        P(None, "gx", "gy", "gz"),
        P("gx", "gy", "gz"),
        P(None, None, "gx", "gy", "gz"),
        P(None, "gx", "gy", "gz"),
        P("gx", "gy", "gz", None),
    )
    return jax.shard_map(
        on_device,
        mesh=mesh,
        in_specs=placed,
        out_specs=(
            P(None, "gx", "gy", "gz"),
            P(None, "gx", "gy", "gz"),
            P(None, "gx", "gy", "gz"),
            P(None, None, "gx", "gy", "gz"),
            P(None, "gx", "gy", "gz", None),
        ),
        check_vma=False,
    )
```

```python
import jax
import jax.numpy as jnp
from jax import lax
from jax.experimental import pallas as pl
from jax.experimental.pallas import tpu as pltpu
from jax.sharding import PartitionSpec as P

MESH = pl.DeviceIdType.MESH
AXES = ("gx", "gy", "gz")
DIRS = (
    (1, 0, 0),
    (0, 1, 0),
    (0, 0, 1),
    (1, 1, 0),
    (1, -1, 0),
    (1, 0, 1),
    (1, 0, -1),
    (0, 1, 1),
    (0, 1, -1),
)
SLOTS = 6
FIELDS = 10
SHEAR = FIELDS
CODES = FIELDS + 3 * SLOTS
FULL = CODES + SLOTS
PACKS = (FULL * 8 + 127) // 128
STEP = 0.05
TINY = 1e-30

ROWS = 24
HEIGHT = 10 * ROWS

PACK_FROM = (
    (0, 0, -1),
    (0, 0, 1),
    (-1, 0, -1),
    (-1, 0, 1),
    (1, 0, -1),
    (1, 0, 1),
    (0, -1, -1),
    (0, -1, 1),
    (0, 1, -1),
    (0, 1, 1),
)
FLAT_FROM = (
    (-1, 0, 0),
    (1, 0, 0),
    (0, -1, 0),
    (0, 1, 0),
    (-1, -1, 0),
    (-1, 1, 0),
    (1, -1, 0),
    (1, 1, 0),
)
SENDERS = FLAT_FROM + PACK_FROM


def plane(x):
    return (x + 1) * ROWS + 8


def step_kernel(
    off_hbm, vel_hbm, spin_hbm, rad_hbm, hist_hbm, con_hbm, leaving_hbm,
    state, arrivals,
    xlo, xhi, ylo, yhi, edges, packs, own_packs, cells, codes, leaving, yrows, rows, outbox,
    pad, pad_up, pad_down, level, rising, falling, side, zside,
    local_sems, send_sems, recv_sems,
):
    here = [lax.axis_index(a) for a in AXES]
    size = [lax.axis_size(a) for a in AXES]

    def exists(step):
        ok = None
        for at, n, s in zip(here, size, step):
            if s == 0:
                continue
            test = at + s < n if s > 0 else at + s >= 0
            ok = test if ok is None else jnp.logical_and(ok, test)
        return ok

    def place(step):
        return tuple(at + s for at, s in zip(here, step))

    loads = [
        pltpu.make_async_copy(off_hbm, cells.at[0:3], local_sems.at[0]),
        pltpu.make_async_copy(vel_hbm, cells.at[3:6], local_sems.at[1]),
        pltpu.make_async_copy(spin_hbm, cells.at[6:9], local_sems.at[2]),
        pltpu.make_async_copy(rad_hbm, cells.at[9:10], local_sems.at[3]),
        pltpu.make_async_copy(hist_hbm, cells.at[SHEAR:CODES], local_sems.at[4]),
        pltpu.make_async_copy(con_hbm, codes, local_sems.at[5]),
        pltpu.make_async_copy(leaving_hbm, leaving, local_sems.at[6]),
    ]
    for load in loads:
        load.start()
    barrier = pltpu.get_barrier_semaphore()
    expected = jnp.int32(0)
    for step in SENDERS:
        there = exists(step)
        expected = expected + there.astype(jnp.int32)

        @pl.when(there)
        def _():
            pl.semaphore_signal(barrier, inc=1, device_id=place(step), device_id_type=MESH)

    for load in loads:
        load.wait()
    for s in range(SLOTS):
        cells[CODES + s] = codes[s].astype(jnp.float32)
    lane = lax.broadcasted_iota(jnp.int32, (8, 128), 1)
    for k in range(PACKS):
        low = jnp.zeros((8, 128), jnp.float32)
        top = jnp.zeros((8, 128), jnp.float32)
        for c in range(k * 16, min(FULL, k * 16 + 16)):
            for x in range(8):
                p = (c % 16) * 8 + x
                value = cells[c, x * 8 : x * 8 + 8, :]
                if p:
                    value = pltpu.roll(value, p, 1)
                low = jnp.where(lane == p, value, low)
                top = jnp.where(lane == (p - 1) % 128, value, top)
        own_packs[0, k] = low
        own_packs[1, k] = top
    for c in range(FULL):
        yrows[0, c] = cells[c, pl.ds(0, 8, stride=8), :]
        yrows[1, c] = cells[c, pl.ds(7, 8, stride=8), :]
    for which, row in enumerate((63, 56, 7, 0)):
        for c in range(FULL if which < 2 else FIELDS):
            rows[which, c : c + 1, :] = cells[c, row : row + 1, :]

    targets = [xlo, xhi, ylo, yhi] + [edges.at[k] for k in range(4)] + [
        packs.at[k] for k in range(len(PACK_FROM))
    ]
    sources = (
        [cells.at[:, 56:64, :], cells.at[0:FIELDS, 0:8, :], yrows.at[1], yrows.at[0]]
        + [rows.at[k] for k in range(4)]
        + [own_packs.at[0 if s[2] > 0 else 1] for s in PACK_FROM]
    )

    def copy(k):
        to = tuple(-s for s in SENDERS[k])
        return pltpu.make_async_remote_copy(
            src_ref=sources[k],
            dst_ref=targets[k],
            send_sem=send_sems.at[k],
            recv_sem=recv_sems.at[k],
            device_id=place(to),
            device_id_type=MESH,
        )

    for k, step in enumerate(SENDERS):

        @pl.when(jnp.logical_not(exists(step)))
        def _():
            targets[k][...] = jnp.zeros(targets[k].shape, jnp.float32)

    pl.semaphore_wait(barrier, expected)
    for k, step in enumerate(SENDERS):

        @pl.when(exists(tuple(-s for s in step)))
        def _():
            copy(k).start()

    for k, step in enumerate(SENDERS):

        @pl.when(exists(step))
        def _():
            copy(k).wait_recv()

        @pl.when(exists(tuple(-s for s in step)))
        def _():
            copy(k).wait_send()

    compute(
        cells.at[0:3], cells.at[3:6], cells.at[6:9], cells.at[9:10], cells.at[SHEAR:CODES],
        codes, leaving, xlo, xhi, ylo, yhi, edges, packs, own_packs,
        state.at[0:3], state.at[3:6], state.at[6:9], state.at[9:27], outbox,
        pad, pad_up, pad_down, level, rising, falling, side, zside,
    )

    last = len(SENDERS)
    fall = pltpu.make_async_remote_copy(
        src_ref=outbox,
        dst_ref=arrivals,
        send_sem=send_sems.at[last],
        recv_sem=recv_sems.at[last],
        device_id=place((0, 0, -1)),
        device_id_type=MESH,
    )

    @pl.when(exists((0, 0, -1)))
    def _():
        fall.start()

    @pl.when(exists((0, 0, 1)))
    def _():
        fall.wait_recv()

    @pl.when(jnp.logical_not(exists((0, 0, 1))))
    def _():
        arrivals[...] = jnp.zeros(arrivals.shape, jnp.float32)

    @pl.when(exists((0, 0, -1)))
    def _():
        fall.wait_send()


def write_kernel(state, arrivals, new_off, new_vel, new_spin, new_hist, entered, sems):
    copies = [
        pltpu.make_async_copy(state.at[9:27], new_hist, sems.at[0]),
        pltpu.make_async_copy(state.at[0:3], new_off, sems.at[1]),
        pltpu.make_async_copy(state.at[3:6], new_vel, sems.at[2]),
        pltpu.make_async_copy(state.at[6:9], new_spin, sems.at[3]),
    ]
    for copy in copies:
        copy.start()
    for c in range(28):
        entered[c] = arrivals[c : c + 1, 0:64]
    for copy in copies:
        copy.wait()


def cross(a, b):
    return [
        a[1] * b[2] - a[2] * b[1],
        a[2] * b[0] - a[0] * b[2],
        a[0] * b[1] - a[1] * b[0],
    ]


def dot3(a, b):
    return a[0] * b[0] + a[1] * b[1] + a[2] * b[2]


def pair(first, second, direction, shear, live):
    sep = []
    for k in range(3):
        gap = second[k] - first[k]
        sep.append(gap + float(direction[k]) if direction[k] else gap)
    square = dot3(sep, sep)
    inverse = lax.rsqrt(square)
    normal = [s * inverse for s in sep]
    radii = first[9] + second[9]
    overlap = jnp.maximum(radii - square * inverse, 0.0)
    product = first[9] * second[9] * overlap
    contact = product * lax.rsqrt(jnp.maximum(product * radii, TINY))
    contact = jnp.where(live, contact, 0.0)
    surface = cross([first[6 + k] + second[6 + k] for k in range(3)], normal)
    relative = [second[3 + k] - first[3 + k] - surface[k] for k in range(3)]
    approach = dot3(relative, normal)
    sliding = [relative[k] - approach * normal[k] for k in range(3)]
    repulsion = contact * jnp.maximum(10.0 * overlap - 2.0 * approach, 0.0)
    along = dot3(shear, normal)
    spring = [shear[k] - along * normal[k] + STEP * sliding[k] for k in range(3)]
    pull = [8.0 * spring[k] + 1.5 * sliding[k] for k in range(3)]
    size = contact * contact * dot3(pull, pull)
    factor = jnp.minimum(1.0, 0.4 * repulsion * lax.rsqrt(jnp.maximum(size, 0.0025)))
    scale = factor * contact
    tangent = [scale * pull[k] for k in range(3)]
    force = [tangent[k] - repulsion * normal[k] for k in range(3)]
    return force, cross(normal, tangent), [factor * spring[k] for k in range(3)]


def pick_shear(load, code, number):
    masks = [code(s) == number for s in range(SLOTS)]
    live = masks[0]
    shear = [jnp.where(masks[0], load(k), 0.0) for k in range(3)]
    for s in range(1, SLOTS):
        live = jnp.logical_or(live, masks[s])
        shear = [jnp.where(masks[s], load(3 * s + k), shear[k]) for k in range(3)]
    return shear, live, masks


def compute(
    off, vel, spin, rad, hist, con, leaving, xlo, xhi, ylo, yhi, edges, packs, own_packs,
    new_off, new_vel, new_spin, new_hist, outbox,
    pad, pad_up, pad_down, level, rising, falling, side, zside,
):
    lane = lax.broadcasted_iota(jnp.int32, (8, 128), 1)
    sub = lax.broadcasted_iota(jnp.int32, (8, 128), 0)
    zero = jnp.zeros((8, 128), jnp.float32)

    def scaled(values):
        return values[:6] + [v * values[9] for v in values[6:9]] + [values[9]]

    for x in range(8):
        rows = pl.ds(plane(x), 8)
        here = slice(x * 8, x * 8 + 8)
        values = [off[k, here] for k in range(3)] + [vel[k, here] for k in range(3)]
        values += [spin[k, here] for k in range(3)] + [rad[0, here]]
        for c, v in enumerate(scaled(values)):
            pad[c, rows, :] = v
    for source, first in ((ylo, plane(0) - 1), (yhi, plane(0) + 8)):
        for c, v in enumerate(scaled([source[c] for c in range(FIELDS)])):
            pad[c, pl.ds(first, 8, stride=ROWS), :] = v
    for c, v in enumerate(scaled([xhi[c] for c in range(FIELDS)])):
        pad[c, pl.ds(plane(8), 8), :] = v
    for which, row in ((2, plane(8) - 1), (3, plane(8) + 8)):
        for c, v in enumerate(scaled([edges[which, c : c + 1, :] for c in range(FIELDS)])):
            pad[c, row : row + 1, :] = v

    def first_pack(pack):
        shift = [pltpu.roll(pack, 128 - 8 * (9 - c), 1) for c in (6, 7, 8)]
        group = lane // 8
        return jnp.where(
            group == 6, pack * shift[0],
            jnp.where(group == 7, pack * shift[1], jnp.where(group == 8, pack * shift[2], pack)),
        )

    def first_top(pack):
        shift = [pltpu.roll(pack, 128 - 8 * (9 - c), 1) for c in (6, 7, 8)]
        group = (lane + 1) // 8
        return jnp.where(
            group == 6, pack * shift[0],
            jnp.where(group == 7, pack * shift[1], jnp.where(group == 8, pack * shift[2], pack)),
        )

    above = [first_pack(packs[k, 0]) for k in (1, 5, 9)]
    below = [first_top(packs[k, 0]) for k in (0, 4, 8)]
    for c in range(FIELDS):
        for x in range(9):
            for tile in range(2 if x < 8 else 1):
                which = 1 if x == 8 else 2 * tile
                p = c * 8 + x % 8
                rows = pl.ds(plane(x) + 8 * tile, 8)
                value = pad[c, rows, :]
                up = pltpu.roll(value, 127, 1)
                pad_up[c, rows, :] = jnp.where(
                    lane == 127, pltpu.roll(above[which], 127 - p, 1), up
                )
                down = pltpu.roll(value, 1, 1)
                pad_down[c, rows, :] = jnp.where(
                    lane == 0, pltpu.roll(below[which], (129 - p) % 128, 1), down
                )

    for total in (level, rising, falling):
        for c in range(6):
            for x in range(9):
                total[c, pl.ds(plane(x), 8), :] = zero
                total[c, pl.ds(plane(x) - 8, 8), :] = zero
                total[c, pl.ds(plane(x) + 8, 8), :] = zero

    def add(total, rows, force, twist, sign):
        for k in range(3):
            total[k, rows, :] = total[k, rows, :] + (force[k] if sign > 0 else -force[k])
            total[3 + k, rows, :] = total[3 + k, rows, :] + twist[k]

    def body(x, carry):
        base = pl.multiple_of((x + 1) * ROWS + 8, 8)
        here = pl.ds(pl.multiple_of(x * 8, 8), 8)
        first = [pad[c, pl.ds(base, 8), :] for c in range(FIELDS)]
        forces = [zero] * 3
        twists = [zero] * 3
        springs = [zero] * (3 * SLOTS)
        for number, (dx, dy, dz) in enumerate(DIRS):
            rows = pl.ds(base + dx * ROWS + dy, 8)
            source = (pad, pad_up, pad_down)[dz]
            total = (level, rising, falling)[dz]
            second = [source[c, rows, :] for c in range(FIELDS)]
            shear, live, masks = pick_shear(
                lambda c: hist[c, here, :], lambda s: con[s, here, :], number
            )
            force, twist, spring = pair(first, second, (dx, dy, dz), shear, live)
            for k in range(3):
                forces[k] = forces[k] + force[k]
                twists[k] = twists[k] + twist[k]
                for s in range(SLOTS):
                    springs[3 * s + k] = jnp.where(masks[s], spring[k], springs[3 * s + k])
            add(total, rows, force, twist, -1)
        add(level, pl.ds(base, 8), forces, twists, 1)
        for c in range(3 * SLOTS):
            new_hist[c, here, :] = springs[c]
        return carry

    lax.fori_loop(0, 8, body, 0)

    def shifted(values, amount):
        return [pltpu.roll(v, amount, 1) for v in values]

    def outer(rows, load, number, second, dead=None, turn=0):
        first = scaled([load(c, rows) for c in range(FIELDS)])
        shear, live, _ = pick_shear(
            lambda c: load(SHEAR + c, rows), lambda s: load(CODES + s, rows), float(number)
        )
        if turn:
            alive = jnp.where(live, 1.0, 0.0)
            moved = shifted(first + shear + [alive], turn)
            first, shear, live = moved[:10], moved[10:13], moved[13] > 0.5
        if dead is not None:
            live = jnp.logical_and(live, jnp.logical_not(dead))
        force, twist, _ = pair(first, second, DIRS[number], shear, live)
        return force, twist

    def load_side(c, rows):
        return side[c, rows, :]

    for c in range(FULL):
        side[c, 8:16, :] = xlo[c]
        side[c, 7:8, :] = edges[0, c : c + 1, :]
        side[c, 16:17, :] = edges[1, c : c + 1, :]
    mine = pl.ds(plane(0), 8)
    second = [pad[c, mine, :] for c in range(FIELDS)]
    for number in (0, 3, 4, 5, 6):
        dx, dy, dz = DIRS[number]
        dead = None if dz == 0 else lane == (0 if dz > 0 else 127)
        force, twist = outer(
            pl.ds(8 - dy, 8), load_side, number, second, dead, (0, 1, 127)[dz]
        )
        add(level, mine, force, twist, -1)
    for c in range(FULL):
        side[c, 8:16, :] = ylo[c]
    mine = pl.ds(plane(0), 8, stride=ROWS)
    second = [pad[c, mine, :] for c in range(FIELDS)]
    for number in (1, 3, 7, 8):
        dx, dy, dz = DIRS[number]
        dead = sub == 0 if dx else (None if dz == 0 else lane == (0 if dz > 0 else 127))
        force, twist = outer(
            pl.ds(8 - dx, 8), load_side, number, second, dead, (0, 1, 127)[dz]
        )
        add(level, mine, force, twist, -1)
    for c in range(FULL):
        side[c, 8:16, :] = yhi[c]
    mine = pl.ds(plane(0) + 7, 8, stride=ROWS)
    second = [pad[c, mine, :] for c in range(FIELDS)]
    force, twist = outer(pl.ds(7, 8), load_side, 4, second, sub == 0)
    add(level, mine, force, twist, -1)

    def spread(pack, c, top):
        p = (c % 16) * 8 - top
        return pltpu.roll(pack, (128 - p) % 128, 1) if p % 128 else pack

    for end in range(2):
        top = 1 - end
        for k in range(PACKS):
            straight, behind, left = packs[end, k], packs[2 + end, k], packs[6 + end, k]
            for c in range(16 * k, min(FULL, 16 * k + 16)):
                before = pltpu.roll(spread(behind, c, top), 120, 1)
                zside[end, c, 8:16, :] = jnp.where(
                    lane == 127, before, spread(straight, c, top)
                )
                zside[end, c, 0:8, :] = spread(left, c, top)

    for end, numbers in ((0, (2, 5, 7)), (1, (6, 8))):
        mine = own_packs[end, 0]
        second = scaled([spread(mine, c, end) for c in range(FIELDS)])
        forces = [zero] * 3
        twists = [zero] * 3
        for number in numbers:
            dx, dy, dz = DIRS[number]
            force, twist = outer(
                pl.ds(8 - dy, 8), lambda c, rows: zside[end, c, rows, :], number, second,
                None, dx,
            )
            forces = [forces[k] + force[k] for k in range(3)]
            twists = [twists[k] + twist[k] for k in range(3)]
        edge = 127 * end
        for x in range(8):
            turn = (edge - x) % 128
            rows = pl.ds(plane(x), 8)
            hold = lane == edge
            add(
                level, rows,
                [jnp.where(hold, pltpu.roll(v, turn, 1) if turn else v, 0.0) for v in forces],
                [jnp.where(hold, pltpu.roll(v, turn, 1) if turn else v, 0.0) for v in twists],
                -1,
            )

    names = leaving[0:1, 0:64]
    wide = jnp.broadcast_to(names, (8, 64))
    deep = lax.broadcasted_iota(jnp.int32, (8, 64), 0)
    starts = [(lax.axis_index(a) * n).astype(jnp.float32) for a, n in zip(AXES, (8, 8, 128))]
    boxes = [jnp.zeros((8, 64), jnp.float32) for _ in range(28)]
    for x in range(8):
        rows = pl.ds(plane(x), 8)
        here = slice(x * 8, x * 8 + 8)
        sums = []
        for c in range(6):
            up = jnp.where(lane == 0, 0.0, pltpu.roll(rising[c, rows, :], 1, 1))
            down = jnp.where(lane == 127, 0.0, pltpu.roll(falling[c, rows, :], 127, 1))
            sums.append(level[c, rows, :] + up + down)
        radius = rad[0, here, :]
        inverse = 1.0 / radius
        push = STEP * inverse * inverse * inverse
        turn = 0.125 * (inverse * inverse) * (inverse * inverse)
        velocity = [vel[k, here, :] + push * sums[k] for k in range(3)]
        velocity[2] = velocity[2] - STEP
        offset = [off[k, here, :] + STEP * velocity[k] for k in range(3)]
        rotation = [spin[k, here, :] + turn * sums[3 + k] for k in range(3)]
        springs = [new_hist[c, here, :] for c in range(3 * SLOTS)]
        bottom = [wide == (x * 8 + deep) * 128 + z for z in range(2)]
        left = [
            jnp.max(jnp.where(b, 1.0, 0.0), axis=1, keepdims=True) for b in bottom
        ]
        staying = 1.0 - jnp.where(lane == 0, left[0], jnp.where(lane == 1, left[1], 0.0))
        lanes = lane.astype(jnp.float32)
        position = [
            offset[0] + (starts[0] + float(x)),
            offset[1] + (starts[1] + sub.astype(jnp.float32)),
            offset[2] + (starts[2] + lanes),
        ]
        for c, v in enumerate(position + velocity + rotation + [radius] + springs):
            for z in range(2):
                value = jnp.broadcast_to(v[:, z : z + 1], (8, 64))
                boxes[c] = boxes[c] + jnp.where(bottom[z], value, 0.0)
        for k in range(3):
            new_off[k, here, :] = offset[k] * staying
            new_vel[k, here, :] = velocity[k] * staying
            new_spin[k, here, :] = rotation[k] * staying
        for c in range(3 * SLOTS):
            new_hist[c, here, :] = springs[c] * staying
    for c in range(28):
        outbox[c : c + 1, 0:64] = jnp.sum(boxes[c], axis=0, keepdims=True)


def on_device(offset, velocity, spin, radius, history, contacts, leaving):
    f32 = jnp.float32
    off = offset.reshape(3, 64, 128)
    vel = velocity.reshape(3, 64, 128)
    spn = spin.reshape(3, 64, 128)
    rad = radius.reshape(1, 64, 128)
    hist = history.reshape(3 * SLOTS, 64, 128)
    con = contacts.reshape(SLOTS, 64, 128)
    vmem = pl.BlockSpec(memory_space=pltpu.VMEM)
    hbm = pl.BlockSpec(memory_space=pltpu.HBM)
    halo_shapes = (
        (FULL, 8, 128),
        (FIELDS, 8, 128),
        (FULL, 8, 128),
        (FULL, 8, 128),
        (4, 40, 128),
        (len(PACK_FROM), PACKS, 8, 128),
        (2, PACKS, 8, 128),
    )
    state, arrivals = pl.pallas_call(
        step_kernel,
        out_shape=[pltpu.VMEM((27, 64, 128), f32), pltpu.VMEM((32, 128), f32)],
        in_specs=[hbm] * 7,
        out_specs=[vmem] * 2,
        scratch_shapes=[pltpu.VMEM(s, f32) for s in halo_shapes]
        + [
            pltpu.VMEM((FULL, 64, 128), f32),
            pltpu.VMEM((SLOTS, 64, 128), jnp.int32),
            pltpu.VMEM((1, 64), jnp.int32),
            pltpu.VMEM((2, FULL, 8, 128), f32),
            pltpu.VMEM((4, 40, 128), f32),
            pltpu.VMEM((32, 128), f32),
            pltpu.VMEM((FIELDS, HEIGHT, 128), f32),
            pltpu.VMEM((FIELDS, HEIGHT, 128), f32),
            pltpu.VMEM((FIELDS, HEIGHT, 128), f32),
            pltpu.VMEM((6, HEIGHT, 128), f32),
            pltpu.VMEM((6, HEIGHT, 128), f32),
            pltpu.VMEM((6, HEIGHT, 128), f32),
            pltpu.VMEM((FULL, ROWS, 128), f32),
            pltpu.VMEM((2, FULL, ROWS, 128), f32),
            pltpu.SemaphoreType.DMA((7,)),
            pltpu.SemaphoreType.DMA((len(SENDERS) + 1,)),
            pltpu.SemaphoreType.DMA((len(SENDERS) + 1,)),
        ],
        compiler_params=pltpu.CompilerParams(
            collective_id=0, has_side_effects=True, vmem_limit_bytes=24 << 20
        ),
        name="step",
    )(*[
        pltpu.with_memory_space_constraint(a, pltpu.HBM)
        for a in (off, vel, spn, rad, hist, con, leaving.reshape(1, 64))
    ])
    moved = jax.ShapeDtypeStruct((3, 64, 128), f32)
    new_off, new_vel, new_spin, new_hist, arrivals = pl.pallas_call(
        write_kernel,
        out_shape=[
            moved, moved, moved,
            jax.ShapeDtypeStruct((3 * SLOTS, 64, 128), f32),
            jax.ShapeDtypeStruct((28, 1, 64), f32),
        ],
        in_specs=[vmem] * 2,
        out_specs=[hbm] * 4 + [vmem],
        scratch_shapes=[pltpu.SemaphoreType.DMA((4,))],
        compiler_params=pltpu.CompilerParams(vmem_limit_bytes=8 << 20),
        name="write",
    )(state, arrivals)
    return (
        new_off.reshape(3, 8, 8, 128),
        new_vel.reshape(3, 8, 8, 128),
        new_spin.reshape(3, 8, 8, 128),
        new_hist.reshape(SLOTS, 3, 8, 8, 128),
        arrivals.reshape(28, 1, 1, 1, 64),
    )


def solution(mesh):
    placed = (
        P(None, "gx", "gy", "gz"),
        P(None, "gx", "gy", "gz"),
        P(None, "gx", "gy", "gz"),
        P("gx", "gy", "gz"),
        P(None, None, "gx", "gy", "gz"),
        P(None, "gx", "gy", "gz"),
        P("gx", "gy", "gz", None),
    )
    return jax.shard_map(
        on_device,
        mesh=mesh,
        in_specs=placed,
        out_specs=(
            P(None, "gx", "gy", "gz"),
            P(None, "gx", "gy", "gz"),
            P(None, "gx", "gy", "gz"),
            P(None, None, "gx", "gy", "gz"),
            P(None, "gx", "gy", "gz", None),
        ),
        check_vma=False,
    )
```

```python
import jax
import jax.numpy as jnp
from jax import lax
from jax.experimental import pallas as pl
from jax.experimental.pallas import tpu as pltpu
from jax.sharding import PartitionSpec as P

MESH = pl.DeviceIdType.MESH
AXES = ("gx", "gy", "gz")
DIRS = (
    (1, 0, 0),
    (0, 1, 0),
    (0, 0, 1),
    (1, 1, 0),
    (1, -1, 0),
    (1, 0, 1),
    (1, 0, -1),
    (0, 1, 1),
    (0, 1, -1),
)
SLOTS = 6
FIELDS = 10
SHEAR = FIELDS
CODES = FIELDS + 3 * SLOTS
FULL = CODES + SLOTS
PACKS = (FULL * 8 + 127) // 128
STEP = 0.05
TINY = 1e-30

ROWS = 24
HEIGHT = 10 * ROWS

PACK_FROM = (
    (0, 0, -1),
    (0, 0, 1),
    (-1, 0, -1),
    (-1, 0, 1),
    (1, 0, -1),
    (1, 0, 1),
    (0, -1, -1),
    (0, -1, 1),
    (0, 1, -1),
    (0, 1, 1),
)
FLAT_FROM = (
    (-1, 0, 0),
    (1, 0, 0),
    (0, -1, 0),
    (0, 1, 0),
    (-1, -1, 0),
    (-1, 1, 0),
    (1, -1, 0),
    (1, 1, 0),
)
SENDERS = FLAT_FROM + PACK_FROM

ALONG_X = (0, 3, 4, 5, 6)
UP_Y = (1, 3, 7, 8)
DOWN_Y = (4,)


def plane(x):
    return (x + 1) * ROWS + 8


def step_kernel(
    off_hbm, vel_hbm, spin_hbm, rad_hbm, hist_hbm, con_hbm, leaving_hbm,
    state, arrivals,
    xlo, xhi, ylo, yhi, edges, packs, own_packs, cells, codes, leaving,
    xrow, ytop, ylow, rows, outbox,
    pad, pad_up, pad_down, level, rising, falling, behind, ahead, zside,
    local_sems, send_sems, recv_sems,
):
    here = [lax.axis_index(a) for a in AXES]
    size = [lax.axis_size(a) for a in AXES]

    def exists(step):
        ok = None
        for at, n, s in zip(here, size, step):
            if s == 0:
                continue
            test = at + s < n if s > 0 else at + s >= 0
            ok = test if ok is None else jnp.logical_and(ok, test)
        return ok

    def place(step):
        return tuple(at + s for at, s in zip(here, step))

    loads = [
        pltpu.make_async_copy(off_hbm, cells.at[0:3], local_sems.at[0]),
        pltpu.make_async_copy(vel_hbm, cells.at[3:6], local_sems.at[1]),
        pltpu.make_async_copy(spin_hbm, cells.at[6:9], local_sems.at[2]),
        pltpu.make_async_copy(rad_hbm, cells.at[9:10], local_sems.at[3]),
        pltpu.make_async_copy(hist_hbm, cells.at[SHEAR:CODES], local_sems.at[4]),
        pltpu.make_async_copy(con_hbm, codes, local_sems.at[5]),
        pltpu.make_async_copy(leaving_hbm, leaving, local_sems.at[6]),
    ]
    for load in loads:
        load.start()
    barrier = pltpu.get_barrier_semaphore()
    expected = jnp.int32(0)
    for step in SENDERS:
        there = exists(step)
        expected = expected + there.astype(jnp.int32)

        @pl.when(there)
        def _():
            pl.semaphore_signal(barrier, inc=1, device_id=place(step), device_id_type=MESH)

    with jax.named_scope("loadwait"):
        for load in loads:
            load.wait()
    with jax.named_scope("pack"):
        for s in range(SLOTS):
            cells[CODES + s] = codes[s].astype(jnp.float32)
        fill_sends(cells, own_packs, xrow, ytop, ylow, rows)

    targets = [xlo, xhi, ylo, yhi] + [edges.at[k] for k in range(4)]
    sources = [xrow, cells.at[0:FIELDS, 0:8, :], ytop, ylow] + [rows.at[k] for k in range(4)]
    for k, s in enumerate(PACK_FROM):
        own = own_packs.at[0 if s[2] > 0 else 1]
        fields_only = s[0] + s[1] > 0
        targets.append(packs.at[k, 0:1] if fields_only else packs.at[k])
        sources.append(own.at[0:1] if fields_only else own)

    def copy(k):
        to = tuple(-s for s in SENDERS[k])
        return pltpu.make_async_remote_copy(
            src_ref=sources[k],
            dst_ref=targets[k],
            send_sem=send_sems.at[k],
            recv_sem=recv_sems.at[k],
            device_id=place(to),
            device_id_type=MESH,
        )

    for k, step in enumerate(SENDERS):

        @pl.when(jnp.logical_not(exists(step)))
        def _():
            targets[k][...] = jnp.zeros(targets[k].shape, jnp.float32)

    with jax.named_scope("barrier"):
        pl.semaphore_wait(barrier, expected)
    for k, step in enumerate(SENDERS):

        @pl.when(exists(tuple(-s for s in step)))
        def _():
            copy(k).start()

    with jax.named_scope("inner"):
        inner_pairs(cells, state, pad, pad_up, pad_down, level, rising, falling)

    for k, step in enumerate(SENDERS):
        with jax.named_scope("recv%d" % k):

            @pl.when(exists(step))
            def _():
                copy(k).wait_recv()

    with jax.named_scope("outer"):
        ends = outer_pairs(
            cells, state, pad, level, behind, ahead, zside, xlo, xhi, ylo, yhi, edges, packs,
            own_packs, xrow, ytop, ylow,
        )
    with jax.named_scope("final"):
        finish(cells, state, leaving, outbox, level, rising, falling, ends)

    last = len(SENDERS)
    fall = pltpu.make_async_remote_copy(
        src_ref=outbox,
        dst_ref=arrivals,
        send_sem=send_sems.at[last],
        recv_sem=recv_sems.at[last],
        device_id=place((0, 0, -1)),
        device_id_type=MESH,
    )

    @pl.when(exists((0, 0, -1)))
    def _():
        fall.start()

    for k, step in enumerate(SENDERS):

        @pl.when(exists(tuple(-s for s in step)))
        def _():
            copy(k).wait_send()

    with jax.named_scope("fall"):

        @pl.when(exists((0, 0, 1)))
        def _():
            fall.wait_recv()

    @pl.when(jnp.logical_not(exists((0, 0, 1))))
    def _():
        arrivals[...] = jnp.zeros(arrivals.shape, jnp.float32)

    @pl.when(exists((0, 0, -1)))
    def _():
        fall.wait_send()


def write_kernel(state, arrivals, new_off, new_vel, new_spin, new_hist, entered, sems):
    copies = [
        pltpu.make_async_copy(state.at[9:27], new_hist, sems.at[0]),
        pltpu.make_async_copy(state.at[0:3], new_off, sems.at[1]),
        pltpu.make_async_copy(state.at[3:6], new_vel, sems.at[2]),
        pltpu.make_async_copy(state.at[6:9], new_spin, sems.at[3]),
    ]
    for copy in copies:
        copy.start()
    for c in range(28):
        entered[c] = arrivals[c : c + 1, 0:64]
    for copy in copies:
        copy.wait()


def cross(a, b):
    return [
        a[1] * b[2] - a[2] * b[1],
        a[2] * b[0] - a[0] * b[2],
        a[0] * b[1] - a[1] * b[0],
    ]


def dot3(a, b):
    return a[0] * b[0] + a[1] * b[1] + a[2] * b[2]


def pair(first, second, direction, shear, live):
    sep = []
    for k in range(3):
        gap = second[k] - first[k]
        sep.append(gap + float(direction[k]) if direction[k] else gap)
    square = dot3(sep, sep)
    inverse = lax.rsqrt(square)
    normal = [s * inverse for s in sep]
    radii = first[9] + second[9]
    overlap = jnp.maximum(radii - square * inverse, 0.0)
    product = first[9] * second[9] * overlap
    contact = product * lax.rsqrt(jnp.maximum(product * radii, TINY))
    contact = jnp.where(live, contact, 0.0)
    surface = cross([first[6 + k] + second[6 + k] for k in range(3)], normal)
    relative = [second[3 + k] - first[3 + k] - surface[k] for k in range(3)]
    approach = dot3(relative, normal)
    sliding = [relative[k] - approach * normal[k] for k in range(3)]
    repulsion = contact * jnp.maximum(10.0 * overlap - 2.0 * approach, 0.0)
    along = dot3(shear, normal)
    spring = [shear[k] - along * normal[k] + STEP * sliding[k] for k in range(3)]
    pull = [8.0 * spring[k] + 1.5 * sliding[k] for k in range(3)]
    size = contact * contact * dot3(pull, pull)
    factor = jnp.minimum(1.0, 0.4 * repulsion * lax.rsqrt(jnp.maximum(size, 0.0025)))
    scale = factor * contact
    tangent = [scale * pull[k] for k in range(3)]
    force = [tangent[k] - repulsion * normal[k] for k in range(3)]
    return force, cross(normal, tangent), [factor * spring[k] for k in range(3)]


def pick_shear(load, numbers):
    codes = [load(CODES + s) for s in range(SLOTS)]
    found = []
    for number in numbers:
        masks = [code == float(number) for code in codes]
        live = masks[0]
        shear = [jnp.where(masks[0], load(SHEAR + k), 0.0) for k in range(3)]
        for s in range(1, SLOTS):
            live = jnp.logical_or(live, masks[s])
            shear = [jnp.where(masks[s], load(SHEAR + 3 * s + k), shear[k]) for k in range(3)]
        found.append((shear, live, masks))
    return found


def scaled(values):
    return values[:6] + [v * values[9] for v in values[6:9]] + [values[9]]


def lanes():
    return lax.broadcasted_iota(jnp.int32, (8, 128), 1)


def fill_sends(cells, own_packs, xrow, ytop, ylow, rows):
    lane = lanes()
    for c in range(FIELDS):
        xrow[c] = cells[c, 56:64, :]
        ytop[c] = cells[c, pl.ds(7, 8, stride=8), :]
        ylow[c] = cells[c, pl.ds(0, 8, stride=8), :]
    for target, span, numbers in (
        (xrow, pl.ds(56, 8), ALONG_X),
        (ytop, pl.ds(7, 8, stride=8), UP_Y),
        (ylow, pl.ds(0, 8, stride=8), DOWN_Y),
    ):
        found = pick_shear(lambda c: cells[c, span, :], numbers)
        for n, (shear, live, _) in enumerate(found):
            for k in range(3):
                target[FIELDS + 4 * n + k] = shear[k]
            target[FIELDS + 4 * n + 3] = jnp.where(live, 1.0, 0.0)
    for which, row, at in ((0, 7, 1), (1, 0, 2)):
        for c in range(FIELDS):
            rows[which, c : c + 1, :] = xrow[c, row : row + 1, :]
        for k in range(4):
            rows[which, FIELDS + k : FIELDS + k + 1, :] = xrow[
                FIELDS + 4 * at + k, row : row + 1, :
            ]
    for which, row in ((2, 7), (3, 0)):
        for c in range(FIELDS):
            rows[which, c : c + 1, :] = cells[c, row : row + 1, :]
    for k in range(PACKS):
        low = jnp.zeros((8, 128), jnp.float32)
        top = jnp.zeros((8, 128), jnp.float32)
        for c in range(k * 16, min(FULL, k * 16 + 16)):
            for x in range(8):
                p = (c % 16) * 8 + x
                value = cells[c, x * 8 : x * 8 + 8, :]
                if p:
                    value = pltpu.roll(value, p, 1)
                low = jnp.where(lane == p, value, low)
                top = jnp.where(lane == (p - 1) % 128, value, top)
        own_packs[0, k] = low
        own_packs[1, k] = top


def inner_pairs(cells, state, pad, pad_up, pad_down, level, rising, falling):
    lane = lanes()
    zero = jnp.zeros((8, 128), jnp.float32)
    row = jnp.zeros((1, 128), jnp.float32)
    for x in range(8):
        here = slice(x * 8, x * 8 + 8)
        span = pl.ds(plane(x), 8)
        for c, v in enumerate(scaled([cells[c, here, :] for c in range(FIELDS)])):
            pad[c, span, :] = v
            pad_up[c, span, :] = jnp.where(lane == 127, 0.0, pltpu.roll(v, 127, 1))
            pad_down[c, span, :] = jnp.where(lane == 0, 0.0, pltpu.roll(v, 1, 1))
            pad[c, plane(x) - 1 : plane(x), :] = row
            for source in (pad, pad_up, pad_down):
                source[c, plane(x) + 8 : plane(x) + 9, :] = row
    for c in range(FIELDS):
        for source in (pad, pad_up, pad_down):
            source[c, pl.ds(plane(8), 8), :] = zero
        pad[c, plane(8) - 1 : plane(8), :] = row
        pad[c, plane(8) + 8 : plane(8) + 9, :] = row
    for total in (level, rising, falling):
        for c in range(6):
            for x in range(9):
                total[c, pl.ds(plane(x), 8), :] = zero
                total[c, plane(x) - 1 : plane(x), :] = row
                total[c, plane(x) + 8 : plane(x) + 9, :] = row

    def body(x, carry):
        base = pl.multiple_of((x + 1) * ROWS + 8, 8)
        here = pl.ds(pl.multiple_of(x * 8, 8), 8)
        first = [pad[c, pl.ds(base, 8), :] for c in range(FIELDS)]
        forces = [zero] * 3
        twists = [zero] * 3
        springs = [zero] * (3 * SLOTS)
        for number, (dx, dy, dz) in enumerate(DIRS):
            span = pl.ds(base + dx * ROWS + dy, 8)
            source = (pad, pad_up, pad_down)[dz]
            total = (level, rising, falling)[dz]
            second = [source[c, span, :] for c in range(FIELDS)]
            ((shear, live, masks),) = pick_shear(lambda c: cells[c, here, :], (number,))
            force, twist, spring = pair(first, second, (dx, dy, dz), shear, live)
            for k in range(3):
                forces[k] = forces[k] + force[k]
                twists[k] = twists[k] + twist[k]
                for s in range(SLOTS):
                    springs[3 * s + k] = jnp.where(masks[s], spring[k], springs[3 * s + k])
                total[k, span, :] = total[k, span, :] - force[k]
                total[3 + k, span, :] = total[3 + k, span, :] + twist[k]
        for k in range(3):
            level[k, pl.ds(base, 8), :] = level[k, pl.ds(base, 8), :] + forces[k]
            level[3 + k, pl.ds(base, 8), :] = level[3 + k, pl.ds(base, 8), :] + twists[k]
        for c in range(3 * SLOTS):
            state[9 + c, here, :] = springs[c]
        return carry

    lax.fori_loop(0, 8, body, 0)


def outer_pairs(
    cells, state, pad, level, behind, ahead, zside, xlo, xhi, ylo, yhi, edges, packs,
    own_packs, xrow, ytop, ylow,
):
    lane = lanes()
    sub = lax.broadcasted_iota(jnp.int32, (8, 128), 0)
    zero = jnp.zeros((8, 128), jnp.float32)

    class Sums:
        def __init__(self):
            self.total = [zero] * 6
            self.springs = [zero] * (3 * SLOTS)

        def own(self, result, masks):
            force, twist, spring = result
            for k in range(3):
                self.total[k] = self.total[k] + force[k]
                self.total[3 + k] = self.total[3 + k] + twist[k]
                for s in range(SLOTS):
                    self.springs[3 * s + k] = jnp.where(
                        masks[s], spring[k], self.springs[3 * s + k]
                    )

        def partner(self, result):
            force, twist, _ = result
            for k in range(3):
                self.total[k] = self.total[k] - force[k]
                self.total[3 + k] = self.total[3 + k] + twist[k]

        def store(self, rows, span):
            for c in range(6):
                level[c, rows, :] = level[c, rows, :] + self.total[c]
            if span is not None:
                for c in range(3 * SLOTS):
                    state[9 + c, span, :] = state[9 + c, span, :] + self.springs[c]

    def turned(values, amount, axis=1):
        return [pltpu.roll(v, amount, axis) for v in values]

    def masks_of(span, number):
        return [cells[CODES + s, span, :] == float(number) for s in range(SLOTS)]

    for c in range(FIELDS + 4 * len(ALONG_X)):
        behind[c, 8:16, :] = xlo[c]
    for c in range(FIELDS):
        behind[c, 7:8, :] = edges[0, c : c + 1, :]
        behind[c, 16:17, :] = edges[1, c : c + 1, :]
        ahead[c, 7:8, :] = edges[2, c : c + 1, :]
        ahead[c, 16:17, :] = edges[3, c : c + 1, :]
        ahead[c, 8:16, :] = xhi[c]
    for k in range(4):
        behind[FIELDS + 4 + k, 7:8, :] = edges[0, FIELDS + k : FIELDS + k + 1, :]
        behind[FIELDS + 8 + k, 16:17, :] = edges[1, FIELDS + k : FIELDS + k + 1, :]

    def pack_scaled(pack, top):
        group = (lane + top) // 8
        for c in (6, 7, 8):
            radius = pltpu.roll(pack, 128 - 8 * (9 - c), 1)
            pack = jnp.where(group == c, pack * radius, pack)
        return pack

    beyond_up = pack_scaled(packs[5, 0], 0)
    beyond_down = pack_scaled(packs[4, 0], 1)
    sums = Sums()
    first = [pad[c, pl.ds(plane(7), 8), :] for c in range(FIELDS)]
    for n, number in enumerate(ALONG_X):
        dx, dy, dz = DIRS[number]
        second = scaled([ahead[c, pl.ds(8 + dy, 8), :] for c in range(FIELDS)])
        if dz > 0:
            second = [
                jnp.where(
                    lane == 127, pltpu.roll(beyond_up, 127 - 8 * c, 1), pltpu.roll(v, 127, 1)
                )
                for c, v in enumerate(second)
            ]
        elif dz < 0:
            second = [
                jnp.where(
                    lane == 0, pltpu.roll(beyond_down, (129 - 8 * c) % 128, 1), pltpu.roll(v, 1, 1)
                )
                for c, v in enumerate(second)
            ]
        at = FIELDS + 4 * n
        shear = [xrow[at + k] for k in range(3)]
        result = pair(first, second, DIRS[number], shear, xrow[at + 3] > 0.5)
        sums.own(result, masks_of(pl.ds(56, 8), number))
    sums.store(pl.ds(plane(7), 8), pl.ds(56, 8))
    sums = Sums()
    second = [pad[c, pl.ds(plane(0), 8), :] for c in range(FIELDS)]
    for n, number in enumerate(ALONG_X):
        dx, dy, dz = DIRS[number]
        span = pl.ds(8 - dy, 8)
        first = scaled([behind[c, span, :] for c in range(FIELDS)])
        first += [behind[FIELDS + 4 * n + k, span, :] for k in range(4)]
        if dz:
            first = turned(first, dz % 128)
        live = first[13] > 0.5
        if dz:
            live = jnp.logical_and(live, lane != (0 if dz > 0 else 127))
        sums.partner(pair(first[:10], second, DIRS[number], first[10:13], live))
    sums.store(pl.ds(plane(0), 8), None)

    top_fields = scaled([yhi[c] for c in range(FIELDS)])
    low_fields = scaled([ylo[c] for c in range(FIELDS)])
    sums = Sums()
    mine_rows = pl.ds(plane(0) + 7, 8, stride=ROWS)
    span = pl.ds(7, 8, stride=8)
    mine = [pad[c, mine_rows, :] for c in range(FIELDS)]
    for n, number in enumerate(UP_Y):
        dx, dy, dz = DIRS[number]
        at = FIELDS + 4 * n
        live = ytop[at + 3] > 0.5
        second = top_fields
        if dx:
            second = turned(second, 7, 0)
            live = jnp.logical_and(live, sub != 7)
        if dz:
            second = turned(second, -dz % 128)
            live = jnp.logical_and(live, lane != (127 if dz > 0 else 0))
        shear = [ytop[at + k] for k in range(3)]
        sums.own(pair(mine, second, DIRS[number], shear, live), masks_of(span, number))
    first = turned(top_fields + [yhi[FIELDS + k] for k in range(4)], 1, 0)
    live = jnp.logical_and(first[13] > 0.5, sub != 0)
    sums.partner(pair(first[:10], mine, DIRS[4], first[10:13], live))
    sums.store(mine_rows, span)

    sums = Sums()
    mine_rows = pl.ds(plane(0), 8, stride=ROWS)
    span = pl.ds(0, 8, stride=8)
    mine = [pad[c, mine_rows, :] for c in range(FIELDS)]
    second = turned(low_fields, 7, 0)
    live = jnp.logical_and(ylow[FIELDS + 3] > 0.5, sub != 7)
    shear = [ylow[FIELDS + k] for k in range(3)]
    sums.own(pair(mine, second, DIRS[4], shear, live), masks_of(span, 4))
    for n, number in enumerate(UP_Y):
        dx, dy, dz = DIRS[number]
        first = low_fields + [ylo[FIELDS + 4 * n + k] for k in range(4)]
        if dx:
            first = turned(first, 1, 0)
        if dz:
            first = turned(first, dz % 128)
        live = first[13] > 0.5
        if dx:
            live = jnp.logical_and(live, sub != 0)
        if dz:
            live = jnp.logical_and(live, lane != (0 if dz > 0 else 127))
        sums.partner(pair(first[:10], mine, DIRS[number], first[10:13], live))
    sums.store(mine_rows, span)

    def spread(pack, c, top):
        p = (c % 16) * 8 - top
        return pltpu.roll(pack, (128 - p) % 128, 1) if p % 128 else pack

    ends = []
    for end, theirs, ours in ((0, (2, 5, 7), (6, 8)), (1, (6, 8), (2, 5, 7))):
        top = 1 - end
        for k in range(PACKS):
            straight, back, left = packs[end, k], packs[2 + end, k], packs[6 + end, k]
            for c in range(16 * k, min(FULL, 16 * k + 16)):
                before = pltpu.roll(spread(back, c, top), 120, 1)
                zside[end, c, 8:16, :] = jnp.where(lane == 127, before, spread(straight, c, top))
                zside[end, c, 0:8, :] = spread(left, c, top)
                if c < FIELDS:
                    zside[end, c, 16:24, :] = spread(packs[8 + end, 0], c, top)
        own = [spread(own_packs[end, c // 16], c, end) for c in range(FULL)]
        mine = scaled(own[:FIELDS])
        sums = Sums()
        for number, (shear, live, masks) in zip(ours, pick_shear(lambda c: own[c], ours)):
            dx, dy, dz = DIRS[number]
            second = scaled([zside[end, c, pl.ds(8 + dy, 8), :] for c in range(FIELDS)])
            if dx:
                second = [jnp.where(lane < 7, v, 0.0) for v in turned(second, 127)]
            sums.own(pair(mine, second, DIRS[number], shear, live), masks)
        for number in theirs:
            dx, dy, dz = DIRS[number]
            span = pl.ds(8 - dy, 8)
            first = scaled([zside[end, c, span, :] for c in range(FIELDS)])
            ((shear, live, _),) = pick_shear(lambda c: zside[end, c, span, :], (number,))
            first = first + shear + [jnp.where(live, 1.0, 0.0)]
            if dx:
                first = turned(first, 1)
            sums.partner(pair(first[:10], mine, DIRS[number], first[10:13], first[13] > 0.5))
        ends.append(sums.total + sums.springs)
    return ends


def finish(cells, state, leaving, outbox, level, rising, falling, ends):
    lane = lanes()
    sub = lax.broadcasted_iota(jnp.int32, (8, 128), 0)
    wide = jnp.broadcast_to(leaving[0:1, 0:64], (8, 64))
    deep = lax.broadcasted_iota(jnp.int32, (8, 64), 0)
    starts = [(lax.axis_index(a) * n).astype(jnp.float32) for a, n in zip(AXES, (8, 8, 128))]
    boxes = [jnp.zeros((8, 64), jnp.float32) for _ in range(28)]
    for x in range(8):
        rows = pl.ds(plane(x), 8)
        here = slice(x * 8, x * 8 + 8)

        def at_ends(c):
            low, top = ends[0][c], ends[1][c]
            low = pltpu.roll(low, 128 - x, 1) if x else low
            return jnp.where(
                lane == 0, low, jnp.where(lane == 127, pltpu.roll(top, 127 - x, 1), 0.0)
            )

        sums = []
        for c in range(6):
            up = jnp.where(lane == 0, 0.0, pltpu.roll(rising[c, rows, :], 1, 1))
            down = jnp.where(lane == 127, 0.0, pltpu.roll(falling[c, rows, :], 127, 1))
            sums.append(level[c, rows, :] + up + down + at_ends(c))
        radius = cells[9, here, :]
        inverse = 1.0 / radius
        push = STEP * inverse * inverse * inverse
        turn = 0.125 * (inverse * inverse) * (inverse * inverse)
        velocity = [cells[3 + k, here, :] + push * sums[k] for k in range(3)]
        velocity[2] = velocity[2] - STEP
        offset = [cells[k, here, :] + STEP * velocity[k] for k in range(3)]
        rotation = [cells[6 + k, here, :] + turn * sums[3 + k] for k in range(3)]
        springs = [state[9 + c, here, :] + at_ends(6 + c) for c in range(3 * SLOTS)]
        bottom = [wide == (x * 8 + deep) * 128 + z for z in range(2)]
        left = [jnp.max(jnp.where(b, 1.0, 0.0), axis=1, keepdims=True) for b in bottom]
        staying = 1.0 - jnp.where(lane == 0, left[0], jnp.where(lane == 1, left[1], 0.0))
        position = [
            offset[0] + (starts[0] + float(x)),
            offset[1] + (starts[1] + sub.astype(jnp.float32)),
            offset[2] + (starts[2] + lane.astype(jnp.float32)),
        ]
        for c, v in enumerate(position + velocity + rotation + [radius] + springs):
            for z in range(2):
                value = jnp.broadcast_to(v[:, z : z + 1], (8, 64))
                boxes[c] = boxes[c] + jnp.where(bottom[z], value, 0.0)
        for c, v in enumerate(offset + velocity + rotation + springs):
            state[c, here, :] = v * staying
    for c in range(28):
        outbox[c : c + 1, 0:64] = jnp.sum(boxes[c], axis=0, keepdims=True)


def on_device(offset, velocity, spin, radius, history, contacts, leaving):
    f32 = jnp.float32
    off = offset.reshape(3, 64, 128)
    vel = velocity.reshape(3, 64, 128)
    spn = spin.reshape(3, 64, 128)
    rad = radius.reshape(1, 64, 128)
    hist = history.reshape(3 * SLOTS, 64, 128)
    con = contacts.reshape(SLOTS, 64, 128)
    vmem = pl.BlockSpec(memory_space=pltpu.VMEM)
    hbm = pl.BlockSpec(memory_space=pltpu.HBM)
    halo_shapes = (
        (FIELDS + 4 * len(ALONG_X), 8, 128),
        (FIELDS, 8, 128),
        (FIELDS + 4 * len(UP_Y), 8, 128),
        (FIELDS + 4 * len(DOWN_Y), 8, 128),
        (4, 16, 128),
        (len(PACK_FROM), PACKS, 8, 128),
        (2, PACKS, 8, 128),
    )
    state, arrivals = pl.pallas_call(
        step_kernel,
        out_shape=[pltpu.VMEM((27, 64, 128), f32), pltpu.VMEM((32, 128), f32)],
        in_specs=[hbm] * 7,
        out_specs=[vmem] * 2,
        scratch_shapes=[pltpu.VMEM(s, f32) for s in halo_shapes]
        + [
            pltpu.VMEM((FULL, 64, 128), f32),
            pltpu.VMEM((SLOTS, 64, 128), jnp.int32),
            pltpu.VMEM((1, 64), jnp.int32),
            pltpu.VMEM((FIELDS + 4 * len(ALONG_X), 8, 128), f32),
            pltpu.VMEM((FIELDS + 4 * len(UP_Y), 8, 128), f32),
            pltpu.VMEM((FIELDS + 4 * len(DOWN_Y), 8, 128), f32),
            pltpu.VMEM((4, 16, 128), f32),
            pltpu.VMEM((32, 128), f32),
            pltpu.VMEM((FIELDS, HEIGHT, 128), f32),
            pltpu.VMEM((FIELDS, HEIGHT, 128), f32),
            pltpu.VMEM((FIELDS, HEIGHT, 128), f32),
            pltpu.VMEM((6, HEIGHT, 128), f32),
            pltpu.VMEM((6, HEIGHT, 128), f32),
            pltpu.VMEM((6, HEIGHT, 128), f32),
            pltpu.VMEM((FIELDS + 4 * len(ALONG_X), ROWS, 128), f32),
            pltpu.VMEM((FIELDS, ROWS, 128), f32),
            pltpu.VMEM((2, FULL, ROWS, 128), f32),
            pltpu.SemaphoreType.DMA((7,)),
            pltpu.SemaphoreType.DMA((len(SENDERS) + 1,)),
            pltpu.SemaphoreType.DMA((len(SENDERS) + 1,)),
        ],
        compiler_params=pltpu.CompilerParams(
            collective_id=0, has_side_effects=True, vmem_limit_bytes=24 << 20
        ),
        name="step",
    )(*[
        pltpu.with_memory_space_constraint(a, pltpu.HBM)
        for a in (off, vel, spn, rad, hist, con, leaving.reshape(1, 64))
    ])
    moved = jax.ShapeDtypeStruct((3, 64, 128), f32)
    new_off, new_vel, new_spin, new_hist, arrivals = pl.pallas_call(
        write_kernel,
        out_shape=[
            moved, moved, moved,
            jax.ShapeDtypeStruct((3 * SLOTS, 64, 128), f32),
            jax.ShapeDtypeStruct((28, 1, 64), f32),
        ],
        in_specs=[vmem] * 2,
        out_specs=[hbm] * 4 + [vmem],
        scratch_shapes=[pltpu.SemaphoreType.DMA((4,))],
        compiler_params=pltpu.CompilerParams(vmem_limit_bytes=8 << 20),
        name="write",
    )(state, arrivals)
    return (
        new_off.reshape(3, 8, 8, 128),
        new_vel.reshape(3, 8, 8, 128),
        new_spin.reshape(3, 8, 8, 128),
        new_hist.reshape(SLOTS, 3, 8, 8, 128),
        arrivals.reshape(28, 1, 1, 1, 64),
    )


def solution(mesh):
    placed = (
        P(None, "gx", "gy", "gz"),
        P(None, "gx", "gy", "gz"),
        P(None, "gx", "gy", "gz"),
        P("gx", "gy", "gz"),
        P(None, None, "gx", "gy", "gz"),
        P(None, "gx", "gy", "gz"),
        P("gx", "gy", "gz", None),
    )
    return jax.shard_map(
        on_device,
        mesh=mesh,
        in_specs=placed,
        out_specs=(
            P(None, "gx", "gy", "gz"),
            P(None, "gx", "gy", "gz"),
            P(None, "gx", "gy", "gz"),
            P(None, None, "gx", "gy", "gz"),
            P(None, "gx", "gy", "gz", None),
        ),
        check_vma=False,
    )
```

```python
import jax
import jax.numpy as jnp
from jax import lax
from jax.experimental import pallas as pl
from jax.experimental.pallas import tpu as pltpu
from jax.sharding import PartitionSpec as P

MESH = pl.DeviceIdType.MESH
AXES = ("gx", "gy", "gz")
DIRS = (
    (1, 0, 0),
    (0, 1, 0),
    (0, 0, 1),
    (1, 1, 0),
    (1, -1, 0),
    (1, 0, 1),
    (1, 0, -1),
    (0, 1, 1),
    (0, 1, -1),
)
SLOTS = 6
FIELDS = 10
SHEAR = FIELDS
CODES = FIELDS + 3 * SLOTS
FULL = CODES + SLOTS
PACKS = (FULL * 8 + 127) // 128
STEP = 0.05
TINY = 1e-30

ROWS = 24
HEIGHT = 10 * ROWS

PACK_FROM = (
    (0, 0, -1),
    (0, 0, 1),
    (-1, 0, -1),
    (-1, 0, 1),
    (1, 0, -1),
    (1, 0, 1),
    (0, -1, -1),
    (0, -1, 1),
    (0, 1, -1),
    (0, 1, 1),
)
FLAT_FROM = (
    (-1, 0, 0),
    (1, 0, 0),
    (0, -1, 0),
    (0, 1, 0),
    (-1, -1, 0),
    (-1, 1, 0),
    (1, -1, 0),
    (1, 1, 0),
)
SENDERS = FLAT_FROM + PACK_FROM

ALONG_X = (0, 3, 4, 5, 6)
UP_Y = (1, 3, 7, 8)
DOWN_Y = (4,)

SEND_ORDER = (8, 9, 14, 15, 16, 17, 10, 11, 12, 13, 4, 5, 6, 7, 2, 3, 0, 1)


def plane(x):
    return (x + 1) * ROWS + 8


def step_kernel(
    off_hbm, vel_hbm, spin_hbm, rad_hbm, hist_hbm, con_hbm, leaving_hbm,
    state, arrivals,
    xlo, xhi, ylo, yhi, edges, packs, own_packs, cells, codes, leaving,
    xrow, ytop, ylow, rows, outbox,
    pad, pad_up, pad_down, level, rising, falling, behind, ahead, zside,
    local_sems, send_sems, recv_sems,
):
    here = [lax.axis_index(a) for a in AXES]
    size = [lax.axis_size(a) for a in AXES]

    def exists(step):
        ok = None
        for at, n, s in zip(here, size, step):
            if s == 0:
                continue
            test = at + s < n if s > 0 else at + s >= 0
            ok = test if ok is None else jnp.logical_and(ok, test)
        return ok

    def place(step):
        return tuple(at + s for at, s in zip(here, step))

    loads = [
        pltpu.make_async_copy(off_hbm, cells.at[0:3], local_sems.at[0]),
        pltpu.make_async_copy(vel_hbm, cells.at[3:6], local_sems.at[1]),
        pltpu.make_async_copy(spin_hbm, cells.at[6:9], local_sems.at[2]),
        pltpu.make_async_copy(rad_hbm, cells.at[9:10], local_sems.at[3]),
        pltpu.make_async_copy(hist_hbm, cells.at[SHEAR:CODES], local_sems.at[4]),
        pltpu.make_async_copy(con_hbm, codes, local_sems.at[5]),
        pltpu.make_async_copy(leaving_hbm, leaving, local_sems.at[6]),
    ]
    for load in loads:
        load.start()
    barrier = pltpu.get_barrier_semaphore()
    expected = jnp.int32(0)
    for step in SENDERS:
        there = exists(step)
        expected = expected + there.astype(jnp.int32)

        @pl.when(there)
        def _():
            pl.semaphore_signal(barrier, inc=1, device_id=place(step), device_id_type=MESH)

    with jax.named_scope("loadwait"):
        for load in loads:
            load.wait()
    with jax.named_scope("pack"):
        for s in range(SLOTS):
            cells[CODES + s] = codes[s].astype(jnp.float32)
        fill_sends(cells, own_packs, xrow, ytop, ylow, rows)

    targets = [xlo, xhi, ylo, yhi] + [edges.at[k] for k in range(4)]
    sources = [xrow, cells.at[0:FIELDS, 0:8, :], ytop, ylow] + [rows.at[k] for k in range(4)]
    for k, s in enumerate(PACK_FROM):
        own = own_packs.at[0 if s[2] > 0 else 1]
        fields_only = s[0] + s[1] > 0
        targets.append(packs.at[k, 0:1] if fields_only else packs.at[k])
        sources.append(own.at[0:1] if fields_only else own)

    def copy(k):
        to = tuple(-s for s in SENDERS[k])
        return pltpu.make_async_remote_copy(
            src_ref=sources[k],
            dst_ref=targets[k],
            send_sem=send_sems.at[k],
            recv_sem=recv_sems.at[k],
            device_id=place(to),
            device_id_type=MESH,
        )

    for k, step in enumerate(SENDERS):

        @pl.when(jnp.logical_not(exists(step)))
        def _():
            targets[k][...] = jnp.zeros(targets[k].shape, jnp.float32)

    with jax.named_scope("barrier"):
        pl.semaphore_wait(barrier, expected)
    for k in SEND_ORDER:

        @pl.when(exists(tuple(-s for s in SENDERS[k])))
        def _():
            copy(k).start()

    with jax.named_scope("inner"):
        inner_pairs(cells, state, pad, pad_up, pad_down, level, rising, falling)

    def receive(which):
        for k in which:

            @pl.when(exists(SENDERS[k]))
            def _():
                copy(k).wait_recv()

    with jax.named_scope("fold"):
        fold(level, rising, falling)
    with jax.named_scope("recvz"):
        receive(range(8, 18, 2))
    with jax.named_scope("floor"):
        end_pairs(0, level, state, zside, packs, own_packs)
    with jax.named_scope("recvy"):
        receive((2, 3))
    with jax.named_scope("ypairs"):
        y_pairs(cells, state, pad, level, ylo, yhi, ytop, ylow)
    with jax.named_scope("recvx"):
        receive((0, 1, 4, 5, 6, 7, 13))
    with jax.named_scope("xpairs"):
        x_pairs(cells, state, pad, level, behind, ahead, xlo, xhi, edges, packs, xrow)
    with jax.named_scope("outbox"):
        fill_outbox(cells, state, leaving, outbox, level)

    last = len(SENDERS)
    fall = pltpu.make_async_remote_copy(
        src_ref=outbox,
        dst_ref=arrivals,
        send_sem=send_sems.at[last],
        recv_sem=recv_sems.at[last],
        device_id=place((0, 0, -1)),
        device_id_type=MESH,
    )

    @pl.when(exists((0, 0, -1)))
    def _():
        fall.start()

    with jax.named_scope("recvtop"):
        receive((9, 11, 15, 17))
    with jax.named_scope("ceiling"):
        end_pairs(1, level, state, zside, packs, own_packs)
    with jax.named_scope("final"):
        finish(cells, state, leaving, level)

    for k, step in enumerate(SENDERS):

        @pl.when(exists(tuple(-s for s in step)))
        def _():
            copy(k).wait_send()

    with jax.named_scope("fall"):

        @pl.when(exists((0, 0, 1)))
        def _():
            fall.wait_recv()

    @pl.when(jnp.logical_not(exists((0, 0, 1))))
    def _():
        arrivals[...] = jnp.zeros(arrivals.shape, jnp.float32)

    @pl.when(exists((0, 0, -1)))
    def _():
        fall.wait_send()


def write_kernel(state, arrivals, new_off, new_vel, new_spin, new_hist, entered, sems):
    copies = [
        pltpu.make_async_copy(state.at[9:27], new_hist, sems.at[0]),
        pltpu.make_async_copy(state.at[0:3], new_off, sems.at[1]),
        pltpu.make_async_copy(state.at[3:6], new_vel, sems.at[2]),
        pltpu.make_async_copy(state.at[6:9], new_spin, sems.at[3]),
    ]
    for copy in copies:
        copy.start()
    for c in range(28):
        entered[c] = arrivals[c : c + 1, 0:64]
    for copy in copies:
        copy.wait()


def cross(a, b):
    return [
        a[1] * b[2] - a[2] * b[1],
        a[2] * b[0] - a[0] * b[2],
        a[0] * b[1] - a[1] * b[0],
    ]


def dot3(a, b):
    return a[0] * b[0] + a[1] * b[1] + a[2] * b[2]


def pair(first, second, direction, shear, live):
    sep = []
    for k in range(3):
        gap = second[k] - first[k]
        sep.append(gap + float(direction[k]) if direction[k] else gap)
    square = dot3(sep, sep)
    inverse = lax.rsqrt(square)
    normal = [s * inverse for s in sep]
    radii = first[9] + second[9]
    overlap = jnp.maximum(radii - square * inverse, 0.0)
    product = first[9] * second[9] * overlap
    contact = product * lax.rsqrt(jnp.maximum(product * radii, TINY))
    contact = jnp.where(live, contact, 0.0)
    surface = cross([first[6 + k] + second[6 + k] for k in range(3)], normal)
    relative = [second[3 + k] - first[3 + k] - surface[k] for k in range(3)]
    approach = dot3(relative, normal)
    sliding = [relative[k] - approach * normal[k] for k in range(3)]
    repulsion = contact * jnp.maximum(10.0 * overlap - 2.0 * approach, 0.0)
    along = dot3(shear, normal)
    spring = [shear[k] - along * normal[k] + STEP * sliding[k] for k in range(3)]
    pull = [8.0 * spring[k] + 1.5 * sliding[k] for k in range(3)]
    size = contact * contact * dot3(pull, pull)
    factor = jnp.minimum(1.0, 0.4 * repulsion * lax.rsqrt(jnp.maximum(size, 0.0025)))
    scale = factor * contact
    tangent = [scale * pull[k] for k in range(3)]
    force = [tangent[k] - repulsion * normal[k] for k in range(3)]
    return force, cross(normal, tangent), [factor * spring[k] for k in range(3)]


def pick_shear(load, numbers):
    codes = [load(CODES + s) for s in range(SLOTS)]
    found = []
    for number in numbers:
        masks = [code == float(number) for code in codes]
        live = masks[0]
        shear = [jnp.where(masks[0], load(SHEAR + k), 0.0) for k in range(3)]
        for s in range(1, SLOTS):
            live = jnp.logical_or(live, masks[s])
            shear = [jnp.where(masks[s], load(SHEAR + 3 * s + k), shear[k]) for k in range(3)]
        found.append((shear, live, masks))
    return found


def scaled(values):
    return values[:6] + [v * values[9] for v in values[6:9]] + [values[9]]


def lanes():
    return lax.broadcasted_iota(jnp.int32, (8, 128), 1)


def fill_sends(cells, own_packs, xrow, ytop, ylow, rows):
    lane = lanes()
    for c in range(FIELDS):
        xrow[c] = cells[c, 56:64, :]
        ytop[c] = cells[c, pl.ds(7, 8, stride=8), :]
        ylow[c] = cells[c, pl.ds(0, 8, stride=8), :]
    for target, span, numbers in (
        (xrow, pl.ds(56, 8), ALONG_X),
        (ytop, pl.ds(7, 8, stride=8), UP_Y),
        (ylow, pl.ds(0, 8, stride=8), DOWN_Y),
    ):
        found = pick_shear(lambda c: cells[c, span, :], numbers)
        for n, (shear, live, _) in enumerate(found):
            for k in range(3):
                target[FIELDS + 4 * n + k] = shear[k]
            target[FIELDS + 4 * n + 3] = jnp.where(live, 1.0, 0.0)
    for which, row, at in ((0, 7, 1), (1, 0, 2)):
        for c in range(FIELDS):
            rows[which, c : c + 1, :] = xrow[c, row : row + 1, :]
        for k in range(4):
            rows[which, FIELDS + k : FIELDS + k + 1, :] = xrow[
                FIELDS + 4 * at + k, row : row + 1, :
            ]
    for which, row in ((2, 7), (3, 0)):
        for c in range(FIELDS):
            rows[which, c : c + 1, :] = cells[c, row : row + 1, :]
    for k in range(PACKS):
        low = jnp.zeros((8, 128), jnp.float32)
        top = jnp.zeros((8, 128), jnp.float32)
        for c in range(k * 16, min(FULL, k * 16 + 16)):
            for x in range(8):
                p = (c % 16) * 8 + x
                value = cells[c, x * 8 : x * 8 + 8, :]
                if p:
                    value = pltpu.roll(value, p, 1)
                low = jnp.where(lane == p, value, low)
                top = jnp.where(lane == (p - 1) % 128, value, top)
        own_packs[0, k] = low
        own_packs[1, k] = top


def inner_pairs(cells, state, pad, pad_up, pad_down, level, rising, falling):
    lane = lanes()
    zero = jnp.zeros((8, 128), jnp.float32)
    row = jnp.zeros((1, 128), jnp.float32)
    for x in range(8):
        here = slice(x * 8, x * 8 + 8)
        span = pl.ds(plane(x), 8)
        for c, v in enumerate(scaled([cells[c, here, :] for c in range(FIELDS)])):
            pad[c, span, :] = v
            pad_up[c, span, :] = jnp.where(lane == 127, 0.0, pltpu.roll(v, 127, 1))
            pad_down[c, span, :] = jnp.where(lane == 0, 0.0, pltpu.roll(v, 1, 1))
            pad[c, plane(x) - 1 : plane(x), :] = row
            for source in (pad, pad_up, pad_down):
                source[c, plane(x) + 8 : plane(x) + 9, :] = row
    for c in range(FIELDS):
        for source in (pad, pad_up, pad_down):
            source[c, pl.ds(plane(8), 8), :] = zero
        pad[c, plane(8) - 1 : plane(8), :] = row
        pad[c, plane(8) + 8 : plane(8) + 9, :] = row
    for total in (level, rising, falling):
        for c in range(6):
            for x in range(9):
                total[c, pl.ds(plane(x), 8), :] = zero
                total[c, plane(x) - 1 : plane(x), :] = row
                total[c, plane(x) + 8 : plane(x) + 9, :] = row

    def body(x, carry):
        base = pl.multiple_of((x + 1) * ROWS + 8, 8)
        here = pl.ds(pl.multiple_of(x * 8, 8), 8)
        first = [pad[c, pl.ds(base, 8), :] for c in range(FIELDS)]
        forces = [zero] * 3
        twists = [zero] * 3
        springs = [zero] * (3 * SLOTS)
        for number, (dx, dy, dz) in enumerate(DIRS):
            span = pl.ds(base + dx * ROWS + dy, 8)
            source = (pad, pad_up, pad_down)[dz]
            total = (level, rising, falling)[dz]
            second = [source[c, span, :] for c in range(FIELDS)]
            ((shear, live, masks),) = pick_shear(lambda c: cells[c, here, :], (number,))
            force, twist, spring = pair(first, second, (dx, dy, dz), shear, live)
            for k in range(3):
                forces[k] = forces[k] + force[k]
                twists[k] = twists[k] + twist[k]
                for s in range(SLOTS):
                    springs[3 * s + k] = jnp.where(masks[s], spring[k], springs[3 * s + k])
                total[k, span, :] = total[k, span, :] - force[k]
                total[3 + k, span, :] = total[3 + k, span, :] + twist[k]
        for k in range(3):
            level[k, pl.ds(base, 8), :] = level[k, pl.ds(base, 8), :] + forces[k]
            level[3 + k, pl.ds(base, 8), :] = level[3 + k, pl.ds(base, 8), :] + twists[k]
        for c in range(3 * SLOTS):
            state[9 + c, here, :] = springs[c]
        return carry

    lax.fori_loop(0, 8, body, 0)


class Sums:
    def __init__(self):
        zero = jnp.zeros((8, 128), jnp.float32)
        self.total = [zero] * 6
        self.springs = [zero] * (3 * SLOTS)

    def own(self, result, masks):
        force, twist, spring = result
        for k in range(3):
            self.total[k] = self.total[k] + force[k]
            self.total[3 + k] = self.total[3 + k] + twist[k]
            for s in range(SLOTS):
                self.springs[3 * s + k] = jnp.where(masks[s], spring[k], self.springs[3 * s + k])

    def partner(self, result):
        force, twist, _ = result
        for k in range(3):
            self.total[k] = self.total[k] - force[k]
            self.total[3 + k] = self.total[3 + k] + twist[k]

    def store(self, level, rows, state, span):
        for c in range(6):
            level[c, rows, :] = level[c, rows, :] + self.total[c]
        if span is not None:
            for c in range(3 * SLOTS):
                state[9 + c, span, :] = state[9 + c, span, :] + self.springs[c]


def turned(values, amount, axis=1):
    return [pltpu.roll(v, amount, axis) for v in values]


def masks_of(cells, span, number):
    return [cells[CODES + s, span, :] == float(number) for s in range(SLOTS)]


def fold(level, rising, falling):
    lane = lanes()
    for x in range(8):
        rows = pl.ds(plane(x), 8)
        for c in range(6):
            up = jnp.where(lane == 0, 0.0, pltpu.roll(rising[c, rows, :], 1, 1))
            down = jnp.where(lane == 127, 0.0, pltpu.roll(falling[c, rows, :], 127, 1))
            level[c, rows, :] = level[c, rows, :] + up + down


def x_pairs(cells, state, pad, level, behind, ahead, xlo, xhi, edges, packs, xrow):
    lane = lanes()
    for c in range(FIELDS + 4 * len(ALONG_X)):
        behind[c, 8:16, :] = xlo[c]
    for c in range(FIELDS):
        behind[c, 7:8, :] = edges[0, c : c + 1, :]
        behind[c, 16:17, :] = edges[1, c : c + 1, :]
        ahead[c, 7:8, :] = edges[2, c : c + 1, :]
        ahead[c, 16:17, :] = edges[3, c : c + 1, :]
        ahead[c, 8:16, :] = xhi[c]
    for k in range(4):
        behind[FIELDS + 4 + k, 7:8, :] = edges[0, FIELDS + k : FIELDS + k + 1, :]
        behind[FIELDS + 8 + k, 16:17, :] = edges[1, FIELDS + k : FIELDS + k + 1, :]

    def pack_scaled(pack, top):
        group = (lane + top) // 8
        for c in (6, 7, 8):
            radius = pltpu.roll(pack, 128 - 8 * (9 - c), 1)
            pack = jnp.where(group == c, pack * radius, pack)
        return pack

    beyond_up = pack_scaled(packs[5, 0], 0)
    beyond_down = pack_scaled(packs[4, 0], 1)
    sums = Sums()
    first = [pad[c, pl.ds(plane(7), 8), :] for c in range(FIELDS)]
    for n, number in enumerate(ALONG_X):
        dx, dy, dz = DIRS[number]
        second = scaled([ahead[c, pl.ds(8 + dy, 8), :] for c in range(FIELDS)])
        if dz > 0:
            second = [
                jnp.where(
                    lane == 127, pltpu.roll(beyond_up, 127 - 8 * c, 1), pltpu.roll(v, 127, 1)
                )
                for c, v in enumerate(second)
            ]
        elif dz < 0:
            second = [
                jnp.where(
                    lane == 0, pltpu.roll(beyond_down, (129 - 8 * c) % 128, 1), pltpu.roll(v, 1, 1)
                )
                for c, v in enumerate(second)
            ]
        at = FIELDS + 4 * n
        shear = [xrow[at + k] for k in range(3)]
        result = pair(first, second, DIRS[number], shear, xrow[at + 3] > 0.5)
        sums.own(result, masks_of(cells, pl.ds(56, 8), number))
    sums.store(level, pl.ds(plane(7), 8), state, pl.ds(56, 8))
    sums = Sums()
    second = [pad[c, pl.ds(plane(0), 8), :] for c in range(FIELDS)]
    for n, number in enumerate(ALONG_X):
        dx, dy, dz = DIRS[number]
        span = pl.ds(8 - dy, 8)
        first = scaled([behind[c, span, :] for c in range(FIELDS)])
        first += [behind[FIELDS + 4 * n + k, span, :] for k in range(4)]
        if dz:
            first = turned(first, dz % 128)
        live = first[13] > 0.5
        if dz:
            live = jnp.logical_and(live, lane != (0 if dz > 0 else 127))
        sums.partner(pair(first[:10], second, DIRS[number], first[10:13], live))
    sums.store(level, pl.ds(plane(0), 8), state, None)


def y_pairs(cells, state, pad, level, ylo, yhi, ytop, ylow):
    lane = lanes()
    sub = lax.broadcasted_iota(jnp.int32, (8, 128), 0)
    top_fields = scaled([yhi[c] for c in range(FIELDS)])
    low_fields = scaled([ylo[c] for c in range(FIELDS)])
    sums = Sums()
    mine_rows = pl.ds(plane(0) + 7, 8, stride=ROWS)
    span = pl.ds(7, 8, stride=8)
    mine = [pad[c, mine_rows, :] for c in range(FIELDS)]
    for n, number in enumerate(UP_Y):
        dx, dy, dz = DIRS[number]
        at = FIELDS + 4 * n
        live = ytop[at + 3] > 0.5
        second = top_fields
        if dx:
            second = turned(second, 7, 0)
            live = jnp.logical_and(live, sub != 7)
        if dz:
            second = turned(second, -dz % 128)
            live = jnp.logical_and(live, lane != (127 if dz > 0 else 0))
        shear = [ytop[at + k] for k in range(3)]
        sums.own(pair(mine, second, DIRS[number], shear, live), masks_of(cells, span, number))
    first = turned(top_fields + [yhi[FIELDS + k] for k in range(4)], 1, 0)
    live = jnp.logical_and(first[13] > 0.5, sub != 0)
    sums.partner(pair(first[:10], mine, DIRS[4], first[10:13], live))
    sums.store(level, mine_rows, state, span)

    sums = Sums()
    mine_rows = pl.ds(plane(0), 8, stride=ROWS)
    span = pl.ds(0, 8, stride=8)
    mine = [pad[c, mine_rows, :] for c in range(FIELDS)]
    second = turned(low_fields, 7, 0)
    live = jnp.logical_and(ylow[FIELDS + 3] > 0.5, sub != 7)
    shear = [ylow[FIELDS + k] for k in range(3)]
    sums.own(pair(mine, second, DIRS[4], shear, live), masks_of(cells, span, 4))
    for n, number in enumerate(UP_Y):
        dx, dy, dz = DIRS[number]
        first = low_fields + [ylo[FIELDS + 4 * n + k] for k in range(4)]
        if dx:
            first = turned(first, 1, 0)
        if dz:
            first = turned(first, dz % 128)
        live = first[13] > 0.5
        if dx:
            live = jnp.logical_and(live, sub != 0)
        if dz:
            live = jnp.logical_and(live, lane != (0 if dz > 0 else 127))
        sums.partner(pair(first[:10], mine, DIRS[number], first[10:13], live))
    sums.store(level, mine_rows, state, span)


def end_pairs(end, level, state, zside, packs, own_packs):
    lane = lanes()
    theirs, ours = (((2, 5, 7), (6, 8)), ((6, 8), (2, 5, 7)))[end]
    top = 1 - end

    def spread(pack, c, top, at=0):
        p = (c % 16) * 8 - top - at
        return pltpu.roll(pack, -p % 128, 1) if p % 128 else pack

    for k in range(PACKS):
        straight, back, left = packs[end, k], packs[2 + end, k], packs[6 + end, k]
        for c in range(16 * k, min(FULL, 16 * k + 16)):
            zside[end, c, 8:16, :] = jnp.where(
                lane == 127, spread(back, c, top, 120), spread(straight, c, top)
            )
            zside[end, c, 0:8, :] = spread(left, c, top)
            if c < FIELDS:
                zside[end, c, 16:24, :] = spread(packs[8 + end, 0], c, top)
    own = [spread(own_packs[end, c // 16], c, end) for c in range(FULL)]
    mine = scaled(own[:FIELDS])
    sums = Sums()
    for number, (shear, live, masks) in zip(ours, pick_shear(lambda c: own[c], ours)):
        dx, dy, dz = DIRS[number]
        second = scaled([zside[end, c, pl.ds(8 + dy, 8), :] for c in range(FIELDS)])
        if dx:
            second = [jnp.where(lane < 7, v, 0.0) for v in turned(second, 127)]
        sums.own(pair(mine, second, DIRS[number], shear, live), masks)
    for number in theirs:
        dx, dy, dz = DIRS[number]
        span = pl.ds(8 - dy, 8)
        first = scaled([zside[end, c, span, :] for c in range(FIELDS)])
        ((shear, live, _),) = pick_shear(lambda c: zside[end, c, span, :], (number,))
        first = first + shear + [jnp.where(live, 1.0, 0.0)]
        if dx:
            first = turned(first, 1)
        sums.partner(pair(first[:10], mine, DIRS[number], first[10:13], first[13] > 0.5))
    edge = 127 * end
    hold = lane == edge
    for x in range(8):
        turn = (edge - x) % 128

        def put(v):
            return jnp.where(hold, pltpu.roll(v, turn, 1) if turn else v, 0.0)

        rows = pl.ds(plane(x), 8)
        here = slice(x * 8, x * 8 + 8)
        for c in range(6):
            level[c, rows, :] = level[c, rows, :] + put(sums.total[c])
        for c in range(3 * SLOTS):
            state[9 + c, here, :] = state[9 + c, here, :] + put(sums.springs[c])


def moved(cells, level, x):
    rows = pl.ds(plane(x), 8)
    here = slice(x * 8, x * 8 + 8)
    sums = [level[c, rows, :] for c in range(6)]
    radius = cells[9, here, :]
    inverse = 1.0 / radius
    push = STEP * inverse * inverse * inverse
    turn = 0.125 * (inverse * inverse) * (inverse * inverse)
    velocity = [cells[3 + k, here, :] + push * sums[k] for k in range(3)]
    velocity[2] = velocity[2] - STEP
    offset = [cells[k, here, :] + STEP * velocity[k] for k in range(3)]
    rotation = [cells[6 + k, here, :] + turn * sums[3 + k] for k in range(3)]
    return offset, velocity, rotation, radius


def fill_outbox(cells, state, leaving, outbox, level):
    lane = lanes()
    sub = lax.broadcasted_iota(jnp.int32, (8, 128), 0)
    names = leaving[0:1, 0:64]
    names = jnp.concatenate([names, jnp.full((1, 64), -1, jnp.int32)], axis=1)
    names = jnp.broadcast_to(names, (8, 128))
    height = jnp.where(names >= 0, names % 128, 0)
    column = jnp.where(names >= 0, names // 128, -1)
    starts = [(lax.axis_index(a) * n).astype(jnp.float32) for a, n in zip(AXES, (8, 8, 128))]
    boxes = [jnp.zeros((8, 128), jnp.float32) for _ in range(28)]
    for x in range(8):
        here = slice(x * 8, x * 8 + 8)
        offset, velocity, rotation, radius = moved(cells, level, x)
        springs = [state[9 + c, here, :] for c in range(3 * SLOTS)]
        position = [
            offset[0] + (starts[0] + float(x)),
            offset[1] + (starts[1] + sub.astype(jnp.float32)),
            offset[2] + (starts[2] + lane.astype(jnp.float32)),
        ]
        chosen = column == x * 8 + sub
        for c, v in enumerate(position + velocity + rotation + [radius] + springs):
            boxes[c] = jnp.where(chosen, jnp.take_along_axis(v, height, axis=1), boxes[c])
    for c in range(28):
        outbox[c : c + 1, :] = jnp.sum(boxes[c], axis=0, keepdims=True)


def finish(cells, state, leaving, level):
    lane = lanes()
    wide = jnp.broadcast_to(leaving[0:1, 0:64], (8, 64))
    deep = lax.broadcasted_iota(jnp.int32, (8, 64), 0)
    for x in range(8):
        here = slice(x * 8, x * 8 + 8)
        offset, velocity, rotation, _ = moved(cells, level, x)
        left = [
            jnp.max(jnp.where(wide == (x * 8 + deep) * 128 + z, 1.0, 0.0), axis=1, keepdims=True)
            for z in range(2)
        ]
        staying = 1.0 - jnp.where(lane == 0, left[0], jnp.where(lane == 1, left[1], 0.0))
        for c, v in enumerate(offset + velocity + rotation):
            state[c, here, :] = v * staying
        for c in range(9, 27):
            state[c, here, :] = state[c, here, :] * staying


def on_device(offset, velocity, spin, radius, history, contacts, leaving):
    f32 = jnp.float32
    off = offset.reshape(3, 64, 128)
    vel = velocity.reshape(3, 64, 128)
    spn = spin.reshape(3, 64, 128)
    rad = radius.reshape(1, 64, 128)
    hist = history.reshape(3 * SLOTS, 64, 128)
    con = contacts.reshape(SLOTS, 64, 128)
    vmem = pl.BlockSpec(memory_space=pltpu.VMEM)
    hbm = pl.BlockSpec(memory_space=pltpu.HBM)
    halo_shapes = (
        (FIELDS + 4 * len(ALONG_X), 8, 128),
        (FIELDS, 8, 128),
        (FIELDS + 4 * len(UP_Y), 8, 128),
        (FIELDS + 4 * len(DOWN_Y), 8, 128),
        (4, 16, 128),
        (len(PACK_FROM), PACKS, 8, 128),
        (2, PACKS, 8, 128),
    )
    state, arrivals = pl.pallas_call(
        step_kernel,
        out_shape=[pltpu.VMEM((27, 64, 128), f32), pltpu.VMEM((32, 128), f32)],
        in_specs=[hbm] * 7,
        out_specs=[vmem] * 2,
        scratch_shapes=[pltpu.VMEM(s, f32) for s in halo_shapes]
        + [
            pltpu.VMEM((FULL, 64, 128), f32),
            pltpu.VMEM((SLOTS, 64, 128), jnp.int32),
            pltpu.VMEM((1, 64), jnp.int32),
            pltpu.VMEM((FIELDS + 4 * len(ALONG_X), 8, 128), f32),
            pltpu.VMEM((FIELDS + 4 * len(UP_Y), 8, 128), f32),
            pltpu.VMEM((FIELDS + 4 * len(DOWN_Y), 8, 128), f32),
            pltpu.VMEM((4, 16, 128), f32),
            pltpu.VMEM((32, 128), f32),
            pltpu.VMEM((FIELDS, HEIGHT, 128), f32),
            pltpu.VMEM((FIELDS, HEIGHT, 128), f32),
            pltpu.VMEM((FIELDS, HEIGHT, 128), f32),
            pltpu.VMEM((6, HEIGHT, 128), f32),
            pltpu.VMEM((6, HEIGHT, 128), f32),
            pltpu.VMEM((6, HEIGHT, 128), f32),
            pltpu.VMEM((FIELDS + 4 * len(ALONG_X), ROWS, 128), f32),
            pltpu.VMEM((FIELDS, ROWS, 128), f32),
            pltpu.VMEM((2, FULL, ROWS, 128), f32),
            pltpu.SemaphoreType.DMA((7,)),
            pltpu.SemaphoreType.DMA((len(SENDERS) + 1,)),
            pltpu.SemaphoreType.DMA((len(SENDERS) + 1,)),
        ],
        compiler_params=pltpu.CompilerParams(
            collective_id=0, has_side_effects=True, vmem_limit_bytes=24 << 20
        ),
        name="step",
    )(*[
        pltpu.with_memory_space_constraint(a, pltpu.HBM)
        for a in (off, vel, spn, rad, hist, con, leaving.reshape(1, 64))
    ])
    moved = jax.ShapeDtypeStruct((3, 64, 128), f32)
    new_off, new_vel, new_spin, new_hist, arrivals = pl.pallas_call(
        write_kernel,
        out_shape=[
            moved, moved, moved,
            jax.ShapeDtypeStruct((3 * SLOTS, 64, 128), f32),
            jax.ShapeDtypeStruct((28, 1, 64), f32),
        ],
        in_specs=[vmem] * 2,
        out_specs=[hbm] * 4 + [vmem],
        scratch_shapes=[pltpu.SemaphoreType.DMA((4,))],
        compiler_params=pltpu.CompilerParams(vmem_limit_bytes=8 << 20),
        name="write",
    )(state, arrivals)
    return (
        new_off.reshape(3, 8, 8, 128),
        new_vel.reshape(3, 8, 8, 128),
        new_spin.reshape(3, 8, 8, 128),
        new_hist.reshape(SLOTS, 3, 8, 8, 128),
        arrivals.reshape(28, 1, 1, 1, 64),
    )


def solution(mesh):
    placed = (
        P(None, "gx", "gy", "gz"),
        P(None, "gx", "gy", "gz"),
        P(None, "gx", "gy", "gz"),
        P("gx", "gy", "gz"),
        P(None, None, "gx", "gy", "gz"),
        P(None, "gx", "gy", "gz"),
        P("gx", "gy", "gz", None),
    )
    return jax.shard_map(
        on_device,
        mesh=mesh,
        in_specs=placed,
        out_specs=(
            P(None, "gx", "gy", "gz"),
            P(None, "gx", "gy", "gz"),
            P(None, "gx", "gy", "gz"),
            P(None, None, "gx", "gy", "gz"),
            P(None, "gx", "gy", "gz", None),
        ),
        check_vma=False,
    )
```

```python
import jax
import jax.numpy as jnp
from jax import lax
from jax.experimental import pallas as pl
from jax.experimental.pallas import tpu as pltpu
from jax.sharding import PartitionSpec as P

MESH = pl.DeviceIdType.MESH
AXES = ("gx", "gy", "gz")
DIRS = (
    (1, 0, 0),
    (0, 1, 0),
    (0, 0, 1),
    (1, 1, 0),
    (1, -1, 0),
    (1, 0, 1),
    (1, 0, -1),
    (0, 1, 1),
    (0, 1, -1),
)
SLOTS = 6
FIELDS = 10
SHEAR = FIELDS
CODES = FIELDS + 3 * SLOTS
FULL = CODES + SLOTS
PACKS = (FULL * 8 + 127) // 128
STEP = 0.05
TINY = 1e-30

ROWS = 24
HEIGHT = 10 * ROWS

PACK_FROM = (
    (0, 0, -1),
    (0, 0, 1),
    (-1, 0, -1),
    (-1, 0, 1),
    (1, 0, -1),
    (1, 0, 1),
    (0, -1, -1),
    (0, -1, 1),
    (0, 1, -1),
    (0, 1, 1),
)
FLAT_FROM = (
    (-1, 0, 0),
    (1, 0, 0),
    (0, -1, 0),
    (0, 1, 0),
    (-1, -1, 0),
    (-1, 1, 0),
    (1, -1, 0),
    (1, 1, 0),
)
SENDERS = FLAT_FROM + PACK_FROM

ALONG_X = (0, 3, 4, 5, 6)
UP_Y = (1, 3, 7, 8)
DOWN_Y = (4,)

SEND_ORDER = (8, 9, 14, 15, 16, 17, 10, 11, 12, 13, 4, 5, 6, 7, 2, 3, 0, 1)


def plane(x):
    return (x + 1) * ROWS + 8


def step_kernel(
    off_hbm, vel_hbm, spin_hbm, rad_hbm, hist_hbm, con_hbm, leaving_hbm,
    state, arrivals,
    xlo, xhi, ylo, yhi, edges, packs, own_packs, cells, codes, leaving,
    xrow, ytop, ylow, rows, corner_x, corner_y, outbox, pad, pad_up, pad_down, level, rising, falling, behind, ahead, zside,
    local_sems, send_sems, recv_sems,
):
    here = [lax.axis_index(a) for a in AXES]
    size = [lax.axis_size(a) for a in AXES]

    def exists(step):
        ok = None
        for at, n, s in zip(here, size, step):
            if s == 0:
                continue
            test = at + s < n if s > 0 else at + s >= 0
            ok = test if ok is None else jnp.logical_and(ok, test)
        return ok

    def place(step):
        return tuple(at + s for at, s in zip(here, step))

    loads = [
        pltpu.make_async_copy(off_hbm, cells.at[0:3], local_sems.at[0]),
        pltpu.make_async_copy(vel_hbm, cells.at[3:6], local_sems.at[1]),
        pltpu.make_async_copy(spin_hbm, cells.at[6:9], local_sems.at[2]),
        pltpu.make_async_copy(rad_hbm, cells.at[9:10], local_sems.at[3]),
        pltpu.make_async_copy(hist_hbm, cells.at[SHEAR:CODES], local_sems.at[4]),
        pltpu.make_async_copy(con_hbm, codes, local_sems.at[5]),
        pltpu.make_async_copy(leaving_hbm, leaving, local_sems.at[6]),
    ]
    for load in loads:
        load.start()
    barrier = pltpu.get_barrier_semaphore()
    expected = jnp.int32(0)
    for step in SENDERS:
        there = exists(step)
        expected = expected + there.astype(jnp.int32)

        @pl.when(there)
        def _():
            pl.semaphore_signal(barrier, inc=1, device_id=place(step), device_id_type=MESH)

    with jax.named_scope("loadwait"):
        for load in loads[:4]:
            load.wait()
    with jax.named_scope("pack"):
        first_pack = fill_fields(cells, xrow, ytop, ylow, rows)
    with jax.named_scope("loadwait2"):
        for load in loads[4:]:
            load.wait()
    with jax.named_scope("pack2"):
        for s in range(SLOTS):
            cells[CODES + s] = codes[s].astype(jnp.float32)
        fill_sends(cells, own_packs, xrow, ytop, ylow, rows, corner_x, corner_y, first_pack)

    targets = [xlo, xhi, ylo, yhi] + [edges.at[k] for k in range(4)]
    sources = [xrow, cells.at[0:FIELDS, 0:8, :], ytop, ylow] + [rows.at[k] for k in range(4)]
    for k, s in enumerate(PACK_FROM):
        end = 0 if s[2] > 0 else 1
        if s[0] + s[1] == 0:
            targets.append(packs.at[k])
            sources.append(own_packs.at[end])
            continue
        targets.append(packs.at[k, 0:1])
        if s[0] + s[1] > 0:
            sources.append(own_packs.at[end, 0:1])
        else:
            sources.append((corner_x if s[0] else corner_y).at[end])

    def copy(k):
        to = tuple(-s for s in SENDERS[k])
        return pltpu.make_async_remote_copy(
            src_ref=sources[k],
            dst_ref=targets[k],
            send_sem=send_sems.at[k],
            recv_sem=recv_sems.at[k],
            device_id=place(to),
            device_id_type=MESH,
        )

    for k, step in enumerate(SENDERS):

        @pl.when(jnp.logical_not(exists(step)))
        def _():
            targets[k][...] = jnp.zeros(targets[k].shape, jnp.float32)

    with jax.named_scope("barrier"):
        pl.semaphore_wait(barrier, expected)
    for k in SEND_ORDER:

        @pl.when(exists(tuple(-s for s in SENDERS[k])))
        def _():
            copy(k).start()

    with jax.named_scope("inner"):
        inner_pairs(cells, state, pad, pad_up, pad_down, level, rising, falling)

    def receive(which):
        for k in which:

            @pl.when(exists(SENDERS[k]))
            def _():
                copy(k).wait_recv()

    with jax.named_scope("fold"):
        fold(level, rising, falling)
    with jax.named_scope("recvz"):
        receive(range(8, 18, 2))
    with jax.named_scope("floor"):
        end_pairs(0, level, state, zside, packs, own_packs)
    with jax.named_scope("recvy"):
        receive((2, 3))
    with jax.named_scope("ypairs"):
        y_pairs(cells, state, pad, level, ylo, yhi, ytop, ylow)
    with jax.named_scope("recvx"):
        receive((0, 1, 4, 5, 6, 7, 13))
    with jax.named_scope("xpairs"):
        x_pairs(cells, state, pad, level, behind, ahead, xlo, xhi, edges, packs, xrow)
    with jax.named_scope("outbox"):
        fill_outbox(cells, state, leaving, outbox, level)

    last = len(SENDERS)
    fall = pltpu.make_async_remote_copy(
        src_ref=outbox,
        dst_ref=arrivals,
        send_sem=send_sems.at[last],
        recv_sem=recv_sems.at[last],
        device_id=place((0, 0, -1)),
        device_id_type=MESH,
    )

    @pl.when(exists((0, 0, -1)))
    def _():
        fall.start()

    with jax.named_scope("recvtop"):
        receive((9, 11, 15, 17))
    with jax.named_scope("ceiling"):
        end_pairs(1, level, state, zside, packs, own_packs)
    with jax.named_scope("final"):
        finish(cells, state, leaving, level)

    for k, step in enumerate(SENDERS):

        @pl.when(exists(tuple(-s for s in step)))
        def _():
            copy(k).wait_send()

    with jax.named_scope("fall"):

        @pl.when(exists((0, 0, 1)))
        def _():
            fall.wait_recv()

    @pl.when(jnp.logical_not(exists((0, 0, 1))))
    def _():
        arrivals[...] = jnp.zeros(arrivals.shape, jnp.float32)

    @pl.when(exists((0, 0, -1)))
    def _():
        fall.wait_send()


def write_kernel(
    state, arrivals, new_off, new_vel, new_spin, new_hist, entered, unpacked, sems
):
    copies = [
        pltpu.make_async_copy(state.at[9:27], new_hist, sems.at[0]),
        pltpu.make_async_copy(state.at[0:3], new_off, sems.at[1]),
        pltpu.make_async_copy(state.at[3:6], new_vel, sems.at[2]),
        pltpu.make_async_copy(state.at[6:9], new_spin, sems.at[3]),
        pltpu.make_async_copy(unpacked, entered, sems.at[4]),
    ]
    for copy in copies[:4]:
        copy.start()
    for c in range(14):
        unpacked[c] = arrivals[c : c + 1, 0:64]
        unpacked[14 + c] = arrivals[c : c + 1, 64:128]
    copies[4].start()
    for copy in copies:
        copy.wait()


def cross(a, b):
    return [
        a[1] * b[2] - a[2] * b[1],
        a[2] * b[0] - a[0] * b[2],
        a[0] * b[1] - a[1] * b[0],
    ]


def dot3(a, b):
    return a[0] * b[0] + a[1] * b[1] + a[2] * b[2]


def pair(first, second, direction, shear, live):
    sep = []
    for k in range(3):
        gap = second[k] - first[k]
        sep.append(gap + float(direction[k]) if direction[k] else gap)
    square = dot3(sep, sep)
    inverse = lax.rsqrt(square)
    normal = [s * inverse for s in sep]
    radii = first[9] + second[9]
    overlap = jnp.maximum(radii - square * inverse, 0.0)
    product = first[9] * second[9] * overlap
    contact = product * lax.rsqrt(jnp.maximum(product * radii, TINY))
    contact = jnp.where(live, contact, 0.0)
    surface = cross([first[6 + k] + second[6 + k] for k in range(3)], normal)
    relative = [second[3 + k] - first[3 + k] - surface[k] for k in range(3)]
    approach = dot3(relative, normal)
    sliding = [relative[k] - approach * normal[k] for k in range(3)]
    repulsion = contact * jnp.maximum(10.0 * overlap - 2.0 * approach, 0.0)
    along = dot3(shear, normal)
    spring = [shear[k] - along * normal[k] + STEP * sliding[k] for k in range(3)]
    pull = [8.0 * spring[k] + 1.5 * sliding[k] for k in range(3)]
    size = contact * contact * dot3(pull, pull)
    factor = jnp.minimum(1.0, 0.4 * repulsion * lax.rsqrt(jnp.maximum(size, 0.0025)))
    scale = factor * contact
    tangent = [scale * pull[k] for k in range(3)]
    force = [tangent[k] - repulsion * normal[k] for k in range(3)]
    return force, cross(normal, tangent), [factor * spring[k] for k in range(3)]


def pick_shear(load, numbers):
    codes = [load(CODES + s) for s in range(SLOTS)]
    found = []
    for number in numbers:
        masks = [code == float(number) for code in codes]
        live = masks[0]
        shear = [jnp.where(masks[0], load(SHEAR + k), 0.0) for k in range(3)]
        for s in range(1, SLOTS):
            live = jnp.logical_or(live, masks[s])
            shear = [jnp.where(masks[s], load(SHEAR + 3 * s + k), shear[k]) for k in range(3)]
        found.append((shear, live, masks))
    return found


def scaled(values):
    return values[:6] + [v * values[9] for v in values[6:9]] + [values[9]]


def lanes():
    return lax.broadcasted_iota(jnp.int32, (8, 128), 1)


def add_packed(cells, channels, low, top):
    lane = lanes()
    for c in channels:
        for x in range(8):
            p = (c % 16) * 8 + x
            value = cells[c, x * 8 : x * 8 + 8, :]
            if p:
                value = pltpu.roll(value, p, 1)
            low = jnp.where(lane == p, value, low)
            top = jnp.where(lane == (p - 1) % 128, value, top)
    return low, top


def fill_fields(cells, xrow, ytop, ylow, rows):
    for c in range(FIELDS):
        xrow[c] = cells[c, 56:64, :]
        ytop[c] = cells[c, pl.ds(7, 8, stride=8), :]
        ylow[c] = cells[c, pl.ds(0, 8, stride=8), :]
        for which, row in enumerate((63, 56, 7, 0)):
            rows[which, c : c + 1, :] = cells[c, row : row + 1, :]
    zero = jnp.zeros((8, 128), jnp.float32)
    return add_packed(cells, range(FIELDS), zero, zero)


def fill_sends(cells, own_packs, xrow, ytop, ylow, rows, corner_x, corner_y, first_pack):
    lane = lanes()
    for target, span, numbers in (
        (xrow, pl.ds(56, 8), ALONG_X),
        (ytop, pl.ds(7, 8, stride=8), UP_Y),
        (ylow, pl.ds(0, 8, stride=8), DOWN_Y),
    ):
        found = pick_shear(lambda c: cells[c, span, :], numbers)
        for n, (shear, live, _) in enumerate(found):
            for k in range(3):
                target[FIELDS + 4 * n + k] = shear[k]
            target[FIELDS + 4 * n + 3] = jnp.where(live, 1.0, 0.0)
    for which, row, at in ((0, 7, 1), (1, 0, 2)):
        for k in range(4):
            rows[which, FIELDS + k : FIELDS + k + 1, :] = xrow[
                FIELDS + 4 * at + k, row : row + 1, :
            ]
    for end, at in ((0, 4), (1, 3)):
        corner = jnp.zeros((8, 128), jnp.float32)
        for j in range(FIELDS + 4):
            value = xrow[j if j < FIELDS else j + 4 * at]
            turn = j + end
            corner = jnp.where(lane == j, pltpu.roll(value, turn, 1) if turn else value, corner)
        corner_x[end, 0] = corner
    for k in range(PACKS):
        if k:
            low = top = jnp.zeros((8, 128), jnp.float32)
        else:
            low, top = first_pack
        channels = range(max(16 * k, FIELDS), min(FULL, 16 * k + 16))
        low, top = add_packed(cells, channels, low, top)
        for end, pack in enumerate((low, top)):
            own_packs[end, k] = pack
            corner_y[end, 0, k : k + 1, :] = pack[7:8, :]
    for end in range(2):
        corner_y[end, 0, PACKS:8, :] = jnp.zeros((8 - PACKS, 128), jnp.float32)


def inner_pairs(cells, state, pad, pad_up, pad_down, level, rising, falling):
    lane = lanes()
    zero = jnp.zeros((8, 128), jnp.float32)
    row = jnp.zeros((1, 128), jnp.float32)
    for x in range(8):
        here = slice(x * 8, x * 8 + 8)
        span = pl.ds(plane(x), 8)
        for c, v in enumerate(scaled([cells[c, here, :] for c in range(FIELDS)])):
            pad[c, span, :] = v
            pad_up[c, span, :] = jnp.where(lane == 127, 0.0, pltpu.roll(v, 127, 1))
            pad_down[c, span, :] = jnp.where(lane == 0, 0.0, pltpu.roll(v, 1, 1))
            pad[c, plane(x) - 1 : plane(x), :] = row
            for source in (pad, pad_up, pad_down):
                source[c, plane(x) + 8 : plane(x) + 9, :] = row
    for c in range(FIELDS):
        for source in (pad, pad_up, pad_down):
            source[c, pl.ds(plane(8), 8), :] = zero
        pad[c, plane(8) - 1 : plane(8), :] = row
        pad[c, plane(8) + 8 : plane(8) + 9, :] = row
    for total in (level, rising, falling):
        for c in range(6):
            for x in range(9):
                total[c, pl.ds(plane(x), 8), :] = zero
                total[c, plane(x) - 1 : plane(x), :] = row
                total[c, plane(x) + 8 : plane(x) + 9, :] = row

    def body(x, carry):
        base = pl.multiple_of((x + 1) * ROWS + 8, 8)
        here = pl.ds(pl.multiple_of(x * 8, 8), 8)
        first = [pad[c, pl.ds(base, 8), :] for c in range(FIELDS)]
        forces = [zero] * 3
        twists = [zero] * 3
        springs = [zero] * (3 * SLOTS)
        for number, (dx, dy, dz) in enumerate(DIRS):
            span = pl.ds(base + dx * ROWS + dy, 8)
            source = (pad, pad_up, pad_down)[dz]
            total = (level, rising, falling)[dz]
            second = [source[c, span, :] for c in range(FIELDS)]
            ((shear, live, masks),) = pick_shear(lambda c: cells[c, here, :], (number,))
            force, twist, spring = pair(first, second, (dx, dy, dz), shear, live)
            for k in range(3):
                forces[k] = forces[k] + force[k]
                twists[k] = twists[k] + twist[k]
                for s in range(SLOTS):
                    springs[3 * s + k] = jnp.where(masks[s], spring[k], springs[3 * s + k])
                total[k, span, :] = total[k, span, :] - force[k]
                total[3 + k, span, :] = total[3 + k, span, :] + twist[k]
        for k in range(3):
            level[k, pl.ds(base, 8), :] = level[k, pl.ds(base, 8), :] + forces[k]
            level[3 + k, pl.ds(base, 8), :] = level[3 + k, pl.ds(base, 8), :] + twists[k]
        for c in range(3 * SLOTS):
            state[9 + c, here, :] = springs[c]
        return carry

    lax.fori_loop(0, 8, body, 0)


class Sums:
    def __init__(self):
        zero = jnp.zeros((8, 128), jnp.float32)
        self.total = [zero] * 6
        self.springs = [zero] * (3 * SLOTS)

    def own(self, result, masks):
        force, twist, spring = result
        for k in range(3):
            self.total[k] = self.total[k] + force[k]
            self.total[3 + k] = self.total[3 + k] + twist[k]
            for s in range(SLOTS):
                self.springs[3 * s + k] = jnp.where(masks[s], spring[k], self.springs[3 * s + k])

    def partner(self, result):
        force, twist, _ = result
        for k in range(3):
            self.total[k] = self.total[k] - force[k]
            self.total[3 + k] = self.total[3 + k] + twist[k]

    def store(self, level, rows, state, span):
        for c in range(6):
            level[c, rows, :] = level[c, rows, :] + self.total[c]
        if span is not None:
            for c in range(3 * SLOTS):
                state[9 + c, span, :] = state[9 + c, span, :] + self.springs[c]


def turned(values, amount, axis=1):
    return [pltpu.roll(v, amount, axis) for v in values]


def masks_of(cells, span, number):
    return [cells[CODES + s, span, :] == float(number) for s in range(SLOTS)]


def fold(level, rising, falling):
    lane = lanes()
    for x in range(8):
        rows = pl.ds(plane(x), 8)
        for c in range(6):
            up = jnp.where(lane == 0, 0.0, pltpu.roll(rising[c, rows, :], 1, 1))
            down = jnp.where(lane == 127, 0.0, pltpu.roll(falling[c, rows, :], 127, 1))
            level[c, rows, :] = level[c, rows, :] + up + down


def x_pairs(cells, state, pad, level, behind, ahead, xlo, xhi, edges, packs, xrow):
    lane = lanes()
    for c in range(FIELDS + 4 * len(ALONG_X)):
        behind[c, 8:16, :] = xlo[c]
    for c in range(FIELDS):
        behind[c, 7:8, :] = edges[0, c : c + 1, :]
        behind[c, 16:17, :] = edges[1, c : c + 1, :]
        ahead[c, 7:8, :] = edges[2, c : c + 1, :]
        ahead[c, 16:17, :] = edges[3, c : c + 1, :]
        ahead[c, 8:16, :] = xhi[c]
    for k in range(4):
        behind[FIELDS + 4 + k, 7:8, :] = edges[0, FIELDS + k : FIELDS + k + 1, :]
        behind[FIELDS + 8 + k, 16:17, :] = edges[1, FIELDS + k : FIELDS + k + 1, :]

    def pack_scaled(pack, top):
        group = (lane + top) // 8
        for c in (6, 7, 8):
            radius = pltpu.roll(pack, 128 - 8 * (9 - c), 1)
            pack = jnp.where(group == c, pack * radius, pack)
        return pack

    beyond_up = pack_scaled(packs[5, 0], 0)
    beyond_down = pack_scaled(packs[4, 0], 1)
    sums = Sums()
    first = [pad[c, pl.ds(plane(7), 8), :] for c in range(FIELDS)]
    for n, number in enumerate(ALONG_X):
        dx, dy, dz = DIRS[number]
        second = scaled([ahead[c, pl.ds(8 + dy, 8), :] for c in range(FIELDS)])
        if dz > 0:
            second = [
                jnp.where(
                    lane == 127, pltpu.roll(beyond_up, 127 - 8 * c, 1), pltpu.roll(v, 127, 1)
                )
                for c, v in enumerate(second)
            ]
        elif dz < 0:
            second = [
                jnp.where(
                    lane == 0, pltpu.roll(beyond_down, (129 - 8 * c) % 128, 1), pltpu.roll(v, 1, 1)
                )
                for c, v in enumerate(second)
            ]
        at = FIELDS + 4 * n
        shear = [xrow[at + k] for k in range(3)]
        result = pair(first, second, DIRS[number], shear, xrow[at + 3] > 0.5)
        sums.own(result, masks_of(cells, pl.ds(56, 8), number))
    sums.store(level, pl.ds(plane(7), 8), state, pl.ds(56, 8))
    sums = Sums()
    second = [pad[c, pl.ds(plane(0), 8), :] for c in range(FIELDS)]
    for n, number in enumerate(ALONG_X):
        dx, dy, dz = DIRS[number]
        span = pl.ds(8 - dy, 8)
        first = scaled([behind[c, span, :] for c in range(FIELDS)])
        first += [behind[FIELDS + 4 * n + k, span, :] for k in range(4)]
        if dz:
            first = turned(first, dz % 128)
        live = first[13] > 0.5
        if dz:
            live = jnp.logical_and(live, lane != (0 if dz > 0 else 127))
        sums.partner(pair(first[:10], second, DIRS[number], first[10:13], live))
    sums.store(level, pl.ds(plane(0), 8), state, None)


def y_pairs(cells, state, pad, level, ylo, yhi, ytop, ylow):
    lane = lanes()
    sub = lax.broadcasted_iota(jnp.int32, (8, 128), 0)
    top_fields = scaled([yhi[c] for c in range(FIELDS)])
    low_fields = scaled([ylo[c] for c in range(FIELDS)])
    sums = Sums()
    mine_rows = pl.ds(plane(0) + 7, 8, stride=ROWS)
    span = pl.ds(7, 8, stride=8)
    mine = [pad[c, mine_rows, :] for c in range(FIELDS)]
    for n, number in enumerate(UP_Y):
        dx, dy, dz = DIRS[number]
        at = FIELDS + 4 * n
        live = ytop[at + 3] > 0.5
        second = top_fields
        if dx:
            second = turned(second, 7, 0)
            live = jnp.logical_and(live, sub != 7)
        if dz:
            second = turned(second, -dz % 128)
            live = jnp.logical_and(live, lane != (127 if dz > 0 else 0))
        shear = [ytop[at + k] for k in range(3)]
        sums.own(pair(mine, second, DIRS[number], shear, live), masks_of(cells, span, number))
    first = turned(top_fields + [yhi[FIELDS + k] for k in range(4)], 1, 0)
    live = jnp.logical_and(first[13] > 0.5, sub != 0)
    sums.partner(pair(first[:10], mine, DIRS[4], first[10:13], live))
    sums.store(level, mine_rows, state, span)

    sums = Sums()
    mine_rows = pl.ds(plane(0), 8, stride=ROWS)
    span = pl.ds(0, 8, stride=8)
    mine = [pad[c, mine_rows, :] for c in range(FIELDS)]
    second = turned(low_fields, 7, 0)
    live = jnp.logical_and(ylow[FIELDS + 3] > 0.5, sub != 7)
    shear = [ylow[FIELDS + k] for k in range(3)]
    sums.own(pair(mine, second, DIRS[4], shear, live), masks_of(cells, span, 4))
    for n, number in enumerate(UP_Y):
        dx, dy, dz = DIRS[number]
        first = low_fields + [ylo[FIELDS + 4 * n + k] for k in range(4)]
        if dx:
            first = turned(first, 1, 0)
        if dz:
            first = turned(first, dz % 128)
        live = first[13] > 0.5
        if dx:
            live = jnp.logical_and(live, sub != 0)
        if dz:
            live = jnp.logical_and(live, lane != (0 if dz > 0 else 127))
        sums.partner(pair(first[:10], mine, DIRS[number], first[10:13], live))
    sums.store(level, mine_rows, state, span)


def end_pairs(end, level, state, zside, packs, own_packs):
    lane = lanes()
    theirs, ours = (((2, 5, 7), (6, 8)), ((6, 8), (2, 5, 7)))[end]
    top = 1 - end

    def spread(pack, c, top):
        p = (c % 16) * 8 - top
        return pltpu.roll(pack, -p % 128, 1) if p % 128 else pack

    back = [
        pltpu.roll(packs[2 + end, 0], -j % 128, 1) if j else packs[2 + end, 0]
        for j in range(FIELDS + 4)
    ]
    back = scaled(back[:FIELDS]) + back[FIELDS:]
    for k in range(PACKS):
        straight, left = packs[end, k], pltpu.roll(packs[6 + end, 0], 7 - k, 0)
        for c in range(16 * k, min(FULL, 16 * k + 16)):
            zside[end, c, 8:16, :] = spread(straight, c, top)
            zside[end, c, 0:8, :] = spread(left, c, top)
            if c < FIELDS:
                zside[end, c, 16:24, :] = spread(packs[8 + end, 0], c, top)
    own = [spread(own_packs[end, c // 16], c, end) for c in range(FULL)]
    mine = scaled(own[:FIELDS])
    sums = Sums()
    for number, (shear, live, masks) in zip(ours, pick_shear(lambda c: own[c], ours)):
        dx, dy, dz = DIRS[number]
        second = scaled([zside[end, c, pl.ds(8 + dy, 8), :] for c in range(FIELDS)])
        if dx:
            second = [jnp.where(lane < 7, v, 0.0) for v in turned(second, 127)]
        sums.own(pair(mine, second, DIRS[number], shear, live), masks)
    for number in theirs:
        dx, dy, dz = DIRS[number]
        span = pl.ds(8 - dy, 8)
        first = scaled([zside[end, c, span, :] for c in range(FIELDS)])
        ((shear, live, _),) = pick_shear(lambda c: zside[end, c, span, :], (number,))
        first = first + shear + [jnp.where(live, 1.0, 0.0)]
        if dx:
            first = [jnp.where(lane == 0, b, v) for b, v in zip(back, turned(first, 1))]
        sums.partner(pair(first[:10], mine, DIRS[number], first[10:13], first[13] > 0.5))
    edge = 127 * end
    hold = lane == edge
    for x in range(8):
        turn = (edge - x) % 128

        def put(v):
            return jnp.where(hold, pltpu.roll(v, turn, 1) if turn else v, 0.0)

        rows = pl.ds(plane(x), 8)
        here = slice(x * 8, x * 8 + 8)
        for c in range(6):
            level[c, rows, :] = level[c, rows, :] + put(sums.total[c])
        for c in range(3 * SLOTS):
            state[9 + c, here, :] = state[9 + c, here, :] + put(sums.springs[c])


def moved(cells, level, x):
    rows = pl.ds(plane(x), 8)
    here = slice(x * 8, x * 8 + 8)
    sums = [level[c, rows, :] for c in range(6)]
    radius = cells[9, here, :]
    inverse = 1.0 / radius
    push = STEP * inverse * inverse * inverse
    turn = 0.125 * (inverse * inverse) * (inverse * inverse)
    velocity = [cells[3 + k, here, :] + push * sums[k] for k in range(3)]
    velocity[2] = velocity[2] - STEP
    offset = [cells[k, here, :] + STEP * velocity[k] for k in range(3)]
    rotation = [cells[6 + k, here, :] + turn * sums[3 + k] for k in range(3)]
    return offset, velocity, rotation, radius


def fill_outbox(cells, state, leaving, outbox, level):
    lane = lanes()
    sub = lax.broadcasted_iota(jnp.int32, (8, 128), 0)
    names = leaving[0:1, 0:64]
    names = jnp.concatenate([names, names], axis=1)
    names = jnp.broadcast_to(names, (8, 128))
    height = jnp.where(names >= 0, names % 128, 0)
    column = jnp.where(names >= 0, names // 128, -1)
    starts = [(lax.axis_index(a) * n).astype(jnp.float32) for a, n in zip(AXES, (8, 8, 128))]
    boxes = [jnp.zeros((8, 128), jnp.float32) for _ in range(14)]
    for x in range(8):
        here = slice(x * 8, x * 8 + 8)
        offset, velocity, rotation, radius = moved(cells, level, x)
        springs = [state[9 + c, here, :] for c in range(3 * SLOTS)]
        position = [
            offset[0] + (starts[0] + float(x)),
            offset[1] + (starts[1] + sub.astype(jnp.float32)),
            offset[2] + (starts[2] + lane.astype(jnp.float32)),
        ]
        chosen = column == x * 8 + sub
        halves = [jnp.logical_and(chosen, lane < 64), jnp.logical_and(chosen, lane >= 64)]
        for c, v in enumerate(position + velocity + rotation + [radius] + springs):
            values = jnp.take_along_axis(v, height, axis=1)
            boxes[c % 14] = jnp.where(halves[c // 14], values, boxes[c % 14])
    for c in range(14):
        outbox[c : c + 1, :] = jnp.sum(boxes[c], axis=0, keepdims=True)


def finish(cells, state, leaving, level):
    lane = lanes()
    wide = jnp.broadcast_to(leaving[0:1, 0:64], (8, 64))
    deep = lax.broadcasted_iota(jnp.int32, (8, 64), 0)
    for x in range(8):
        here = slice(x * 8, x * 8 + 8)
        offset, velocity, rotation, _ = moved(cells, level, x)
        left = [
            jnp.max(jnp.where(wide == (x * 8 + deep) * 128 + z, 1.0, 0.0), axis=1, keepdims=True)
            for z in range(2)
        ]
        staying = 1.0 - jnp.where(lane == 0, left[0], jnp.where(lane == 1, left[1], 0.0))
        for c, v in enumerate(offset + velocity + rotation):
            state[c, here, :] = v * staying
        for c in range(9, 27):
            state[c, here, :] = state[c, here, :] * staying


def on_device(offset, velocity, spin, radius, history, contacts, leaving):
    f32 = jnp.float32
    off = offset.reshape(3, 64, 128)
    vel = velocity.reshape(3, 64, 128)
    spn = spin.reshape(3, 64, 128)
    rad = radius.reshape(1, 64, 128)
    hist = history.reshape(3 * SLOTS, 64, 128)
    con = contacts.reshape(SLOTS, 64, 128)
    vmem = pl.BlockSpec(memory_space=pltpu.VMEM)
    hbm = pl.BlockSpec(memory_space=pltpu.HBM)
    halo_shapes = (
        (FIELDS + 4 * len(ALONG_X), 8, 128),
        (FIELDS, 8, 128),
        (FIELDS + 4 * len(UP_Y), 8, 128),
        (FIELDS + 4 * len(DOWN_Y), 8, 128),
        (4, 16, 128),
        (len(PACK_FROM), PACKS, 8, 128),
        (2, PACKS, 8, 128),
    )
    state, arrivals = pl.pallas_call(
        step_kernel,
        out_shape=[pltpu.VMEM((27, 64, 128), f32), pltpu.VMEM((16, 128), f32)],
        in_specs=[hbm] * 7,
        out_specs=[vmem] * 2,
        scratch_shapes=[pltpu.VMEM(s, f32) for s in halo_shapes]
        + [
            pltpu.VMEM((FULL, 64, 128), f32),
            pltpu.VMEM((SLOTS, 64, 128), jnp.int32),
            pltpu.VMEM((1, 64), jnp.int32),
            pltpu.VMEM((FIELDS + 4 * len(ALONG_X), 8, 128), f32),
            pltpu.VMEM((FIELDS + 4 * len(UP_Y), 8, 128), f32),
            pltpu.VMEM((FIELDS + 4 * len(DOWN_Y), 8, 128), f32),
            pltpu.VMEM((4, 16, 128), f32),
            pltpu.VMEM((2, 1, 8, 128), f32),
            pltpu.VMEM((2, 1, 8, 128), f32),
            pltpu.VMEM((16, 128), f32),
            pltpu.VMEM((FIELDS, HEIGHT, 128), f32),
            pltpu.VMEM((FIELDS, HEIGHT, 128), f32),
            pltpu.VMEM((FIELDS, HEIGHT, 128), f32),
            pltpu.VMEM((6, HEIGHT, 128), f32),
            pltpu.VMEM((6, HEIGHT, 128), f32),
            pltpu.VMEM((6, HEIGHT, 128), f32),
            pltpu.VMEM((FIELDS + 4 * len(ALONG_X), ROWS, 128), f32),
            pltpu.VMEM((FIELDS, ROWS, 128), f32),
            pltpu.VMEM((2, FULL, ROWS, 128), f32),
            pltpu.SemaphoreType.DMA((7,)),
            pltpu.SemaphoreType.DMA((len(SENDERS) + 1,)),
            pltpu.SemaphoreType.DMA((len(SENDERS) + 1,)),
        ],
        compiler_params=pltpu.CompilerParams(
            collective_id=0, has_side_effects=True, vmem_limit_bytes=24 << 20
        ),
        name="step",
    )(*[
        pltpu.with_memory_space_constraint(a, pltpu.HBM)
        for a in (off, vel, spn, rad, hist, con, leaving.reshape(1, 64))
    ])
    moved = jax.ShapeDtypeStruct((3, 64, 128), f32)
    new_off, new_vel, new_spin, new_hist, arrivals = pl.pallas_call(
        write_kernel,
        out_shape=[
            moved, moved, moved,
            jax.ShapeDtypeStruct((3 * SLOTS, 64, 128), f32),
            jax.ShapeDtypeStruct((28, 1, 64), f32),
        ],
        in_specs=[vmem] * 2,
        out_specs=[hbm] * 5,
        scratch_shapes=[pltpu.VMEM((28, 1, 64), f32), pltpu.SemaphoreType.DMA((5,))],
        compiler_params=pltpu.CompilerParams(vmem_limit_bytes=8 << 20),
        name="write",
    )(state, arrivals)
    return (
        new_off.reshape(3, 8, 8, 128),
        new_vel.reshape(3, 8, 8, 128),
        new_spin.reshape(3, 8, 8, 128),
        new_hist.reshape(SLOTS, 3, 8, 8, 128),
        arrivals.reshape(28, 1, 1, 1, 64),
    )


def solution(mesh):
    placed = (
        P(None, "gx", "gy", "gz"),
        P(None, "gx", "gy", "gz"),
        P(None, "gx", "gy", "gz"),
        P("gx", "gy", "gz"),
        P(None, None, "gx", "gy", "gz"),
        P(None, "gx", "gy", "gz"),
        P("gx", "gy", "gz", None),
    )
    return jax.shard_map(
        on_device,
        mesh=mesh,
        in_specs=placed,
        out_specs=(
            P(None, "gx", "gy", "gz"),
            P(None, "gx", "gy", "gz"),
            P(None, "gx", "gy", "gz"),
            P(None, None, "gx", "gy", "gz"),
            P(None, "gx", "gy", "gz", None),
        ),
        check_vma=False,
    )
```

```python
import jax
import jax.numpy as jnp
from jax import lax
from jax.experimental import pallas as pl
from jax.experimental.pallas import tpu as pltpu
from jax.sharding import PartitionSpec as P

MESH = pl.DeviceIdType.MESH
AXES = ("gx", "gy", "gz")
DIRS = (
    (1, 0, 0),
    (0, 1, 0),
    (0, 0, 1),
    (1, 1, 0),
    (1, -1, 0),
    (1, 0, 1),
    (1, 0, -1),
    (0, 1, 1),
    (0, 1, -1),
)
SLOTS = 6
FIELDS = 10
SHEAR = FIELDS
CODES = FIELDS + 3 * SLOTS
FULL = CODES + SLOTS
PACKS = (FULL * 8 + 127) // 128
STEP = 0.05
TINY = 1e-30

ROWS = 24
HEIGHT = 10 * ROWS

PACK_FROM = (
    (0, 0, -1),
    (0, 0, 1),
    (-1, 0, -1),
    (-1, 0, 1),
    (1, 0, -1),
    (1, 0, 1),
    (0, -1, -1),
    (0, -1, 1),
    (0, 1, -1),
    (0, 1, 1),
)
FLAT_FROM = (
    (-1, 0, 0),
    (1, 0, 0),
    (0, -1, 0),
    (0, 1, 0),
    (-1, -1, 0),
    (-1, 1, 0),
    (1, -1, 0),
    (1, 1, 0),
)
SENDERS = FLAT_FROM + PACK_FROM

ALONG_X = (0, 3, 4, 5, 6)
UP_Y = (1, 3, 7, 8)
DOWN_Y = (4,)

SEND_ORDER = (10, 12, 14, 16, 4, 5, 6, 7, 8, 2, 0, 3, 1, 11, 13, 15, 17, 9)


def plane(x):
    return (x + 1) * ROWS + 8


def step_kernel(*refs):
    pl.run_scoped(
        lambda local_sems, send_sems: step_body(*refs, local_sems, send_sems),
        pltpu.SemaphoreType.DMA((7,)),
        pltpu.SemaphoreType.DMA((len(SENDERS) + 1,)),
    )


def step_body(
    off_hbm, vel_hbm, spin_hbm, rad_hbm, hist_hbm, con_hbm, leaving_hbm,
    state, arrivals,
    xlo, xhi, ylo, yhi, edges, packs, own_packs, cells, codes, leaving,
    xrow, ytop, ylow, rows, corner_x, corner_y, outbox, pad, pad_up, pad_down, level, rising, falling, behind, ahead, zside,
    recv_sems, local_sems, send_sems,
):
    here = [lax.axis_index(a) for a in AXES]
    size = [lax.axis_size(a) for a in AXES]

    def exists(step):
        ok = None
        for at, n, s in zip(here, size, step):
            if s == 0:
                continue
            test = at + s < n if s > 0 else at + s >= 0
            ok = test if ok is None else jnp.logical_and(ok, test)
        return ok

    def place(step):
        return tuple(at + s for at, s in zip(here, step))

    loads = [
        pltpu.make_async_copy(off_hbm, cells.at[0:3], local_sems.at[0]),
        pltpu.make_async_copy(vel_hbm, cells.at[3:6], local_sems.at[1]),
        pltpu.make_async_copy(spin_hbm, cells.at[6:9], local_sems.at[2]),
        pltpu.make_async_copy(rad_hbm, cells.at[9:10], local_sems.at[3]),
        pltpu.make_async_copy(hist_hbm, cells.at[SHEAR:CODES], local_sems.at[4]),
        pltpu.make_async_copy(con_hbm, codes, local_sems.at[5]),
        pltpu.make_async_copy(leaving_hbm, leaving, local_sems.at[6]),
    ]
    barrier = pltpu.get_barrier_semaphore()
    expected = jnp.int32(0)
    for step in SENDERS[4:] + SENDERS[:4]:
        there = exists(step)
        expected = expected + there.astype(jnp.int32)

        @pl.when(there)
        def _():
            pl.semaphore_signal(barrier, inc=1, device_id=place(step), device_id_type=MESH)

    for load in loads:
        load.start()
    with jax.named_scope("loadwait"):
        for load in loads[:4]:
            load.wait()
    with jax.named_scope("pack"):
        first_pack = fill_fields(cells, xrow, ytop, ylow, rows)
    with jax.named_scope("loadwait2"):
        for load in loads[4:]:
            load.wait()
    with jax.named_scope("pack2"):
        for s in range(SLOTS):
            cells[CODES + s] = codes[s].astype(jnp.float32)
        fill_sends(cells, own_packs, xrow, ytop, ylow, rows, corner_x, corner_y, first_pack)

    targets = [xlo, xhi, ylo, yhi] + [edges.at[k] for k in range(4)]
    sources = [xrow, cells.at[0:FIELDS, 0:8, :], ytop, ylow] + [rows.at[k] for k in range(4)]
    for k, s in enumerate(PACK_FROM):
        end = 0 if s[2] > 0 else 1
        if s[0] + s[1] == 0:
            targets.append(packs.at[k])
            sources.append(own_packs.at[end])
            continue
        targets.append(packs.at[k, 0:1])
        if s[0] + s[1] > 0:
            sources.append(own_packs.at[end, 0:1])
        else:
            sources.append((corner_x if s[0] else corner_y).at[end])

    def copy(k):
        to = tuple(-s for s in SENDERS[k])
        return pltpu.make_async_remote_copy(
            src_ref=sources[k],
            dst_ref=targets[k],
            send_sem=send_sems.at[k],
            recv_sem=recv_sems.at[k],
            device_id=place(to),
            device_id_type=MESH,
        )

    for k, step in enumerate(SENDERS):

        @pl.when(jnp.logical_not(exists(step)))
        def _():
            targets[k][...] = jnp.zeros(targets[k].shape, jnp.float32)

    with jax.named_scope("barrier"):
        pl.semaphore_wait(barrier, expected)
    for k in SEND_ORDER:

        @pl.when(exists(tuple(-s for s in SENDERS[k])))
        def _():
            copy(k).start()

    with jax.named_scope("inner"):
        inner_pairs(cells, state, pad, pad_up, pad_down, level, rising, falling)

    def receive(which):
        for k in which:

            @pl.when(exists(SENDERS[k]))
            def _():
                copy(k).wait_recv()

    with jax.named_scope("fold"):
        fold(level, rising, falling)
    with jax.named_scope("recvz"):
        receive(range(8, 18, 2))
    with jax.named_scope("floor"):
        end_pairs(0, level, state, zside, packs, own_packs)
    with jax.named_scope("recvy"):
        receive((2, 3))
    with jax.named_scope("ypairs"):
        y_high(cells, state, pad, level, yhi, ytop)
        y_low(cells, state, pad, level, ylo, ylow)
    with jax.named_scope("outbox"):
        boxes = [jnp.zeros((8, 128), jnp.float32)] * 14
        boxes = gather_leaving(boxes, range(1, 7), cells, state, leaving, level)
    with jax.named_scope("recvx"):
        receive((0, 1, 4, 5, 6, 7))
    with jax.named_scope("xpairs"):
        x_ahead(cells, state, pad, level, ahead, xhi, edges, xrow)
        x_behind(pad, level, behind, xlo, edges)
    with jax.named_scope("outbox2"):
        boxes = gather_leaving(boxes, (0, 7), cells, state, leaving, level)
        for c in range(14):
            outbox[c : c + 1, :] = jnp.sum(boxes[c], axis=0, keepdims=True)

    last = len(SENDERS)
    fall = pltpu.make_async_remote_copy(
        src_ref=outbox,
        dst_ref=arrivals,
        send_sem=send_sems.at[last],
        recv_sem=recv_sems.at[last],
        device_id=place((0, 0, -1)),
        device_id_type=MESH,
    )

    @pl.when(exists((0, 0, -1)))
    def _():
        fall.start()

    with jax.named_scope("recvtop"):
        receive((9, 11, 13, 15, 17))
    with jax.named_scope("ceiling"):
        end_pairs(1, level, state, zside, packs, own_packs)
    with jax.named_scope("final"):
        finish(cells, state, leaving, level)

    for k, step in enumerate(SENDERS):

        @pl.when(exists(tuple(-s for s in step)))
        def _():
            copy(k).wait_send()

    with jax.named_scope("fall"):

        @pl.when(exists((0, 0, 1)))
        def _():
            fall.wait_recv()

    @pl.when(jnp.logical_not(exists((0, 0, 1))))
    def _():
        arrivals[...] = jnp.zeros(arrivals.shape, jnp.float32)

    @pl.when(exists((0, 0, -1)))
    def _():
        fall.wait_send()


def write_kernel(
    state, arrivals, new_off, new_vel, new_spin, new_hist, entered, unpacked, sems
):
    copies = [
        pltpu.make_async_copy(state.at[9:27], new_hist, sems.at[0]),
        pltpu.make_async_copy(state.at[0:3], new_off, sems.at[1]),
        pltpu.make_async_copy(state.at[3:6], new_vel, sems.at[2]),
        pltpu.make_async_copy(state.at[6:9], new_spin, sems.at[3]),
        pltpu.make_async_copy(unpacked, entered, sems.at[4]),
    ]
    for copy in copies[:4]:
        copy.start()
    for c in range(14):
        unpacked[c] = arrivals[c : c + 1, 0:64]
        unpacked[14 + c] = arrivals[c : c + 1, 64:128]
    copies[4].start()
    for copy in copies:
        copy.wait()


def cross(a, b):
    return [
        a[1] * b[2] - a[2] * b[1],
        a[2] * b[0] - a[0] * b[2],
        a[0] * b[1] - a[1] * b[0],
    ]


def dot3(a, b):
    return a[0] * b[0] + a[1] * b[1] + a[2] * b[2]


def pair(first, second, direction, shear, live):
    sep = []
    for k in range(3):
        gap = second[k] - first[k]
        sep.append(gap + float(direction[k]) if direction[k] else gap)
    square = dot3(sep, sep)
    inverse = lax.rsqrt(square)
    normal = [s * inverse for s in sep]
    radii = first[9] + second[9]
    overlap = jnp.maximum(radii - square * inverse, 0.0)
    product = first[9] * second[9] * overlap
    contact = product * lax.rsqrt(jnp.maximum(product * radii, TINY))
    contact = jnp.where(live, contact, 0.0)
    surface = cross([first[6 + k] + second[6 + k] for k in range(3)], normal)
    relative = [second[3 + k] - first[3 + k] - surface[k] for k in range(3)]
    approach = dot3(relative, normal)
    sliding = [relative[k] - approach * normal[k] for k in range(3)]
    repulsion = contact * jnp.maximum(10.0 * overlap - 2.0 * approach, 0.0)
    along = dot3(shear, normal)
    spring = [shear[k] - along * normal[k] + STEP * sliding[k] for k in range(3)]
    pull = [8.0 * spring[k] + 1.5 * sliding[k] for k in range(3)]
    size = contact * contact * dot3(pull, pull)
    factor = jnp.minimum(1.0, 0.4 * repulsion * lax.rsqrt(jnp.maximum(size, 0.0025)))
    scale = factor * contact
    tangent = [scale * pull[k] for k in range(3)]
    force = [tangent[k] - repulsion * normal[k] for k in range(3)]
    return force, cross(normal, tangent), [factor * spring[k] for k in range(3)]


def pick_shear(load, numbers):
    codes = [load(CODES + s) for s in range(SLOTS)]
    found = []
    for number in numbers:
        masks = [code == float(number) for code in codes]
        live = masks[0]
        shear = [jnp.where(masks[0], load(SHEAR + k), 0.0) for k in range(3)]
        for s in range(1, SLOTS):
            live = jnp.logical_or(live, masks[s])
            shear = [jnp.where(masks[s], load(SHEAR + 3 * s + k), shear[k]) for k in range(3)]
        found.append((shear, live, masks))
    return found


def scaled(values):
    return values[:6] + [v * values[9] for v in values[6:9]] + [values[9]]


def lanes():
    return lax.broadcasted_iota(jnp.int32, (8, 128), 1)


def add_packed(cells, channels, low, top):
    lane = lanes()
    for c in channels:
        for x in range(8):
            p = (c % 16) * 8 + x
            value = cells[c, x * 8 : x * 8 + 8, :]
            if p:
                value = pltpu.roll(value, p, 1)
            low = jnp.where(lane == p, value, low)
            top = jnp.where(lane == (p - 1) % 128, value, top)
    return low, top


def fill_fields(cells, xrow, ytop, ylow, rows):
    for c in range(FIELDS):
        xrow[c] = cells[c, 56:64, :]
        ytop[c] = cells[c, pl.ds(7, 8, stride=8), :]
        ylow[c] = cells[c, pl.ds(0, 8, stride=8), :]
        for which, row in enumerate((63, 56, 7, 0)):
            rows[which, c : c + 1, :] = cells[c, row : row + 1, :]
    zero = jnp.zeros((8, 128), jnp.float32)
    return add_packed(cells, range(FIELDS), zero, zero)


def fill_sends(cells, own_packs, xrow, ytop, ylow, rows, corner_x, corner_y, first_pack):
    lane = lanes()
    for target, span, numbers in (
        (xrow, pl.ds(56, 8), ALONG_X),
        (ytop, pl.ds(7, 8, stride=8), UP_Y),
        (ylow, pl.ds(0, 8, stride=8), DOWN_Y),
    ):
        found = pick_shear(lambda c: cells[c, span, :], numbers)
        for n, (shear, live, _) in enumerate(found):
            for k in range(3):
                target[FIELDS + 4 * n + k] = shear[k]
            target[FIELDS + 4 * n + 3] = jnp.where(live, 1.0, 0.0)
    for which, row, at in ((0, 7, 1), (1, 0, 2)):
        for k in range(4):
            rows[which, FIELDS + k : FIELDS + k + 1, :] = xrow[
                FIELDS + 4 * at + k, row : row + 1, :
            ]
    for end, at in ((0, 4), (1, 3)):
        corner = jnp.zeros((8, 128), jnp.float32)
        for j in range(FIELDS + 4):
            value = xrow[j if j < FIELDS else j + 4 * at]
            turn = j + end
            corner = jnp.where(lane == j, pltpu.roll(value, turn, 1) if turn else value, corner)
        corner_x[end, 0] = corner
    for k in range(PACKS):
        if k:
            low = top = jnp.zeros((8, 128), jnp.float32)
        else:
            low, top = first_pack
        channels = range(max(16 * k, FIELDS), min(FULL, 16 * k + 16))
        low, top = add_packed(cells, channels, low, top)
        for end, pack in enumerate((low, top)):
            own_packs[end, k] = pack
            corner_y[end, 0, k : k + 1, :] = pack[7:8, :]
    for end in range(2):
        corner_y[end, 0, PACKS:8, :] = jnp.zeros((8 - PACKS, 128), jnp.float32)


def inner_pairs(cells, state, pad, pad_up, pad_down, level, rising, falling):
    lane = lanes()
    zero = jnp.zeros((8, 128), jnp.float32)
    row = jnp.zeros((1, 128), jnp.float32)
    for x in range(8):
        here = slice(x * 8, x * 8 + 8)
        span = pl.ds(plane(x), 8)
        for c, v in enumerate(scaled([cells[c, here, :] for c in range(FIELDS)])):
            pad[c, span, :] = v
            pad_up[c, span, :] = jnp.where(lane == 127, 0.0, pltpu.roll(v, 127, 1))
            pad_down[c, span, :] = jnp.where(lane == 0, 0.0, pltpu.roll(v, 1, 1))
            pad[c, plane(x) - 1 : plane(x), :] = row
            for source in (pad, pad_up, pad_down):
                source[c, plane(x) + 8 : plane(x) + 9, :] = row
    for c in range(FIELDS):
        for source in (pad, pad_up, pad_down):
            source[c, pl.ds(plane(8), 8), :] = zero
        pad[c, plane(8) - 1 : plane(8), :] = row
        pad[c, plane(8) + 8 : plane(8) + 9, :] = row
    for total in (level, rising, falling):
        for c in range(6):
            for x in range(9):
                total[c, pl.ds(plane(x), 8), :] = zero
                total[c, plane(x) - 1 : plane(x), :] = row
                total[c, plane(x) + 8 : plane(x) + 9, :] = row

    def body(x, carry):
        base = pl.multiple_of((x + 1) * ROWS + 8, 8)
        here = pl.ds(pl.multiple_of(x * 8, 8), 8)
        first = [pad[c, pl.ds(base, 8), :] for c in range(FIELDS)]
        forces = [zero] * 3
        twists = [zero] * 3
        springs = [zero] * (3 * SLOTS)
        for number, (dx, dy, dz) in enumerate(DIRS):
            span = pl.ds(base + dx * ROWS + dy, 8)
            source = (pad, pad_up, pad_down)[dz]
            total = (level, rising, falling)[dz]
            second = [source[c, span, :] for c in range(FIELDS)]
            ((shear, live, masks),) = pick_shear(lambda c: cells[c, here, :], (number,))
            force, twist, spring = pair(first, second, (dx, dy, dz), shear, live)
            for k in range(3):
                forces[k] = forces[k] + force[k]
                twists[k] = twists[k] + twist[k]
                for s in range(SLOTS):
                    springs[3 * s + k] = jnp.where(masks[s], spring[k], springs[3 * s + k])
                total[k, span, :] = total[k, span, :] - force[k]
                total[3 + k, span, :] = total[3 + k, span, :] + twist[k]
        for k in range(3):
            level[k, pl.ds(base, 8), :] = level[k, pl.ds(base, 8), :] + forces[k]
            level[3 + k, pl.ds(base, 8), :] = level[3 + k, pl.ds(base, 8), :] + twists[k]
        for c in range(3 * SLOTS):
            state[9 + c, here, :] = springs[c]
        return carry

    lax.fori_loop(0, 8, body, 0)


class Sums:
    def __init__(self):
        zero = jnp.zeros((8, 128), jnp.float32)
        self.total = [zero] * 6
        self.springs = [zero] * (3 * SLOTS)

    def own(self, result, masks):
        force, twist, spring = result
        for k in range(3):
            self.total[k] = self.total[k] + force[k]
            self.total[3 + k] = self.total[3 + k] + twist[k]
            for s in range(SLOTS):
                self.springs[3 * s + k] = jnp.where(masks[s], spring[k], self.springs[3 * s + k])

    def partner(self, result):
        force, twist, _ = result
        for k in range(3):
            self.total[k] = self.total[k] - force[k]
            self.total[3 + k] = self.total[3 + k] + twist[k]

    def store(self, level, rows, state, span):
        for c in range(6):
            level[c, rows, :] = level[c, rows, :] + self.total[c]
        if span is not None:
            for c in range(3 * SLOTS):
                state[9 + c, span, :] = state[9 + c, span, :] + self.springs[c]


def turned(values, amount, axis=1):
    return [pltpu.roll(v, amount, axis) for v in values]


def masks_of(cells, span, number):
    return [cells[CODES + s, span, :] == float(number) for s in range(SLOTS)]


def fold(level, rising, falling):
    lane = lanes()
    for x in range(8):
        rows = pl.ds(plane(x), 8)
        for c in range(6):
            up = jnp.where(lane == 0, 0.0, pltpu.roll(rising[c, rows, :], 1, 1))
            down = jnp.where(lane == 127, 0.0, pltpu.roll(falling[c, rows, :], 127, 1))
            level[c, rows, :] = level[c, rows, :] + up + down


def x_ahead(cells, state, pad, level, ahead, xhi, edges, xrow):
    lane = lanes()
    for c in range(FIELDS):
        ahead[c, 7:8, :] = edges[2, c : c + 1, :]
        ahead[c, 16:17, :] = edges[3, c : c + 1, :]
        ahead[c, 8:16, :] = xhi[c]

    sums = Sums()
    first = [pad[c, pl.ds(plane(7), 8), :] for c in range(FIELDS)]
    for n, number in enumerate(ALONG_X):
        dx, dy, dz = DIRS[number]
        second = scaled([ahead[c, pl.ds(8 + dy, 8), :] for c in range(FIELDS)])
        if dz:
            edge = 127 if dz > 0 else 0
            second = [jnp.where(lane == edge, 0.0, v) for v in turned(second, -dz % 128)]
        at = FIELDS + 4 * n
        shear = [xrow[at + k] for k in range(3)]
        result = pair(first, second, DIRS[number], shear, xrow[at + 3] > 0.5)
        sums.own(result, masks_of(cells, pl.ds(56, 8), number))
    sums.store(level, pl.ds(plane(7), 8), state, pl.ds(56, 8))


def x_behind(pad, level, behind, xlo, edges):
    lane = lanes()
    for c in range(FIELDS + 4 * len(ALONG_X)):
        behind[c, 8:16, :] = xlo[c]
    for c in range(FIELDS):
        behind[c, 7:8, :] = edges[0, c : c + 1, :]
        behind[c, 16:17, :] = edges[1, c : c + 1, :]
    for k in range(4):
        behind[FIELDS + 4 + k, 7:8, :] = edges[0, FIELDS + k : FIELDS + k + 1, :]
        behind[FIELDS + 8 + k, 16:17, :] = edges[1, FIELDS + k : FIELDS + k + 1, :]
    sums = Sums()
    second = [pad[c, pl.ds(plane(0), 8), :] for c in range(FIELDS)]
    for n, number in enumerate(ALONG_X):
        dx, dy, dz = DIRS[number]
        span = pl.ds(8 - dy, 8)
        first = scaled([behind[c, span, :] for c in range(FIELDS)])
        first += [behind[FIELDS + 4 * n + k, span, :] for k in range(4)]
        if dz:
            first = turned(first, dz % 128)
        live = first[13] > 0.5
        if dz:
            live = jnp.logical_and(live, lane != (0 if dz > 0 else 127))
        sums.partner(pair(first[:10], second, DIRS[number], first[10:13], live))
    sums.store(level, pl.ds(plane(0), 8), None, None)


def y_high(cells, state, pad, level, yhi, ytop):
    lane = lanes()
    sub = lax.broadcasted_iota(jnp.int32, (8, 128), 0)
    top_fields = scaled([yhi[c] for c in range(FIELDS)])
    sums = Sums()
    mine_rows = pl.ds(plane(0) + 7, 8, stride=ROWS)
    span = pl.ds(7, 8, stride=8)
    mine = [pad[c, mine_rows, :] for c in range(FIELDS)]
    for n, number in enumerate(UP_Y):
        dx, dy, dz = DIRS[number]
        at = FIELDS + 4 * n
        live = ytop[at + 3] > 0.5
        second = top_fields
        if dx:
            second = turned(second, 7, 0)
            live = jnp.logical_and(live, sub != 7)
        if dz:
            second = turned(second, -dz % 128)
            live = jnp.logical_and(live, lane != (127 if dz > 0 else 0))
        shear = [ytop[at + k] for k in range(3)]
        sums.own(pair(mine, second, DIRS[number], shear, live), masks_of(cells, span, number))
    first = turned(top_fields + [yhi[FIELDS + k] for k in range(4)], 1, 0)
    live = jnp.logical_and(first[13] > 0.5, sub != 0)
    sums.partner(pair(first[:10], mine, DIRS[4], first[10:13], live))
    sums.store(level, mine_rows, state, span)


def y_low(cells, state, pad, level, ylo, ylow):
    lane = lanes()
    sub = lax.broadcasted_iota(jnp.int32, (8, 128), 0)
    low_fields = scaled([ylo[c] for c in range(FIELDS)])
    sums = Sums()
    mine_rows = pl.ds(plane(0), 8, stride=ROWS)
    span = pl.ds(0, 8, stride=8)
    mine = [pad[c, mine_rows, :] for c in range(FIELDS)]
    second = turned(low_fields, 7, 0)
    live = jnp.logical_and(ylow[FIELDS + 3] > 0.5, sub != 7)
    shear = [ylow[FIELDS + k] for k in range(3)]
    sums.own(pair(mine, second, DIRS[4], shear, live), masks_of(cells, span, 4))
    for n, number in enumerate(UP_Y):
        dx, dy, dz = DIRS[number]
        first = low_fields + [ylo[FIELDS + 4 * n + k] for k in range(4)]
        if dx:
            first = turned(first, 1, 0)
        if dz:
            first = turned(first, dz % 128)
        live = first[13] > 0.5
        if dx:
            live = jnp.logical_and(live, sub != 0)
        if dz:
            live = jnp.logical_and(live, lane != (0 if dz > 0 else 127))
        sums.partner(pair(first[:10], mine, DIRS[number], first[10:13], live))
    sums.store(level, mine_rows, state, span)


def end_pairs(end, level, state, zside, packs, own_packs):
    lane = lanes()
    theirs, ours = (((2, 5, 7), (6, 8)), ((6, 8), (2, 5, 7)))[end]
    top = 1 - end

    def spread(pack, c, top):
        p = (c % 16) * 8 - top
        return pltpu.roll(pack, -p % 128, 1) if p % 128 else pack

    back = [
        pltpu.roll(packs[2 + end, 0], -j % 128, 1) if j else packs[2 + end, 0]
        for j in range(FIELDS + 4)
    ]
    back = scaled(back[:FIELDS]) + back[FIELDS:]
    beyond = scaled(
        [pltpu.roll(packs[4 + end, 0], (7 - 8 * c + top) % 128, 1) for c in range(FIELDS)]
    )
    for k in range(PACKS):
        straight, left = packs[end, k], pltpu.roll(packs[6 + end, 0], 7 - k, 0)
        for c in range(16 * k, min(FULL, 16 * k + 16)):
            zside[end, c, 8:16, :] = spread(straight, c, top)
            zside[end, c, 0:8, :] = spread(left, c, top)
            if c < FIELDS:
                zside[end, c, 16:24, :] = spread(packs[8 + end, 0], c, top)
    own = [spread(own_packs[end, c // 16], c, end) for c in range(FULL)]
    mine = scaled(own[:FIELDS])
    sums = Sums()
    for number, (shear, live, masks) in zip(ours, pick_shear(lambda c: own[c], ours)):
        dx, dy, dz = DIRS[number]
        second = scaled([zside[end, c, pl.ds(8 + dy, 8), :] for c in range(FIELDS)])
        if dx:
            second = [
                jnp.where(lane < 7, v, jnp.where(lane == 7, b, 0.0))
                for b, v in zip(beyond, turned(second, 127))
            ]
        sums.own(pair(mine, second, DIRS[number], shear, live), masks)
    for number in theirs:
        dx, dy, dz = DIRS[number]
        span = pl.ds(8 - dy, 8)
        first = scaled([zside[end, c, span, :] for c in range(FIELDS)])
        ((shear, live, _),) = pick_shear(lambda c: zside[end, c, span, :], (number,))
        first = first + shear + [jnp.where(live, 1.0, 0.0)]
        if dx:
            first = [jnp.where(lane == 0, b, v) for b, v in zip(back, turned(first, 1))]
        sums.partner(pair(first[:10], mine, DIRS[number], first[10:13], first[13] > 0.5))
    edge = 127 * end
    hold = lane == edge
    for x in range(8):
        turn = (edge - x) % 128

        def put(v):
            return jnp.where(hold, pltpu.roll(v, turn, 1) if turn else v, 0.0)

        rows = pl.ds(plane(x), 8)
        here = slice(x * 8, x * 8 + 8)
        for c in range(6):
            level[c, rows, :] = level[c, rows, :] + put(sums.total[c])
        for c in range(3 * SLOTS):
            state[9 + c, here, :] = state[9 + c, here, :] + put(sums.springs[c])


def moved(cells, level, x):
    rows = pl.ds(plane(x), 8)
    here = slice(x * 8, x * 8 + 8)
    sums = [level[c, rows, :] for c in range(6)]
    radius = cells[9, here, :]
    inverse = 1.0 / radius
    push = STEP * inverse * inverse * inverse
    turn = 0.125 * (inverse * inverse) * (inverse * inverse)
    velocity = [cells[3 + k, here, :] + push * sums[k] for k in range(3)]
    velocity[2] = velocity[2] - STEP
    offset = [cells[k, here, :] + STEP * velocity[k] for k in range(3)]
    rotation = [cells[6 + k, here, :] + turn * sums[3 + k] for k in range(3)]
    return offset, velocity, rotation, radius


def gather_leaving(boxes, planes, cells, state, leaving, level):
    boxes = list(boxes)
    lane = lanes()
    sub = lax.broadcasted_iota(jnp.int32, (8, 128), 0)
    names = leaving[0:1, 0:64]
    names = jnp.concatenate([names, names], axis=1)
    names = jnp.broadcast_to(names, (8, 128))
    height = jnp.where(names >= 0, names % 128, 0)
    column = jnp.where(names >= 0, names // 128, -1)
    starts = [(lax.axis_index(a) * n).astype(jnp.float32) for a, n in zip(AXES, (8, 8, 128))]
    for x in planes:
        here = slice(x * 8, x * 8 + 8)
        offset, velocity, rotation, radius = moved(cells, level, x)
        springs = [state[9 + c, here, :] for c in range(3 * SLOTS)]
        position = [
            offset[0] + (starts[0] + float(x)),
            offset[1] + (starts[1] + sub.astype(jnp.float32)),
            offset[2] + (starts[2] + lane.astype(jnp.float32)),
        ]
        chosen = column == x * 8 + sub
        halves = [jnp.logical_and(chosen, lane < 64), jnp.logical_and(chosen, lane >= 64)]
        for c, v in enumerate(position + velocity + rotation + [radius] + springs):
            values = jnp.take_along_axis(v, height, axis=1)
            boxes[c % 14] = jnp.where(halves[c // 14], values, boxes[c % 14])
    return boxes


def finish(cells, state, leaving, level):
    lane = lanes()
    wide = jnp.broadcast_to(leaving[0:1, 0:64], (8, 64))
    deep = lax.broadcasted_iota(jnp.int32, (8, 64), 0)
    for x in range(8):
        here = slice(x * 8, x * 8 + 8)
        offset, velocity, rotation, _ = moved(cells, level, x)
        left = [
            jnp.max(jnp.where(wide == (x * 8 + deep) * 128 + z, 1.0, 0.0), axis=1, keepdims=True)
            for z in range(2)
        ]
        staying = 1.0 - jnp.where(lane == 0, left[0], jnp.where(lane == 1, left[1], 0.0))
        for c, v in enumerate(offset + velocity + rotation):
            state[c, here, :] = v * staying
        for c in range(9, 27):
            state[c, here, :] = state[c, here, :] * staying


def on_device(offset, velocity, spin, radius, history, contacts, leaving):
    f32 = jnp.float32
    off = offset.reshape(3, 64, 128)
    vel = velocity.reshape(3, 64, 128)
    spn = spin.reshape(3, 64, 128)
    rad = radius.reshape(1, 64, 128)
    hist = history.reshape(3 * SLOTS, 64, 128)
    con = contacts.reshape(SLOTS, 64, 128)
    vmem = pl.BlockSpec(memory_space=pltpu.VMEM)
    hbm = pl.BlockSpec(memory_space=pltpu.HBM)
    halo_shapes = (
        (FIELDS + 4 * len(ALONG_X), 8, 128),
        (FIELDS, 8, 128),
        (FIELDS + 4 * len(UP_Y), 8, 128),
        (FIELDS + 4 * len(DOWN_Y), 8, 128),
        (4, 16, 128),
        (len(PACK_FROM), PACKS, 8, 128),
        (2, PACKS, 8, 128),
    )
    state, arrivals = pl.pallas_call(
        step_kernel,
        out_shape=[pltpu.VMEM((27, 64, 128), f32), pltpu.VMEM((16, 128), f32)],
        in_specs=[hbm] * 7,
        out_specs=[vmem] * 2,
        scratch_shapes=[pltpu.VMEM(s, f32) for s in halo_shapes]
        + [
            pltpu.VMEM((FULL, 64, 128), f32),
            pltpu.VMEM((SLOTS, 64, 128), jnp.int32),
            pltpu.VMEM((1, 64), jnp.int32),
            pltpu.VMEM((FIELDS + 4 * len(ALONG_X), 8, 128), f32),
            pltpu.VMEM((FIELDS + 4 * len(UP_Y), 8, 128), f32),
            pltpu.VMEM((FIELDS + 4 * len(DOWN_Y), 8, 128), f32),
            pltpu.VMEM((4, 16, 128), f32),
            pltpu.VMEM((2, 1, 8, 128), f32),
            pltpu.VMEM((2, 1, 8, 128), f32),
            pltpu.VMEM((16, 128), f32),
            pltpu.VMEM((FIELDS, HEIGHT, 128), f32),
            pltpu.VMEM((FIELDS, HEIGHT, 128), f32),
            pltpu.VMEM((FIELDS, HEIGHT, 128), f32),
            pltpu.VMEM((6, HEIGHT, 128), f32),
            pltpu.VMEM((6, HEIGHT, 128), f32),
            pltpu.VMEM((6, HEIGHT, 128), f32),
            pltpu.VMEM((FIELDS + 4 * len(ALONG_X), ROWS, 128), f32),
            pltpu.VMEM((FIELDS, ROWS, 128), f32),
            pltpu.VMEM((2, FULL, ROWS, 128), f32),
            pltpu.SemaphoreType.DMA((len(SENDERS) + 1,)),
        ],
        compiler_params=pltpu.CompilerParams(
            collective_id=0, has_side_effects=True, vmem_limit_bytes=24 << 20
        ),
        name="step",
    )(*[
        pltpu.with_memory_space_constraint(a, pltpu.HBM)
        for a in (off, vel, spn, rad, hist, con, leaving.reshape(1, 64))
    ])
    moved = jax.ShapeDtypeStruct((3, 64, 128), f32)
    new_off, new_vel, new_spin, new_hist, arrivals = pl.pallas_call(
        write_kernel,
        out_shape=[
            moved, moved, moved,
            jax.ShapeDtypeStruct((3 * SLOTS, 64, 128), f32),
            jax.ShapeDtypeStruct((28, 1, 64), f32),
        ],
        in_specs=[vmem] * 2,
        out_specs=[hbm] * 5,
        scratch_shapes=[pltpu.VMEM((28, 1, 64), f32), pltpu.SemaphoreType.DMA((5,))],
        compiler_params=pltpu.CompilerParams(vmem_limit_bytes=8 << 20),
        name="write",
    )(state, arrivals)
    return (
        new_off.reshape(3, 8, 8, 128),
        new_vel.reshape(3, 8, 8, 128),
        new_spin.reshape(3, 8, 8, 128),
        new_hist.reshape(SLOTS, 3, 8, 8, 128),
        arrivals.reshape(28, 1, 1, 1, 64),
    )


def solution(mesh):
    placed = (
        P(None, "gx", "gy", "gz"),
        P(None, "gx", "gy", "gz"),
        P(None, "gx", "gy", "gz"),
        P("gx", "gy", "gz"),
        P(None, None, "gx", "gy", "gz"),
        P(None, "gx", "gy", "gz"),
        P("gx", "gy", "gz", None),
    )
    return jax.shard_map(
        on_device,
        mesh=mesh,
        in_specs=placed,
        out_specs=(
            P(None, "gx", "gy", "gz"),
            P(None, "gx", "gy", "gz"),
            P(None, "gx", "gy", "gz"),
            P(None, None, "gx", "gy", "gz"),
            P(None, "gx", "gy", "gz", None),
        ),
        check_vma=False,
    )
```

```python
import jax
import jax.numpy as jnp
from jax import lax
from jax.experimental import pallas as pl
from jax.experimental.pallas import tpu as pltpu
from jax.sharding import PartitionSpec as P

MESH = pl.DeviceIdType.MESH
AXES = ("gx", "gy", "gz")
DIRS = (
    (1, 0, 0),
    (0, 1, 0),
    (0, 0, 1),
    (1, 1, 0),
    (1, -1, 0),
    (1, 0, 1),
    (1, 0, -1),
    (0, 1, 1),
    (0, 1, -1),
)
SLOTS = 6
FIELDS = 10
SHEAR = FIELDS
CODES = FIELDS + 3 * SLOTS
FULL = CODES + SLOTS
PACKS = (FULL * 8 + 127) // 128
STEP = 0.05
TINY = 1e-30

ROWS = 24
HEIGHT = 10 * ROWS

PACK_FROM = (
    (0, 0, -1),
    (0, 0, 1),
    (-1, 0, -1),
    (-1, 0, 1),
    (1, 0, -1),
    (1, 0, 1),
    (0, -1, -1),
    (0, -1, 1),
    (0, 1, -1),
    (0, 1, 1),
)
FLAT_FROM = (
    (-1, 0, 0),
    (1, 0, 0),
    (0, -1, 0),
    (0, 1, 0),
    (-1, -1, 0),
    (-1, 1, 0),
    (1, -1, 0),
    (1, 1, 0),
)
SENDERS = FLAT_FROM + PACK_FROM

ALONG_X = (0, 3, 4, 5, 6)
UP_Y = (1, 3, 7, 8)
DOWN_Y = (4,)

SEND_ORDER = (10, 12, 14, 16, 4, 5, 6, 7, 8, 2, 0, 3, 1, 11, 13, 15, 17, 9)


def plane(x):
    return (x + 1) * ROWS + 8


def step_kernel(*refs):
    pl.run_scoped(
        lambda local_sems, send_sems: step_body(*refs, local_sems, send_sems),
        pltpu.SemaphoreType.DMA((7,)),
        pltpu.SemaphoreType.DMA((len(SENDERS) + 1,)),
    )


def step_body(
    off_hbm, vel_hbm, spin_hbm, rad_hbm, hist_hbm, con_hbm, leaving_hbm,
    state, arrivals,
    xlo, xhi, ylo, yhi, edges, packs, own_packs, cells, codes, leaving,
    xrow, ytop, ylow, rows, corner_x, corner_y, outbox, found, pad, pad_up, pad_down, level, rising, falling, behind, ahead, zside,
    recv_sems, local_sems, send_sems,
):
    here = [lax.axis_index(a) for a in AXES]
    size = [lax.axis_size(a) for a in AXES]

    def exists(step):
        ok = None
        for at, n, s in zip(here, size, step):
            if s == 0:
                continue
            test = at + s < n if s > 0 else at + s >= 0
            ok = test if ok is None else jnp.logical_and(ok, test)
        return ok

    def place(step):
        return tuple(at + s for at, s in zip(here, step))

    loads = [
        pltpu.make_async_copy(off_hbm, cells.at[0:3], local_sems.at[0]),
        pltpu.make_async_copy(vel_hbm, cells.at[3:6], local_sems.at[1]),
        pltpu.make_async_copy(spin_hbm, cells.at[6:9], local_sems.at[2]),
        pltpu.make_async_copy(rad_hbm, cells.at[9:10], local_sems.at[3]),
        pltpu.make_async_copy(hist_hbm, cells.at[SHEAR:CODES], local_sems.at[4]),
        pltpu.make_async_copy(con_hbm, codes, local_sems.at[5]),
        pltpu.make_async_copy(leaving_hbm, leaving, local_sems.at[6]),
    ]
    barrier = pltpu.get_barrier_semaphore()
    expected = jnp.int32(0)
    for step in SENDERS[4:] + SENDERS[:4]:
        there = exists(step)
        expected = expected + there.astype(jnp.int32)

        @pl.when(there)
        def _():
            pl.semaphore_signal(barrier, inc=1, device_id=place(step), device_id_type=MESH)

    for load in loads:
        load.start()
    with jax.named_scope("loadwait"):
        for load in loads[:4]:
            load.wait()
    with jax.named_scope("pack"):
        first_pack = fill_fields(cells, xrow, ytop, ylow, rows)
    with jax.named_scope("loadwait2"):
        for load in loads[4:]:
            load.wait()
    with jax.named_scope("pack2"):
        for s in range(SLOTS):
            cells[CODES + s] = codes[s].astype(jnp.float32)
        fill_sends(cells, own_packs, xrow, ytop, ylow, rows, corner_x, corner_y, first_pack)

    targets = [xlo, xhi, ylo, yhi] + [edges.at[k] for k in range(4)]
    sources = [xrow, cells.at[0:FIELDS, 0:8, :], ytop, ylow] + [rows.at[k] for k in range(4)]
    for k, s in enumerate(PACK_FROM):
        end = 0 if s[2] > 0 else 1
        if s[0] + s[1] == 0:
            targets.append(packs.at[k])
            sources.append(own_packs.at[end])
            continue
        targets.append(packs.at[k, 0:1])
        if s[0] + s[1] > 0:
            sources.append(own_packs.at[end, 0:1])
        else:
            sources.append((corner_x if s[0] else corner_y).at[end])

    def copy(k):
        to = tuple(-s for s in SENDERS[k])
        return pltpu.make_async_remote_copy(
            src_ref=sources[k],
            dst_ref=targets[k],
            send_sem=send_sems.at[k],
            recv_sem=recv_sems.at[k],
            device_id=place(to),
            device_id_type=MESH,
        )

    for k, step in enumerate(SENDERS):

        @pl.when(jnp.logical_not(exists(step)))
        def _():
            targets[k][...] = jnp.zeros(targets[k].shape, jnp.float32)

    with jax.named_scope("fill"):
        fill_padded(cells, pad, pad_up, pad_down, level, rising, falling)
    with jax.named_scope("barrier"):
        pl.semaphore_wait(barrier, expected)
    for k in SEND_ORDER:

        @pl.when(exists(tuple(-s for s in SENDERS[k])))
        def _():
            copy(k).start()

    with jax.named_scope("inner"):
        inner_pairs(cells, state, pad, pad_up, pad_down, level, rising, falling)

    def receive(which):
        for k in which:

            @pl.when(exists(SENDERS[k]))
            def _():
                copy(k).wait_recv()

    with jax.named_scope("fold"):
        fold(level, rising, falling)
    with jax.named_scope("gather"):
        who = leaving_cells(leaving)
        gather_inner(found, cells, state, level, who)
    with jax.named_scope("recvz"):
        receive(range(8, 18, 2))
    with jax.named_scope("floor"):
        floor = end_pairs(0, zside, packs, own_packs)
        x, y, z, live = who
        floor.collect(found, x, (y == below()) & (z == 0) & live)
    with jax.named_scope("recvy"):
        receive((2, 3))
    with jax.named_scope("ypairs"):
        y_high(cells, state, pad, level, yhi, ytop, found, who)
        y_low(cells, state, pad, level, ylo, ylow, found, who)
    with jax.named_scope("recvx"):
        receive((0, 1, 4, 5, 6, 7))
    with jax.named_scope("xpairs"):
        x_ahead(cells, state, pad, level, ahead, xhi, edges, xrow, found, who)
        x_behind(pad, level, behind, xlo, edges, found, who)
    with jax.named_scope("outbox"):
        fill_outbox(found, outbox, who)

    last = len(SENDERS)
    fall = pltpu.make_async_remote_copy(
        src_ref=outbox,
        dst_ref=arrivals,
        send_sem=send_sems.at[last],
        recv_sem=recv_sems.at[last],
        device_id=place((0, 0, -1)),
        device_id_type=MESH,
    )

    @pl.when(exists((0, 0, -1)))
    def _():
        fall.start()

    with jax.named_scope("spread"):
        spread_end(0, floor, level, state)
    with jax.named_scope("recvtop"):
        receive((9, 11, 13, 15, 17))
    with jax.named_scope("ceiling"):
        spread_end(1, end_pairs(1, zside, packs, own_packs), level, state)
    with jax.named_scope("final"):
        finish(cells, state, leaving, level)

    for k, step in enumerate(SENDERS):

        @pl.when(exists(tuple(-s for s in step)))
        def _():
            copy(k).wait_send()

    with jax.named_scope("fall"):

        @pl.when(exists((0, 0, 1)))
        def _():
            fall.wait_recv()

    @pl.when(jnp.logical_not(exists((0, 0, 1))))
    def _():
        arrivals[...] = jnp.zeros(arrivals.shape, jnp.float32)

    @pl.when(exists((0, 0, -1)))
    def _():
        fall.wait_send()


def write_kernel(
    state, arrivals, new_off, new_vel, new_spin, new_hist, entered, unpacked, sems
):
    copies = [
        pltpu.make_async_copy(state.at[9:27], new_hist, sems.at[0]),
        pltpu.make_async_copy(state.at[0:3], new_off, sems.at[1]),
        pltpu.make_async_copy(state.at[3:6], new_vel, sems.at[2]),
        pltpu.make_async_copy(state.at[6:9], new_spin, sems.at[3]),
        pltpu.make_async_copy(unpacked, entered, sems.at[4]),
    ]
    for copy in copies[:4]:
        copy.start()
    for c in range(14):
        unpacked[c] = arrivals[c : c + 1, 0:64]
        unpacked[14 + c] = arrivals[c : c + 1, 64:128]
    copies[4].start()
    for copy in copies:
        copy.wait()


def cross(a, b):
    return [
        a[1] * b[2] - a[2] * b[1],
        a[2] * b[0] - a[0] * b[2],
        a[0] * b[1] - a[1] * b[0],
    ]


def dot3(a, b):
    return a[0] * b[0] + a[1] * b[1] + a[2] * b[2]


def pair(first, second, direction, shear, live):
    sep = []
    for k in range(3):
        gap = second[k] - first[k]
        sep.append(gap + float(direction[k]) if direction[k] else gap)
    square = dot3(sep, sep)
    inverse = lax.rsqrt(square)
    normal = [s * inverse for s in sep]
    radii = first[9] + second[9]
    overlap = jnp.maximum(radii - square * inverse, 0.0)
    product = first[9] * second[9] * overlap
    contact = product * lax.rsqrt(jnp.maximum(product * radii, TINY))
    contact = jnp.where(live, contact, 0.0)
    surface = cross([first[6 + k] + second[6 + k] for k in range(3)], normal)
    relative = [second[3 + k] - first[3 + k] - surface[k] for k in range(3)]
    approach = dot3(relative, normal)
    sliding = [relative[k] - approach * normal[k] for k in range(3)]
    repulsion = contact * jnp.maximum(10.0 * overlap - 2.0 * approach, 0.0)
    along = dot3(shear, normal)
    spring = [shear[k] - along * normal[k] + STEP * sliding[k] for k in range(3)]
    pull = [8.0 * spring[k] + 1.5 * sliding[k] for k in range(3)]
    size = contact * contact * dot3(pull, pull)
    factor = jnp.minimum(1.0, 0.4 * repulsion * lax.rsqrt(jnp.maximum(size, 0.0025)))
    scale = factor * contact
    tangent = [scale * pull[k] for k in range(3)]
    force = [tangent[k] - repulsion * normal[k] for k in range(3)]
    return force, cross(normal, tangent), [factor * spring[k] for k in range(3)]


def pick_shear(load, numbers):
    codes = [load(CODES + s) for s in range(SLOTS)]
    found = []
    for number in numbers:
        masks = [code == float(number) for code in codes]
        live = masks[0]
        shear = [jnp.where(masks[0], load(SHEAR + k), 0.0) for k in range(3)]
        for s in range(1, SLOTS):
            live = jnp.logical_or(live, masks[s])
            shear = [jnp.where(masks[s], load(SHEAR + 3 * s + k), shear[k]) for k in range(3)]
        found.append((shear, live, masks))
    return found


def scaled(values):
    return values[:6] + [v * values[9] for v in values[6:9]] + [values[9]]


def lanes():
    return lax.broadcasted_iota(jnp.int32, (8, 128), 1)


def add_packed(cells, channels, low, top):
    lane = lanes()
    for c in channels:
        for x in range(8):
            p = (c % 16) * 8 + x
            value = cells[c, x * 8 : x * 8 + 8, :]
            if p:
                value = pltpu.roll(value, p, 1)
            low = jnp.where(lane == p, value, low)
            top = jnp.where(lane == (p - 1) % 128, value, top)
    return low, top


def fill_fields(cells, xrow, ytop, ylow, rows):
    for c in range(FIELDS):
        xrow[c] = cells[c, 56:64, :]
        ytop[c] = cells[c, pl.ds(7, 8, stride=8), :]
        ylow[c] = cells[c, pl.ds(0, 8, stride=8), :]
        for which, row in enumerate((63, 56, 7, 0)):
            rows[which, c : c + 1, :] = cells[c, row : row + 1, :]
    zero = jnp.zeros((8, 128), jnp.float32)
    return add_packed(cells, range(FIELDS), zero, zero)


def fill_sends(cells, own_packs, xrow, ytop, ylow, rows, corner_x, corner_y, first_pack):
    lane = lanes()
    for target, span, numbers in (
        (xrow, pl.ds(56, 8), ALONG_X),
        (ytop, pl.ds(7, 8, stride=8), UP_Y),
        (ylow, pl.ds(0, 8, stride=8), DOWN_Y),
    ):
        found = pick_shear(lambda c: cells[c, span, :], numbers)
        for n, (shear, live, _) in enumerate(found):
            for k in range(3):
                target[FIELDS + 4 * n + k] = shear[k]
            target[FIELDS + 4 * n + 3] = jnp.where(live, 1.0, 0.0)
    for which, row, at in ((0, 7, 1), (1, 0, 2)):
        for k in range(4):
            rows[which, FIELDS + k : FIELDS + k + 1, :] = xrow[
                FIELDS + 4 * at + k, row : row + 1, :
            ]
    for end, at in ((0, 4), (1, 3)):
        corner = jnp.zeros((8, 128), jnp.float32)
        for j in range(FIELDS + 4):
            value = xrow[j if j < FIELDS else j + 4 * at]
            turn = j + end
            corner = jnp.where(lane == j, pltpu.roll(value, turn, 1) if turn else value, corner)
        corner_x[end, 0] = corner
    for k in range(PACKS):
        if k:
            low = top = jnp.zeros((8, 128), jnp.float32)
        else:
            low, top = first_pack
        channels = range(max(16 * k, FIELDS), min(FULL, 16 * k + 16))
        low, top = add_packed(cells, channels, low, top)
        for end, pack in enumerate((low, top)):
            own_packs[end, k] = pack
            corner_y[end, 0, k : k + 1, :] = pack[7:8, :]
    for end in range(2):
        corner_y[end, 0, PACKS:8, :] = jnp.zeros((8 - PACKS, 128), jnp.float32)


def fill_padded(cells, pad, pad_up, pad_down, level, rising, falling):
    lane = lanes()
    zero = jnp.zeros((8, 128), jnp.float32)
    row = jnp.zeros((1, 128), jnp.float32)
    for x in range(8):
        here = slice(x * 8, x * 8 + 8)
        span = pl.ds(plane(x), 8)
        for c, v in enumerate(scaled([cells[c, here, :] for c in range(FIELDS)])):
            pad[c, span, :] = v
            pad_up[c, span, :] = jnp.where(lane == 127, 0.0, pltpu.roll(v, 127, 1))
            pad_down[c, span, :] = jnp.where(lane == 0, 0.0, pltpu.roll(v, 1, 1))
            pad[c, plane(x) - 1 : plane(x), :] = row
            for source in (pad, pad_up, pad_down):
                source[c, plane(x) + 8 : plane(x) + 9, :] = row
    for c in range(FIELDS):
        for source in (pad, pad_up, pad_down):
            source[c, pl.ds(plane(8), 8), :] = zero
        pad[c, plane(8) - 1 : plane(8), :] = row
        pad[c, plane(8) + 8 : plane(8) + 9, :] = row
    for total in (level, rising, falling):
        for c in range(6):
            for x in range(9):
                total[c, pl.ds(plane(x), 8), :] = zero
                total[c, plane(x) - 1 : plane(x), :] = row
                total[c, plane(x) + 8 : plane(x) + 9, :] = row


def inner_pairs(cells, state, pad, pad_up, pad_down, level, rising, falling):
    zero = jnp.zeros((8, 128), jnp.float32)

    def body(x, carry):
        base = pl.multiple_of((x + 1) * ROWS + 8, 8)
        here = pl.ds(pl.multiple_of(x * 8, 8), 8)
        first = [pad[c, pl.ds(base, 8), :] for c in range(FIELDS)]
        forces = [zero] * 3
        twists = [zero] * 3
        springs = [zero] * (3 * SLOTS)
        for number, (dx, dy, dz) in enumerate(DIRS):
            span = pl.ds(base + dx * ROWS + dy, 8)
            source = (pad, pad_up, pad_down)[dz]
            total = (level, rising, falling)[dz]
            second = [source[c, span, :] for c in range(FIELDS)]
            ((shear, live, masks),) = pick_shear(lambda c: cells[c, here, :], (number,))
            force, twist, spring = pair(first, second, (dx, dy, dz), shear, live)
            for k in range(3):
                forces[k] = forces[k] + force[k]
                twists[k] = twists[k] + twist[k]
                for s in range(SLOTS):
                    springs[3 * s + k] = jnp.where(masks[s], spring[k], springs[3 * s + k])
                total[k, span, :] = total[k, span, :] - force[k]
                total[3 + k, span, :] = total[3 + k, span, :] + twist[k]
        for k in range(3):
            level[k, pl.ds(base, 8), :] = level[k, pl.ds(base, 8), :] + forces[k]
            level[3 + k, pl.ds(base, 8), :] = level[3 + k, pl.ds(base, 8), :] + twists[k]
        for c in range(3 * SLOTS):
            state[9 + c, here, :] = springs[c]
        return carry

    lax.fori_loop(0, 8, body, 0)


class Sums:
    def __init__(self):
        zero = jnp.zeros((8, 128), jnp.float32)
        self.total = [zero] * 6
        self.springs = [zero] * (3 * SLOTS)

    def own(self, result, masks):
        force, twist, spring = result
        for k in range(3):
            self.total[k] = self.total[k] + force[k]
            self.total[3 + k] = self.total[3 + k] + twist[k]
            for s in range(SLOTS):
                self.springs[3 * s + k] = jnp.where(masks[s], spring[k], self.springs[3 * s + k])

    def partner(self, result):
        force, twist, _ = result
        for k in range(3):
            self.total[k] = self.total[k] - force[k]
            self.total[3 + k] = self.total[3 + k] + twist[k]

    def collect(self, found, index, mask):
        for c, v in enumerate(self.total + self.springs):
            value = jnp.take_along_axis(v, index, axis=1)
            found[FIELDS + c] = found[FIELDS + c] + jnp.where(mask, value, 0.0)

    def store(self, level, rows, state, span):
        for c in range(6):
            level[c, rows, :] = level[c, rows, :] + self.total[c]
        if span is not None:
            for c in range(3 * SLOTS):
                state[9 + c, span, :] = state[9 + c, span, :] + self.springs[c]


def turned(values, amount, axis=1):
    return [pltpu.roll(v, amount, axis) for v in values]


def masks_of(cells, span, number):
    return [cells[CODES + s, span, :] == float(number) for s in range(SLOTS)]


def fold(level, rising, falling):
    lane = lanes()
    for x in range(8):
        rows = pl.ds(plane(x), 8)
        for c in range(6):
            up = jnp.where(lane == 0, 0.0, pltpu.roll(rising[c, rows, :], 1, 1))
            down = jnp.where(lane == 127, 0.0, pltpu.roll(falling[c, rows, :], 127, 1))
            level[c, rows, :] = level[c, rows, :] + up + down


def x_ahead(cells, state, pad, level, ahead, xhi, edges, xrow, found, who):
    lane = lanes()
    for c in range(FIELDS):
        ahead[c, 7:8, :] = edges[2, c : c + 1, :]
        ahead[c, 16:17, :] = edges[3, c : c + 1, :]
        ahead[c, 8:16, :] = xhi[c]

    sums = Sums()
    first = [pad[c, pl.ds(plane(7), 8), :] for c in range(FIELDS)]
    for n, number in enumerate(ALONG_X):
        dx, dy, dz = DIRS[number]
        second = scaled([ahead[c, pl.ds(8 + dy, 8), :] for c in range(FIELDS)])
        if dz:
            edge = 127 if dz > 0 else 0
            second = [jnp.where(lane == edge, 0.0, v) for v in turned(second, -dz % 128)]
        at = FIELDS + 4 * n
        shear = [xrow[at + k] for k in range(3)]
        result = pair(first, second, DIRS[number], shear, xrow[at + 3] > 0.5)
        sums.own(result, masks_of(cells, pl.ds(56, 8), number))
    sums.store(level, pl.ds(plane(7), 8), state, pl.ds(56, 8))
    x, y, z, live = who
    sums.collect(found, z, ((y == below()) & (x == 7)) & live)


def x_behind(pad, level, behind, xlo, edges, found, who):
    lane = lanes()
    for c in range(FIELDS + 4 * len(ALONG_X)):
        behind[c, 8:16, :] = xlo[c]
    for c in range(FIELDS):
        behind[c, 7:8, :] = edges[0, c : c + 1, :]
        behind[c, 16:17, :] = edges[1, c : c + 1, :]
    for k in range(4):
        behind[FIELDS + 4 + k, 7:8, :] = edges[0, FIELDS + k : FIELDS + k + 1, :]
        behind[FIELDS + 8 + k, 16:17, :] = edges[1, FIELDS + k : FIELDS + k + 1, :]
    sums = Sums()
    second = [pad[c, pl.ds(plane(0), 8), :] for c in range(FIELDS)]
    for n, number in enumerate(ALONG_X):
        dx, dy, dz = DIRS[number]
        span = pl.ds(8 - dy, 8)
        first = scaled([behind[c, span, :] for c in range(FIELDS)])
        first += [behind[FIELDS + 4 * n + k, span, :] for k in range(4)]
        if dz:
            first = turned(first, dz % 128)
        live = first[13] > 0.5
        if dz:
            live = jnp.logical_and(live, lane != (0 if dz > 0 else 127))
        sums.partner(pair(first[:10], second, DIRS[number], first[10:13], live))
    sums.store(level, pl.ds(plane(0), 8), None, None)
    x, y, z, live = who
    sums.collect(found, z, ((y == below()) & (x == 0)) & live)


def y_high(cells, state, pad, level, yhi, ytop, found, who):
    lane = lanes()
    sub = lax.broadcasted_iota(jnp.int32, (8, 128), 0)
    top_fields = scaled([yhi[c] for c in range(FIELDS)])
    sums = Sums()
    mine_rows = pl.ds(plane(0) + 7, 8, stride=ROWS)
    span = pl.ds(7, 8, stride=8)
    mine = [pad[c, mine_rows, :] for c in range(FIELDS)]
    for n, number in enumerate(UP_Y):
        dx, dy, dz = DIRS[number]
        at = FIELDS + 4 * n
        live = ytop[at + 3] > 0.5
        second = top_fields
        if dx:
            second = turned(second, 7, 0)
            live = jnp.logical_and(live, sub != 7)
        if dz:
            second = turned(second, -dz % 128)
            live = jnp.logical_and(live, lane != (127 if dz > 0 else 0))
        shear = [ytop[at + k] for k in range(3)]
        sums.own(pair(mine, second, DIRS[number], shear, live), masks_of(cells, span, number))
    first = turned(top_fields + [yhi[FIELDS + k] for k in range(4)], 1, 0)
    live = jnp.logical_and(first[13] > 0.5, sub != 0)
    sums.partner(pair(first[:10], mine, DIRS[4], first[10:13], live))
    sums.store(level, mine_rows, state, span)
    x, y, z, live = who
    sums.collect(found, z, ((x == below()) & (y == 7)) & live)


def y_low(cells, state, pad, level, ylo, ylow, found, who):
    lane = lanes()
    sub = lax.broadcasted_iota(jnp.int32, (8, 128), 0)
    low_fields = scaled([ylo[c] for c in range(FIELDS)])
    sums = Sums()
    mine_rows = pl.ds(plane(0), 8, stride=ROWS)
    span = pl.ds(0, 8, stride=8)
    mine = [pad[c, mine_rows, :] for c in range(FIELDS)]
    second = turned(low_fields, 7, 0)
    live = jnp.logical_and(ylow[FIELDS + 3] > 0.5, sub != 7)
    shear = [ylow[FIELDS + k] for k in range(3)]
    sums.own(pair(mine, second, DIRS[4], shear, live), masks_of(cells, span, 4))
    for n, number in enumerate(UP_Y):
        dx, dy, dz = DIRS[number]
        first = low_fields + [ylo[FIELDS + 4 * n + k] for k in range(4)]
        if dx:
            first = turned(first, 1, 0)
        if dz:
            first = turned(first, dz % 128)
        live = first[13] > 0.5
        if dx:
            live = jnp.logical_and(live, sub != 0)
        if dz:
            live = jnp.logical_and(live, lane != (0 if dz > 0 else 127))
        sums.partner(pair(first[:10], mine, DIRS[number], first[10:13], live))
    sums.store(level, mine_rows, state, span)
    x, y, z, live = who
    sums.collect(found, z, ((x == below()) & (y == 0)) & live)


def end_pairs(end, zside, packs, own_packs):
    lane = lanes()
    theirs, ours = (((2, 5, 7), (6, 8)), ((6, 8), (2, 5, 7)))[end]
    top = 1 - end

    def spread(pack, c, top):
        p = (c % 16) * 8 - top
        return pltpu.roll(pack, -p % 128, 1) if p % 128 else pack

    back = [
        pltpu.roll(packs[2 + end, 0], -j % 128, 1) if j else packs[2 + end, 0]
        for j in range(FIELDS + 4)
    ]
    back = scaled(back[:FIELDS]) + back[FIELDS:]
    beyond = scaled(
        [pltpu.roll(packs[4 + end, 0], (7 - 8 * c + top) % 128, 1) for c in range(FIELDS)]
    )
    for k in range(PACKS):
        straight, left = packs[end, k], pltpu.roll(packs[6 + end, 0], 7 - k, 0)
        for c in range(16 * k, min(FULL, 16 * k + 16)):
            zside[end, c, 8:16, :] = spread(straight, c, top)
            zside[end, c, 0:8, :] = spread(left, c, top)
            if c < FIELDS:
                zside[end, c, 16:24, :] = spread(packs[8 + end, 0], c, top)
    own = [spread(own_packs[end, c // 16], c, end) for c in range(FULL)]
    mine = scaled(own[:FIELDS])
    sums = Sums()
    for number, (shear, live, masks) in zip(ours, pick_shear(lambda c: own[c], ours)):
        dx, dy, dz = DIRS[number]
        second = scaled([zside[end, c, pl.ds(8 + dy, 8), :] for c in range(FIELDS)])
        if dx:
            second = [
                jnp.where(lane < 7, v, jnp.where(lane == 7, b, 0.0))
                for b, v in zip(beyond, turned(second, 127))
            ]
        sums.own(pair(mine, second, DIRS[number], shear, live), masks)
    for number in theirs:
        dx, dy, dz = DIRS[number]
        span = pl.ds(8 - dy, 8)
        first = scaled([zside[end, c, span, :] for c in range(FIELDS)])
        ((shear, live, _),) = pick_shear(lambda c: zside[end, c, span, :], (number,))
        first = first + shear + [jnp.where(live, 1.0, 0.0)]
        if dx:
            first = [jnp.where(lane == 0, b, v) for b, v in zip(back, turned(first, 1))]
        sums.partner(pair(first[:10], mine, DIRS[number], first[10:13], first[13] > 0.5))
    return sums


def spread_end(end, sums, level, state):
    lane = lanes()
    edge = 127 * end
    hold = lane == edge
    for x in range(8):
        turn = (edge - x) % 128

        def put(v):
            return jnp.where(hold, pltpu.roll(v, turn, 1) if turn else v, 0.0)

        rows = pl.ds(plane(x), 8)
        here = slice(x * 8, x * 8 + 8)
        for c in range(6):
            level[c, rows, :] = level[c, rows, :] + put(sums.total[c])
        for c in range(3 * SLOTS):
            state[9 + c, here, :] = state[9 + c, here, :] + put(sums.springs[c])


def moved(cells, level, x):
    rows = pl.ds(plane(x), 8)
    here = slice(x * 8, x * 8 + 8)
    sums = [level[c, rows, :] for c in range(6)]
    radius = cells[9, here, :]
    inverse = 1.0 / radius
    push = STEP * inverse * inverse * inverse
    turn = 0.125 * (inverse * inverse) * (inverse * inverse)
    velocity = [cells[3 + k, here, :] + push * sums[k] for k in range(3)]
    velocity[2] = velocity[2] - STEP
    offset = [cells[k, here, :] + STEP * velocity[k] for k in range(3)]
    rotation = [cells[6 + k, here, :] + turn * sums[3 + k] for k in range(3)]
    return offset, velocity, rotation, radius


def below():
    return lax.broadcasted_iota(jnp.int32, (8, 128), 0)


def leaving_cells(leaving):
    names = leaving[0:1, 0:64]
    names = jnp.broadcast_to(jnp.concatenate([names, names], axis=1), (8, 128))
    live = names >= 0
    names = jnp.where(live, names, 0)
    return names // 1024, names // 128 % 8, names % 128, live


def gather_inner(found, cells, state, level, who):
    x_of, y_of, z_of, live = who
    row = (y_of == below()) & live
    zero = jnp.zeros((8, 128), jnp.float32)
    values = [zero] * (FIELDS + 6 + 3 * SLOTS)
    for x in range(8):
        here = slice(x * 8, x * 8 + 8)
        chosen = row & (x_of == x)
        parts = [cells[c, here, :] for c in range(FIELDS)]
        parts += [level[c, pl.ds(plane(x), 8), :] for c in range(6)]
        parts += [state[9 + c, here, :] for c in range(3 * SLOTS)]
        for c, v in enumerate(parts):
            values[c] = jnp.where(chosen, jnp.take_along_axis(v, z_of, axis=1), values[c])
    for c, v in enumerate(values):
        found[c] = v


def fill_outbox(found, outbox, who):
    lane = lanes()[0:1]
    rows = [
        jnp.sum(found[c], axis=0, keepdims=True) for c in range(FIELDS + 6 + 3 * SLOTS)
    ]
    live = who[3][0:1]
    cell = [w[0:1].astype(jnp.float32) for w in who[:3]]
    starts = [(lax.axis_index(a) * n).astype(jnp.float32) for a, n in zip(AXES, (8, 8, 128))]
    radius = rows[9]
    inverse = 1.0 / jnp.where(live, radius, 1.0)
    push = STEP * inverse * inverse * inverse
    turn = 0.125 * (inverse * inverse) * (inverse * inverse)
    velocity = [rows[3 + k] + push * rows[10 + k] for k in range(3)]
    velocity[2] = jnp.where(live, velocity[2] - STEP, 0.0)
    position = [
        jnp.where(live, rows[k] + STEP * velocity[k] + (starts[k] + cell[k]), 0.0)
        for k in range(3)
    ]
    rotation = [rows[6 + k] + turn * rows[13 + k] for k in range(3)]
    values = position + velocity + rotation + [radius] + rows[16:]
    for c in range(14):
        outbox[c : c + 1, :] = jnp.where(lane < 64, values[c], values[14 + c])


def finish(cells, state, leaving, level):
    lane = lanes()
    wide = jnp.broadcast_to(leaving[0:1, 0:64], (8, 64))
    deep = lax.broadcasted_iota(jnp.int32, (8, 64), 0)
    for x in range(8):
        here = slice(x * 8, x * 8 + 8)
        offset, velocity, rotation, _ = moved(cells, level, x)
        left = [
            jnp.max(jnp.where(wide == (x * 8 + deep) * 128 + z, 1.0, 0.0), axis=1, keepdims=True)
            for z in range(2)
        ]
        staying = 1.0 - jnp.where(lane == 0, left[0], jnp.where(lane == 1, left[1], 0.0))
        for c, v in enumerate(offset + velocity + rotation):
            state[c, here, :] = v * staying
        for c in range(9, 27):
            state[c, here, :] = state[c, here, :] * staying


def on_device(offset, velocity, spin, radius, history, contacts, leaving):
    f32 = jnp.float32
    off = offset.reshape(3, 64, 128)
    vel = velocity.reshape(3, 64, 128)
    spn = spin.reshape(3, 64, 128)
    rad = radius.reshape(1, 64, 128)
    hist = history.reshape(3 * SLOTS, 64, 128)
    con = contacts.reshape(SLOTS, 64, 128)
    vmem = pl.BlockSpec(memory_space=pltpu.VMEM)
    hbm = pl.BlockSpec(memory_space=pltpu.HBM)
    halo_shapes = (
        (FIELDS + 4 * len(ALONG_X), 8, 128),
        (FIELDS, 8, 128),
        (FIELDS + 4 * len(UP_Y), 8, 128),
        (FIELDS + 4 * len(DOWN_Y), 8, 128),
        (4, 16, 128),
        (len(PACK_FROM), PACKS, 8, 128),
        (2, PACKS, 8, 128),
    )
    state, arrivals = pl.pallas_call(
        step_kernel,
        out_shape=[pltpu.VMEM((27, 64, 128), f32), pltpu.VMEM((16, 128), f32)],
        in_specs=[hbm] * 7,
        out_specs=[vmem] * 2,
        scratch_shapes=[pltpu.VMEM(s, f32) for s in halo_shapes]
        + [
            pltpu.VMEM((FULL, 64, 128), f32),
            pltpu.VMEM((SLOTS, 64, 128), jnp.int32),
            pltpu.VMEM((1, 64), jnp.int32),
            pltpu.VMEM((FIELDS + 4 * len(ALONG_X), 8, 128), f32),
            pltpu.VMEM((FIELDS + 4 * len(UP_Y), 8, 128), f32),
            pltpu.VMEM((FIELDS + 4 * len(DOWN_Y), 8, 128), f32),
            pltpu.VMEM((4, 16, 128), f32),
            pltpu.VMEM((2, 1, 8, 128), f32),
            pltpu.VMEM((2, 1, 8, 128), f32),
            pltpu.VMEM((16, 128), f32),
            pltpu.VMEM((FIELDS + 6 + 3 * SLOTS, 8, 128), f32),
            pltpu.VMEM((FIELDS, HEIGHT, 128), f32),
            pltpu.VMEM((FIELDS, HEIGHT, 128), f32),
            pltpu.VMEM((FIELDS, HEIGHT, 128), f32),
            pltpu.VMEM((6, HEIGHT, 128), f32),
            pltpu.VMEM((6, HEIGHT, 128), f32),
            pltpu.VMEM((6, HEIGHT, 128), f32),
            pltpu.VMEM((FIELDS + 4 * len(ALONG_X), ROWS, 128), f32),
            pltpu.VMEM((FIELDS, ROWS, 128), f32),
            pltpu.VMEM((2, FULL, ROWS, 128), f32),
            pltpu.SemaphoreType.DMA((len(SENDERS) + 1,)),
        ],
        compiler_params=pltpu.CompilerParams(
            collective_id=0, has_side_effects=True, vmem_limit_bytes=24 << 20
        ),
        name="step",
    )(*[
        pltpu.with_memory_space_constraint(a, pltpu.HBM)
        for a in (off, vel, spn, rad, hist, con, leaving.reshape(1, 64))
    ])
    moved = jax.ShapeDtypeStruct((3, 64, 128), f32)
    new_off, new_vel, new_spin, new_hist, arrivals = pl.pallas_call(
        write_kernel,
        out_shape=[
            moved, moved, moved,
            jax.ShapeDtypeStruct((3 * SLOTS, 64, 128), f32),
            jax.ShapeDtypeStruct((28, 1, 64), f32),
        ],
        in_specs=[vmem] * 2,
        out_specs=[hbm] * 5,
        scratch_shapes=[pltpu.VMEM((28, 1, 64), f32), pltpu.SemaphoreType.DMA((5,))],
        compiler_params=pltpu.CompilerParams(vmem_limit_bytes=8 << 20),
        name="write",
    )(state, arrivals)
    return (
        new_off.reshape(3, 8, 8, 128),
        new_vel.reshape(3, 8, 8, 128),
        new_spin.reshape(3, 8, 8, 128),
        new_hist.reshape(SLOTS, 3, 8, 8, 128),
        arrivals.reshape(28, 1, 1, 1, 64),
    )


def solution(mesh):
    placed = (
        P(None, "gx", "gy", "gz"),
        P(None, "gx", "gy", "gz"),
        P(None, "gx", "gy", "gz"),
        P("gx", "gy", "gz"),
        P(None, None, "gx", "gy", "gz"),
        P(None, "gx", "gy", "gz"),
        P("gx", "gy", "gz", None),
    )
    return jax.shard_map(
        on_device,
        mesh=mesh,
        in_specs=placed,
        out_specs=(
            P(None, "gx", "gy", "gz"),
            P(None, "gx", "gy", "gz"),
            P(None, "gx", "gy", "gz"),
            P(None, None, "gx", "gy", "gz"),
            P(None, "gx", "gy", "gz", None),
        ),
        check_vma=False,
    )
```

```python
import jax
import jax.numpy as jnp
from jax import lax
from jax.experimental import pallas as pl
from jax.experimental.pallas import tpu as pltpu
from jax.sharding import PartitionSpec as P

MESH = pl.DeviceIdType.MESH
AXES = ("gx", "gy", "gz")
DIRS = (
    (1, 0, 0),
    (0, 1, 0),
    (0, 0, 1),
    (1, 1, 0),
    (1, -1, 0),
    (1, 0, 1),
    (1, 0, -1),
    (0, 1, 1),
    (0, 1, -1),
)
SLOTS = 6
FIELDS = 10
SHEAR = FIELDS
CODES = FIELDS + 3 * SLOTS
FULL = CODES + SLOTS
PACKS = (FULL * 8 + 127) // 128
STEP = 0.05
TINY = 1e-30

ROWS = 24
HEIGHT = 10 * ROWS

PACK_FROM = (
    (0, 0, -1),
    (0, 0, 1),
    (-1, 0, -1),
    (-1, 0, 1),
    (1, 0, -1),
    (1, 0, 1),
    (0, -1, -1),
    (0, -1, 1),
    (0, 1, -1),
    (0, 1, 1),
)
FLAT_FROM = (
    (-1, 0, 0),
    (1, 0, 0),
    (0, -1, 0),
    (0, 1, 0),
    (-1, -1, 0),
    (-1, 1, 0),
    (1, -1, 0),
    (1, 1, 0),
)
SENDERS = FLAT_FROM + PACK_FROM

ALONG_X = (0, 3, 4, 5, 6)
UP_Y = (1, 3, 7, 8)
DOWN_Y = (4,)

SEND_ORDER = (10, 12, 14, 16, 4, 5, 6, 7, 8, 2, 0, 3, 1, 11, 13, 15, 17, 9)


def plane(x):
    return (x + 1) * ROWS + 8


def step_kernel(*refs):
    pl.run_scoped(
        lambda local_sems, send_sems: step_body(*refs, local_sems, send_sems),
        pltpu.SemaphoreType.DMA((7,)),
        pltpu.SemaphoreType.DMA((len(SENDERS) + 1,)),
    )


def step_body(
    off_hbm, vel_hbm, spin_hbm, rad_hbm, hist_hbm, con_hbm, leaving_hbm,
    state, arrivals,
    xlo, xhi, ylo, yhi, edges, packs, own_packs, cells, codes, leaving,
    xrow, ytop, ylow, rows, corner_x, corner_y, outbox, found, marks, pad, pad_up, pad_down, level, rising, falling, behind, ahead, zside,
    recv_sems, local_sems, send_sems,
):
    here = [lax.axis_index(a) for a in AXES]
    size = [lax.axis_size(a) for a in AXES]

    def exists(step):
        ok = None
        for at, n, s in zip(here, size, step):
            if s == 0:
                continue
            test = at + s < n if s > 0 else at + s >= 0
            ok = test if ok is None else jnp.logical_and(ok, test)
        return ok

    def place(step):
        return tuple(at + s for at, s in zip(here, step))

    loads = [
        pltpu.make_async_copy(off_hbm, cells.at[0:3], local_sems.at[0]),
        pltpu.make_async_copy(vel_hbm, cells.at[3:6], local_sems.at[1]),
        pltpu.make_async_copy(spin_hbm, cells.at[6:9], local_sems.at[2]),
        pltpu.make_async_copy(rad_hbm, cells.at[9:10], local_sems.at[3]),
        pltpu.make_async_copy(hist_hbm, cells.at[SHEAR:CODES], local_sems.at[4]),
        pltpu.make_async_copy(con_hbm, codes, local_sems.at[5]),
        pltpu.make_async_copy(leaving_hbm, leaving, local_sems.at[6]),
    ]
    barrier = pltpu.get_barrier_semaphore()
    expected = jnp.int32(0)
    for step in SENDERS[4:] + SENDERS[:4]:
        there = exists(step)
        expected = expected + there.astype(jnp.int32)

        @pl.when(there)
        def _():
            pl.semaphore_signal(barrier, inc=1, device_id=place(step), device_id_type=MESH)

    for load in loads:
        load.start()
    with jax.named_scope("loadwait"):
        for load in loads[:4]:
            load.wait()
    with jax.named_scope("pack"):
        first_pack = fill_fields(cells, xrow, ytop, ylow, rows)
    with jax.named_scope("loadwait2"):
        for load in loads[4:]:
            load.wait()
    with jax.named_scope("pack2"):
        for s in range(SLOTS):
            cells[CODES + s] = codes[s].astype(jnp.float32)
        fill_sends(cells, own_packs, xrow, ytop, ylow, rows, corner_x, corner_y, first_pack)

    targets = [xlo, xhi, ylo, yhi] + [edges.at[k] for k in range(4)]
    sources = [xrow, cells.at[0:FIELDS, 0:8, :], ytop, ylow] + [rows.at[k] for k in range(4)]
    for k, s in enumerate(PACK_FROM):
        end = 0 if s[2] > 0 else 1
        if s[0] + s[1] == 0:
            targets.append(packs.at[k])
            sources.append(own_packs.at[end])
            continue
        targets.append(packs.at[k, 0:1])
        if s[0] + s[1] > 0:
            sources.append(own_packs.at[end, 0:1])
        else:
            sources.append((corner_x if s[0] else corner_y).at[end])

    def copy(k):
        to = tuple(-s for s in SENDERS[k])
        return pltpu.make_async_remote_copy(
            src_ref=sources[k],
            dst_ref=targets[k],
            send_sem=send_sems.at[k],
            recv_sem=recv_sems.at[k],
            device_id=place(to),
            device_id_type=MESH,
        )

    for k, step in enumerate(SENDERS):

        @pl.when(jnp.logical_not(exists(step)))
        def _():
            targets[k][...] = jnp.zeros(targets[k].shape, jnp.float32)

    with jax.named_scope("fill"):
        fill_padded(cells, pad, pad_up, pad_down, level, rising, falling)
        gather_fields(found, cells, leaving, marks)
    with jax.named_scope("barrier"):
        pl.semaphore_wait(barrier, expected)
    for k in SEND_ORDER:

        @pl.when(exists(tuple(-s for s in SENDERS[k])))
        def _():
            copy(k).start()

    with jax.named_scope("inner"):
        inner_pairs(cells, state, pad, pad_up, pad_down, level, rising, falling, found, marks)

    def receive(which):
        for k in which:

            @pl.when(exists(SENDERS[k]))
            def _():
                copy(k).wait_recv()

    with jax.named_scope("fold"):
        fold(level, rising, falling, found, marks)
        who = leaving_cells(leaving)
    with jax.named_scope("recvz"):
        receive(range(8, 18, 2))
    with jax.named_scope("floor"):
        floor = end_pairs(0, zside, packs, own_packs)
        x, y, z, live = who
        floor.collect(found, x, (y == below()) & (z == 0) & live)
    with jax.named_scope("recvy"):
        receive((2, 3))
    with jax.named_scope("ypairs"):
        y_high(cells, state, pad, level, yhi, ytop, found, who)
        y_low(cells, state, pad, level, ylo, ylow, found, who)
    with jax.named_scope("recvx"):
        receive((0, 1, 4, 5, 6, 7))
    with jax.named_scope("xpairs"):
        x_ahead(cells, state, pad, level, ahead, xhi, edges, xrow, found, who)
        x_behind(pad, level, behind, xlo, edges, found, who)
    with jax.named_scope("outbox"):
        fill_outbox(found, outbox, who)

    last = len(SENDERS)
    fall = pltpu.make_async_remote_copy(
        src_ref=outbox,
        dst_ref=arrivals,
        send_sem=send_sems.at[last],
        recv_sem=recv_sems.at[last],
        device_id=place((0, 0, -1)),
        device_id_type=MESH,
    )

    @pl.when(exists((0, 0, -1)))
    def _():
        fall.start()

    with jax.named_scope("spread"):
        spread_end(0, floor, level, state)
    with jax.named_scope("recvtop"):
        receive((9, 11, 13, 15, 17))
    with jax.named_scope("ceiling"):
        spread_end(1, end_pairs(1, zside, packs, own_packs), level, state)
    with jax.named_scope("final"):
        finish(cells, state, leaving, level)

    for k, step in enumerate(SENDERS):

        @pl.when(exists(tuple(-s for s in step)))
        def _():
            copy(k).wait_send()

    with jax.named_scope("fall"):

        @pl.when(exists((0, 0, 1)))
        def _():
            fall.wait_recv()

    @pl.when(jnp.logical_not(exists((0, 0, 1))))
    def _():
        arrivals[...] = jnp.zeros(arrivals.shape, jnp.float32)

    @pl.when(exists((0, 0, -1)))
    def _():
        fall.wait_send()


def write_kernel(
    state, arrivals, new_off, new_vel, new_spin, new_hist, entered, unpacked, sems
):
    copies = [
        pltpu.make_async_copy(state.at[9:27], new_hist, sems.at[0]),
        pltpu.make_async_copy(state.at[0:3], new_off, sems.at[1]),
        pltpu.make_async_copy(state.at[3:6], new_vel, sems.at[2]),
        pltpu.make_async_copy(state.at[6:9], new_spin, sems.at[3]),
        pltpu.make_async_copy(unpacked, entered, sems.at[4]),
    ]
    for copy in copies[:4]:
        copy.start()
    for c in range(14):
        unpacked[c] = arrivals[c : c + 1, 0:64]
        unpacked[14 + c] = arrivals[c : c + 1, 64:128]
    copies[4].start()
    for copy in copies:
        copy.wait()


def cross(a, b):
    return [
        a[1] * b[2] - a[2] * b[1],
        a[2] * b[0] - a[0] * b[2],
        a[0] * b[1] - a[1] * b[0],
    ]


def dot3(a, b):
    return a[0] * b[0] + a[1] * b[1] + a[2] * b[2]


def pair(first, second, direction, shear, live):
    sep = []
    for k in range(3):
        gap = second[k] - first[k]
        sep.append(gap + float(direction[k]) if direction[k] else gap)
    square = dot3(sep, sep)
    inverse = lax.rsqrt(square)
    normal = [s * inverse for s in sep]
    radii = first[9] + second[9]
    overlap = jnp.maximum(radii - square * inverse, 0.0)
    product = first[9] * second[9] * overlap
    contact = product * lax.rsqrt(jnp.maximum(product * radii, TINY))
    contact = jnp.where(live, contact, 0.0)
    surface = cross([first[6 + k] + second[6 + k] for k in range(3)], normal)
    relative = [second[3 + k] - first[3 + k] - surface[k] for k in range(3)]
    approach = dot3(relative, normal)
    sliding = [relative[k] - approach * normal[k] for k in range(3)]
    repulsion = contact * jnp.maximum(10.0 * overlap - 2.0 * approach, 0.0)
    along = dot3(shear, normal)
    spring = [shear[k] - along * normal[k] + STEP * sliding[k] for k in range(3)]
    pull = [8.0 * spring[k] + 1.5 * sliding[k] for k in range(3)]
    size = contact * contact * dot3(pull, pull)
    factor = jnp.minimum(1.0, 0.4 * repulsion * lax.rsqrt(jnp.maximum(size, 0.0025)))
    scale = factor * contact
    tangent = [scale * pull[k] for k in range(3)]
    force = [tangent[k] - repulsion * normal[k] for k in range(3)]
    return force, cross(normal, tangent), [factor * spring[k] for k in range(3)]


def pick_shear(load, numbers):
    codes = [load(CODES + s) for s in range(SLOTS)]
    found = []
    for number in numbers:
        masks = [code == float(number) for code in codes]
        live = masks[0]
        shear = [jnp.where(masks[0], load(SHEAR + k), 0.0) for k in range(3)]
        for s in range(1, SLOTS):
            live = jnp.logical_or(live, masks[s])
            shear = [jnp.where(masks[s], load(SHEAR + 3 * s + k), shear[k]) for k in range(3)]
        found.append((shear, live, masks))
    return found


def scaled(values):
    return values[:6] + [v * values[9] for v in values[6:9]] + [values[9]]


def lanes():
    return lax.broadcasted_iota(jnp.int32, (8, 128), 1)


def add_packed(cells, channels, low, top):
    lane = lanes()
    for c in channels:
        for x in range(8):
            p = (c % 16) * 8 + x
            value = cells[c, x * 8 : x * 8 + 8, :]
            if p:
                value = pltpu.roll(value, p, 1)
            low = jnp.where(lane == p, value, low)
            top = jnp.where(lane == (p - 1) % 128, value, top)
    return low, top


def fill_fields(cells, xrow, ytop, ylow, rows):
    for c in range(FIELDS):
        xrow[c] = cells[c, 56:64, :]
        ytop[c] = cells[c, pl.ds(7, 8, stride=8), :]
        ylow[c] = cells[c, pl.ds(0, 8, stride=8), :]
        for which, row in enumerate((63, 56, 7, 0)):
            rows[which, c : c + 1, :] = cells[c, row : row + 1, :]
    zero = jnp.zeros((8, 128), jnp.float32)
    return add_packed(cells, range(FIELDS), zero, zero)


def fill_sends(cells, own_packs, xrow, ytop, ylow, rows, corner_x, corner_y, first_pack):
    lane = lanes()
    for target, span, numbers in (
        (xrow, pl.ds(56, 8), ALONG_X),
        (ytop, pl.ds(7, 8, stride=8), UP_Y),
        (ylow, pl.ds(0, 8, stride=8), DOWN_Y),
    ):
        found = pick_shear(lambda c: cells[c, span, :], numbers)
        for n, (shear, live, _) in enumerate(found):
            for k in range(3):
                target[FIELDS + 4 * n + k] = shear[k]
            target[FIELDS + 4 * n + 3] = jnp.where(live, 1.0, 0.0)
    for which, row, at in ((0, 7, 1), (1, 0, 2)):
        for k in range(4):
            rows[which, FIELDS + k : FIELDS + k + 1, :] = xrow[
                FIELDS + 4 * at + k, row : row + 1, :
            ]
    for end, at in ((0, 4), (1, 3)):
        corner = jnp.zeros((8, 128), jnp.float32)
        for j in range(FIELDS + 4):
            value = xrow[j if j < FIELDS else j + 4 * at]
            turn = j + end
            corner = jnp.where(lane == j, pltpu.roll(value, turn, 1) if turn else value, corner)
        corner_x[end, 0] = corner
    for k in range(PACKS):
        if k:
            low = top = jnp.zeros((8, 128), jnp.float32)
        else:
            low, top = first_pack
        channels = range(max(16 * k, FIELDS), min(FULL, 16 * k + 16))
        low, top = add_packed(cells, channels, low, top)
        for end, pack in enumerate((low, top)):
            own_packs[end, k] = pack
            corner_y[end, 0, k : k + 1, :] = pack[7:8, :]
    for end in range(2):
        corner_y[end, 0, PACKS:8, :] = jnp.zeros((8 - PACKS, 128), jnp.float32)


def fill_padded(cells, pad, pad_up, pad_down, level, rising, falling):
    lane = lanes()
    zero = jnp.zeros((8, 128), jnp.float32)
    row = jnp.zeros((1, 128), jnp.float32)
    for x in range(8):
        here = slice(x * 8, x * 8 + 8)
        span = pl.ds(plane(x), 8)
        for c, v in enumerate(scaled([cells[c, here, :] for c in range(FIELDS)])):
            pad[c, span, :] = v
            pad_up[c, span, :] = jnp.where(lane == 127, 0.0, pltpu.roll(v, 127, 1))
            pad_down[c, span, :] = jnp.where(lane == 0, 0.0, pltpu.roll(v, 1, 1))
            pad[c, plane(x) - 1 : plane(x), :] = row
            for source in (pad, pad_up, pad_down):
                source[c, plane(x) + 8 : plane(x) + 9, :] = row
    for c in range(FIELDS):
        for source in (pad, pad_up, pad_down):
            source[c, pl.ds(plane(8), 8), :] = zero
        pad[c, plane(8) - 1 : plane(8), :] = row
        pad[c, plane(8) + 8 : plane(8) + 9, :] = row
    for total in (level, rising, falling):
        for c in range(6):
            for x in range(9):
                total[c, pl.ds(plane(x), 8), :] = zero
                total[c, plane(x) - 1 : plane(x), :] = row
                total[c, plane(x) + 8 : plane(x) + 9, :] = row


def inner_pairs(cells, state, pad, pad_up, pad_down, level, rising, falling, found, marks):
    zero = jnp.zeros((8, 128), jnp.float32)

    def body(x, carry):
        base = pl.multiple_of((x + 1) * ROWS + 8, 8)
        here = pl.ds(pl.multiple_of(x * 8, 8), 8)
        first = [pad[c, pl.ds(base, 8), :] for c in range(FIELDS)]
        forces = [zero] * 3
        twists = [zero] * 3
        springs = [zero] * (3 * SLOTS)
        for number, (dx, dy, dz) in enumerate(DIRS):
            span = pl.ds(base + dx * ROWS + dy, 8)
            source = (pad, pad_up, pad_down)[dz]
            total = (level, rising, falling)[dz]
            second = [source[c, span, :] for c in range(FIELDS)]
            ((shear, live, masks),) = pick_shear(lambda c: cells[c, here, :], (number,))
            force, twist, spring = pair(first, second, (dx, dy, dz), shear, live)
            for k in range(3):
                forces[k] = forces[k] + force[k]
                twists[k] = twists[k] + twist[k]
                for s in range(SLOTS):
                    springs[3 * s + k] = jnp.where(masks[s], spring[k], springs[3 * s + k])
                total[k, span, :] = total[k, span, :] - force[k]
                total[3 + k, span, :] = total[3 + k, span, :] + twist[k]
        for k in range(3):
            level[k, pl.ds(base, 8), :] = level[k, pl.ds(base, 8), :] + forces[k]
            level[3 + k, pl.ds(base, 8), :] = level[3 + k, pl.ds(base, 8), :] + twists[k]
        height, chosen = marks[0], marks[1] == x
        for c in range(3 * SLOTS):
            state[9 + c, here, :] = springs[c]
            value = jnp.take_along_axis(springs[c], height, axis=1)
            found[FIELDS + 6 + c] = jnp.where(chosen, value, found[FIELDS + 6 + c])
        return carry

    lax.fori_loop(0, 8, body, 0)


class Sums:
    def __init__(self):
        zero = jnp.zeros((8, 128), jnp.float32)
        self.total = [zero] * 6
        self.springs = [zero] * (3 * SLOTS)

    def own(self, result, masks):
        force, twist, spring = result
        for k in range(3):
            self.total[k] = self.total[k] + force[k]
            self.total[3 + k] = self.total[3 + k] + twist[k]
            for s in range(SLOTS):
                self.springs[3 * s + k] = jnp.where(masks[s], spring[k], self.springs[3 * s + k])

    def partner(self, result):
        force, twist, _ = result
        for k in range(3):
            self.total[k] = self.total[k] - force[k]
            self.total[3 + k] = self.total[3 + k] + twist[k]

    def collect(self, found, index, mask):
        for c, v in enumerate(self.total + self.springs):
            value = jnp.take_along_axis(v, index, axis=1)
            found[FIELDS + c] = found[FIELDS + c] + jnp.where(mask, value, 0.0)

    def store(self, level, rows, state, span):
        for c in range(6):
            level[c, rows, :] = level[c, rows, :] + self.total[c]
        if span is not None:
            for c in range(3 * SLOTS):
                state[9 + c, span, :] = state[9 + c, span, :] + self.springs[c]


def turned(values, amount, axis=1):
    return [pltpu.roll(v, amount, axis) for v in values]


def masks_of(cells, span, number):
    return [cells[CODES + s, span, :] == float(number) for s in range(SLOTS)]


def fold(level, rising, falling, found, marks):
    lane = lanes()
    sums = [jnp.zeros((8, 128), jnp.float32)] * 6
    for x in range(8):
        rows = pl.ds(plane(x), 8)
        for c in range(6):
            up = jnp.where(lane == 0, 0.0, pltpu.roll(rising[c, rows, :], 1, 1))
            down = jnp.where(lane == 127, 0.0, pltpu.roll(falling[c, rows, :], 127, 1))
            total = level[c, rows, :] + up + down
            level[c, rows, :] = total
            value = jnp.take_along_axis(total, marks[0], axis=1)
            sums[c] = jnp.where(marks[1] == x, value, sums[c])
    for c in range(6):
        found[FIELDS + c] = sums[c]


def x_ahead(cells, state, pad, level, ahead, xhi, edges, xrow, found, who):
    lane = lanes()
    for c in range(FIELDS):
        ahead[c, 7:8, :] = edges[2, c : c + 1, :]
        ahead[c, 16:17, :] = edges[3, c : c + 1, :]
        ahead[c, 8:16, :] = xhi[c]

    sums = Sums()
    first = [pad[c, pl.ds(plane(7), 8), :] for c in range(FIELDS)]
    for n, number in enumerate(ALONG_X):
        dx, dy, dz = DIRS[number]
        second = scaled([ahead[c, pl.ds(8 + dy, 8), :] for c in range(FIELDS)])
        if dz:
            edge = 127 if dz > 0 else 0
            second = [jnp.where(lane == edge, 0.0, v) for v in turned(second, -dz % 128)]
        at = FIELDS + 4 * n
        shear = [xrow[at + k] for k in range(3)]
        result = pair(first, second, DIRS[number], shear, xrow[at + 3] > 0.5)
        sums.own(result, masks_of(cells, pl.ds(56, 8), number))
    sums.store(level, pl.ds(plane(7), 8), state, pl.ds(56, 8))
    x, y, z, live = who
    sums.collect(found, z, ((y == below()) & (x == 7)) & live)


def x_behind(pad, level, behind, xlo, edges, found, who):
    lane = lanes()
    for c in range(FIELDS + 4 * len(ALONG_X)):
        behind[c, 8:16, :] = xlo[c]
    for c in range(FIELDS):
        behind[c, 7:8, :] = edges[0, c : c + 1, :]
        behind[c, 16:17, :] = edges[1, c : c + 1, :]
    for k in range(4):
        behind[FIELDS + 4 + k, 7:8, :] = edges[0, FIELDS + k : FIELDS + k + 1, :]
        behind[FIELDS + 8 + k, 16:17, :] = edges[1, FIELDS + k : FIELDS + k + 1, :]
    sums = Sums()
    second = [pad[c, pl.ds(plane(0), 8), :] for c in range(FIELDS)]
    for n, number in enumerate(ALONG_X):
        dx, dy, dz = DIRS[number]
        span = pl.ds(8 - dy, 8)
        first = scaled([behind[c, span, :] for c in range(FIELDS)])
        first += [behind[FIELDS + 4 * n + k, span, :] for k in range(4)]
        if dz:
            first = turned(first, dz % 128)
        live = first[13] > 0.5
        if dz:
            live = jnp.logical_and(live, lane != (0 if dz > 0 else 127))
        sums.partner(pair(first[:10], second, DIRS[number], first[10:13], live))
    sums.store(level, pl.ds(plane(0), 8), None, None)
    x, y, z, live = who
    sums.collect(found, z, ((y == below()) & (x == 0)) & live)


def y_high(cells, state, pad, level, yhi, ytop, found, who):
    lane = lanes()
    sub = lax.broadcasted_iota(jnp.int32, (8, 128), 0)
    top_fields = scaled([yhi[c] for c in range(FIELDS)])
    sums = Sums()
    mine_rows = pl.ds(plane(0) + 7, 8, stride=ROWS)
    span = pl.ds(7, 8, stride=8)
    mine = [pad[c, mine_rows, :] for c in range(FIELDS)]
    for n, number in enumerate(UP_Y):
        dx, dy, dz = DIRS[number]
        at = FIELDS + 4 * n
        live = ytop[at + 3] > 0.5
        second = top_fields
        if dx:
            second = turned(second, 7, 0)
            live = jnp.logical_and(live, sub != 7)
        if dz:
            second = turned(second, -dz % 128)
            live = jnp.logical_and(live, lane != (127 if dz > 0 else 0))
        shear = [ytop[at + k] for k in range(3)]
        sums.own(pair(mine, second, DIRS[number], shear, live), masks_of(cells, span, number))
    first = turned(top_fields + [yhi[FIELDS + k] for k in range(4)], 1, 0)
    live = jnp.logical_and(first[13] > 0.5, sub != 0)
    sums.partner(pair(first[:10], mine, DIRS[4], first[10:13], live))
    sums.store(level, mine_rows, state, span)
    x, y, z, live = who
    sums.collect(found, z, ((x == below()) & (y == 7)) & live)


def y_low(cells, state, pad, level, ylo, ylow, found, who):
    lane = lanes()
    sub = lax.broadcasted_iota(jnp.int32, (8, 128), 0)
    low_fields = scaled([ylo[c] for c in range(FIELDS)])
    sums = Sums()
    mine_rows = pl.ds(plane(0), 8, stride=ROWS)
    span = pl.ds(0, 8, stride=8)
    mine = [pad[c, mine_rows, :] for c in range(FIELDS)]
    second = turned(low_fields, 7, 0)
    live = jnp.logical_and(ylow[FIELDS + 3] > 0.5, sub != 7)
    shear = [ylow[FIELDS + k] for k in range(3)]
    sums.own(pair(mine, second, DIRS[4], shear, live), masks_of(cells, span, 4))
    for n, number in enumerate(UP_Y):
        dx, dy, dz = DIRS[number]
        first = low_fields + [ylo[FIELDS + 4 * n + k] for k in range(4)]
        if dx:
            first = turned(first, 1, 0)
        if dz:
            first = turned(first, dz % 128)
        live = first[13] > 0.5
        if dx:
            live = jnp.logical_and(live, sub != 0)
        if dz:
            live = jnp.logical_and(live, lane != (0 if dz > 0 else 127))
        sums.partner(pair(first[:10], mine, DIRS[number], first[10:13], live))
    sums.store(level, mine_rows, state, span)
    x, y, z, live = who
    sums.collect(found, z, ((x == below()) & (y == 0)) & live)


def end_pairs(end, zside, packs, own_packs):
    lane = lanes()
    theirs, ours = (((2, 5, 7), (6, 8)), ((6, 8), (2, 5, 7)))[end]
    top = 1 - end

    def spread(pack, c, top):
        p = (c % 16) * 8 - top
        return pltpu.roll(pack, -p % 128, 1) if p % 128 else pack

    back = [
        pltpu.roll(packs[2 + end, 0], -j % 128, 1) if j else packs[2 + end, 0]
        for j in range(FIELDS + 4)
    ]
    back = scaled(back[:FIELDS]) + back[FIELDS:]
    beyond = scaled(
        [pltpu.roll(packs[4 + end, 0], (7 - 8 * c + top) % 128, 1) for c in range(FIELDS)]
    )
    for k in range(PACKS):
        straight, left = packs[end, k], pltpu.roll(packs[6 + end, 0], 7 - k, 0)
        for c in range(16 * k, min(FULL, 16 * k + 16)):
            zside[end, c, 8:16, :] = spread(straight, c, top)
            zside[end, c, 0:8, :] = spread(left, c, top)
            if c < FIELDS:
                zside[end, c, 16:24, :] = spread(packs[8 + end, 0], c, top)
    own = [spread(own_packs[end, c // 16], c, end) for c in range(FULL)]
    mine = scaled(own[:FIELDS])
    sums = Sums()
    for number, (shear, live, masks) in zip(ours, pick_shear(lambda c: own[c], ours)):
        dx, dy, dz = DIRS[number]
        second = scaled([zside[end, c, pl.ds(8 + dy, 8), :] for c in range(FIELDS)])
        if dx:
            second = [
                jnp.where(lane < 7, v, jnp.where(lane == 7, b, 0.0))
                for b, v in zip(beyond, turned(second, 127))
            ]
        sums.own(pair(mine, second, DIRS[number], shear, live), masks)
    for number in theirs:
        dx, dy, dz = DIRS[number]
        span = pl.ds(8 - dy, 8)
        first = scaled([zside[end, c, span, :] for c in range(FIELDS)])
        ((shear, live, _),) = pick_shear(lambda c: zside[end, c, span, :], (number,))
        first = first + shear + [jnp.where(live, 1.0, 0.0)]
        if dx:
            first = [jnp.where(lane == 0, b, v) for b, v in zip(back, turned(first, 1))]
        sums.partner(pair(first[:10], mine, DIRS[number], first[10:13], first[13] > 0.5))
    return sums


def spread_end(end, sums, level, state):
    lane = lanes()
    edge = 127 * end
    hold = lane == edge
    for x in range(8):
        turn = (edge - x) % 128

        def put(v):
            return jnp.where(hold, pltpu.roll(v, turn, 1) if turn else v, 0.0)

        rows = pl.ds(plane(x), 8)
        here = slice(x * 8, x * 8 + 8)
        for c in range(6):
            level[c, rows, :] = level[c, rows, :] + put(sums.total[c])
        for c in range(3 * SLOTS):
            state[9 + c, here, :] = state[9 + c, here, :] + put(sums.springs[c])


def moved(cells, level, x):
    rows = pl.ds(plane(x), 8)
    here = slice(x * 8, x * 8 + 8)
    sums = [level[c, rows, :] for c in range(6)]
    radius = cells[9, here, :]
    inverse = 1.0 / radius
    push = STEP * inverse * inverse * inverse
    turn = 0.125 * (inverse * inverse) * (inverse * inverse)
    velocity = [cells[3 + k, here, :] + push * sums[k] for k in range(3)]
    velocity[2] = velocity[2] - STEP
    offset = [cells[k, here, :] + STEP * velocity[k] for k in range(3)]
    rotation = [cells[6 + k, here, :] + turn * sums[3 + k] for k in range(3)]
    return offset, velocity, rotation, radius


def below():
    return lax.broadcasted_iota(jnp.int32, (8, 128), 0)


def leaving_cells(leaving):
    names = leaving[0:1, 0:64]
    names = jnp.broadcast_to(jnp.concatenate([names, names], axis=1), (8, 128))
    live = names >= 0
    names = jnp.where(live, names, 0)
    return names // 1024, names // 128 % 8, names % 128, live


def gather_fields(found, cells, leaving, marks):
    x_of, y_of, z_of, live = leaving_cells(leaving)
    plane_of = jnp.where((y_of == below()) & live, x_of, -1)
    marks[0] = z_of
    marks[1] = plane_of
    zero = jnp.zeros((8, 128), jnp.float32)
    values = [zero] * FIELDS
    for x in range(8):
        here = slice(x * 8, x * 8 + 8)
        for c in range(FIELDS):
            value = jnp.take_along_axis(cells[c, here, :], z_of, axis=1)
            values[c] = jnp.where(plane_of == x, value, values[c])
    for c in range(FIELDS):
        found[c] = values[c]
    for c in range(3 * SLOTS):
        found[FIELDS + 6 + c] = zero


def fill_outbox(found, outbox, who):
    lane = lanes()[0:1]
    rows = [
        jnp.sum(found[c], axis=0, keepdims=True) for c in range(FIELDS + 6 + 3 * SLOTS)
    ]
    live = who[3][0:1]
    cell = [w[0:1].astype(jnp.float32) for w in who[:3]]
    starts = [(lax.axis_index(a) * n).astype(jnp.float32) for a, n in zip(AXES, (8, 8, 128))]
    radius = rows[9]
    inverse = 1.0 / jnp.where(live, radius, 1.0)
    push = STEP * inverse * inverse * inverse
    turn = 0.125 * (inverse * inverse) * (inverse * inverse)
    velocity = [rows[3 + k] + push * rows[10 + k] for k in range(3)]
    velocity[2] = jnp.where(live, velocity[2] - STEP, 0.0)
    position = [
        jnp.where(live, rows[k] + STEP * velocity[k] + (starts[k] + cell[k]), 0.0)
        for k in range(3)
    ]
    rotation = [rows[6 + k] + turn * rows[13 + k] for k in range(3)]
    values = position + velocity + rotation + [radius] + rows[16:]
    for c in range(14):
        outbox[c : c + 1, :] = jnp.where(lane < 64, values[c], values[14 + c])


def finish(cells, state, leaving, level):
    lane = lanes()
    wide = jnp.broadcast_to(leaving[0:1, 0:64], (8, 64))
    deep = lax.broadcasted_iota(jnp.int32, (8, 64), 0)
    for x in range(8):
        here = slice(x * 8, x * 8 + 8)
        offset, velocity, rotation, _ = moved(cells, level, x)
        left = [
            jnp.max(jnp.where(wide == (x * 8 + deep) * 128 + z, 1.0, 0.0), axis=1, keepdims=True)
            for z in range(2)
        ]
        staying = 1.0 - jnp.where(lane == 0, left[0], jnp.where(lane == 1, left[1], 0.0))
        for c, v in enumerate(offset + velocity + rotation):
            state[c, here, :] = v * staying
        for c in range(9, 27):
            state[c, here, :] = state[c, here, :] * staying


def on_device(offset, velocity, spin, radius, history, contacts, leaving):
    f32 = jnp.float32
    off = offset.reshape(3, 64, 128)
    vel = velocity.reshape(3, 64, 128)
    spn = spin.reshape(3, 64, 128)
    rad = radius.reshape(1, 64, 128)
    hist = history.reshape(3 * SLOTS, 64, 128)
    con = contacts.reshape(SLOTS, 64, 128)
    vmem = pl.BlockSpec(memory_space=pltpu.VMEM)
    hbm = pl.BlockSpec(memory_space=pltpu.HBM)
    halo_shapes = (
        (FIELDS + 4 * len(ALONG_X), 8, 128),
        (FIELDS, 8, 128),
        (FIELDS + 4 * len(UP_Y), 8, 128),
        (FIELDS + 4 * len(DOWN_Y), 8, 128),
        (4, 16, 128),
        (len(PACK_FROM), PACKS, 8, 128),
        (2, PACKS, 8, 128),
    )
    state, arrivals = pl.pallas_call(
        step_kernel,
        out_shape=[pltpu.VMEM((27, 64, 128), f32), pltpu.VMEM((16, 128), f32)],
        in_specs=[hbm] * 7,
        out_specs=[vmem] * 2,
        scratch_shapes=[pltpu.VMEM(s, f32) for s in halo_shapes]
        + [
            pltpu.VMEM((FULL, 64, 128), f32),
            pltpu.VMEM((SLOTS, 64, 128), jnp.int32),
            pltpu.VMEM((1, 64), jnp.int32),
            pltpu.VMEM((FIELDS + 4 * len(ALONG_X), 8, 128), f32),
            pltpu.VMEM((FIELDS + 4 * len(UP_Y), 8, 128), f32),
            pltpu.VMEM((FIELDS + 4 * len(DOWN_Y), 8, 128), f32),
            pltpu.VMEM((4, 16, 128), f32),
            pltpu.VMEM((2, 1, 8, 128), f32),
            pltpu.VMEM((2, 1, 8, 128), f32),
            pltpu.VMEM((16, 128), f32),
            pltpu.VMEM((FIELDS + 6 + 3 * SLOTS, 8, 128), f32),
            pltpu.VMEM((2, 8, 128), jnp.int32),
            pltpu.VMEM((FIELDS, HEIGHT, 128), f32),
            pltpu.VMEM((FIELDS, HEIGHT, 128), f32),
            pltpu.VMEM((FIELDS, HEIGHT, 128), f32),
            pltpu.VMEM((6, HEIGHT, 128), f32),
            pltpu.VMEM((6, HEIGHT, 128), f32),
            pltpu.VMEM((6, HEIGHT, 128), f32),
            pltpu.VMEM((FIELDS + 4 * len(ALONG_X), ROWS, 128), f32),
            pltpu.VMEM((FIELDS, ROWS, 128), f32),
            pltpu.VMEM((2, FULL, ROWS, 128), f32),
            pltpu.SemaphoreType.DMA((len(SENDERS) + 1,)),
        ],
        compiler_params=pltpu.CompilerParams(
            collective_id=0, has_side_effects=True, vmem_limit_bytes=24 << 20
        ),
        name="step",
    )(*[
        pltpu.with_memory_space_constraint(a, pltpu.HBM)
        for a in (off, vel, spn, rad, hist, con, leaving.reshape(1, 64))
    ])
    moved = jax.ShapeDtypeStruct((3, 64, 128), f32)
    new_off, new_vel, new_spin, new_hist, arrivals = pl.pallas_call(
        write_kernel,
        out_shape=[
            moved, moved, moved,
            jax.ShapeDtypeStruct((3 * SLOTS, 64, 128), f32),
            jax.ShapeDtypeStruct((28, 1, 64), f32),
        ],
        in_specs=[vmem] * 2,
        out_specs=[hbm] * 5,
        scratch_shapes=[pltpu.VMEM((28, 1, 64), f32), pltpu.SemaphoreType.DMA((5,))],
        compiler_params=pltpu.CompilerParams(vmem_limit_bytes=8 << 20),
        name="write",
    )(state, arrivals)
    return (
        new_off.reshape(3, 8, 8, 128),
        new_vel.reshape(3, 8, 8, 128),
        new_spin.reshape(3, 8, 8, 128),
        new_hist.reshape(SLOTS, 3, 8, 8, 128),
        arrivals.reshape(28, 1, 1, 1, 64),
    )


def solution(mesh):
    placed = (
        P(None, "gx", "gy", "gz"),
        P(None, "gx", "gy", "gz"),
        P(None, "gx", "gy", "gz"),
        P("gx", "gy", "gz"),
        P(None, None, "gx", "gy", "gz"),
        P(None, "gx", "gy", "gz"),
        P("gx", "gy", "gz", None),
    )
    return jax.shard_map(
        on_device,
        mesh=mesh,
        in_specs=placed,
        out_specs=(
            P(None, "gx", "gy", "gz"),
            P(None, "gx", "gy", "gz"),
            P(None, "gx", "gy", "gz"),
            P(None, None, "gx", "gy", "gz"),
            P(None, "gx", "gy", "gz", None),
        ),
        check_vma=False,
    )
```

```python
import jax
import jax.numpy as jnp
from jax import lax
from jax.experimental import pallas as pl
from jax.experimental.pallas import tpu as pltpu
from jax.sharding import PartitionSpec as P

MESH = pl.DeviceIdType.MESH
AXES = ("gx", "gy", "gz")
DIRS = (
    (1, 0, 0),
    (0, 1, 0),
    (0, 0, 1),
    (1, 1, 0),
    (1, -1, 0),
    (1, 0, 1),
    (1, 0, -1),
    (0, 1, 1),
    (0, 1, -1),
)
SLOTS = 6
FIELDS = 10
SHEAR = FIELDS
CODES = FIELDS + 3 * SLOTS
FULL = CODES + SLOTS
PACKS = (FULL * 8 + 127) // 128
STEP = 0.05
TINY = 1e-30

ROWS = 24
HEIGHT = 10 * ROWS

PACK_FROM = (
    (0, 0, -1),
    (0, 0, 1),
    (-1, 0, -1),
    (-1, 0, 1),
    (1, 0, -1),
    (1, 0, 1),
    (0, -1, -1),
    (0, -1, 1),
    (0, 1, -1),
    (0, 1, 1),
)
FLAT_FROM = (
    (-1, 0, 0),
    (1, 0, 0),
    (0, -1, 0),
    (0, 1, 0),
    (-1, -1, 0),
    (-1, 1, 0),
    (1, -1, 0),
    (1, 1, 0),
)
SENDERS = FLAT_FROM + PACK_FROM

ALONG_X = (0, 3, 4, 5, 6)
UP_Y = (1, 3, 7, 8)
DOWN_Y = (4,)

SEND_ORDER = (10, 12, 14, 16, 4, 5, 6, 7, 8, 2, 0, 3, 1, 11, 13, 15, 17, 9)


def plane(x):
    return (x + 1) * ROWS + 8


def step_kernel(*refs):
    pl.run_scoped(
        lambda *sems: step_body(*refs, *sems),
        pltpu.SemaphoreType.DMA((len(SENDERS) + 1,)),
        pltpu.SemaphoreType.DMA((7,)),
        pltpu.SemaphoreType.DMA((len(SENDERS) + 1,)),
    )


def step_body(
    off_hbm, vel_hbm, spin_hbm, rad_hbm, hist_hbm, con_hbm, leaving_hbm,
    state, arrivals,
    xlo, xhi, ylo, yhi, edges, packs, own_packs, cells, codes, leaving,
    xrow, ytop, ylow, rows, corner_x, corner_y, outbox, found, marks, pad, pad_up, pad_down, level, rising, falling, behind, ahead, zside,
    recv_sems, local_sems, send_sems,
):
    here = [lax.axis_index(a) for a in AXES]
    size = [lax.axis_size(a) for a in AXES]

    def exists(step):
        ok = None
        for at, n, s in zip(here, size, step):
            if s == 0:
                continue
            test = at + s < n if s > 0 else at + s >= 0
            ok = test if ok is None else jnp.logical_and(ok, test)
        return ok

    def place(step):
        return tuple(at + s for at, s in zip(here, step))

    loads = [
        pltpu.make_async_copy(off_hbm, cells.at[0:3], local_sems.at[0]),
        pltpu.make_async_copy(vel_hbm, cells.at[3:6], local_sems.at[1]),
        pltpu.make_async_copy(spin_hbm, cells.at[6:9], local_sems.at[2]),
        pltpu.make_async_copy(rad_hbm, cells.at[9:10], local_sems.at[3]),
        pltpu.make_async_copy(hist_hbm, cells.at[SHEAR:CODES], local_sems.at[4]),
        pltpu.make_async_copy(con_hbm, codes, local_sems.at[5]),
        pltpu.make_async_copy(leaving_hbm, leaving, local_sems.at[6]),
    ]
    barrier = pltpu.get_barrier_semaphore()
    expected = jnp.int32(0)
    for step in SENDERS[4:] + SENDERS[:4]:
        there = exists(step)
        expected = expected + there.astype(jnp.int32)

        @pl.when(there)
        def _():
            pl.semaphore_signal(barrier, inc=1, device_id=place(step), device_id_type=MESH)

    for load in loads:
        load.start()
    with jax.named_scope("loadwait"):
        for load in loads[:4]:
            load.wait()
    with jax.named_scope("pack"):
        first_pack = fill_fields(cells, xrow, ytop, ylow, rows)
    with jax.named_scope("loadwait2"):
        for load in loads[4:]:
            load.wait()
    with jax.named_scope("pack2"):
        for s in range(SLOTS):
            cells[CODES + s] = codes[s].astype(jnp.float32)
        fill_sends(cells, own_packs, xrow, ytop, ylow, rows, corner_x, corner_y, first_pack)

    targets = [xlo, xhi, ylo, yhi] + [edges.at[k] for k in range(4)]
    sources = [xrow, cells.at[0:FIELDS, 0:8, :], ytop, ylow] + [rows.at[k] for k in range(4)]
    for k, s in enumerate(PACK_FROM):
        end = 0 if s[2] > 0 else 1
        if s[0] + s[1] == 0:
            targets.append(packs.at[k])
            sources.append(own_packs.at[end])
            continue
        targets.append(packs.at[k, 0:1])
        if s[0] + s[1] > 0:
            sources.append(own_packs.at[end, 0:1])
        else:
            sources.append((corner_x if s[0] else corner_y).at[end])

    def copy(k):
        to = tuple(-s for s in SENDERS[k])
        return pltpu.make_async_remote_copy(
            src_ref=sources[k],
            dst_ref=targets[k],
            send_sem=send_sems.at[k],
            recv_sem=recv_sems.at[k],
            device_id=place(to),
            device_id_type=MESH,
        )

    for k, step in enumerate(SENDERS):

        @pl.when(jnp.logical_not(exists(step)))
        def _():
            targets[k][...] = jnp.zeros(targets[k].shape, jnp.float32)

    with jax.named_scope("fill"):
        fill_padded(cells, pad, pad_up, pad_down, level, rising, falling)
        gather_fields(found, cells, leaving, marks)
    with jax.named_scope("barrier"):
        pl.semaphore_wait(barrier, expected)
    for k in SEND_ORDER:

        @pl.when(exists(tuple(-s for s in SENDERS[k])))
        def _():
            copy(k).start()

    with jax.named_scope("inner"):
        inner_pairs(cells, state, pad, pad_up, pad_down, level, rising, falling, found, marks)

    def receive(which):
        for k in which:

            @pl.when(exists(SENDERS[k]))
            def _():
                copy(k).wait_recv()

    with jax.named_scope("fold"):
        fold(level, rising, falling, found, marks)
        who = leaving_cells(leaving)
    with jax.named_scope("recvz"):
        receive(range(8, 18, 2))
    with jax.named_scope("floor"):
        floor = end_pairs(0, zside, packs, own_packs)
        x, y, z, live = who
        floor.collect(found, x, (y == below()) & (z == 0) & live)
    with jax.named_scope("recvy"):
        receive((2, 3))
    with jax.named_scope("ypairs"):
        y_high(cells, state, pad, level, yhi, ytop, found, who)
        y_low(cells, state, pad, level, ylo, ylow, found, who)
    with jax.named_scope("recvx"):
        receive((0, 1, 4, 5, 6, 7))
    with jax.named_scope("xpairs"):
        x_ahead(cells, state, pad, level, ahead, xhi, edges, xrow, found, who)
        x_behind(pad, level, behind, xlo, edges, found, who)
    with jax.named_scope("outbox"):
        fill_outbox(found, outbox, who)

    last = len(SENDERS)
    fall = pltpu.make_async_remote_copy(
        src_ref=outbox,
        dst_ref=arrivals,
        send_sem=send_sems.at[last],
        recv_sem=recv_sems.at[last],
        device_id=place((0, 0, -1)),
        device_id_type=MESH,
    )

    @pl.when(exists((0, 0, -1)))
    def _():
        fall.start()

    with jax.named_scope("spread"):
        spread_end(0, floor, level, state)
    with jax.named_scope("recvtop"):
        receive((9, 11, 13, 15, 17))
    with jax.named_scope("ceiling"):
        spread_end(1, end_pairs(1, zside, packs, own_packs), level, state)
    with jax.named_scope("final"):
        finish(cells, state, leaving, level)

    for k, step in enumerate(SENDERS):

        @pl.when(exists(tuple(-s for s in step)))
        def _():
            copy(k).wait_send()

    with jax.named_scope("fall"):

        @pl.when(exists((0, 0, 1)))
        def _():
            fall.wait_recv()

    @pl.when(jnp.logical_not(exists((0, 0, 1))))
    def _():
        arrivals[...] = jnp.zeros(arrivals.shape, jnp.float32)

    @pl.when(exists((0, 0, -1)))
    def _():
        fall.wait_send()


def write_kernel(*refs):
    pl.run_scoped(lambda sems: write_body(*refs, sems), pltpu.SemaphoreType.DMA((5,)))


def write_body(
    state, arrivals, new_off, new_vel, new_spin, new_hist, entered, unpacked, sems
):
    copies = [
        pltpu.make_async_copy(state.at[9:27], new_hist, sems.at[0]),
        pltpu.make_async_copy(state.at[0:3], new_off, sems.at[1]),
        pltpu.make_async_copy(state.at[3:6], new_vel, sems.at[2]),
        pltpu.make_async_copy(state.at[6:9], new_spin, sems.at[3]),
        pltpu.make_async_copy(unpacked, entered, sems.at[4]),
    ]
    for copy in copies[:4]:
        copy.start()
    for c in range(14):
        unpacked[c] = arrivals[c : c + 1, 0:64]
        unpacked[14 + c] = arrivals[c : c + 1, 64:128]
    copies[4].start()
    for copy in copies:
        copy.wait()


def cross(a, b):
    return [
        a[1] * b[2] - a[2] * b[1],
        a[2] * b[0] - a[0] * b[2],
        a[0] * b[1] - a[1] * b[0],
    ]


def dot3(a, b):
    return a[0] * b[0] + a[1] * b[1] + a[2] * b[2]


def pair(first, second, direction, shear, live):
    sep = []
    for k in range(3):
        gap = second[k] - first[k]
        sep.append(gap + float(direction[k]) if direction[k] else gap)
    square = dot3(sep, sep)
    inverse = lax.rsqrt(square)
    normal = [s * inverse for s in sep]
    radii = first[9] + second[9]
    overlap = jnp.maximum(radii - square * inverse, 0.0)
    product = first[9] * second[9] * overlap
    contact = product * lax.rsqrt(jnp.maximum(product * radii, TINY))
    contact = jnp.where(live, contact, 0.0)
    surface = cross([first[6 + k] + second[6 + k] for k in range(3)], normal)
    relative = [second[3 + k] - first[3 + k] - surface[k] for k in range(3)]
    approach = dot3(relative, normal)
    sliding = [relative[k] - approach * normal[k] for k in range(3)]
    repulsion = contact * jnp.maximum(10.0 * overlap - 2.0 * approach, 0.0)
    along = dot3(shear, normal)
    spring = [shear[k] - along * normal[k] + STEP * sliding[k] for k in range(3)]
    pull = [8.0 * spring[k] + 1.5 * sliding[k] for k in range(3)]
    size = contact * contact * dot3(pull, pull)
    factor = jnp.minimum(1.0, 0.4 * repulsion * lax.rsqrt(jnp.maximum(size, 0.0025)))
    scale = factor * contact
    tangent = [scale * pull[k] for k in range(3)]
    force = [tangent[k] - repulsion * normal[k] for k in range(3)]
    return force, cross(normal, tangent), [factor * spring[k] for k in range(3)]


def pick_shear(load, numbers):
    codes = [load(CODES + s) for s in range(SLOTS)]
    found = []
    for number in numbers:
        masks = [code == float(number) for code in codes]
        live = masks[0]
        shear = [jnp.where(masks[0], load(SHEAR + k), 0.0) for k in range(3)]
        for s in range(1, SLOTS):
            live = jnp.logical_or(live, masks[s])
            shear = [jnp.where(masks[s], load(SHEAR + 3 * s + k), shear[k]) for k in range(3)]
        found.append((shear, live, masks))
    return found


def scaled(values):
    return values[:6] + [v * values[9] for v in values[6:9]] + [values[9]]


def lanes():
    return lax.broadcasted_iota(jnp.int32, (8, 128), 1)


def add_packed(cells, channels, low, top):
    lane = lanes()
    for c in channels:
        for x in range(8):
            p = (c % 16) * 8 + x
            value = cells[c, x * 8 : x * 8 + 8, :]
            if p:
                value = pltpu.roll(value, p, 1)
            low = jnp.where(lane == p, value, low)
            top = jnp.where(lane == (p - 1) % 128, value, top)
    return low, top


def fill_fields(cells, xrow, ytop, ylow, rows):
    for c in range(FIELDS):
        xrow[c] = cells[c, 56:64, :]
        ytop[c] = cells[c, pl.ds(7, 8, stride=8), :]
        ylow[c] = cells[c, pl.ds(0, 8, stride=8), :]
        for which, row in enumerate((63, 56, 7, 0)):
            rows[which, c : c + 1, :] = cells[c, row : row + 1, :]
    zero = jnp.zeros((8, 128), jnp.float32)
    return add_packed(cells, range(FIELDS), zero, zero)


def fill_sends(cells, own_packs, xrow, ytop, ylow, rows, corner_x, corner_y, first_pack):
    lane = lanes()
    for target, span, numbers in (
        (xrow, pl.ds(56, 8), ALONG_X),
        (ytop, pl.ds(7, 8, stride=8), UP_Y),
        (ylow, pl.ds(0, 8, stride=8), DOWN_Y),
    ):
        found = pick_shear(lambda c: cells[c, span, :], numbers)
        for n, (shear, live, _) in enumerate(found):
            for k in range(3):
                target[FIELDS + 4 * n + k] = shear[k]
            target[FIELDS + 4 * n + 3] = jnp.where(live, 1.0, 0.0)
    for which, row, at in ((0, 7, 1), (1, 0, 2)):
        for k in range(4):
            rows[which, FIELDS + k : FIELDS + k + 1, :] = xrow[
                FIELDS + 4 * at + k, row : row + 1, :
            ]
    for end, at in ((0, 4), (1, 3)):
        corner = jnp.zeros((8, 128), jnp.float32)
        for j in range(FIELDS + 4):
            value = xrow[j if j < FIELDS else j + 4 * at]
            turn = j + end
            corner = jnp.where(lane == j, pltpu.roll(value, turn, 1) if turn else value, corner)
        corner_x[end, 0] = corner
    for k in range(PACKS):
        if k:
            low = top = jnp.zeros((8, 128), jnp.float32)
        else:
            low, top = first_pack
        channels = range(max(16 * k, FIELDS), min(FULL, 16 * k + 16))
        low, top = add_packed(cells, channels, low, top)
        for end, pack in enumerate((low, top)):
            own_packs[end, k] = pack
            corner_y[end, 0, k : k + 1, :] = pack[7:8, :]
    for end in range(2):
        corner_y[end, 0, PACKS:8, :] = jnp.zeros((8 - PACKS, 128), jnp.float32)


def fill_padded(cells, pad, pad_up, pad_down, level, rising, falling):
    lane = lanes()
    zero = jnp.zeros((8, 128), jnp.float32)
    row = jnp.zeros((1, 128), jnp.float32)
    for x in range(8):
        here = slice(x * 8, x * 8 + 8)
        span = pl.ds(plane(x), 8)
        for c, v in enumerate(scaled([cells[c, here, :] for c in range(FIELDS)])):
            pad[c, span, :] = v
            pad_up[c, span, :] = jnp.where(lane == 127, 0.0, pltpu.roll(v, 127, 1))
            pad_down[c, span, :] = jnp.where(lane == 0, 0.0, pltpu.roll(v, 1, 1))
            pad[c, plane(x) - 1 : plane(x), :] = row
            for source in (pad, pad_up, pad_down):
                source[c, plane(x) + 8 : plane(x) + 9, :] = row
    for c in range(FIELDS):
        for source in (pad, pad_up, pad_down):
            source[c, pl.ds(plane(8), 8), :] = zero
        pad[c, plane(8) - 1 : plane(8), :] = row
        pad[c, plane(8) + 8 : plane(8) + 9, :] = row
    for total in (level, rising, falling):
        for c in range(6):
            for x in range(9):
                total[c, pl.ds(plane(x), 8), :] = zero
                total[c, plane(x) - 1 : plane(x), :] = row
                total[c, plane(x) + 8 : plane(x) + 9, :] = row


def inner_pairs(cells, state, pad, pad_up, pad_down, level, rising, falling, found, marks):
    zero = jnp.zeros((8, 128), jnp.float32)

    def body(x, carry):
        base = pl.multiple_of((x + 1) * ROWS + 8, 8)
        here = pl.ds(pl.multiple_of(x * 8, 8), 8)
        first = [pad[c, pl.ds(base, 8), :] for c in range(FIELDS)]
        forces = [zero] * 3
        twists = [zero] * 3
        springs = [zero] * (3 * SLOTS)
        for number, (dx, dy, dz) in enumerate(DIRS):
            span = pl.ds(base + dx * ROWS + dy, 8)
            source = (pad, pad_up, pad_down)[dz]
            total = (level, rising, falling)[dz]
            second = [source[c, span, :] for c in range(FIELDS)]
            ((shear, live, masks),) = pick_shear(lambda c: cells[c, here, :], (number,))
            force, twist, spring = pair(first, second, (dx, dy, dz), shear, live)
            for k in range(3):
                forces[k] = forces[k] + force[k]
                twists[k] = twists[k] + twist[k]
                for s in range(SLOTS):
                    springs[3 * s + k] = jnp.where(masks[s], spring[k], springs[3 * s + k])
                total[k, span, :] = total[k, span, :] - force[k]
                total[3 + k, span, :] = total[3 + k, span, :] + twist[k]
        for k in range(3):
            level[k, pl.ds(base, 8), :] = level[k, pl.ds(base, 8), :] + forces[k]
            level[3 + k, pl.ds(base, 8), :] = level[3 + k, pl.ds(base, 8), :] + twists[k]
        height, chosen = marks[0], marks[1] == x
        for c in range(3 * SLOTS):
            state[9 + c, here, :] = springs[c]
            value = jnp.take_along_axis(springs[c], height, axis=1)
            found[FIELDS + 6 + c] = jnp.where(chosen, value, found[FIELDS + 6 + c])
        return carry

    lax.fori_loop(0, 8, body, 0)


class Sums:
    def __init__(self):
        zero = jnp.zeros((8, 128), jnp.float32)
        self.total = [zero] * 6
        self.springs = [zero] * (3 * SLOTS)

    def own(self, result, masks):
        force, twist, spring = result
        for k in range(3):
            self.total[k] = self.total[k] + force[k]
            self.total[3 + k] = self.total[3 + k] + twist[k]
            for s in range(SLOTS):
                self.springs[3 * s + k] = jnp.where(masks[s], spring[k], self.springs[3 * s + k])

    def partner(self, result):
        force, twist, _ = result
        for k in range(3):
            self.total[k] = self.total[k] - force[k]
            self.total[3 + k] = self.total[3 + k] + twist[k]

    def collect(self, found, index, mask):
        for c, v in enumerate(self.total + self.springs):
            value = jnp.take_along_axis(v, index, axis=1)
            found[FIELDS + c] = found[FIELDS + c] + jnp.where(mask, value, 0.0)

    def store(self, level, rows, state, span):
        for c in range(6):
            level[c, rows, :] = level[c, rows, :] + self.total[c]
        if span is not None:
            for c in range(3 * SLOTS):
                state[9 + c, span, :] = state[9 + c, span, :] + self.springs[c]


def turned(values, amount, axis=1):
    return [pltpu.roll(v, amount, axis) for v in values]


def masks_of(cells, span, number):
    return [cells[CODES + s, span, :] == float(number) for s in range(SLOTS)]


def fold(level, rising, falling, found, marks):
    lane = lanes()
    sums = [jnp.zeros((8, 128), jnp.float32)] * 6
    for x in range(8):
        rows = pl.ds(plane(x), 8)
        for c in range(6):
            up = jnp.where(lane == 0, 0.0, pltpu.roll(rising[c, rows, :], 1, 1))
            down = jnp.where(lane == 127, 0.0, pltpu.roll(falling[c, rows, :], 127, 1))
            total = level[c, rows, :] + up + down
            level[c, rows, :] = total
            value = jnp.take_along_axis(total, marks[0], axis=1)
            sums[c] = jnp.where(marks[1] == x, value, sums[c])
    for c in range(6):
        found[FIELDS + c] = sums[c]


def x_ahead(cells, state, pad, level, ahead, xhi, edges, xrow, found, who):
    lane = lanes()
    for c in range(FIELDS):
        ahead[c, 7:8, :] = edges[2, c : c + 1, :]
        ahead[c, 16:17, :] = edges[3, c : c + 1, :]
        ahead[c, 8:16, :] = xhi[c]

    sums = Sums()
    first = [pad[c, pl.ds(plane(7), 8), :] for c in range(FIELDS)]
    for n, number in enumerate(ALONG_X):
        dx, dy, dz = DIRS[number]
        second = scaled([ahead[c, pl.ds(8 + dy, 8), :] for c in range(FIELDS)])
        if dz:
            edge = 127 if dz > 0 else 0
            second = [jnp.where(lane == edge, 0.0, v) for v in turned(second, -dz % 128)]
        at = FIELDS + 4 * n
        shear = [xrow[at + k] for k in range(3)]
        result = pair(first, second, DIRS[number], shear, xrow[at + 3] > 0.5)
        sums.own(result, masks_of(cells, pl.ds(56, 8), number))
    sums.store(level, pl.ds(plane(7), 8), state, pl.ds(56, 8))
    x, y, z, live = who
    sums.collect(found, z, ((y == below()) & (x == 7)) & live)


def x_behind(pad, level, behind, xlo, edges, found, who):
    lane = lanes()
    for c in range(FIELDS + 4 * len(ALONG_X)):
        behind[c, 8:16, :] = xlo[c]
    for c in range(FIELDS):
        behind[c, 7:8, :] = edges[0, c : c + 1, :]
        behind[c, 16:17, :] = edges[1, c : c + 1, :]
    for k in range(4):
        behind[FIELDS + 4 + k, 7:8, :] = edges[0, FIELDS + k : FIELDS + k + 1, :]
        behind[FIELDS + 8 + k, 16:17, :] = edges[1, FIELDS + k : FIELDS + k + 1, :]
    sums = Sums()
    second = [pad[c, pl.ds(plane(0), 8), :] for c in range(FIELDS)]
    for n, number in enumerate(ALONG_X):
        dx, dy, dz = DIRS[number]
        span = pl.ds(8 - dy, 8)
        first = scaled([behind[c, span, :] for c in range(FIELDS)])
        first += [behind[FIELDS + 4 * n + k, span, :] for k in range(4)]
        if dz:
            first = turned(first, dz % 128)
        live = first[13] > 0.5
        if dz:
            live = jnp.logical_and(live, lane != (0 if dz > 0 else 127))
        sums.partner(pair(first[:10], second, DIRS[number], first[10:13], live))
    sums.store(level, pl.ds(plane(0), 8), None, None)
    x, y, z, live = who
    sums.collect(found, z, ((y == below()) & (x == 0)) & live)


def y_high(cells, state, pad, level, yhi, ytop, found, who):
    lane = lanes()
    sub = lax.broadcasted_iota(jnp.int32, (8, 128), 0)
    top_fields = scaled([yhi[c] for c in range(FIELDS)])
    sums = Sums()
    mine_rows = pl.ds(plane(0) + 7, 8, stride=ROWS)
    span = pl.ds(7, 8, stride=8)
    mine = [pad[c, mine_rows, :] for c in range(FIELDS)]
    for n, number in enumerate(UP_Y):
        dx, dy, dz = DIRS[number]
        at = FIELDS + 4 * n
        live = ytop[at + 3] > 0.5
        second = top_fields
        if dx:
            second = turned(second, 7, 0)
            live = jnp.logical_and(live, sub != 7)
        if dz:
            second = turned(second, -dz % 128)
            live = jnp.logical_and(live, lane != (127 if dz > 0 else 0))
        shear = [ytop[at + k] for k in range(3)]
        sums.own(pair(mine, second, DIRS[number], shear, live), masks_of(cells, span, number))
    first = turned(top_fields + [yhi[FIELDS + k] for k in range(4)], 1, 0)
    live = jnp.logical_and(first[13] > 0.5, sub != 0)
    sums.partner(pair(first[:10], mine, DIRS[4], first[10:13], live))
    sums.store(level, mine_rows, state, span)
    x, y, z, live = who
    sums.collect(found, z, ((x == below()) & (y == 7)) & live)


def y_low(cells, state, pad, level, ylo, ylow, found, who):
    lane = lanes()
    sub = lax.broadcasted_iota(jnp.int32, (8, 128), 0)
    low_fields = scaled([ylo[c] for c in range(FIELDS)])
    sums = Sums()
    mine_rows = pl.ds(plane(0), 8, stride=ROWS)
    span = pl.ds(0, 8, stride=8)
    mine = [pad[c, mine_rows, :] for c in range(FIELDS)]
    second = turned(low_fields, 7, 0)
    live = jnp.logical_and(ylow[FIELDS + 3] > 0.5, sub != 7)
    shear = [ylow[FIELDS + k] for k in range(3)]
    sums.own(pair(mine, second, DIRS[4], shear, live), masks_of(cells, span, 4))
    for n, number in enumerate(UP_Y):
        dx, dy, dz = DIRS[number]
        first = low_fields + [ylo[FIELDS + 4 * n + k] for k in range(4)]
        if dx:
            first = turned(first, 1, 0)
        if dz:
            first = turned(first, dz % 128)
        live = first[13] > 0.5
        if dx:
            live = jnp.logical_and(live, sub != 0)
        if dz:
            live = jnp.logical_and(live, lane != (0 if dz > 0 else 127))
        sums.partner(pair(first[:10], mine, DIRS[number], first[10:13], live))
    sums.store(level, mine_rows, state, span)
    x, y, z, live = who
    sums.collect(found, z, ((x == below()) & (y == 0)) & live)


def end_pairs(end, zside, packs, own_packs):
    lane = lanes()
    theirs, ours = (((2, 5, 7), (6, 8)), ((6, 8), (2, 5, 7)))[end]
    top = 1 - end

    def spread(pack, c, top):
        p = (c % 16) * 8 - top
        return pltpu.roll(pack, -p % 128, 1) if p % 128 else pack

    back = [
        pltpu.roll(packs[2 + end, 0], -j % 128, 1) if j else packs[2 + end, 0]
        for j in range(FIELDS + 4)
    ]
    back = scaled(back[:FIELDS]) + back[FIELDS:]
    beyond = scaled(
        [pltpu.roll(packs[4 + end, 0], (7 - 8 * c + top) % 128, 1) for c in range(FIELDS)]
    )
    for k in range(PACKS):
        straight, left = packs[end, k], pltpu.roll(packs[6 + end, 0], 7 - k, 0)
        for c in range(16 * k, min(FULL, 16 * k + 16)):
            zside[end, c, 8:16, :] = spread(straight, c, top)
            zside[end, c, 0:8, :] = spread(left, c, top)
            if c < FIELDS:
                zside[end, c, 16:24, :] = spread(packs[8 + end, 0], c, top)
    own = [spread(own_packs[end, c // 16], c, end) for c in range(FULL)]
    mine = scaled(own[:FIELDS])
    sums = Sums()
    for number, (shear, live, masks) in zip(ours, pick_shear(lambda c: own[c], ours)):
        dx, dy, dz = DIRS[number]
        second = scaled([zside[end, c, pl.ds(8 + dy, 8), :] for c in range(FIELDS)])
        if dx:
            second = [
                jnp.where(lane < 7, v, jnp.where(lane == 7, b, 0.0))
                for b, v in zip(beyond, turned(second, 127))
            ]
        sums.own(pair(mine, second, DIRS[number], shear, live), masks)
    for number in theirs:
        dx, dy, dz = DIRS[number]
        span = pl.ds(8 - dy, 8)
        first = scaled([zside[end, c, span, :] for c in range(FIELDS)])
        ((shear, live, _),) = pick_shear(lambda c: zside[end, c, span, :], (number,))
        first = first + shear + [jnp.where(live, 1.0, 0.0)]
        if dx:
            first = [jnp.where(lane == 0, b, v) for b, v in zip(back, turned(first, 1))]
        sums.partner(pair(first[:10], mine, DIRS[number], first[10:13], first[13] > 0.5))
    return sums


def spread_end(end, sums, level, state):
    lane = lanes()
    edge = 127 * end
    hold = lane == edge
    for x in range(8):
        turn = (edge - x) % 128

        def put(v):
            return jnp.where(hold, pltpu.roll(v, turn, 1) if turn else v, 0.0)

        rows = pl.ds(plane(x), 8)
        here = slice(x * 8, x * 8 + 8)
        for c in range(6):
            level[c, rows, :] = level[c, rows, :] + put(sums.total[c])
        for c in range(3 * SLOTS):
            state[9 + c, here, :] = state[9 + c, here, :] + put(sums.springs[c])


def moved(cells, level, x):
    rows = pl.ds(plane(x), 8)
    here = slice(x * 8, x * 8 + 8)
    sums = [level[c, rows, :] for c in range(6)]
    radius = cells[9, here, :]
    inverse = 1.0 / radius
    push = STEP * inverse * inverse * inverse
    turn = 0.125 * (inverse * inverse) * (inverse * inverse)
    velocity = [cells[3 + k, here, :] + push * sums[k] for k in range(3)]
    velocity[2] = velocity[2] - STEP
    offset = [cells[k, here, :] + STEP * velocity[k] for k in range(3)]
    rotation = [cells[6 + k, here, :] + turn * sums[3 + k] for k in range(3)]
    return offset, velocity, rotation, radius


def below():
    return lax.broadcasted_iota(jnp.int32, (8, 128), 0)


def leaving_cells(leaving):
    names = leaving[0:1, 0:64]
    names = jnp.broadcast_to(jnp.concatenate([names, names], axis=1), (8, 128))
    live = names >= 0
    names = jnp.where(live, names, 0)
    return names // 1024, names // 128 % 8, names % 128, live


def gather_fields(found, cells, leaving, marks):
    x_of, y_of, z_of, live = leaving_cells(leaving)
    plane_of = jnp.where((y_of == below()) & live, x_of, -1)
    marks[0] = z_of
    marks[1] = plane_of
    zero = jnp.zeros((8, 128), jnp.float32)
    values = [zero] * FIELDS
    for x in range(8):
        here = slice(x * 8, x * 8 + 8)
        for c in range(FIELDS):
            value = jnp.take_along_axis(cells[c, here, :], z_of, axis=1)
            values[c] = jnp.where(plane_of == x, value, values[c])
    for c in range(FIELDS):
        found[c] = values[c]
    for c in range(3 * SLOTS):
        found[FIELDS + 6 + c] = zero


def fill_outbox(found, outbox, who):
    lane = lanes()[0:1]
    rows = [
        jnp.sum(found[c], axis=0, keepdims=True) for c in range(FIELDS + 6 + 3 * SLOTS)
    ]
    live = who[3][0:1]
    cell = [w[0:1].astype(jnp.float32) for w in who[:3]]
    starts = [(lax.axis_index(a) * n).astype(jnp.float32) for a, n in zip(AXES, (8, 8, 128))]
    radius = rows[9]
    inverse = 1.0 / jnp.where(live, radius, 1.0)
    push = STEP * inverse * inverse * inverse
    turn = 0.125 * (inverse * inverse) * (inverse * inverse)
    velocity = [rows[3 + k] + push * rows[10 + k] for k in range(3)]
    velocity[2] = jnp.where(live, velocity[2] - STEP, 0.0)
    position = [
        jnp.where(live, rows[k] + STEP * velocity[k] + (starts[k] + cell[k]), 0.0)
        for k in range(3)
    ]
    rotation = [rows[6 + k] + turn * rows[13 + k] for k in range(3)]
    values = position + velocity + rotation + [radius] + rows[16:]
    for c in range(14):
        outbox[c : c + 1, :] = jnp.where(lane < 64, values[c], values[14 + c])


def finish(cells, state, leaving, level):
    lane = lanes()
    wide = jnp.broadcast_to(leaving[0:1, 0:64], (8, 64))
    deep = lax.broadcasted_iota(jnp.int32, (8, 64), 0)
    for x in range(8):
        here = slice(x * 8, x * 8 + 8)
        offset, velocity, rotation, _ = moved(cells, level, x)
        left = [
            jnp.max(jnp.where(wide == (x * 8 + deep) * 128 + z, 1.0, 0.0), axis=1, keepdims=True)
            for z in range(2)
        ]
        staying = 1.0 - jnp.where(lane == 0, left[0], jnp.where(lane == 1, left[1], 0.0))
        for c, v in enumerate(offset + velocity + rotation):
            state[c, here, :] = v * staying
        for c in range(9, 27):
            state[c, here, :] = state[c, here, :] * staying


def on_device(offset, velocity, spin, radius, history, contacts, leaving):
    f32 = jnp.float32
    off = offset.reshape(3, 64, 128)
    vel = velocity.reshape(3, 64, 128)
    spn = spin.reshape(3, 64, 128)
    rad = radius.reshape(1, 64, 128)
    hist = history.reshape(3 * SLOTS, 64, 128)
    con = contacts.reshape(SLOTS, 64, 128)
    vmem = pl.BlockSpec(memory_space=pltpu.VMEM)
    hbm = pl.BlockSpec(memory_space=pltpu.HBM)
    halo_shapes = (
        (FIELDS + 4 * len(ALONG_X), 8, 128),
        (FIELDS, 8, 128),
        (FIELDS + 4 * len(UP_Y), 8, 128),
        (FIELDS + 4 * len(DOWN_Y), 8, 128),
        (4, 16, 128),
        (len(PACK_FROM), PACKS, 8, 128),
        (2, PACKS, 8, 128),
    )
    state, arrivals = pl.pallas_call(
        step_kernel,
        out_shape=[pltpu.VMEM((27, 64, 128), f32), pltpu.VMEM((16, 128), f32)],
        in_specs=[hbm] * 7,
        out_specs=[vmem] * 2,
        scratch_shapes=[pltpu.VMEM(s, f32) for s in halo_shapes]
        + [
            pltpu.VMEM((FULL, 64, 128), f32),
            pltpu.VMEM((SLOTS, 64, 128), jnp.int32),
            pltpu.VMEM((1, 64), jnp.int32),
            pltpu.VMEM((FIELDS + 4 * len(ALONG_X), 8, 128), f32),
            pltpu.VMEM((FIELDS + 4 * len(UP_Y), 8, 128), f32),
            pltpu.VMEM((FIELDS + 4 * len(DOWN_Y), 8, 128), f32),
            pltpu.VMEM((4, 16, 128), f32),
            pltpu.VMEM((2, 1, 8, 128), f32),
            pltpu.VMEM((2, 1, 8, 128), f32),
            pltpu.VMEM((16, 128), f32),
            pltpu.VMEM((FIELDS + 6 + 3 * SLOTS, 8, 128), f32),
            pltpu.VMEM((2, 8, 128), jnp.int32),
            pltpu.VMEM((FIELDS, HEIGHT, 128), f32),
            pltpu.VMEM((FIELDS, HEIGHT, 128), f32),
            pltpu.VMEM((FIELDS, HEIGHT, 128), f32),
            pltpu.VMEM((6, HEIGHT, 128), f32),
            pltpu.VMEM((6, HEIGHT, 128), f32),
            pltpu.VMEM((6, HEIGHT, 128), f32),
            pltpu.VMEM((FIELDS + 4 * len(ALONG_X), ROWS, 128), f32),
            pltpu.VMEM((FIELDS, ROWS, 128), f32),
            pltpu.VMEM((2, FULL, ROWS, 128), f32),
        ],
        compiler_params=pltpu.CompilerParams(
            collective_id=0, has_side_effects=True, vmem_limit_bytes=24 << 20
        ),
        name="step",
    )(*[
        pltpu.with_memory_space_constraint(a, pltpu.HBM)
        for a in (off, vel, spn, rad, hist, con, leaving.reshape(1, 64))
    ])
    moved = jax.ShapeDtypeStruct((3, 64, 128), f32)
    new_off, new_vel, new_spin, new_hist, arrivals = pl.pallas_call(
        write_kernel,
        out_shape=[
            moved, moved, moved,
            jax.ShapeDtypeStruct((3 * SLOTS, 64, 128), f32),
            jax.ShapeDtypeStruct((28, 1, 64), f32),
        ],
        in_specs=[vmem] * 2,
        out_specs=[hbm] * 5,
        scratch_shapes=[pltpu.VMEM((28, 1, 64), f32)],
        compiler_params=pltpu.CompilerParams(vmem_limit_bytes=8 << 20),
        name="write",
    )(state, arrivals)
    return (
        new_off.reshape(3, 8, 8, 128),
        new_vel.reshape(3, 8, 8, 128),
        new_spin.reshape(3, 8, 8, 128),
        new_hist.reshape(SLOTS, 3, 8, 8, 128),
        arrivals.reshape(28, 1, 1, 1, 64),
    )


def solution(mesh):
    placed = (
        P(None, "gx", "gy", "gz"),
        P(None, "gx", "gy", "gz"),
        P(None, "gx", "gy", "gz"),
        P("gx", "gy", "gz"),
        P(None, None, "gx", "gy", "gz"),
        P(None, "gx", "gy", "gz"),
        P("gx", "gy", "gz", None),
    )
    return jax.shard_map(
        on_device,
        mesh=mesh,
        in_specs=placed,
        out_specs=(
            P(None, "gx", "gy", "gz"),
            P(None, "gx", "gy", "gz"),
            P(None, "gx", "gy", "gz"),
            P(None, None, "gx", "gy", "gz"),
            P(None, "gx", "gy", "gz", None),
        ),
        check_vma=False,
    )
```

```python
import jax
import jax.numpy as jnp
from jax import lax
from jax.experimental import pallas as pl
from jax.experimental.pallas import tpu as pltpu
from jax.sharding import PartitionSpec as P

MESH = pl.DeviceIdType.MESH
AXES = ("gx", "gy", "gz")
DIRS = (
    (1, 0, 0),
    (0, 1, 0),
    (0, 0, 1),
    (1, 1, 0),
    (1, -1, 0),
    (1, 0, 1),
    (1, 0, -1),
    (0, 1, 1),
    (0, 1, -1),
)
SLOTS = 6
FIELDS = 10
SHEAR = FIELDS
CODES = FIELDS + 3 * SLOTS
FULL = CODES + SLOTS
PACKS = (FULL * 8 + 127) // 128
STEP = 0.05
TINY = 1e-30

ROWS = 24
HEIGHT = 10 * ROWS

PACK_FROM = (
    (0, 0, -1),
    (0, 0, 1),
    (-1, 0, -1),
    (-1, 0, 1),
    (1, 0, -1),
    (1, 0, 1),
    (0, -1, -1),
    (0, -1, 1),
    (0, 1, -1),
    (0, 1, 1),
)
FLAT_FROM = (
    (-1, 0, 0),
    (1, 0, 0),
    (0, -1, 0),
    (0, 1, 0),
    (-1, -1, 0),
    (-1, 1, 0),
    (1, -1, 0),
    (1, 1, 0),
)
SENDERS = FLAT_FROM + PACK_FROM

ALONG_X = (0, 3, 4, 5, 6)
UP_Y = (1, 3, 7, 8)
DOWN_Y = (4,)

SEND_ORDER = (10, 12, 14, 16, 4, 5, 6, 7, 8, 2, 0, 3, 1, 11, 13, 15, 17, 9)


def plane(x):
    return (x + 1) * ROWS + 8


def step_kernel(*refs):
    pl.run_scoped(
        lambda *sems: step_body(*refs, *sems),
        pltpu.SemaphoreType.DMA((len(SENDERS) + 1,)),
        pltpu.SemaphoreType.DMA((7,)),
        pltpu.SemaphoreType.DMA((len(SENDERS) + 1,)),
    )


def step_body(
    off_hbm, vel_hbm, spin_hbm, rad_hbm, hist_hbm, con_hbm, leaving_hbm,
    state, arrivals,
    xlo, xhi, ylo, yhi, edges, packs, own_packs, cells, codes, leaving,
    xrow, ytop, ylow, rows, corner_x, corner_y, outbox, found, marks, pad, pad_up, pad_down, level, rising, falling, behind, ahead, zside,
    recv_sems, local_sems, send_sems,
):
    here = [lax.axis_index(a) for a in AXES]
    size = [lax.axis_size(a) for a in AXES]

    def exists(step):
        ok = None
        for at, n, s in zip(here, size, step):
            if s == 0:
                continue
            test = at + s < n if s > 0 else at + s >= 0
            ok = test if ok is None else jnp.logical_and(ok, test)
        return ok

    def place(step):
        return tuple(at + s for at, s in zip(here, step))

    loads = [
        pltpu.make_async_copy(off_hbm, cells.at[0:3], local_sems.at[0]),
        pltpu.make_async_copy(vel_hbm, cells.at[3:6], local_sems.at[1]),
        pltpu.make_async_copy(spin_hbm, cells.at[6:9], local_sems.at[2]),
        pltpu.make_async_copy(rad_hbm, cells.at[9:10], local_sems.at[3]),
        pltpu.make_async_copy(hist_hbm, cells.at[SHEAR:CODES], local_sems.at[4]),
        pltpu.make_async_copy(con_hbm, codes, local_sems.at[5]),
        pltpu.make_async_copy(leaving_hbm, leaving, local_sems.at[6]),
    ]
    barrier = pltpu.get_barrier_semaphore()
    expected = jnp.int32(0)
    for step in SENDERS[4:] + SENDERS[:4]:
        there = exists(step)
        expected = expected + there.astype(jnp.int32)

        @pl.when(there)
        def _():
            pl.semaphore_signal(barrier, inc=1, device_id=place(step), device_id_type=MESH)

    for load in loads:
        load.start()
    with jax.named_scope("loadwait"):
        for load in loads[:4]:
            load.wait()
    with jax.named_scope("pack"):
        first_pack = fill_fields(cells, xrow, ytop, ylow, rows)
    with jax.named_scope("loadwait2"):
        for load in loads[4:]:
            load.wait()
    with jax.named_scope("pack2"):
        for s in range(SLOTS):
            cells[CODES + s] = codes[s].astype(jnp.float32)
        fill_sends(cells, own_packs, xrow, ytop, ylow, rows, corner_x, corner_y, first_pack)

    targets = [xlo, xhi, ylo, yhi] + [edges.at[k] for k in range(4)]
    sources = [xrow, cells.at[0:FIELDS, 0:8, :], ytop, ylow] + [rows.at[k] for k in range(4)]
    for k, s in enumerate(PACK_FROM):
        end = 0 if s[2] > 0 else 1
        if s[0] + s[1] == 0:
            targets.append(packs.at[k])
            sources.append(own_packs.at[end])
            continue
        targets.append(packs.at[k, 0:1])
        if s[0] + s[1] > 0:
            sources.append(own_packs.at[end, 0:1])
        else:
            sources.append((corner_x if s[0] else corner_y).at[end])

    def copy(k):
        to = tuple(-s for s in SENDERS[k])
        return pltpu.make_async_remote_copy(
            src_ref=sources[k],
            dst_ref=targets[k],
            send_sem=send_sems.at[k],
            recv_sem=recv_sems.at[k],
            device_id=place(to),
            device_id_type=MESH,
        )

    for k, step in enumerate(SENDERS):

        @pl.when(jnp.logical_not(exists(step)))
        def _():
            targets[k][...] = jnp.zeros(targets[k].shape, jnp.float32)

    with jax.named_scope("fill"):
        fill_padded(cells, pad, pad_up, pad_down, level, rising, falling)
        gather_fields(found, cells, leaving, marks)
    with jax.named_scope("barrier"):
        pl.semaphore_wait(barrier, expected)
    for k in SEND_ORDER:

        @pl.when(exists(tuple(-s for s in SENDERS[k])))
        def _():
            copy(k).start()

    with jax.named_scope("inner"):
        inner_pairs(cells, state, pad, pad_up, pad_down, level, rising, falling, found, marks)

    def receive(which):
        for k in which:

            @pl.when(exists(SENDERS[k]))
            def _():
                copy(k).wait_recv()

    with jax.named_scope("fold"):
        fold(level, rising, falling, found, marks)
        who = leaving_cells(leaving)
    with jax.named_scope("recvz"):
        receive(range(8, 18, 2))
    with jax.named_scope("floor"):
        floor = end_pairs(0, zside, packs, own_packs)
        x, y, z, live = who
        floor.collect(found, x, (y == below()) & (z == 0) & live)
    with jax.named_scope("recvy"):
        receive((2, 3))
    with jax.named_scope("ypairs"):
        y_high(cells, state, pad, level, yhi, ytop, found, who)
        y_low(cells, state, pad, level, ylo, ylow, found, who)
    with jax.named_scope("recvx"):
        receive((0, 1, 4, 5, 6, 7))
    with jax.named_scope("xpairs"):
        x_ahead(cells, state, pad, level, ahead, xhi, edges, xrow, found, who)
        x_behind(pad, level, behind, xlo, edges, found, who)
    with jax.named_scope("outbox"):
        fill_outbox(found, outbox, who)

    last = len(SENDERS)
    fall = pltpu.make_async_remote_copy(
        src_ref=outbox,
        dst_ref=arrivals,
        send_sem=send_sems.at[last],
        recv_sem=recv_sems.at[last],
        device_id=place((0, 0, -1)),
        device_id_type=MESH,
    )

    @pl.when(exists((0, 0, -1)))
    def _():
        fall.start()

    with jax.named_scope("spread"):
        spread_end(0, floor, level, state)
    with jax.named_scope("recvtop"):
        receive((9, 11, 13, 15, 17))
    with jax.named_scope("ceiling"):
        spread_end(1, end_pairs(1, zside, packs, own_packs), level, state)
    with jax.named_scope("final"):
        finish(cells, state, leaving, level)

    for k, step in enumerate(SENDERS):

        @pl.when(exists(tuple(-s for s in step)))
        def _():
            copy(k).wait_send()

    with jax.named_scope("fall"):

        @pl.when(exists((0, 0, 1)))
        def _():
            fall.wait_recv()

    @pl.when(jnp.logical_not(exists((0, 0, 1))))
    def _():
        arrivals[...] = jnp.zeros(arrivals.shape, jnp.float32)

    @pl.when(exists((0, 0, -1)))
    def _():
        fall.wait_send()


def write_kernel(*refs):
    pl.run_scoped(lambda sems: write_body(*refs, sems), pltpu.SemaphoreType.DMA((5,)))


def write_body(
    state, arrivals, new_off, new_vel, new_spin, new_hist, entered, unpacked, sems
):
    copies = [
        pltpu.make_async_copy(state.at[9:27], new_hist, sems.at[0]),
        pltpu.make_async_copy(state.at[0:3], new_off, sems.at[1]),
        pltpu.make_async_copy(state.at[3:6], new_vel, sems.at[2]),
        pltpu.make_async_copy(state.at[6:9], new_spin, sems.at[3]),
        pltpu.make_async_copy(unpacked, entered, sems.at[4]),
    ]
    for copy in copies[:4]:
        copy.start()
    for c in range(14):
        unpacked[c] = arrivals[c : c + 1, 0:64]
        unpacked[14 + c] = arrivals[c : c + 1, 64:128]
    copies[4].start()
    for copy in copies:
        copy.wait()


def cross(a, b):
    return [
        a[1] * b[2] - a[2] * b[1],
        a[2] * b[0] - a[0] * b[2],
        a[0] * b[1] - a[1] * b[0],
    ]


def dot3(a, b):
    return a[0] * b[0] + a[1] * b[1] + a[2] * b[2]


def pair(first, second, direction, shear, live):
    sep = []
    for k in range(3):
        gap = second[k] - first[k]
        sep.append(gap + float(direction[k]) if direction[k] else gap)
    square = dot3(sep, sep)
    inverse = lax.rsqrt(square)
    normal = [s * inverse for s in sep]
    radii = first[9] + second[9]
    overlap = jnp.maximum(radii - square * inverse, 0.0)
    product = first[9] * second[9] * overlap
    contact = product * lax.rsqrt(jnp.maximum(product * radii, TINY))
    contact = jnp.where(live, contact, 0.0)
    surface = cross([first[6 + k] + second[6 + k] for k in range(3)], normal)
    relative = [second[3 + k] - first[3 + k] - surface[k] for k in range(3)]
    approach = dot3(relative, normal)
    sliding = [relative[k] - approach * normal[k] for k in range(3)]
    repulsion = contact * jnp.maximum(10.0 * overlap - 2.0 * approach, 0.0)
    along = dot3(shear, normal)
    spring = [shear[k] - along * normal[k] + STEP * sliding[k] for k in range(3)]
    pull = [8.0 * spring[k] + 1.5 * sliding[k] for k in range(3)]
    size = contact * contact * dot3(pull, pull)
    factor = jnp.minimum(1.0, 0.4 * repulsion * lax.rsqrt(jnp.maximum(size, 0.0025)))
    scale = factor * contact
    tangent = [scale * pull[k] for k in range(3)]
    force = [tangent[k] - repulsion * normal[k] for k in range(3)]
    return force, cross(normal, tangent), [factor * spring[k] for k in range(3)]


def pick_shear(load, numbers):
    codes = [load(CODES + s) for s in range(SLOTS)]
    found = []
    for number in numbers:
        masks = [code == float(number) for code in codes]
        live = masks[0]
        shear = [jnp.where(masks[0], load(SHEAR + k), 0.0) for k in range(3)]
        for s in range(1, SLOTS):
            live = jnp.logical_or(live, masks[s])
            shear = [jnp.where(masks[s], load(SHEAR + 3 * s + k), shear[k]) for k in range(3)]
        found.append((shear, live, masks))
    return found


def scaled(values):
    return values[:6] + [v * values[9] for v in values[6:9]] + [values[9]]


def lanes():
    return lax.broadcasted_iota(jnp.int32, (8, 128), 1)


def add_packed(cells, channels, low, top):
    lane = lanes()
    for c in channels:
        for x in range(8):
            p = (c % 16) * 8 + x
            value = cells[c, x * 8 : x * 8 + 8, :]
            if p:
                value = pltpu.roll(value, p, 1)
            low = jnp.where(lane == p, value, low)
            top = jnp.where(lane == (p - 1) % 128, value, top)
    return low, top


def fill_fields(cells, xrow, ytop, ylow, rows):
    for c in range(FIELDS):
        xrow[c] = cells[c, 56:64, :]
        ytop[c] = cells[c, pl.ds(7, 8, stride=8), :]
        ylow[c] = cells[c, pl.ds(0, 8, stride=8), :]
        for which, row in enumerate((63, 56, 7, 0)):
            rows[which, c : c + 1, :] = cells[c, row : row + 1, :]
    zero = jnp.zeros((8, 128), jnp.float32)
    return add_packed(cells, range(FIELDS), zero, zero)


def fill_sends(cells, own_packs, xrow, ytop, ylow, rows, corner_x, corner_y, first_pack):
    lane = lanes()
    for target, span, numbers in (
        (xrow, pl.ds(56, 8), ALONG_X),
        (ytop, pl.ds(7, 8, stride=8), UP_Y),
        (ylow, pl.ds(0, 8, stride=8), DOWN_Y),
    ):
        found = pick_shear(lambda c: cells[c, span, :], numbers)
        for n, (shear, live, _) in enumerate(found):
            for k in range(3):
                target[FIELDS + 4 * n + k] = shear[k]
            target[FIELDS + 4 * n + 3] = jnp.where(live, 1.0, 0.0)
    for which, row, at in ((0, 7, 1), (1, 0, 2)):
        for k in range(4):
            rows[which, FIELDS + k : FIELDS + k + 1, :] = xrow[
                FIELDS + 4 * at + k, row : row + 1, :
            ]
    for end, at in ((0, 4), (1, 3)):
        corner = jnp.zeros((8, 128), jnp.float32)
        for j in range(FIELDS + 4):
            value = xrow[j if j < FIELDS else j + 4 * at]
            turn = j + end
            corner = jnp.where(lane == j, pltpu.roll(value, turn, 1) if turn else value, corner)
        corner_x[end, 0] = corner
    for k in range(PACKS):
        if k:
            low = top = jnp.zeros((8, 128), jnp.float32)
        else:
            low, top = first_pack
        channels = range(max(16 * k, FIELDS), min(FULL, 16 * k + 16))
        low, top = add_packed(cells, channels, low, top)
        for end, pack in enumerate((low, top)):
            own_packs[end, k] = pack
            corner_y[end, 0, k : k + 1, :] = pack[7:8, :]
    for end in range(2):
        corner_y[end, 0, PACKS:8, :] = jnp.zeros((8 - PACKS, 128), jnp.float32)


def fill_padded(cells, pad, pad_up, pad_down, level, rising, falling):
    lane = lanes()
    zero = jnp.zeros((8, 128), jnp.float32)
    row = jnp.zeros((1, 128), jnp.float32)
    for x in range(8):
        here = slice(x * 8, x * 8 + 8)
        span = pl.ds(plane(x), 8)
        for c, v in enumerate(scaled([cells[c, here, :] for c in range(FIELDS)])):
            pad[c, span, :] = v
            pad_up[c, span, :] = jnp.where(lane == 127, 0.0, pltpu.roll(v, 127, 1))
            pad_down[c, span, :] = jnp.where(lane == 0, 0.0, pltpu.roll(v, 1, 1))
            pad[c, plane(x) - 1 : plane(x), :] = row
            for source in (pad, pad_up, pad_down):
                source[c, plane(x) + 8 : plane(x) + 9, :] = row
    for c in range(FIELDS):
        for source in (pad, pad_up, pad_down):
            source[c, pl.ds(plane(8), 8), :] = zero
        pad[c, plane(8) - 1 : plane(8), :] = row
        pad[c, plane(8) + 8 : plane(8) + 9, :] = row
    for total in (level, rising, falling):
        for c in range(6):
            for x in range(9):
                total[c, pl.ds(plane(x), 8), :] = zero
                total[c, plane(x) - 1 : plane(x), :] = row
                total[c, plane(x) + 8 : plane(x) + 9, :] = row


def inner_pairs(cells, state, pad, pad_up, pad_down, level, rising, falling, found, marks):
    zero = jnp.zeros((8, 128), jnp.float32)

    def body(x, carry):
        base = pl.multiple_of((x + 1) * ROWS + 8, 8)
        here = pl.ds(pl.multiple_of(x * 8, 8), 8)
        first = [pad[c, pl.ds(base, 8), :] for c in range(FIELDS)]
        forces = [zero] * 3
        twists = [zero] * 3
        springs = [zero] * (3 * SLOTS)
        for number, (dx, dy, dz) in enumerate(DIRS):
            span = pl.ds(base + dx * ROWS + dy, 8)
            source = (pad, pad_up, pad_down)[dz]
            total = (level, rising, falling)[dz]
            second = [source[c, span, :] for c in range(FIELDS)]
            ((shear, live, masks),) = pick_shear(lambda c: cells[c, here, :], (number,))
            force, twist, spring = pair(first, second, (dx, dy, dz), shear, live)
            for k in range(3):
                forces[k] = forces[k] + force[k]
                twists[k] = twists[k] + twist[k]
                for s in range(SLOTS):
                    springs[3 * s + k] = jnp.where(masks[s], spring[k], springs[3 * s + k])
                total[k, span, :] = total[k, span, :] - force[k]
                total[3 + k, span, :] = total[3 + k, span, :] + twist[k]
        for k in range(3):
            level[k, pl.ds(base, 8), :] = level[k, pl.ds(base, 8), :] + forces[k]
            level[3 + k, pl.ds(base, 8), :] = level[3 + k, pl.ds(base, 8), :] + twists[k]
        height, chosen = marks[0], marks[1] == x
        for c in range(3 * SLOTS):
            state[9 + c, here, :] = springs[c]
            value = jnp.take_along_axis(springs[c], height, axis=1)
            found[FIELDS + 6 + c] = jnp.where(chosen, value, found[FIELDS + 6 + c])
        return carry

    lax.fori_loop(0, 8, body, 0)


class Sums:
    def __init__(self):
        zero = jnp.zeros((8, 128), jnp.float32)
        self.total = [zero] * 6
        self.springs = [zero] * (3 * SLOTS)

    def own(self, result, masks):
        force, twist, spring = result
        for k in range(3):
            self.total[k] = self.total[k] + force[k]
            self.total[3 + k] = self.total[3 + k] + twist[k]
            for s in range(SLOTS):
                self.springs[3 * s + k] = jnp.where(masks[s], spring[k], self.springs[3 * s + k])

    def partner(self, result):
        force, twist, _ = result
        for k in range(3):
            self.total[k] = self.total[k] - force[k]
            self.total[3 + k] = self.total[3 + k] + twist[k]

    def collect(self, found, index, mask):
        for c, v in enumerate(self.total + self.springs):
            value = jnp.take_along_axis(v, index, axis=1)
            found[FIELDS + c] = found[FIELDS + c] + jnp.where(mask, value, 0.0)

    def store(self, level, rows, state, span):
        for c in range(6):
            level[c, rows, :] = level[c, rows, :] + self.total[c]
        if span is not None:
            for c in range(3 * SLOTS):
                state[9 + c, span, :] = state[9 + c, span, :] + self.springs[c]


def turned(values, amount, axis=1):
    return [pltpu.roll(v, amount, axis) for v in values]


def masks_of(cells, span, number):
    return [cells[CODES + s, span, :] == float(number) for s in range(SLOTS)]


def fold(level, rising, falling, found, marks):
    lane = lanes()
    sums = [jnp.zeros((8, 128), jnp.float32)] * 6
    for x in range(8):
        rows = pl.ds(plane(x), 8)
        for c in range(6):
            up = jnp.where(lane == 0, 0.0, pltpu.roll(rising[c, rows, :], 1, 1))
            down = jnp.where(lane == 127, 0.0, pltpu.roll(falling[c, rows, :], 127, 1))
            total = level[c, rows, :] + up + down
            level[c, rows, :] = total
    for x in range(8):
        for c in range(6):
            total = level[c, pl.ds(plane(x), 8), :]
            value = jnp.take_along_axis(total, marks[0], axis=1)
            sums[c] = jnp.where(marks[1] == x, value, sums[c])
    for c in range(6):
        found[FIELDS + c] = sums[c]


def x_ahead(cells, state, pad, level, ahead, xhi, edges, xrow, found, who):
    lane = lanes()
    for c in range(FIELDS):
        ahead[c, 7:8, :] = edges[2, c : c + 1, :]
        ahead[c, 16:17, :] = edges[3, c : c + 1, :]
        ahead[c, 8:16, :] = xhi[c]

    sums = Sums()
    first = [pad[c, pl.ds(plane(7), 8), :] for c in range(FIELDS)]
    for n, number in enumerate(ALONG_X):
        dx, dy, dz = DIRS[number]
        second = scaled([ahead[c, pl.ds(8 + dy, 8), :] for c in range(FIELDS)])
        if dz:
            edge = 127 if dz > 0 else 0
            second = [jnp.where(lane == edge, 0.0, v) for v in turned(second, -dz % 128)]
        at = FIELDS + 4 * n
        shear = [xrow[at + k] for k in range(3)]
        result = pair(first, second, DIRS[number], shear, xrow[at + 3] > 0.5)
        sums.own(result, masks_of(cells, pl.ds(56, 8), number))
    sums.store(level, pl.ds(plane(7), 8), state, pl.ds(56, 8))
    x, y, z, live = who
    sums.collect(found, z, ((y == below()) & (x == 7)) & live)


def x_behind(pad, level, behind, xlo, edges, found, who):
    lane = lanes()
    for c in range(FIELDS + 4 * len(ALONG_X)):
        behind[c, 8:16, :] = xlo[c]
    for c in range(FIELDS):
        behind[c, 7:8, :] = edges[0, c : c + 1, :]
        behind[c, 16:17, :] = edges[1, c : c + 1, :]
    for k in range(4):
        behind[FIELDS + 4 + k, 7:8, :] = edges[0, FIELDS + k : FIELDS + k + 1, :]
        behind[FIELDS + 8 + k, 16:17, :] = edges[1, FIELDS + k : FIELDS + k + 1, :]
    sums = Sums()
    second = [pad[c, pl.ds(plane(0), 8), :] for c in range(FIELDS)]
    for n, number in enumerate(ALONG_X):
        dx, dy, dz = DIRS[number]
        span = pl.ds(8 - dy, 8)
        first = scaled([behind[c, span, :] for c in range(FIELDS)])
        first += [behind[FIELDS + 4 * n + k, span, :] for k in range(4)]
        if dz:
            first = turned(first, dz % 128)
        live = first[13] > 0.5
        if dz:
            live = jnp.logical_and(live, lane != (0 if dz > 0 else 127))
        sums.partner(pair(first[:10], second, DIRS[number], first[10:13], live))
    sums.store(level, pl.ds(plane(0), 8), None, None)
    x, y, z, live = who
    sums.collect(found, z, ((y == below()) & (x == 0)) & live)


def y_high(cells, state, pad, level, yhi, ytop, found, who):
    lane = lanes()
    sub = lax.broadcasted_iota(jnp.int32, (8, 128), 0)
    top_fields = scaled([yhi[c] for c in range(FIELDS)])
    sums = Sums()
    mine_rows = pl.ds(plane(0) + 7, 8, stride=ROWS)
    span = pl.ds(7, 8, stride=8)
    mine = [pad[c, mine_rows, :] for c in range(FIELDS)]
    for n, number in enumerate(UP_Y):
        dx, dy, dz = DIRS[number]
        at = FIELDS + 4 * n
        live = ytop[at + 3] > 0.5
        second = top_fields
        if dx:
            second = turned(second, 7, 0)
            live = jnp.logical_and(live, sub != 7)
        if dz:
            second = turned(second, -dz % 128)
            live = jnp.logical_and(live, lane != (127 if dz > 0 else 0))
        shear = [ytop[at + k] for k in range(3)]
        sums.own(pair(mine, second, DIRS[number], shear, live), masks_of(cells, span, number))
    first = turned(top_fields + [yhi[FIELDS + k] for k in range(4)], 1, 0)
    live = jnp.logical_and(first[13] > 0.5, sub != 0)
    sums.partner(pair(first[:10], mine, DIRS[4], first[10:13], live))
    sums.store(level, mine_rows, state, span)
    x, y, z, live = who
    sums.collect(found, z, ((x == below()) & (y == 7)) & live)


def y_low(cells, state, pad, level, ylo, ylow, found, who):
    lane = lanes()
    sub = lax.broadcasted_iota(jnp.int32, (8, 128), 0)
    low_fields = scaled([ylo[c] for c in range(FIELDS)])
    sums = Sums()
    mine_rows = pl.ds(plane(0), 8, stride=ROWS)
    span = pl.ds(0, 8, stride=8)
    mine = [pad[c, mine_rows, :] for c in range(FIELDS)]
    second = turned(low_fields, 7, 0)
    live = jnp.logical_and(ylow[FIELDS + 3] > 0.5, sub != 7)
    shear = [ylow[FIELDS + k] for k in range(3)]
    sums.own(pair(mine, second, DIRS[4], shear, live), masks_of(cells, span, 4))
    for n, number in enumerate(UP_Y):
        dx, dy, dz = DIRS[number]
        first = low_fields + [ylo[FIELDS + 4 * n + k] for k in range(4)]
        if dx:
            first = turned(first, 1, 0)
        if dz:
            first = turned(first, dz % 128)
        live = first[13] > 0.5
        if dx:
            live = jnp.logical_and(live, sub != 0)
        if dz:
            live = jnp.logical_and(live, lane != (0 if dz > 0 else 127))
        sums.partner(pair(first[:10], mine, DIRS[number], first[10:13], live))
    sums.store(level, mine_rows, state, span)
    x, y, z, live = who
    sums.collect(found, z, ((x == below()) & (y == 0)) & live)


def end_pairs(end, zside, packs, own_packs):
    lane = lanes()
    theirs, ours = (((2, 5, 7), (6, 8)), ((6, 8), (2, 5, 7)))[end]
    top = 1 - end

    def spread(pack, c, top):
        p = (c % 16) * 8 - top
        return pltpu.roll(pack, -p % 128, 1) if p % 128 else pack

    back = [
        pltpu.roll(packs[2 + end, 0], -j % 128, 1) if j else packs[2 + end, 0]
        for j in range(FIELDS + 4)
    ]
    back = scaled(back[:FIELDS]) + back[FIELDS:]
    beyond = scaled(
        [pltpu.roll(packs[4 + end, 0], (7 - 8 * c + top) % 128, 1) for c in range(FIELDS)]
    )
    for k in range(PACKS):
        straight, left = packs[end, k], pltpu.roll(packs[6 + end, 0], 7 - k, 0)
        for c in range(16 * k, min(FULL, 16 * k + 16)):
            zside[end, c, 8:16, :] = spread(straight, c, top)
            zside[end, c, 0:8, :] = spread(left, c, top)
            if c < FIELDS:
                zside[end, c, 16:24, :] = spread(packs[8 + end, 0], c, top)
    own = [spread(own_packs[end, c // 16], c, end) for c in range(FULL)]
    mine = scaled(own[:FIELDS])
    sums = Sums()
    for number, (shear, live, masks) in zip(ours, pick_shear(lambda c: own[c], ours)):
        dx, dy, dz = DIRS[number]
        second = scaled([zside[end, c, pl.ds(8 + dy, 8), :] for c in range(FIELDS)])
        if dx:
            second = [
                jnp.where(lane < 7, v, jnp.where(lane == 7, b, 0.0))
                for b, v in zip(beyond, turned(second, 127))
            ]
        sums.own(pair(mine, second, DIRS[number], shear, live), masks)
    for number in theirs:
        dx, dy, dz = DIRS[number]
        span = pl.ds(8 - dy, 8)
        first = scaled([zside[end, c, span, :] for c in range(FIELDS)])
        ((shear, live, _),) = pick_shear(lambda c: zside[end, c, span, :], (number,))
        first = first + shear + [jnp.where(live, 1.0, 0.0)]
        if dx:
            first = [jnp.where(lane == 0, b, v) for b, v in zip(back, turned(first, 1))]
        sums.partner(pair(first[:10], mine, DIRS[number], first[10:13], first[13] > 0.5))
    return sums


def spread_end(end, sums, level, state):
    lane = lanes()
    edge = 127 * end
    hold = lane == edge
    for x in range(8):
        turn = (edge - x) % 128

        def put(v):
            return jnp.where(hold, pltpu.roll(v, turn, 1) if turn else v, 0.0)

        rows = pl.ds(plane(x), 8)
        here = slice(x * 8, x * 8 + 8)
        for c in range(6):
            level[c, rows, :] = level[c, rows, :] + put(sums.total[c])
        for c in range(3 * SLOTS):
            state[9 + c, here, :] = state[9 + c, here, :] + put(sums.springs[c])


def moved(cells, level, x):
    rows = pl.ds(plane(x), 8)
    here = slice(x * 8, x * 8 + 8)
    sums = [level[c, rows, :] for c in range(6)]
    radius = cells[9, here, :]
    inverse = 1.0 / radius
    push = STEP * inverse * inverse * inverse
    turn = 0.125 * (inverse * inverse) * (inverse * inverse)
    velocity = [cells[3 + k, here, :] + push * sums[k] for k in range(3)]
    velocity[2] = velocity[2] - STEP
    offset = [cells[k, here, :] + STEP * velocity[k] for k in range(3)]
    rotation = [cells[6 + k, here, :] + turn * sums[3 + k] for k in range(3)]
    return offset, velocity, rotation, radius


def below():
    return lax.broadcasted_iota(jnp.int32, (8, 128), 0)


def leaving_cells(leaving):
    names = leaving[0:1, 0:64]
    names = jnp.broadcast_to(jnp.concatenate([names, names], axis=1), (8, 128))
    live = names >= 0
    names = jnp.where(live, names, 0)
    return names // 1024, names // 128 % 8, names % 128, live


def gather_fields(found, cells, leaving, marks):
    x_of, y_of, z_of, live = leaving_cells(leaving)
    plane_of = jnp.where((y_of == below()) & live, x_of, -1)
    marks[0] = z_of
    marks[1] = plane_of
    zero = jnp.zeros((8, 128), jnp.float32)
    values = [zero] * FIELDS
    for x in range(8):
        here = slice(x * 8, x * 8 + 8)
        for c in range(FIELDS):
            value = jnp.take_along_axis(cells[c, here, :], z_of, axis=1)
            values[c] = jnp.where(plane_of == x, value, values[c])
    for c in range(FIELDS):
        found[c] = values[c]
    for c in range(3 * SLOTS):
        found[FIELDS + 6 + c] = zero


def fill_outbox(found, outbox, who):
    lane = lanes()[0:1]
    rows = [
        jnp.sum(found[c], axis=0, keepdims=True) for c in range(FIELDS + 6 + 3 * SLOTS)
    ]
    live = who[3][0:1]
    cell = [w[0:1].astype(jnp.float32) for w in who[:3]]
    starts = [(lax.axis_index(a) * n).astype(jnp.float32) for a, n in zip(AXES, (8, 8, 128))]
    radius = rows[9]
    inverse = 1.0 / jnp.where(live, radius, 1.0)
    push = STEP * inverse * inverse * inverse
    turn = 0.125 * (inverse * inverse) * (inverse * inverse)
    velocity = [rows[3 + k] + push * rows[10 + k] for k in range(3)]
    velocity[2] = jnp.where(live, velocity[2] - STEP, 0.0)
    position = [
        jnp.where(live, rows[k] + STEP * velocity[k] + (starts[k] + cell[k]), 0.0)
        for k in range(3)
    ]
    rotation = [rows[6 + k] + turn * rows[13 + k] for k in range(3)]
    values = position + velocity + rotation + [radius] + rows[16:]
    for c in range(14):
        outbox[c : c + 1, :] = jnp.where(lane < 64, values[c], values[14 + c])


def finish(cells, state, leaving, level):
    lane = lanes()
    wide = jnp.broadcast_to(leaving[0:1, 0:64], (8, 64))
    deep = lax.broadcasted_iota(jnp.int32, (8, 64), 0)
    for x in range(8):
        here = slice(x * 8, x * 8 + 8)
        offset, velocity, rotation, _ = moved(cells, level, x)
        left = [
            jnp.max(jnp.where(wide == (x * 8 + deep) * 128 + z, 1.0, 0.0), axis=1, keepdims=True)
            for z in range(2)
        ]
        staying = 1.0 - jnp.where(lane == 0, left[0], jnp.where(lane == 1, left[1], 0.0))
        for c, v in enumerate(offset + velocity + rotation):
            state[c, here, :] = v * staying
        for c in range(9, 27):
            state[c, here, :] = state[c, here, :] * staying


def on_device(offset, velocity, spin, radius, history, contacts, leaving):
    f32 = jnp.float32
    off = offset.reshape(3, 64, 128)
    vel = velocity.reshape(3, 64, 128)
    spn = spin.reshape(3, 64, 128)
    rad = radius.reshape(1, 64, 128)
    hist = history.reshape(3 * SLOTS, 64, 128)
    con = contacts.reshape(SLOTS, 64, 128)
    vmem = pl.BlockSpec(memory_space=pltpu.VMEM)
    hbm = pl.BlockSpec(memory_space=pltpu.HBM)
    halo_shapes = (
        (FIELDS + 4 * len(ALONG_X), 8, 128),
        (FIELDS, 8, 128),
        (FIELDS + 4 * len(UP_Y), 8, 128),
        (FIELDS + 4 * len(DOWN_Y), 8, 128),
        (4, 16, 128),
        (len(PACK_FROM), PACKS, 8, 128),
        (2, PACKS, 8, 128),
    )
    state, arrivals = pl.pallas_call(
        step_kernel,
        out_shape=[pltpu.VMEM((27, 64, 128), f32), pltpu.VMEM((16, 128), f32)],
        in_specs=[hbm] * 7,
        out_specs=[vmem] * 2,
        scratch_shapes=[pltpu.VMEM(s, f32) for s in halo_shapes]
        + [
            pltpu.VMEM((FULL, 64, 128), f32),
            pltpu.VMEM((SLOTS, 64, 128), jnp.int32),
            pltpu.VMEM((1, 64), jnp.int32),
            pltpu.VMEM((FIELDS + 4 * len(ALONG_X), 8, 128), f32),
            pltpu.VMEM((FIELDS + 4 * len(UP_Y), 8, 128), f32),
            pltpu.VMEM((FIELDS + 4 * len(DOWN_Y), 8, 128), f32),
            pltpu.VMEM((4, 16, 128), f32),
            pltpu.VMEM((2, 1, 8, 128), f32),
            pltpu.VMEM((2, 1, 8, 128), f32),
            pltpu.VMEM((16, 128), f32),
            pltpu.VMEM((FIELDS + 6 + 3 * SLOTS, 8, 128), f32),
            pltpu.VMEM((2, 8, 128), jnp.int32),
            pltpu.VMEM((FIELDS, HEIGHT, 128), f32),
            pltpu.VMEM((FIELDS, HEIGHT, 128), f32),
            pltpu.VMEM((FIELDS, HEIGHT, 128), f32),
            pltpu.VMEM((6, HEIGHT, 128), f32),
            pltpu.VMEM((6, HEIGHT, 128), f32),
            pltpu.VMEM((6, HEIGHT, 128), f32),
            pltpu.VMEM((FIELDS + 4 * len(ALONG_X), ROWS, 128), f32),
            pltpu.VMEM((FIELDS, ROWS, 128), f32),
            pltpu.VMEM((2, FULL, ROWS, 128), f32),
        ],
        compiler_params=pltpu.CompilerParams(
            collective_id=0, has_side_effects=True, vmem_limit_bytes=24 << 20
        ),
        name="step",
    )(*[
        pltpu.with_memory_space_constraint(a, pltpu.HBM)
        for a in (off, vel, spn, rad, hist, con, leaving.reshape(1, 64))
    ])
    moved = jax.ShapeDtypeStruct((3, 64, 128), f32)
    new_off, new_vel, new_spin, new_hist, arrivals = pl.pallas_call(
        write_kernel,
        out_shape=[
            moved, moved, moved,
            jax.ShapeDtypeStruct((3 * SLOTS, 64, 128), f32),
            jax.ShapeDtypeStruct((28, 1, 64), f32),
        ],
        in_specs=[vmem] * 2,
        out_specs=[hbm] * 5,
        scratch_shapes=[pltpu.VMEM((28, 1, 64), f32)],
        compiler_params=pltpu.CompilerParams(vmem_limit_bytes=8 << 20),
        name="write",
    )(state, arrivals)
    return (
        new_off.reshape(3, 8, 8, 128),
        new_vel.reshape(3, 8, 8, 128),
        new_spin.reshape(3, 8, 8, 128),
        new_hist.reshape(SLOTS, 3, 8, 8, 128),
        arrivals.reshape(28, 1, 1, 1, 64),
    )


def solution(mesh):
    placed = (
        P(None, "gx", "gy", "gz"),
        P(None, "gx", "gy", "gz"),
        P(None, "gx", "gy", "gz"),
        P("gx", "gy", "gz"),
        P(None, None, "gx", "gy", "gz"),
        P(None, "gx", "gy", "gz"),
        P("gx", "gy", "gz", None),
    )
    return jax.shard_map(
        on_device,
        mesh=mesh,
        in_specs=placed,
        out_specs=(
            P(None, "gx", "gy", "gz"),
            P(None, "gx", "gy", "gz"),
            P(None, "gx", "gy", "gz"),
            P(None, None, "gx", "gy", "gz"),
            P(None, "gx", "gy", "gz", None),
        ),
        check_vma=False,
    )
```

```python
import jax
import jax.numpy as jnp
from jax import lax
from jax.experimental import pallas as pl
from jax.experimental.pallas import tpu as pltpu
from jax.sharding import PartitionSpec as P

MESH = pl.DeviceIdType.MESH
AXES = ("gx", "gy", "gz")
DIRS = (
    (1, 0, 0),
    (0, 1, 0),
    (0, 0, 1),
    (1, 1, 0),
    (1, -1, 0),
    (1, 0, 1),
    (1, 0, -1),
    (0, 1, 1),
    (0, 1, -1),
)
SLOTS = 6
FIELDS = 10
SHEAR = FIELDS
CODES = FIELDS + 3 * SLOTS
FULL = CODES + SLOTS
PACKS = (FULL * 8 + 127) // 128
STEP = 0.05
TINY = 1e-30

ROWS = 24
HEIGHT = 10 * ROWS

PACK_FROM = (
    (0, 0, -1),
    (0, 0, 1),
    (-1, 0, -1),
    (-1, 0, 1),
    (1, 0, -1),
    (1, 0, 1),
    (0, -1, -1),
    (0, -1, 1),
    (0, 1, -1),
    (0, 1, 1),
)
FLAT_FROM = (
    (-1, 0, 0),
    (1, 0, 0),
    (0, -1, 0),
    (0, 1, 0),
    (-1, -1, 0),
    (-1, 1, 0),
    (1, -1, 0),
    (1, 1, 0),
)
SENDERS = FLAT_FROM + PACK_FROM

ALONG_X = (0, 3, 4, 5, 6)
UP_Y = (1, 3, 7, 8)
DOWN_Y = (4,)

SEND_ORDER = (10, 12, 14, 16, 4, 5, 6, 7, 8, 2, 0, 3, 1, 11, 13, 15, 17, 9)


def plane(x):
    return (x + 1) * ROWS + 8


def step_kernel(*refs):
    pl.run_scoped(
        lambda *sems: step_body(*refs, *sems),
        pltpu.SemaphoreType.DMA((len(SENDERS) + 1,)),
        pltpu.SemaphoreType.DMA((7,)),
        pltpu.SemaphoreType.DMA((len(SENDERS) + 1,)),
    )


def step_body(
    off_hbm, vel_hbm, spin_hbm, rad_hbm, hist_hbm, con_hbm, leaving_hbm,
    state, arrivals,
    xlo, xhi, ylo, yhi, edges, packs, own_packs, cells, codes, leaving,
    xrow, ytop, ylow, rows, corner_x, corner_y, outbox, found, marks, pad, pad_up, pad_down, level, rising, falling, behind, ahead, zside,
    recv_sems, local_sems, send_sems,
):
    here = [lax.axis_index(a) for a in AXES]
    size = [lax.axis_size(a) for a in AXES]

    def exists(step):
        ok = None
        for at, n, s in zip(here, size, step):
            if s == 0:
                continue
            test = at + s < n if s > 0 else at + s >= 0
            ok = test if ok is None else jnp.logical_and(ok, test)
        return ok

    def place(step):
        return tuple(at + s for at, s in zip(here, step))

    loads = [
        pltpu.make_async_copy(off_hbm, cells.at[0:3], local_sems.at[0]),
        pltpu.make_async_copy(vel_hbm, cells.at[3:6], local_sems.at[1]),
        pltpu.make_async_copy(spin_hbm, cells.at[6:9], local_sems.at[2]),
        pltpu.make_async_copy(rad_hbm, cells.at[9:10], local_sems.at[3]),
        pltpu.make_async_copy(hist_hbm, cells.at[SHEAR:CODES], local_sems.at[4]),
        pltpu.make_async_copy(con_hbm, codes, local_sems.at[5]),
        pltpu.make_async_copy(leaving_hbm, leaving, local_sems.at[6]),
    ]
    barrier = pltpu.get_barrier_semaphore()
    expected = jnp.int32(0)
    for step in SENDERS[4:] + SENDERS[:4]:
        there = exists(step)
        expected = expected + there.astype(jnp.int32)

        @pl.when(there)
        def _():
            pl.semaphore_signal(barrier, inc=1, device_id=place(step), device_id_type=MESH)

    for load in loads:
        load.start()
    with jax.named_scope("loadwait"):
        for load in loads[:4]:
            load.wait()
    with jax.named_scope("pack"):
        first_pack = fill_fields(cells, xrow, ytop, ylow, rows)
    with jax.named_scope("loadwait2"):
        for load in loads[4:]:
            load.wait()
    with jax.named_scope("pack2"):
        for s in range(SLOTS):
            cells[CODES + s] = codes[s].astype(jnp.float32)
        fill_sends(cells, own_packs, xrow, ytop, ylow, rows, corner_x, corner_y, first_pack)

    targets = [xlo, xhi, ylo, yhi] + [edges.at[k] for k in range(4)]
    sources = [xrow, cells.at[0:FIELDS, 0:8, :], ytop, ylow] + [rows.at[k] for k in range(4)]
    for k, s in enumerate(PACK_FROM):
        end = 0 if s[2] > 0 else 1
        if s[0] + s[1] == 0:
            targets.append(packs.at[k])
            sources.append(own_packs.at[end])
            continue
        targets.append(packs.at[k, 0:1])
        if s[0] + s[1] > 0:
            sources.append(own_packs.at[end, 0:1])
        else:
            sources.append((corner_x if s[0] else corner_y).at[end])

    def copy(k):
        to = tuple(-s for s in SENDERS[k])
        return pltpu.make_async_remote_copy(
            src_ref=sources[k],
            dst_ref=targets[k],
            send_sem=send_sems.at[k],
            recv_sem=recv_sems.at[k],
            device_id=place(to),
            device_id_type=MESH,
        )

    for k, step in enumerate(SENDERS):

        @pl.when(jnp.logical_not(exists(step)))
        def _():
            targets[k][...] = jnp.zeros(targets[k].shape, jnp.float32)

    with jax.named_scope("fill"):
        fill_padded(cells, pad, pad_up, pad_down, level, rising, falling)
        gather_fields(found, cells, leaving, marks)
    with jax.named_scope("barrier"):
        pl.semaphore_wait(barrier, expected)
    for k in SEND_ORDER:

        @pl.when(exists(tuple(-s for s in SENDERS[k])))
        def _():
            copy(k).start()

    with jax.named_scope("inner"):
        inner_pairs(cells, state, pad, pad_up, pad_down, level, rising, falling, found, marks)

    def receive(which):
        for k in which:

            @pl.when(exists(SENDERS[k]))
            def _():
                copy(k).wait_recv()

    with jax.named_scope("fold"):
        fold(level, rising, falling, found, marks)
        who = leaving_cells(leaving)
    with jax.named_scope("recvz"):
        receive(range(8, 18, 2))
    with jax.named_scope("floor"):
        floor = end_pairs(0, zside, packs, own_packs)
        x, y, z, live = who
        floor.collect(found, x, (y == below()) & (z == 0) & live)
    with jax.named_scope("recvy"):
        receive((2, 3))
    with jax.named_scope("ypairs"):
        later = [
            y_high(cells, state, pad, level, yhi, ytop, found, who),
            y_low(cells, state, pad, level, ylo, ylow, found, who),
        ]
    with jax.named_scope("recvx"):
        receive((0, 1, 4, 5, 6, 7))
    with jax.named_scope("xpairs"):
        x_ahead(cells, state, pad, level, ahead, xhi, edges, xrow, found, who)
        x_behind(pad, level, behind, xlo, edges, found, who)
    with jax.named_scope("outbox"):
        fill_outbox(found, outbox, who)

    last = len(SENDERS)
    fall = pltpu.make_async_remote_copy(
        src_ref=outbox,
        dst_ref=arrivals,
        send_sem=send_sems.at[last],
        recv_sem=recv_sems.at[last],
        device_id=place((0, 0, -1)),
        device_id_type=MESH,
    )

    @pl.when(exists((0, 0, -1)))
    def _():
        fall.start()

    with jax.named_scope("spread"):
        for sums, *where in later:
            sums.store(*where)
        spread_end(0, floor, level, state)
    with jax.named_scope("recvtop"):
        receive((9, 11, 13, 15, 17))
    with jax.named_scope("ceiling"):
        spread_end(1, end_pairs(1, zside, packs, own_packs), level, state)
    with jax.named_scope("final"):
        finish(cells, state, leaving, level)

    for k, step in enumerate(SENDERS):

        @pl.when(exists(tuple(-s for s in step)))
        def _():
            copy(k).wait_send()

    with jax.named_scope("fall"):

        @pl.when(exists((0, 0, 1)))
        def _():
            fall.wait_recv()

    @pl.when(jnp.logical_not(exists((0, 0, 1))))
    def _():
        arrivals[...] = jnp.zeros(arrivals.shape, jnp.float32)

    @pl.when(exists((0, 0, -1)))
    def _():
        fall.wait_send()


def write_kernel(*refs):
    pl.run_scoped(lambda sems: write_body(*refs, sems), pltpu.SemaphoreType.DMA((5,)))


def write_body(
    state, arrivals, new_off, new_vel, new_spin, new_hist, entered, unpacked, sems
):
    copies = [
        pltpu.make_async_copy(state.at[9:27], new_hist, sems.at[0]),
        pltpu.make_async_copy(state.at[0:3], new_off, sems.at[1]),
        pltpu.make_async_copy(state.at[3:6], new_vel, sems.at[2]),
        pltpu.make_async_copy(state.at[6:9], new_spin, sems.at[3]),
        pltpu.make_async_copy(unpacked, entered, sems.at[4]),
    ]
    for copy in copies[:4]:
        copy.start()
    for c in range(14):
        unpacked[c] = arrivals[c : c + 1, 0:64]
        unpacked[14 + c] = arrivals[c : c + 1, 64:128]
    copies[4].start()
    for copy in copies:
        copy.wait()


def cross(a, b):
    return [
        a[1] * b[2] - a[2] * b[1],
        a[2] * b[0] - a[0] * b[2],
        a[0] * b[1] - a[1] * b[0],
    ]


def dot3(a, b):
    return a[0] * b[0] + a[1] * b[1] + a[2] * b[2]


def pair(first, second, direction, shear, live):
    sep = []
    for k in range(3):
        gap = second[k] - first[k]
        sep.append(gap + float(direction[k]) if direction[k] else gap)
    square = dot3(sep, sep)
    inverse = lax.rsqrt(square)
    normal = [s * inverse for s in sep]
    radii = first[9] + second[9]
    overlap = jnp.maximum(radii - square * inverse, 0.0)
    product = first[9] * second[9] * overlap
    contact = product * lax.rsqrt(jnp.maximum(product * radii, TINY))
    contact = jnp.where(live, contact, 0.0)
    surface = cross([first[6 + k] + second[6 + k] for k in range(3)], normal)
    relative = [second[3 + k] - first[3 + k] - surface[k] for k in range(3)]
    approach = dot3(relative, normal)
    sliding = [relative[k] - approach * normal[k] for k in range(3)]
    repulsion = contact * jnp.maximum(10.0 * overlap - 2.0 * approach, 0.0)
    along = dot3(shear, normal)
    spring = [shear[k] - along * normal[k] + STEP * sliding[k] for k in range(3)]
    pull = [8.0 * spring[k] + 1.5 * sliding[k] for k in range(3)]
    size = contact * contact * dot3(pull, pull)
    factor = jnp.minimum(1.0, 0.4 * repulsion * lax.rsqrt(jnp.maximum(size, 0.0025)))
    scale = factor * contact
    tangent = [scale * pull[k] for k in range(3)]
    force = [tangent[k] - repulsion * normal[k] for k in range(3)]
    return force, cross(normal, tangent), [factor * spring[k] for k in range(3)]


def pick_shear(load, numbers):
    codes = [load(CODES + s) for s in range(SLOTS)]
    found = []
    for number in numbers:
        masks = [code == float(number) for code in codes]
        live = masks[0]
        shear = [jnp.where(masks[0], load(SHEAR + k), 0.0) for k in range(3)]
        for s in range(1, SLOTS):
            live = jnp.logical_or(live, masks[s])
            shear = [jnp.where(masks[s], load(SHEAR + 3 * s + k), shear[k]) for k in range(3)]
        found.append((shear, live, masks))
    return found


def scaled(values):
    return values[:6] + [v * values[9] for v in values[6:9]] + [values[9]]


def lanes():
    return lax.broadcasted_iota(jnp.int32, (8, 128), 1)


def add_packed(cells, channels, low, top):
    lane = lanes()
    for c in channels:
        for x in range(8):
            p = (c % 16) * 8 + x
            value = cells[c, x * 8 : x * 8 + 8, :]
            if p:
                value = pltpu.roll(value, p, 1)
            low = jnp.where(lane == p, value, low)
            top = jnp.where(lane == (p - 1) % 128, value, top)
    return low, top


def fill_fields(cells, xrow, ytop, ylow, rows):
    for c in range(FIELDS):
        xrow[c] = cells[c, 56:64, :]
        ytop[c] = cells[c, pl.ds(7, 8, stride=8), :]
        ylow[c] = cells[c, pl.ds(0, 8, stride=8), :]
        for which, row in enumerate((63, 56, 7, 0)):
            rows[which, c : c + 1, :] = cells[c, row : row + 1, :]
    zero = jnp.zeros((8, 128), jnp.float32)
    return add_packed(cells, range(FIELDS), zero, zero)


def fill_sends(cells, own_packs, xrow, ytop, ylow, rows, corner_x, corner_y, first_pack):
    lane = lanes()
    for target, span, numbers in (
        (xrow, pl.ds(56, 8), ALONG_X),
        (ytop, pl.ds(7, 8, stride=8), UP_Y),
        (ylow, pl.ds(0, 8, stride=8), DOWN_Y),
    ):
        found = pick_shear(lambda c: cells[c, span, :], numbers)
        for n, (shear, live, _) in enumerate(found):
            for k in range(3):
                target[FIELDS + 4 * n + k] = shear[k]
            target[FIELDS + 4 * n + 3] = jnp.where(live, 1.0, 0.0)
    for which, row, at in ((0, 7, 1), (1, 0, 2)):
        for k in range(4):
            rows[which, FIELDS + k : FIELDS + k + 1, :] = xrow[
                FIELDS + 4 * at + k, row : row + 1, :
            ]
    for end, at in ((0, 4), (1, 3)):
        corner = jnp.zeros((8, 128), jnp.float32)
        for j in range(FIELDS + 4):
            value = xrow[j if j < FIELDS else j + 4 * at]
            turn = j + end
            corner = jnp.where(lane == j, pltpu.roll(value, turn, 1) if turn else value, corner)
        corner_x[end, 0] = corner
    for k in range(PACKS):
        if k:
            low = top = jnp.zeros((8, 128), jnp.float32)
        else:
            low, top = first_pack
        channels = range(max(16 * k, FIELDS), min(FULL, 16 * k + 16))
        low, top = add_packed(cells, channels, low, top)
        for end, pack in enumerate((low, top)):
            own_packs[end, k] = pack
            corner_y[end, 0, k : k + 1, :] = pack[7:8, :]
    for end in range(2):
        corner_y[end, 0, PACKS:8, :] = jnp.zeros((8 - PACKS, 128), jnp.float32)


def fill_padded(cells, pad, pad_up, pad_down, level, rising, falling):
    lane = lanes()
    zero = jnp.zeros((8, 128), jnp.float32)
    row = jnp.zeros((1, 128), jnp.float32)
    for x in range(8):
        here = slice(x * 8, x * 8 + 8)
        span = pl.ds(plane(x), 8)
        for c, v in enumerate(scaled([cells[c, here, :] for c in range(FIELDS)])):
            pad[c, span, :] = v
            pad_up[c, span, :] = jnp.where(lane == 127, 0.0, pltpu.roll(v, 127, 1))
            pad_down[c, span, :] = jnp.where(lane == 0, 0.0, pltpu.roll(v, 1, 1))
            pad[c, plane(x) - 1 : plane(x), :] = row
            for source in (pad, pad_up, pad_down):
                source[c, plane(x) + 8 : plane(x) + 9, :] = row
    for c in range(FIELDS):
        for source in (pad, pad_up, pad_down):
            source[c, pl.ds(plane(8), 8), :] = zero
        pad[c, plane(8) - 1 : plane(8), :] = row
        pad[c, plane(8) + 8 : plane(8) + 9, :] = row
    for total in (level, rising, falling):
        for c in range(6):
            for x in range(9):
                total[c, pl.ds(plane(x), 8), :] = zero
                total[c, plane(x) - 1 : plane(x), :] = row
                total[c, plane(x) + 8 : plane(x) + 9, :] = row


def inner_pairs(cells, state, pad, pad_up, pad_down, level, rising, falling, found, marks):
    zero = jnp.zeros((8, 128), jnp.float32)

    def body(x, carry):
        base = pl.multiple_of((x + 1) * ROWS + 8, 8)
        here = pl.ds(pl.multiple_of(x * 8, 8), 8)
        first = [pad[c, pl.ds(base, 8), :] for c in range(FIELDS)]
        forces = [zero] * 3
        twists = [zero] * 3
        springs = [zero] * (3 * SLOTS)
        for number, (dx, dy, dz) in enumerate(DIRS):
            span = pl.ds(base + dx * ROWS + dy, 8)
            source = (pad, pad_up, pad_down)[dz]
            total = (level, rising, falling)[dz]
            second = [source[c, span, :] for c in range(FIELDS)]
            ((shear, live, masks),) = pick_shear(lambda c: cells[c, here, :], (number,))
            force, twist, spring = pair(first, second, (dx, dy, dz), shear, live)
            for k in range(3):
                forces[k] = forces[k] + force[k]
                twists[k] = twists[k] + twist[k]
                for s in range(SLOTS):
                    springs[3 * s + k] = jnp.where(masks[s], spring[k], springs[3 * s + k])
                total[k, span, :] = total[k, span, :] - force[k]
                total[3 + k, span, :] = total[3 + k, span, :] + twist[k]
        for k in range(3):
            level[k, pl.ds(base, 8), :] = level[k, pl.ds(base, 8), :] + forces[k]
            level[3 + k, pl.ds(base, 8), :] = level[3 + k, pl.ds(base, 8), :] + twists[k]
        height, chosen = marks[0], marks[1] == x
        for c in range(3 * SLOTS):
            state[9 + c, here, :] = springs[c]
            value = jnp.take_along_axis(springs[c], height, axis=1)
            found[FIELDS + 6 + c] = jnp.where(chosen, value, found[FIELDS + 6 + c])
        return carry

    lax.fori_loop(0, 8, body, 0)


class Sums:
    def __init__(self):
        zero = jnp.zeros((8, 128), jnp.float32)
        self.total = [zero] * 6
        self.springs = [zero] * (3 * SLOTS)

    def own(self, result, masks):
        force, twist, spring = result
        for k in range(3):
            self.total[k] = self.total[k] + force[k]
            self.total[3 + k] = self.total[3 + k] + twist[k]
            for s in range(SLOTS):
                self.springs[3 * s + k] = jnp.where(masks[s], spring[k], self.springs[3 * s + k])

    def partner(self, result):
        force, twist, _ = result
        for k in range(3):
            self.total[k] = self.total[k] - force[k]
            self.total[3 + k] = self.total[3 + k] + twist[k]

    def collect(self, found, index, mask):
        for c, v in enumerate(self.total + self.springs):
            value = jnp.take_along_axis(v, index, axis=1)
            found[FIELDS + c] = found[FIELDS + c] + jnp.where(mask, value, 0.0)

    def store(self, level, rows, state, span):
        for c in range(6):
            level[c, rows, :] = level[c, rows, :] + self.total[c]
        if span is not None:
            for c in range(3 * SLOTS):
                state[9 + c, span, :] = state[9 + c, span, :] + self.springs[c]


def turned(values, amount, axis=1):
    return [pltpu.roll(v, amount, axis) for v in values]


def masks_of(cells, span, number):
    return [cells[CODES + s, span, :] == float(number) for s in range(SLOTS)]


def fold(level, rising, falling, found, marks):
    lane = lanes()
    sums = [jnp.zeros((8, 128), jnp.float32)] * 6
    for x in range(8):
        rows = pl.ds(plane(x), 8)
        for c in range(6):
            up = jnp.where(lane == 0, 0.0, pltpu.roll(rising[c, rows, :], 1, 1))
            down = jnp.where(lane == 127, 0.0, pltpu.roll(falling[c, rows, :], 127, 1))
            total = level[c, rows, :] + up + down
            level[c, rows, :] = total
    for x in range(8):
        for c in range(6):
            total = level[c, pl.ds(plane(x), 8), :]
            value = jnp.take_along_axis(total, marks[0], axis=1)
            sums[c] = jnp.where(marks[1] == x, value, sums[c])
    for c in range(6):
        found[FIELDS + c] = sums[c]


def x_ahead(cells, state, pad, level, ahead, xhi, edges, xrow, found, who):
    lane = lanes()
    for c in range(FIELDS):
        ahead[c, 7:8, :] = edges[2, c : c + 1, :]
        ahead[c, 16:17, :] = edges[3, c : c + 1, :]
        ahead[c, 8:16, :] = xhi[c]

    sums = Sums()
    first = [pad[c, pl.ds(plane(7), 8), :] for c in range(FIELDS)]
    for n, number in enumerate(ALONG_X):
        dx, dy, dz = DIRS[number]
        second = scaled([ahead[c, pl.ds(8 + dy, 8), :] for c in range(FIELDS)])
        if dz:
            edge = 127 if dz > 0 else 0
            second = [jnp.where(lane == edge, 0.0, v) for v in turned(second, -dz % 128)]
        at = FIELDS + 4 * n
        shear = [xrow[at + k] for k in range(3)]
        result = pair(first, second, DIRS[number], shear, xrow[at + 3] > 0.5)
        sums.own(result, masks_of(cells, pl.ds(56, 8), number))
    sums.store(level, pl.ds(plane(7), 8), state, pl.ds(56, 8))
    x, y, z, live = who
    sums.collect(found, z, ((y == below()) & (x == 7)) & live)


def x_behind(pad, level, behind, xlo, edges, found, who):
    lane = lanes()
    for c in range(FIELDS + 4 * len(ALONG_X)):
        behind[c, 8:16, :] = xlo[c]
    for c in range(FIELDS):
        behind[c, 7:8, :] = edges[0, c : c + 1, :]
        behind[c, 16:17, :] = edges[1, c : c + 1, :]
    for k in range(4):
        behind[FIELDS + 4 + k, 7:8, :] = edges[0, FIELDS + k : FIELDS + k + 1, :]
        behind[FIELDS + 8 + k, 16:17, :] = edges[1, FIELDS + k : FIELDS + k + 1, :]
    sums = Sums()
    second = [pad[c, pl.ds(plane(0), 8), :] for c in range(FIELDS)]
    for n, number in enumerate(ALONG_X):
        dx, dy, dz = DIRS[number]
        span = pl.ds(8 - dy, 8)
        first = scaled([behind[c, span, :] for c in range(FIELDS)])
        first += [behind[FIELDS + 4 * n + k, span, :] for k in range(4)]
        if dz:
            first = turned(first, dz % 128)
        live = first[13] > 0.5
        if dz:
            live = jnp.logical_and(live, lane != (0 if dz > 0 else 127))
        sums.partner(pair(first[:10], second, DIRS[number], first[10:13], live))
    sums.store(level, pl.ds(plane(0), 8), None, None)
    x, y, z, live = who
    sums.collect(found, z, ((y == below()) & (x == 0)) & live)


def y_high(cells, state, pad, level, yhi, ytop, found, who):
    lane = lanes()
    sub = lax.broadcasted_iota(jnp.int32, (8, 128), 0)
    top_fields = scaled([yhi[c] for c in range(FIELDS)])
    sums = Sums()
    mine_rows = pl.ds(plane(0) + 7, 8, stride=ROWS)
    span = pl.ds(7, 8, stride=8)
    mine = [pad[c, mine_rows, :] for c in range(FIELDS)]
    for n, number in enumerate(UP_Y):
        dx, dy, dz = DIRS[number]
        at = FIELDS + 4 * n
        live = ytop[at + 3] > 0.5
        second = top_fields
        if dx:
            second = turned(second, 7, 0)
            live = jnp.logical_and(live, sub != 7)
        if dz:
            second = turned(second, -dz % 128)
            live = jnp.logical_and(live, lane != (127 if dz > 0 else 0))
        shear = [ytop[at + k] for k in range(3)]
        sums.own(pair(mine, second, DIRS[number], shear, live), masks_of(cells, span, number))
    first = turned(top_fields + [yhi[FIELDS + k] for k in range(4)], 1, 0)
    live = jnp.logical_and(first[13] > 0.5, sub != 0)
    sums.partner(pair(first[:10], mine, DIRS[4], first[10:13], live))
    x, y, z, live = who
    sums.collect(found, z, ((x == below()) & (y == 7)) & live)
    return sums, level, mine_rows, state, span


def y_low(cells, state, pad, level, ylo, ylow, found, who):
    lane = lanes()
    sub = lax.broadcasted_iota(jnp.int32, (8, 128), 0)
    low_fields = scaled([ylo[c] for c in range(FIELDS)])
    sums = Sums()
    mine_rows = pl.ds(plane(0), 8, stride=ROWS)
    span = pl.ds(0, 8, stride=8)
    mine = [pad[c, mine_rows, :] for c in range(FIELDS)]
    second = turned(low_fields, 7, 0)
    live = jnp.logical_and(ylow[FIELDS + 3] > 0.5, sub != 7)
    shear = [ylow[FIELDS + k] for k in range(3)]
    sums.own(pair(mine, second, DIRS[4], shear, live), masks_of(cells, span, 4))
    for n, number in enumerate(UP_Y):
        dx, dy, dz = DIRS[number]
        first = low_fields + [ylo[FIELDS + 4 * n + k] for k in range(4)]
        if dx:
            first = turned(first, 1, 0)
        if dz:
            first = turned(first, dz % 128)
        live = first[13] > 0.5
        if dx:
            live = jnp.logical_and(live, sub != 0)
        if dz:
            live = jnp.logical_and(live, lane != (0 if dz > 0 else 127))
        sums.partner(pair(first[:10], mine, DIRS[number], first[10:13], live))
    x, y, z, live = who
    sums.collect(found, z, ((x == below()) & (y == 0)) & live)
    return sums, level, mine_rows, state, span


def end_pairs(end, zside, packs, own_packs):
    lane = lanes()
    theirs, ours = (((2, 5, 7), (6, 8)), ((6, 8), (2, 5, 7)))[end]
    top = 1 - end

    def spread(pack, c, top):
        p = (c % 16) * 8 - top
        return pltpu.roll(pack, -p % 128, 1) if p % 128 else pack

    back = [
        pltpu.roll(packs[2 + end, 0], -j % 128, 1) if j else packs[2 + end, 0]
        for j in range(FIELDS + 4)
    ]
    back = scaled(back[:FIELDS]) + back[FIELDS:]
    beyond = scaled(
        [pltpu.roll(packs[4 + end, 0], (7 - 8 * c + top) % 128, 1) for c in range(FIELDS)]
    )
    for k in range(PACKS):
        straight, left = packs[end, k], pltpu.roll(packs[6 + end, 0], 7 - k, 0)
        for c in range(16 * k, min(FULL, 16 * k + 16)):
            zside[end, c, 8:16, :] = spread(straight, c, top)
            zside[end, c, 0:8, :] = spread(left, c, top)
            if c < FIELDS:
                zside[end, c, 16:24, :] = spread(packs[8 + end, 0], c, top)
    own = [spread(own_packs[end, c // 16], c, end) for c in range(FULL)]
    mine = scaled(own[:FIELDS])
    sums = Sums()
    for number, (shear, live, masks) in zip(ours, pick_shear(lambda c: own[c], ours)):
        dx, dy, dz = DIRS[number]
        second = scaled([zside[end, c, pl.ds(8 + dy, 8), :] for c in range(FIELDS)])
        if dx:
            second = [
                jnp.where(lane < 7, v, jnp.where(lane == 7, b, 0.0))
                for b, v in zip(beyond, turned(second, 127))
            ]
        sums.own(pair(mine, second, DIRS[number], shear, live), masks)
    for number in theirs:
        dx, dy, dz = DIRS[number]
        span = pl.ds(8 - dy, 8)
        first = scaled([zside[end, c, span, :] for c in range(FIELDS)])
        ((shear, live, _),) = pick_shear(lambda c: zside[end, c, span, :], (number,))
        first = first + shear + [jnp.where(live, 1.0, 0.0)]
        if dx:
            first = [jnp.where(lane == 0, b, v) for b, v in zip(back, turned(first, 1))]
        sums.partner(pair(first[:10], mine, DIRS[number], first[10:13], first[13] > 0.5))
    return sums


def spread_end(end, sums, level, state):
    lane = lanes()
    edge = 127 * end
    hold = lane == edge
    for x in range(8):
        turn = (edge - x) % 128

        def put(v):
            return jnp.where(hold, pltpu.roll(v, turn, 1) if turn else v, 0.0)

        rows = pl.ds(plane(x), 8)
        here = slice(x * 8, x * 8 + 8)
        for c in range(6):
            level[c, rows, :] = level[c, rows, :] + put(sums.total[c])
        for c in range(3 * SLOTS):
            state[9 + c, here, :] = state[9 + c, here, :] + put(sums.springs[c])


def moved(cells, level, x):
    rows = pl.ds(plane(x), 8)
    here = slice(x * 8, x * 8 + 8)
    sums = [level[c, rows, :] for c in range(6)]
    radius = cells[9, here, :]
    inverse = 1.0 / radius
    push = STEP * inverse * inverse * inverse
    turn = 0.125 * (inverse * inverse) * (inverse * inverse)
    velocity = [cells[3 + k, here, :] + push * sums[k] for k in range(3)]
    velocity[2] = velocity[2] - STEP
    offset = [cells[k, here, :] + STEP * velocity[k] for k in range(3)]
    rotation = [cells[6 + k, here, :] + turn * sums[3 + k] for k in range(3)]
    return offset, velocity, rotation, radius


def below():
    return lax.broadcasted_iota(jnp.int32, (8, 128), 0)


def leaving_cells(leaving):
    names = leaving[0:1, 0:64]
    names = jnp.broadcast_to(jnp.concatenate([names, names], axis=1), (8, 128))
    live = names >= 0
    names = jnp.where(live, names, 0)
    return names // 1024, names // 128 % 8, names % 128, live


def gather_fields(found, cells, leaving, marks):
    x_of, y_of, z_of, live = leaving_cells(leaving)
    plane_of = jnp.where((y_of == below()) & live, x_of, -1)
    marks[0] = z_of
    marks[1] = plane_of
    zero = jnp.zeros((8, 128), jnp.float32)
    values = [zero] * FIELDS
    for x in range(8):
        here = slice(x * 8, x * 8 + 8)
        for c in range(FIELDS):
            value = jnp.take_along_axis(cells[c, here, :], z_of, axis=1)
            values[c] = jnp.where(plane_of == x, value, values[c])
    for c in range(FIELDS):
        found[c] = values[c]
    for c in range(3 * SLOTS):
        found[FIELDS + 6 + c] = zero


def fill_outbox(found, outbox, who):
    lane = lanes()[0:1]
    rows = [
        jnp.sum(found[c], axis=0, keepdims=True) for c in range(FIELDS + 6 + 3 * SLOTS)
    ]
    live = who[3][0:1]
    cell = [w[0:1].astype(jnp.float32) for w in who[:3]]
    starts = [(lax.axis_index(a) * n).astype(jnp.float32) for a, n in zip(AXES, (8, 8, 128))]
    radius = rows[9]
    inverse = 1.0 / jnp.where(live, radius, 1.0)
    push = STEP * inverse * inverse * inverse
    turn = 0.125 * (inverse * inverse) * (inverse * inverse)
    velocity = [rows[3 + k] + push * rows[10 + k] for k in range(3)]
    velocity[2] = jnp.where(live, velocity[2] - STEP, 0.0)
    position = [
        jnp.where(live, rows[k] + STEP * velocity[k] + (starts[k] + cell[k]), 0.0)
        for k in range(3)
    ]
    rotation = [rows[6 + k] + turn * rows[13 + k] for k in range(3)]
    values = position + velocity + rotation + [radius] + rows[16:]
    for c in range(14):
        outbox[c : c + 1, :] = jnp.where(lane < 64, values[c], values[14 + c])


def finish(cells, state, leaving, level):
    lane = lanes()
    wide = jnp.broadcast_to(leaving[0:1, 0:64], (8, 64))
    deep = lax.broadcasted_iota(jnp.int32, (8, 64), 0)
    for x in range(8):
        here = slice(x * 8, x * 8 + 8)
        offset, velocity, rotation, _ = moved(cells, level, x)
        left = [
            jnp.max(jnp.where(wide == (x * 8 + deep) * 128 + z, 1.0, 0.0), axis=1, keepdims=True)
            for z in range(2)
        ]
        staying = 1.0 - jnp.where(lane == 0, left[0], jnp.where(lane == 1, left[1], 0.0))
        for c, v in enumerate(offset + velocity + rotation):
            state[c, here, :] = v * staying
        for c in range(9, 27):
            state[c, here, :] = state[c, here, :] * staying


def on_device(offset, velocity, spin, radius, history, contacts, leaving):
    f32 = jnp.float32
    off = offset.reshape(3, 64, 128)
    vel = velocity.reshape(3, 64, 128)
    spn = spin.reshape(3, 64, 128)
    rad = radius.reshape(1, 64, 128)
    hist = history.reshape(3 * SLOTS, 64, 128)
    con = contacts.reshape(SLOTS, 64, 128)
    vmem = pl.BlockSpec(memory_space=pltpu.VMEM)
    hbm = pl.BlockSpec(memory_space=pltpu.HBM)
    halo_shapes = (
        (FIELDS + 4 * len(ALONG_X), 8, 128),
        (FIELDS, 8, 128),
        (FIELDS + 4 * len(UP_Y), 8, 128),
        (FIELDS + 4 * len(DOWN_Y), 8, 128),
        (4, 16, 128),
        (len(PACK_FROM), PACKS, 8, 128),
        (2, PACKS, 8, 128),
    )
    state, arrivals = pl.pallas_call(
        step_kernel,
        out_shape=[pltpu.VMEM((27, 64, 128), f32), pltpu.VMEM((16, 128), f32)],
        in_specs=[hbm] * 7,
        out_specs=[vmem] * 2,
        scratch_shapes=[pltpu.VMEM(s, f32) for s in halo_shapes]
        + [
            pltpu.VMEM((FULL, 64, 128), f32),
            pltpu.VMEM((SLOTS, 64, 128), jnp.int32),
            pltpu.VMEM((1, 64), jnp.int32),
            pltpu.VMEM((FIELDS + 4 * len(ALONG_X), 8, 128), f32),
            pltpu.VMEM((FIELDS + 4 * len(UP_Y), 8, 128), f32),
            pltpu.VMEM((FIELDS + 4 * len(DOWN_Y), 8, 128), f32),
            pltpu.VMEM((4, 16, 128), f32),
            pltpu.VMEM((2, 1, 8, 128), f32),
            pltpu.VMEM((2, 1, 8, 128), f32),
            pltpu.VMEM((16, 128), f32),
            pltpu.VMEM((FIELDS + 6 + 3 * SLOTS, 8, 128), f32),
            pltpu.VMEM((2, 8, 128), jnp.int32),
            pltpu.VMEM((FIELDS, HEIGHT, 128), f32),
            pltpu.VMEM((FIELDS, HEIGHT, 128), f32),
            pltpu.VMEM((FIELDS, HEIGHT, 128), f32),
            pltpu.VMEM((6, HEIGHT, 128), f32),
            pltpu.VMEM((6, HEIGHT, 128), f32),
            pltpu.VMEM((6, HEIGHT, 128), f32),
            pltpu.VMEM((FIELDS + 4 * len(ALONG_X), ROWS, 128), f32),
            pltpu.VMEM((FIELDS, ROWS, 128), f32),
            pltpu.VMEM((2, FULL, ROWS, 128), f32),
        ],
        compiler_params=pltpu.CompilerParams(
            collective_id=0, has_side_effects=True, vmem_limit_bytes=24 << 20
        ),
        name="step",
    )(*[
        pltpu.with_memory_space_constraint(a, pltpu.HBM)
        for a in (off, vel, spn, rad, hist, con, leaving.reshape(1, 64))
    ])
    moved = jax.ShapeDtypeStruct((3, 64, 128), f32)
    new_off, new_vel, new_spin, new_hist, arrivals = pl.pallas_call(
        write_kernel,
        out_shape=[
            moved, moved, moved,
            jax.ShapeDtypeStruct((3 * SLOTS, 64, 128), f32),
            jax.ShapeDtypeStruct((28, 1, 64), f32),
        ],
        in_specs=[vmem] * 2,
        out_specs=[hbm] * 5,
        scratch_shapes=[pltpu.VMEM((28, 1, 64), f32)],
        compiler_params=pltpu.CompilerParams(vmem_limit_bytes=8 << 20),
        name="write",
    )(state, arrivals)
    return (
        new_off.reshape(3, 8, 8, 128),
        new_vel.reshape(3, 8, 8, 128),
        new_spin.reshape(3, 8, 8, 128),
        new_hist.reshape(SLOTS, 3, 8, 8, 128),
        arrivals.reshape(28, 1, 1, 1, 64),
    )


def solution(mesh):
    placed = (
        P(None, "gx", "gy", "gz"),
        P(None, "gx", "gy", "gz"),
        P(None, "gx", "gy", "gz"),
        P("gx", "gy", "gz"),
        P(None, None, "gx", "gy", "gz"),
        P(None, "gx", "gy", "gz"),
        P("gx", "gy", "gz", None),
    )
    return jax.shard_map(
        on_device,
        mesh=mesh,
        in_specs=placed,
        out_specs=(
            P(None, "gx", "gy", "gz"),
            P(None, "gx", "gy", "gz"),
            P(None, "gx", "gy", "gz"),
            P(None, None, "gx", "gy", "gz"),
            P(None, "gx", "gy", "gz", None),
        ),
        check_vma=False,
    )
```

```python
import jax
import jax.numpy as jnp
from jax import lax
from jax.experimental import pallas as pl
from jax.experimental.pallas import tpu as pltpu
from jax.sharding import PartitionSpec as P

MESH = pl.DeviceIdType.MESH
AXES = ("gx", "gy", "gz")
DIRS = (
    (1, 0, 0),
    (0, 1, 0),
    (0, 0, 1),
    (1, 1, 0),
    (1, -1, 0),
    (1, 0, 1),
    (1, 0, -1),
    (0, 1, 1),
    (0, 1, -1),
)
SLOTS = 6
FIELDS = 10
SHEAR = FIELDS
CODES = FIELDS + 3 * SLOTS
FULL = CODES + SLOTS
PACKS = (FULL * 8 + 127) // 128
STEP = 0.05
TINY = 1e-30

ROWS = 24
HEIGHT = 10 * ROWS

PACK_FROM = (
    (0, 0, -1),
    (0, 0, 1),
    (-1, 0, -1),
    (-1, 0, 1),
    (1, 0, -1),
    (1, 0, 1),
    (0, -1, -1),
    (0, -1, 1),
    (0, 1, -1),
    (0, 1, 1),
)
FLAT_FROM = (
    (-1, 0, 0),
    (1, 0, 0),
    (0, -1, 0),
    (0, 1, 0),
    (-1, -1, 0),
    (-1, 1, 0),
    (1, -1, 0),
    (1, 1, 0),
)
SENDERS = FLAT_FROM + PACK_FROM

ALONG_X = (0, 3, 4, 5, 6)
UP_Y = (1, 3, 7, 8)
DOWN_Y = (4,)

SEND_ORDER = (10, 12, 14, 16, 4, 5, 6, 7, 8, 2, 0, 3, 1, 11, 13, 15, 17, 9)


def plane(x):
    return (x + 1) * ROWS + 8


def step_kernel(*refs):
    pl.run_scoped(
        lambda *sems: step_body(*refs, *sems),
        pltpu.SemaphoreType.DMA((len(SENDERS) + 1,)),
        pltpu.SemaphoreType.DMA((7,)),
        pltpu.SemaphoreType.DMA((len(SENDERS) + 1,)),
    )


def step_body(
    off_hbm, vel_hbm, spin_hbm, rad_hbm, hist_hbm, con_hbm, leaving_hbm,
    state, arrivals,
    xlo, xhi, ylo, yhi, edges, packs, own_packs, cells, codes, leaving,
    xrow, ytop, ylow, rows, corner_x, corner_y, outbox, found, marks, pad, pad_up, pad_down, level, rising, falling, behind, ahead, zside,
    recv_sems, local_sems, send_sems,
):
    here = [lax.axis_index(a) for a in AXES]
    size = [lax.axis_size(a) for a in AXES]

    def exists(step):
        ok = None
        for at, n, s in zip(here, size, step):
            if s == 0:
                continue
            test = at + s < n if s > 0 else at + s >= 0
            ok = test if ok is None else jnp.logical_and(ok, test)
        return ok

    def place(step):
        return tuple(at + s for at, s in zip(here, step))

    loads = [
        pltpu.make_async_copy(off_hbm, cells.at[0:3], local_sems.at[0]),
        pltpu.make_async_copy(vel_hbm, cells.at[3:6], local_sems.at[1]),
        pltpu.make_async_copy(spin_hbm, cells.at[6:9], local_sems.at[2]),
        pltpu.make_async_copy(rad_hbm, cells.at[9:10], local_sems.at[3]),
        pltpu.make_async_copy(hist_hbm, cells.at[SHEAR:CODES], local_sems.at[4]),
        pltpu.make_async_copy(con_hbm, codes, local_sems.at[5]),
        pltpu.make_async_copy(leaving_hbm, leaving, local_sems.at[6]),
    ]
    barrier = pltpu.get_barrier_semaphore()
    expected = jnp.int32(0)
    for step in SENDERS[4:] + SENDERS[:4]:
        there = exists(step)
        expected = expected + there.astype(jnp.int32)

        @pl.when(there)
        def _():
            pl.semaphore_signal(barrier, inc=1, device_id=place(step), device_id_type=MESH)

    for load in loads:
        load.start()
    with jax.named_scope("loadwait"):
        for load in loads[:4]:
            load.wait()
    with jax.named_scope("pack"):
        first_pack = fill_fields(cells, xrow, ytop, ylow, rows)
    with jax.named_scope("loadwait2"):
        for load in loads[4:]:
            load.wait()
    with jax.named_scope("pack2"):
        for s in range(SLOTS):
            cells[CODES + s] = codes[s].astype(jnp.float32)
        fill_sends(cells, own_packs, xrow, ytop, ylow, rows, corner_x, corner_y, first_pack)

    targets = [xlo, xhi, ylo, yhi] + [edges.at[k] for k in range(4)]
    sources = [xrow, cells.at[0:FIELDS, 0:8, :], ytop, ylow] + [rows.at[k] for k in range(4)]
    for k, s in enumerate(PACK_FROM):
        end = 0 if s[2] > 0 else 1
        if s[0] + s[1] == 0:
            targets.append(packs.at[k])
            sources.append(own_packs.at[end])
            continue
        targets.append(packs.at[k, 0:1])
        if s[0] + s[1] > 0:
            sources.append(own_packs.at[end, 0:1])
        else:
            sources.append((corner_x if s[0] else corner_y).at[end])

    def copy(k):
        to = tuple(-s for s in SENDERS[k])
        return pltpu.make_async_remote_copy(
            src_ref=sources[k],
            dst_ref=targets[k],
            send_sem=send_sems.at[k],
            recv_sem=recv_sems.at[k],
            device_id=place(to),
            device_id_type=MESH,
        )

    for k, step in enumerate(SENDERS):

        @pl.when(jnp.logical_not(exists(step)))
        def _():
            targets[k][...] = jnp.zeros(targets[k].shape, jnp.float32)

    with jax.named_scope("fill"):
        fill_padded(cells, pad, pad_up, pad_down, level, rising, falling)
        gather_fields(found, cells, leaving, marks)
    with jax.named_scope("barrier"):
        pl.semaphore_wait(barrier, expected)
    for k in SEND_ORDER:

        @pl.when(exists(tuple(-s for s in SENDERS[k])))
        def _():
            copy(k).start()

    with jax.named_scope("inner"):
        inner_pairs(cells, state, pad, pad_up, pad_down, level, rising, falling, found, marks)

    def receive(which):
        for k in which:

            @pl.when(exists(SENDERS[k]))
            def _():
                copy(k).wait_recv()

    with jax.named_scope("fold"):
        fold(level, rising, falling, found, marks)
        who = leaving_cells(leaving)
    with jax.named_scope("recvz"):
        receive(range(8, 18, 2))
    with jax.named_scope("floor"):
        floor = end_pairs(0, zside, packs, own_packs)
        x, y, z, live = who
        floor.collect(found, x, (y == below()) & (z == 0) & live)
    with jax.named_scope("recvy"):
        receive((2, 3))
    with jax.named_scope("ypairs"):
        y_high(cells, state, pad, level, yhi, ytop, found, who)
        y_low(cells, state, pad, level, ylo, ylow, found, who)
    with jax.named_scope("recvx"):
        receive((0, 1, 4, 5, 6, 7))
    with jax.named_scope("xpairs"):
        x_ahead(cells, state, pad, level, ahead, xhi, edges, xrow, found, who)
        x_behind(pad, level, behind, xlo, edges, found, who)
    with jax.named_scope("outbox"):
        fill_outbox(found, outbox, who)

    last = len(SENDERS)
    fall = pltpu.make_async_remote_copy(
        src_ref=outbox,
        dst_ref=arrivals,
        send_sem=send_sems.at[last],
        recv_sem=recv_sems.at[last],
        device_id=place((0, 0, -1)),
        device_id_type=MESH,
    )

    @pl.when(exists((0, 0, -1)))
    def _():
        fall.start()

    with jax.named_scope("spread"):
        spread_end(0, floor, level, state)
    with jax.named_scope("recvtop"):
        receive((9, 11, 13, 15, 17))
    with jax.named_scope("ceiling"):
        spread_end(1, end_pairs(1, zside, packs, own_packs), level, state)
    with jax.named_scope("final"):
        finish(cells, state, leaving, level)

    for k, step in enumerate(SENDERS):

        @pl.when(exists(tuple(-s for s in step)))
        def _():
            copy(k).wait_send()

    with jax.named_scope("fall"):

        @pl.when(exists((0, 0, 1)))
        def _():
            fall.wait_recv()

    @pl.when(jnp.logical_not(exists((0, 0, 1))))
    def _():
        arrivals[...] = jnp.zeros(arrivals.shape, jnp.float32)

    @pl.when(exists((0, 0, -1)))
    def _():
        fall.wait_send()


def write_kernel(*refs):
    pl.run_scoped(lambda sems: write_body(*refs, sems), pltpu.SemaphoreType.DMA((5,)))


def write_body(
    state, arrivals, new_off, new_vel, new_spin, new_hist, entered, unpacked, sems
):
    copies = [
        pltpu.make_async_copy(state.at[9:27], new_hist, sems.at[0]),
        pltpu.make_async_copy(state.at[0:3], new_off, sems.at[1]),
        pltpu.make_async_copy(state.at[3:6], new_vel, sems.at[2]),
        pltpu.make_async_copy(state.at[6:9], new_spin, sems.at[3]),
        pltpu.make_async_copy(unpacked, entered, sems.at[4]),
    ]
    for copy in copies[:4]:
        copy.start()
    for c in range(14):
        unpacked[c] = arrivals[c : c + 1, 0:64]
        unpacked[14 + c] = arrivals[c : c + 1, 64:128]
    copies[4].start()
    for copy in copies:
        copy.wait()


def cross(a, b):
    return [
        a[1] * b[2] - a[2] * b[1],
        a[2] * b[0] - a[0] * b[2],
        a[0] * b[1] - a[1] * b[0],
    ]


def dot3(a, b):
    return a[0] * b[0] + a[1] * b[1] + a[2] * b[2]


def pair(first, second, direction, shear, live):
    sep = []
    for k in range(3):
        gap = second[k] - first[k]
        sep.append(gap + float(direction[k]) if direction[k] else gap)
    square = dot3(sep, sep)
    inverse = lax.rsqrt(square)
    normal = [s * inverse for s in sep]
    radii = first[9] + second[9]
    overlap = jnp.maximum(radii - square * inverse, 0.0)
    product = first[9] * second[9] * overlap
    contact = product * lax.rsqrt(jnp.maximum(product * radii, TINY))
    contact = jnp.where(live, contact, 0.0)
    surface = cross([first[6 + k] + second[6 + k] for k in range(3)], normal)
    relative = [second[3 + k] - first[3 + k] - surface[k] for k in range(3)]
    approach = dot3(relative, normal)
    sliding = [relative[k] - approach * normal[k] for k in range(3)]
    repulsion = contact * jnp.maximum(10.0 * overlap - 2.0 * approach, 0.0)
    along = dot3(shear, normal)
    spring = [shear[k] - along * normal[k] + STEP * sliding[k] for k in range(3)]
    pull = [8.0 * spring[k] + 1.5 * sliding[k] for k in range(3)]
    size = contact * contact * dot3(pull, pull)
    factor = jnp.minimum(1.0, 0.4 * repulsion * lax.rsqrt(jnp.maximum(size, 0.0025)))
    scale = factor * contact
    tangent = [scale * pull[k] for k in range(3)]
    force = [tangent[k] - repulsion * normal[k] for k in range(3)]
    return force, cross(normal, tangent), [factor * spring[k] for k in range(3)]


def pick_shear(load, numbers):
    codes = [load(CODES + s) for s in range(SLOTS)]
    found = []
    for number in numbers:
        masks = [code == float(number) for code in codes]
        live = masks[0]
        shear = [jnp.where(masks[0], load(SHEAR + k), 0.0) for k in range(3)]
        for s in range(1, SLOTS):
            live = jnp.logical_or(live, masks[s])
            shear = [jnp.where(masks[s], load(SHEAR + 3 * s + k), shear[k]) for k in range(3)]
        found.append((shear, live, masks))
    return found


def scaled(values):
    return values[:6] + [v * values[9] for v in values[6:9]] + [values[9]]


def lanes():
    return lax.broadcasted_iota(jnp.int32, (8, 128), 1)


def add_packed(cells, channels, low, top):
    lane = lanes()
    for c in channels:
        for x in range(8):
            p = (c % 16) * 8 + x
            value = cells[c, x * 8 : x * 8 + 8, :]
            if p:
                value = pltpu.roll(value, p, 1)
            low = jnp.where(lane == p, value, low)
            top = jnp.where(lane == (p - 1) % 128, value, top)
    return low, top


def fill_fields(cells, xrow, ytop, ylow, rows):
    for c in range(FIELDS):
        xrow[c] = cells[c, 56:64, :]
        ytop[c] = cells[c, pl.ds(7, 8, stride=8), :]
        ylow[c] = cells[c, pl.ds(0, 8, stride=8), :]
        for which, row in enumerate((63, 56, 7, 0)):
            rows[which, c : c + 1, :] = cells[c, row : row + 1, :]
    zero = jnp.zeros((8, 128), jnp.float32)
    return add_packed(cells, range(FIELDS), zero, zero)


def fill_sends(cells, own_packs, xrow, ytop, ylow, rows, corner_x, corner_y, first_pack):
    lane = lanes()
    for target, span, numbers in (
        (xrow, pl.ds(56, 8), ALONG_X),
        (ytop, pl.ds(7, 8, stride=8), UP_Y),
        (ylow, pl.ds(0, 8, stride=8), DOWN_Y),
    ):
        found = pick_shear(lambda c: cells[c, span, :], numbers)
        for n, (shear, live, _) in enumerate(found):
            for k in range(3):
                target[FIELDS + 4 * n + k] = shear[k]
            target[FIELDS + 4 * n + 3] = jnp.where(live, 1.0, 0.0)
    for which, row, at in ((0, 7, 1), (1, 0, 2)):
        for k in range(4):
            rows[which, FIELDS + k : FIELDS + k + 1, :] = xrow[
                FIELDS + 4 * at + k, row : row + 1, :
            ]
    for end, at in ((0, 4), (1, 3)):
        corner = jnp.zeros((8, 128), jnp.float32)
        for j in range(FIELDS + 4):
            value = xrow[j if j < FIELDS else j + 4 * at]
            turn = j + end
            corner = jnp.where(lane == j, pltpu.roll(value, turn, 1) if turn else value, corner)
        corner_x[end, 0] = corner
    for k in range(PACKS):
        if k:
            low = top = jnp.zeros((8, 128), jnp.float32)
        else:
            low, top = first_pack
        channels = range(max(16 * k, FIELDS), min(FULL, 16 * k + 16))
        low, top = add_packed(cells, channels, low, top)
        for end, pack in enumerate((low, top)):
            own_packs[end, k] = pack
            corner_y[end, 0, k : k + 1, :] = pack[7:8, :]
    for end in range(2):
        corner_y[end, 0, PACKS:8, :] = jnp.zeros((8 - PACKS, 128), jnp.float32)


def fill_padded(cells, pad, pad_up, pad_down, level, rising, falling):
    lane = lanes()
    zero = jnp.zeros((8, 128), jnp.float32)
    row = jnp.zeros((1, 128), jnp.float32)
    for x in range(8):
        here = slice(x * 8, x * 8 + 8)
        span = pl.ds(plane(x), 8)
        for c, v in enumerate(scaled([cells[c, here, :] for c in range(FIELDS)])):
            pad[c, span, :] = v
            pad_up[c, span, :] = jnp.where(lane == 127, 0.0, pltpu.roll(v, 127, 1))
            pad_down[c, span, :] = jnp.where(lane == 0, 0.0, pltpu.roll(v, 1, 1))
            pad[c, plane(x) - 1 : plane(x), :] = row
            for source in (pad, pad_up, pad_down):
                source[c, plane(x) + 8 : plane(x) + 9, :] = row
    for c in range(FIELDS):
        for source in (pad, pad_up, pad_down):
            source[c, pl.ds(plane(8), 8), :] = zero
        pad[c, plane(8) - 1 : plane(8), :] = row
        pad[c, plane(8) + 8 : plane(8) + 9, :] = row
    for total in (level, rising, falling):
        for c in range(6):
            for x in range(8):
                total[c, pl.ds(plane(x), 8), :] = zero


def inner_pairs(cells, state, pad, pad_up, pad_down, level, rising, falling, found, marks):
    zero = jnp.zeros((8, 128), jnp.float32)

    def body(x, carry):
        base = pl.multiple_of((x + 1) * ROWS + 8, 8)
        here = pl.ds(pl.multiple_of(x * 8, 8), 8)
        first = [pad[c, pl.ds(base, 8), :] for c in range(FIELDS)]
        forces = [zero] * 3
        twists = [zero] * 3
        springs = [zero] * (3 * SLOTS)
        for number, (dx, dy, dz) in enumerate(DIRS):
            span = pl.ds(base + dx * ROWS + dy, 8)
            source = (pad, pad_up, pad_down)[dz]
            total = (level, rising, falling)[dz]
            second = [source[c, span, :] for c in range(FIELDS)]
            ((shear, live, masks),) = pick_shear(lambda c: cells[c, here, :], (number,))
            force, twist, spring = pair(first, second, (dx, dy, dz), shear, live)
            for k in range(3):
                forces[k] = forces[k] + force[k]
                twists[k] = twists[k] + twist[k]
                for s in range(SLOTS):
                    springs[3 * s + k] = jnp.where(masks[s], spring[k], springs[3 * s + k])
                total[k, span, :] = total[k, span, :] - force[k]
                total[3 + k, span, :] = total[3 + k, span, :] + twist[k]
        for k in range(3):
            level[k, pl.ds(base, 8), :] = level[k, pl.ds(base, 8), :] + forces[k]
            level[3 + k, pl.ds(base, 8), :] = level[3 + k, pl.ds(base, 8), :] + twists[k]
        height, chosen = marks[0], marks[1] == x
        for c in range(3 * SLOTS):
            state[9 + c, here, :] = springs[c]
            value = jnp.take_along_axis(springs[c], height, axis=1)
            found[FIELDS + 6 + c] = jnp.where(chosen, value, found[FIELDS + 6 + c])
        return carry

    lax.fori_loop(0, 8, body, 0)


class Sums:
    def __init__(self):
        zero = jnp.zeros((8, 128), jnp.float32)
        self.total = [zero] * 6
        self.springs = [zero] * (3 * SLOTS)

    def own(self, result, masks):
        force, twist, spring = result
        for k in range(3):
            self.total[k] = self.total[k] + force[k]
            self.total[3 + k] = self.total[3 + k] + twist[k]
            for s in range(SLOTS):
                self.springs[3 * s + k] = jnp.where(masks[s], spring[k], self.springs[3 * s + k])

    def partner(self, result):
        force, twist, _ = result
        for k in range(3):
            self.total[k] = self.total[k] - force[k]
            self.total[3 + k] = self.total[3 + k] + twist[k]

    def collect(self, found, index, mask):
        for c, v in enumerate(self.total + self.springs):
            value = jnp.take_along_axis(v, index, axis=1)
            found[FIELDS + c] = found[FIELDS + c] + jnp.where(mask, value, 0.0)

    def store(self, level, rows, state, span):
        for c in range(6):
            level[c, rows, :] = level[c, rows, :] + self.total[c]
        if span is not None:
            for c in range(3 * SLOTS):
                state[9 + c, span, :] = state[9 + c, span, :] + self.springs[c]


def turned(values, amount, axis=1):
    return [pltpu.roll(v, amount, axis) for v in values]


def masks_of(cells, span, number):
    return [cells[CODES + s, span, :] == float(number) for s in range(SLOTS)]


def fold(level, rising, falling, found, marks):
    lane = lanes()
    sums = [jnp.zeros((8, 128), jnp.float32)] * 6
    for x in range(8):
        rows = pl.ds(plane(x), 8)
        for c in range(6):
            up = jnp.where(lane == 0, 0.0, pltpu.roll(rising[c, rows, :], 1, 1))
            down = jnp.where(lane == 127, 0.0, pltpu.roll(falling[c, rows, :], 127, 1))
            total = level[c, rows, :] + up + down
            level[c, rows, :] = total
    for x in range(8):
        for c in range(6):
            total = level[c, pl.ds(plane(x), 8), :]
            value = jnp.take_along_axis(total, marks[0], axis=1)
            sums[c] = jnp.where(marks[1] == x, value, sums[c])
    for c in range(6):
        found[FIELDS + c] = sums[c]


def x_ahead(cells, state, pad, level, ahead, xhi, edges, xrow, found, who):
    lane = lanes()
    for c in range(FIELDS):
        ahead[c, 7:8, :] = edges[2, c : c + 1, :]
        ahead[c, 16:17, :] = edges[3, c : c + 1, :]
        ahead[c, 8:16, :] = xhi[c]

    sums = Sums()
    first = [pad[c, pl.ds(plane(7), 8), :] for c in range(FIELDS)]
    for n, number in enumerate(ALONG_X):
        dx, dy, dz = DIRS[number]
        second = scaled([ahead[c, pl.ds(8 + dy, 8), :] for c in range(FIELDS)])
        if dz:
            edge = 127 if dz > 0 else 0
            second = [jnp.where(lane == edge, 0.0, v) for v in turned(second, -dz % 128)]
        at = FIELDS + 4 * n
        shear = [xrow[at + k] for k in range(3)]
        result = pair(first, second, DIRS[number], shear, xrow[at + 3] > 0.5)
        sums.own(result, masks_of(cells, pl.ds(56, 8), number))
    sums.store(level, pl.ds(plane(7), 8), state, pl.ds(56, 8))
    x, y, z, live = who
    sums.collect(found, z, ((y == below()) & (x == 7)) & live)


def x_behind(pad, level, behind, xlo, edges, found, who):
    lane = lanes()
    for c in range(FIELDS + 4 * len(ALONG_X)):
        behind[c, 8:16, :] = xlo[c]
    for c in range(FIELDS):
        behind[c, 7:8, :] = edges[0, c : c + 1, :]
        behind[c, 16:17, :] = edges[1, c : c + 1, :]
    for k in range(4):
        behind[FIELDS + 4 + k, 7:8, :] = edges[0, FIELDS + k : FIELDS + k + 1, :]
        behind[FIELDS + 8 + k, 16:17, :] = edges[1, FIELDS + k : FIELDS + k + 1, :]
    sums = Sums()
    second = [pad[c, pl.ds(plane(0), 8), :] for c in range(FIELDS)]
    for n, number in enumerate(ALONG_X):
        dx, dy, dz = DIRS[number]
        span = pl.ds(8 - dy, 8)
        first = scaled([behind[c, span, :] for c in range(FIELDS)])
        first += [behind[FIELDS + 4 * n + k, span, :] for k in range(4)]
        if dz:
            first = turned(first, dz % 128)
        live = first[13] > 0.5
        if dz:
            live = jnp.logical_and(live, lane != (0 if dz > 0 else 127))
        sums.partner(pair(first[:10], second, DIRS[number], first[10:13], live))
    sums.store(level, pl.ds(plane(0), 8), None, None)
    x, y, z, live = who
    sums.collect(found, z, ((y == below()) & (x == 0)) & live)


def y_high(cells, state, pad, level, yhi, ytop, found, who):
    lane = lanes()
    sub = lax.broadcasted_iota(jnp.int32, (8, 128), 0)
    top_fields = scaled([yhi[c] for c in range(FIELDS)])
    sums = Sums()
    mine_rows = pl.ds(plane(0) + 7, 8, stride=ROWS)
    span = pl.ds(7, 8, stride=8)
    mine = [pad[c, mine_rows, :] for c in range(FIELDS)]
    for n, number in enumerate(UP_Y):
        dx, dy, dz = DIRS[number]
        at = FIELDS + 4 * n
        live = ytop[at + 3] > 0.5
        second = top_fields
        if dx:
            second = turned(second, 7, 0)
            live = jnp.logical_and(live, sub != 7)
        if dz:
            second = turned(second, -dz % 128)
            live = jnp.logical_and(live, lane != (127 if dz > 0 else 0))
        shear = [ytop[at + k] for k in range(3)]
        sums.own(pair(mine, second, DIRS[number], shear, live), masks_of(cells, span, number))
    first = turned(top_fields + [yhi[FIELDS + k] for k in range(4)], 1, 0)
    live = jnp.logical_and(first[13] > 0.5, sub != 0)
    sums.partner(pair(first[:10], mine, DIRS[4], first[10:13], live))
    sums.store(level, mine_rows, state, span)
    x, y, z, live = who
    sums.collect(found, z, ((x == below()) & (y == 7)) & live)


def y_low(cells, state, pad, level, ylo, ylow, found, who):
    lane = lanes()
    sub = lax.broadcasted_iota(jnp.int32, (8, 128), 0)
    low_fields = scaled([ylo[c] for c in range(FIELDS)])
    sums = Sums()
    mine_rows = pl.ds(plane(0), 8, stride=ROWS)
    span = pl.ds(0, 8, stride=8)
    mine = [pad[c, mine_rows, :] for c in range(FIELDS)]
    second = turned(low_fields, 7, 0)
    live = jnp.logical_and(ylow[FIELDS + 3] > 0.5, sub != 7)
    shear = [ylow[FIELDS + k] for k in range(3)]
    sums.own(pair(mine, second, DIRS[4], shear, live), masks_of(cells, span, 4))
    for n, number in enumerate(UP_Y):
        dx, dy, dz = DIRS[number]
        first = low_fields + [ylo[FIELDS + 4 * n + k] for k in range(4)]
        if dx:
            first = turned(first, 1, 0)
        if dz:
            first = turned(first, dz % 128)
        live = first[13] > 0.5
        if dx:
            live = jnp.logical_and(live, sub != 0)
        if dz:
            live = jnp.logical_and(live, lane != (0 if dz > 0 else 127))
        sums.partner(pair(first[:10], mine, DIRS[number], first[10:13], live))
    sums.store(level, mine_rows, state, span)
    x, y, z, live = who
    sums.collect(found, z, ((x == below()) & (y == 0)) & live)


def end_pairs(end, zside, packs, own_packs):
    lane = lanes()
    theirs, ours = (((2, 5, 7), (6, 8)), ((6, 8), (2, 5, 7)))[end]
    top = 1 - end

    def spread(pack, c, top):
        p = (c % 16) * 8 - top
        return pltpu.roll(pack, -p % 128, 1) if p % 128 else pack

    back = [
        pltpu.roll(packs[2 + end, 0], -j % 128, 1) if j else packs[2 + end, 0]
        for j in range(FIELDS + 4)
    ]
    back = scaled(back[:FIELDS]) + back[FIELDS:]
    beyond = scaled(
        [pltpu.roll(packs[4 + end, 0], (7 - 8 * c + top) % 128, 1) for c in range(FIELDS)]
    )
    for k in range(PACKS):
        straight, left = packs[end, k], pltpu.roll(packs[6 + end, 0], 7 - k, 0)
        for c in range(16 * k, min(FULL, 16 * k + 16)):
            zside[end, c, 8:16, :] = spread(straight, c, top)
            zside[end, c, 0:8, :] = spread(left, c, top)
            if c < FIELDS:
                zside[end, c, 16:24, :] = spread(packs[8 + end, 0], c, top)
    own = [spread(own_packs[end, c // 16], c, end) for c in range(FULL)]
    mine = scaled(own[:FIELDS])
    sums = Sums()
    for number, (shear, live, masks) in zip(ours, pick_shear(lambda c: own[c], ours)):
        dx, dy, dz = DIRS[number]
        second = scaled([zside[end, c, pl.ds(8 + dy, 8), :] for c in range(FIELDS)])
        if dx:
            second = [
                jnp.where(lane < 7, v, jnp.where(lane == 7, b, 0.0))
                for b, v in zip(beyond, turned(second, 127))
            ]
        sums.own(pair(mine, second, DIRS[number], shear, live), masks)
    for number in theirs:
        dx, dy, dz = DIRS[number]
        span = pl.ds(8 - dy, 8)
        first = scaled([zside[end, c, span, :] for c in range(FIELDS)])
        ((shear, live, _),) = pick_shear(lambda c: zside[end, c, span, :], (number,))
        first = first + shear + [jnp.where(live, 1.0, 0.0)]
        if dx:
            first = [jnp.where(lane == 0, b, v) for b, v in zip(back, turned(first, 1))]
        sums.partner(pair(first[:10], mine, DIRS[number], first[10:13], first[13] > 0.5))
    return sums


def spread_end(end, sums, level, state):
    lane = lanes()
    edge = 127 * end
    hold = lane == edge
    for x in range(8):
        turn = (edge - x) % 128

        def put(v):
            return jnp.where(hold, pltpu.roll(v, turn, 1) if turn else v, 0.0)

        rows = pl.ds(plane(x), 8)
        here = slice(x * 8, x * 8 + 8)
        for c in range(6):
            level[c, rows, :] = level[c, rows, :] + put(sums.total[c])
        for c in range(3 * SLOTS):
            state[9 + c, here, :] = state[9 + c, here, :] + put(sums.springs[c])


def moved(cells, level, x):
    rows = pl.ds(plane(x), 8)
    here = slice(x * 8, x * 8 + 8)
    sums = [level[c, rows, :] for c in range(6)]
    radius = cells[9, here, :]
    inverse = 1.0 / radius
    push = STEP * inverse * inverse * inverse
    turn = 0.125 * (inverse * inverse) * (inverse * inverse)
    velocity = [cells[3 + k, here, :] + push * sums[k] for k in range(3)]
    velocity[2] = velocity[2] - STEP
    offset = [cells[k, here, :] + STEP * velocity[k] for k in range(3)]
    rotation = [cells[6 + k, here, :] + turn * sums[3 + k] for k in range(3)]
    return offset, velocity, rotation, radius


def below():
    return lax.broadcasted_iota(jnp.int32, (8, 128), 0)


def leaving_cells(leaving):
    names = leaving[0:1, 0:64]
    names = jnp.broadcast_to(jnp.concatenate([names, names], axis=1), (8, 128))
    live = names >= 0
    names = jnp.where(live, names, 0)
    return names // 1024, names // 128 % 8, names % 128, live


def gather_fields(found, cells, leaving, marks):
    x_of, y_of, z_of, live = leaving_cells(leaving)
    plane_of = jnp.where((y_of == below()) & live, x_of, -1)
    marks[0] = z_of
    marks[1] = plane_of
    zero = jnp.zeros((8, 128), jnp.float32)
    values = [zero] * FIELDS
    for x in range(8):
        here = slice(x * 8, x * 8 + 8)
        for c in range(FIELDS):
            value = jnp.take_along_axis(cells[c, here, :], z_of, axis=1)
            values[c] = jnp.where(plane_of == x, value, values[c])
    for c in range(FIELDS):
        found[c] = values[c]
    for c in range(3 * SLOTS):
        found[FIELDS + 6 + c] = zero


def fill_outbox(found, outbox, who):
    lane = lanes()[0:1]
    rows = [
        jnp.sum(found[c], axis=0, keepdims=True) for c in range(FIELDS + 6 + 3 * SLOTS)
    ]
    live = who[3][0:1]
    cell = [w[0:1].astype(jnp.float32) for w in who[:3]]
    starts = [(lax.axis_index(a) * n).astype(jnp.float32) for a, n in zip(AXES, (8, 8, 128))]
    radius = rows[9]
    inverse = 1.0 / jnp.where(live, radius, 1.0)
    push = STEP * inverse * inverse * inverse
    turn = 0.125 * (inverse * inverse) * (inverse * inverse)
    velocity = [rows[3 + k] + push * rows[10 + k] for k in range(3)]
    velocity[2] = jnp.where(live, velocity[2] - STEP, 0.0)
    position = [
        jnp.where(live, rows[k] + STEP * velocity[k] + (starts[k] + cell[k]), 0.0)
        for k in range(3)
    ]
    rotation = [rows[6 + k] + turn * rows[13 + k] for k in range(3)]
    values = position + velocity + rotation + [radius] + rows[16:]
    for c in range(14):
        outbox[c : c + 1, :] = jnp.where(lane < 64, values[c], values[14 + c])


def finish(cells, state, leaving, level):
    lane = lanes()
    wide = jnp.broadcast_to(leaving[0:1, 0:64], (8, 64))
    deep = lax.broadcasted_iota(jnp.int32, (8, 64), 0)
    for x in range(8):
        here = slice(x * 8, x * 8 + 8)
        offset, velocity, rotation, _ = moved(cells, level, x)
        left = [
            jnp.max(jnp.where(wide == (x * 8 + deep) * 128 + z, 1.0, 0.0), axis=1, keepdims=True)
            for z in range(2)
        ]
        staying = 1.0 - jnp.where(lane == 0, left[0], jnp.where(lane == 1, left[1], 0.0))
        for c, v in enumerate(offset + velocity + rotation):
            state[c, here, :] = v * staying
        for c in range(9, 27):
            state[c, here, :] = state[c, here, :] * staying


def on_device(offset, velocity, spin, radius, history, contacts, leaving):
    f32 = jnp.float32
    off = offset.reshape(3, 64, 128)
    vel = velocity.reshape(3, 64, 128)
    spn = spin.reshape(3, 64, 128)
    rad = radius.reshape(1, 64, 128)
    hist = history.reshape(3 * SLOTS, 64, 128)
    con = contacts.reshape(SLOTS, 64, 128)
    vmem = pl.BlockSpec(memory_space=pltpu.VMEM)
    hbm = pl.BlockSpec(memory_space=pltpu.HBM)
    halo_shapes = (
        (FIELDS + 4 * len(ALONG_X), 8, 128),
        (FIELDS, 8, 128),
        (FIELDS + 4 * len(UP_Y), 8, 128),
        (FIELDS + 4 * len(DOWN_Y), 8, 128),
        (4, 16, 128),
        (len(PACK_FROM), PACKS, 8, 128),
        (2, PACKS, 8, 128),
    )
    state, arrivals = pl.pallas_call(
        step_kernel,
        out_shape=[pltpu.VMEM((27, 64, 128), f32), pltpu.VMEM((16, 128), f32)],
        in_specs=[hbm] * 7,
        out_specs=[vmem] * 2,
        scratch_shapes=[pltpu.VMEM(s, f32) for s in halo_shapes]
        + [
            pltpu.VMEM((FULL, 64, 128), f32),
            pltpu.VMEM((SLOTS, 64, 128), jnp.int32),
            pltpu.VMEM((1, 64), jnp.int32),
            pltpu.VMEM((FIELDS + 4 * len(ALONG_X), 8, 128), f32),
            pltpu.VMEM((FIELDS + 4 * len(UP_Y), 8, 128), f32),
            pltpu.VMEM((FIELDS + 4 * len(DOWN_Y), 8, 128), f32),
            pltpu.VMEM((4, 16, 128), f32),
            pltpu.VMEM((2, 1, 8, 128), f32),
            pltpu.VMEM((2, 1, 8, 128), f32),
            pltpu.VMEM((16, 128), f32),
            pltpu.VMEM((FIELDS + 6 + 3 * SLOTS, 8, 128), f32),
            pltpu.VMEM((2, 8, 128), jnp.int32),
            pltpu.VMEM((FIELDS, HEIGHT, 128), f32),
            pltpu.VMEM((FIELDS, HEIGHT, 128), f32),
            pltpu.VMEM((FIELDS, HEIGHT, 128), f32),
            pltpu.VMEM((6, HEIGHT, 128), f32),
            pltpu.VMEM((6, HEIGHT, 128), f32),
            pltpu.VMEM((6, HEIGHT, 128), f32),
            pltpu.VMEM((FIELDS + 4 * len(ALONG_X), ROWS, 128), f32),
            pltpu.VMEM((FIELDS, ROWS, 128), f32),
            pltpu.VMEM((2, FULL, ROWS, 128), f32),
        ],
        compiler_params=pltpu.CompilerParams(
            collective_id=0, has_side_effects=True, vmem_limit_bytes=24 << 20
        ),
        name="step",
    )(*[
        pltpu.with_memory_space_constraint(a, pltpu.HBM)
        for a in (off, vel, spn, rad, hist, con, leaving.reshape(1, 64))
    ])
    moved = jax.ShapeDtypeStruct((3, 64, 128), f32)
    new_off, new_vel, new_spin, new_hist, arrivals = pl.pallas_call(
        write_kernel,
        out_shape=[
            moved, moved, moved,
            jax.ShapeDtypeStruct((3 * SLOTS, 64, 128), f32),
            jax.ShapeDtypeStruct((28, 1, 64), f32),
        ],
        in_specs=[vmem] * 2,
        out_specs=[hbm] * 5,
        scratch_shapes=[pltpu.VMEM((28, 1, 64), f32)],
        compiler_params=pltpu.CompilerParams(vmem_limit_bytes=8 << 20),
        name="write",
    )(state, arrivals)
    return (
        new_off.reshape(3, 8, 8, 128),
        new_vel.reshape(3, 8, 8, 128),
        new_spin.reshape(3, 8, 8, 128),
        new_hist.reshape(SLOTS, 3, 8, 8, 128),
        arrivals.reshape(28, 1, 1, 1, 64),
    )


def solution(mesh):
    placed = (
        P(None, "gx", "gy", "gz"),
        P(None, "gx", "gy", "gz"),
        P(None, "gx", "gy", "gz"),
        P("gx", "gy", "gz"),
        P(None, None, "gx", "gy", "gz"),
        P(None, "gx", "gy", "gz"),
        P("gx", "gy", "gz", None),
    )
    return jax.shard_map(
        on_device,
        mesh=mesh,
        in_specs=placed,
        out_specs=(
            P(None, "gx", "gy", "gz"),
            P(None, "gx", "gy", "gz"),
            P(None, "gx", "gy", "gz"),
            P(None, None, "gx", "gy", "gz"),
            P(None, "gx", "gy", "gz", None),
        ),
        check_vma=False,
    )
```
